32 devices in a mesh: seq: 4 (over z), fsdp: 8 (over y, x, core).
Axes of the slice: x: 2, y: 2, z: 4, core: 2. Of those that a mesh axis runs over, the one named last changes fastest.
Arguments:
- tokens: float32 [16, 1024, 1536], P('fsdp', 'seq'), may hold values from -6 to 6
- cotangent: float32 [16, 1024, 1536], P('fsdp', 'seq'), may hold values from -6 to 6
- attention_gain: bfloat16 [1536], P('fsdp'), may hold values from 0.5 to 1.5
- feedforward_gain: bfloat16 [1536], P('fsdp'), may hold values from 0.5 to 1.5
- query_weight: bfloat16 [1536, 1536], P('fsdp'), may hold values from -1 to 1
- key_matrix: bfloat16 [1536, 768], P('fsdp'), may hold values from -16 to 16
- value_matrix: bfloat16 [1536, 768], P('fsdp'), may hold values from -0.15625 to 0.15625
- out_weight: bfloat16 [1536, 1536], P('fsdp'), may hold values from -1.25 to 1.25
- gate_weight: bfloat16 [1536, 4096], P('fsdp'), may hold values from -0.15625 to 0.15625
- up_weight: bfloat16 [1536, 4096], P('fsdp'), may hold values from -0.15625 to 0.15625
- down_weight: bfloat16 [4096, 1536], P('fsdp'), may hold values from -0.09375 to 0.09375
Outputs:
- block_out: float32 [16, 1024, 1536], P('fsdp', 'seq')
- grad_tokens: float32 [16, 1024, 1536], P('fsdp', 'seq')
- grad_attention_gain: float32 [1536], P('fsdp')
- grad_feedforward_gain: float32 [1536], P('fsdp')
- grad_query: float32 [1536, 1536], P('fsdp')
- grad_key: float32 [1536, 768], P('fsdp')
- grad_value: float32 [1536, 768], P('fsdp')
- grad_out: float32 [1536, 1536], P('fsdp')
- grad_gate: float32 [1536, 4096], P('fsdp')
- grad_up: float32 [1536, 4096], P('fsdp')
- grad_down: float32 [4096, 1536], P('fsdp')
The draws below stay inside these ranges and needn't reach their ends.
All inputs are finite; a program needn't handle non-finite values.
Results may differ from the reference program's by a relative error of at most 0.024.
The reference program's roundings to bfloat16 on the way count: a program that leaves them out, or rounds other values in their place, can miss the bound.
Values may be sent and summed in bfloat16 or wider, within the bound.
A program may use at most 320 MiB of HBM per device.

```python
import math
import jax
import jax.numpy as jnp
from jax import lax

MODEL_WIDTH = 1536
QUERY_HEADS = 16
KEY_VALUE_HEADS = 8
HEAD_DIM = 96
FF = 4096
LEN = 1024
SEQS = 16


def query_shared(key):
    random_noise = jax.random.normal(jax.random.fold_in(key, 11), (MODEL_WIDTH, QUERY_HEADS * HEAD_DIM), jnp.float32)
    return jnp.clip(random_noise, -4.0, 4.0) / math.sqrt(MODEL_WIDTH)


def draw_query_weight(key, part):
    return query_shared(key).astype(jnp.bfloat16)


def draw_key_matrix(key, part):
    random_noise = jax.random.normal(jax.random.fold_in(key, 12), (MODEL_WIDTH, KEY_VALUE_HEADS * HEAD_DIM), jnp.float32)
    random_noise = jnp.clip(random_noise, -4.0, 4.0) / math.sqrt(MODEL_WIDTH)
    return random_noise.astype(jnp.bfloat16)


def draw_tokens(key, part):
    base = jax.random.normal(jax.random.fold_in(key, 21), (SEQS, LEN, MODEL_WIDTH), jnp.float32)
    base = jnp.clip(base, -6.0, 6.0)
    return base


def block_levels(stream_key, extent, split, low, high):
    gain = 1.0
    for dim, blocks in split:
        steps = jax.random.uniform(jax.random.fold_in(jax.random.fold_in(stream_key, 6), dim), (blocks,), jnp.float32, low / len(split), high / len(split))
        gain = gain * jnp.repeat(jnp.exp(steps), extent[dim] // blocks).reshape((-1,) + (1,) * (len(extent) - 1 - dim))
    return gain


def gaussian(key, dims, deviation, most, cuts=(), kind=jnp.bfloat16):
    entries = jax.random.normal(key, dims, jnp.float32) * deviation
    if len(cuts) > 0:
        entries = block_levels(key, dims, cuts, -0.22, 0.18) * entries
    return jnp.clip(entries, min=-most, max=most).astype(kind)


def setup_inputs(seed: int = 0) -> dict:
    splits = jax.random.split(jax.random.key(seed), 12)
    tokens = draw_tokens(jax.random.fold_in(splits[11], 71), 0)
    cotangent = gaussian(splits[1], (SEQS, LEN, MODEL_WIDTH), 1.0, 6.0, ((0, 8), (1, 4)), jnp.float32)
    attention_gain = jnp.clip(1.0 + 0.1 * jax.random.normal(splits[2], (MODEL_WIDTH,), jnp.float32), 0.5, 1.5).astype(jnp.bfloat16)
    feedforward_gain = jnp.clip(1.0 + 0.1 * jax.random.normal(splits[3], (MODEL_WIDTH,), jnp.float32), 0.5, 1.5).astype(jnp.bfloat16)
    query_weight = draw_query_weight(jax.random.fold_in(splits[11], 71), 0)
    key_matrix = draw_key_matrix(jax.random.fold_in(splits[11], 71), 0)
    value_matrix = gaussian(splits[6], (MODEL_WIDTH, KEY_VALUE_HEADS * HEAD_DIM), MODEL_WIDTH ** -0.5, 0.15625, ((0, 8),))
    out_weight = gaussian(splits[7], (QUERY_HEADS * HEAD_DIM, MODEL_WIDTH), (QUERY_HEADS * HEAD_DIM // 64) ** -0.5, 1.25, ((0, 8),))
    gate_weight = gaussian(splits[8], (MODEL_WIDTH, FF), MODEL_WIDTH ** -0.5, 0.15625, ((0, 8),))
    up_weight = gaussian(splits[9], (MODEL_WIDTH, FF), MODEL_WIDTH ** -0.5, 0.15625, ((0, 8),))
    down_weight = gaussian(splits[10], (FF, MODEL_WIDTH), FF ** -0.5, 0.09375, ((0, 8),))
    return {"tokens": tokens, "cotangent": cotangent, "attention_gain": attention_gain, "feedforward_gain": feedforward_gain, "query_weight": query_weight, "key_matrix": key_matrix, "value_matrix": value_matrix, "out_weight": out_weight, "gate_weight": gate_weight, "up_weight": up_weight, "down_weight": down_weight}


norm_eps = 1e-05
rope_base = 100000.0
masked_score = -1e+30

def as_wide(values):
    return lax.optimization_barrier(values).astype(jnp.float32)

def rope_tables(positions, head_size):
    half = head_size // 2
    freqs = rope_base ** (-(2.0 * jnp.arange(half, dtype=jnp.float32)) / head_size)
    angles = positions.astype(jnp.float32)[:, None] * freqs[None, :]
    return (jnp.cos(angles), jnp.sin(angles))

def rotate_halves(values, cosine, sine):
    half = values.shape[-1] // 2
    first = values[..., :half]
    second = values[..., half:]
    return jnp.concatenate([first * cosine - second * sine, second * cosine + first * sine], axis=-1)

def reverse_rotation(grads, cosine, sine):
    half = grads.shape[-1] // 2
    first = grads[..., :half]
    second = grads[..., half:]
    return jnp.concatenate([first * cosine + second * sine, second * cosine - first * sine], axis=-1)

def masked_scores(query_rows, key_rows, scale):
    sequence_length = query_rows.shape[0]
    scores = jnp.einsum('qhgd,khd->hgqk', as_wide(query_rows), as_wide(key_rows)) * scale
    causal = jnp.arange(sequence_length)[:, None] >= jnp.arange(sequence_length)[None, :]
    return jnp.where(causal, scores, masked_score)

def attend_forward(query_rows, key_rows, value_matrix_rows, scale):
    scores = masked_scores(query_rows, key_rows, scale)
    top_score = lax.optimization_barrier(jnp.max(scores, axis=-1, keepdims=True))
    log_total = top_score + jnp.log(lax.optimization_barrier(jnp.sum(jnp.exp(scores - top_score), axis=-1, keepdims=True)))
    probs = jnp.exp(scores - log_total).astype(jnp.bfloat16)
    attended = jnp.einsum('hgqk,khd->qhgd', as_wide(probs), as_wide(value_matrix_rows)).astype(jnp.bfloat16)
    return (attended, log_total)

def attend_backward(query_rows, key_rows, value_matrix_rows, attended, log_total, attended_gradient, scale):
    scores = masked_scores(query_rows, key_rows, scale)
    probs = jnp.exp(scores - log_total)
    delta = jnp.einsum('qhgd,qhgd->hgq', as_wide(attended_gradient), as_wide(attended))[..., None]
    probs_low = probs.astype(jnp.bfloat16)
    value_gradients = jnp.einsum('hgqk,qhgd->khd', as_wide(probs_low), as_wide(attended_gradient))
    grad_probs = jnp.einsum('qhgd,khd->hgqk', as_wide(attended_gradient), as_wide(value_matrix_rows))
    grad_scores = (probs * (grad_probs - delta) * scale).astype(jnp.bfloat16)
    grad_queries = jnp.einsum('hgqk,khd->qhgd', as_wide(grad_scores), as_wide(key_rows))
    key_gradients = jnp.einsum('hgqk,qhgd->khd', as_wide(grad_scores), as_wide(query_rows))
    return (grad_queries, key_gradients, value_gradients)

def one_sequence(tokens, cotangent, attention_gain, feedforward_gain, query_weight, key_matrix, value_matrix, out_weight, gate_weight, up_weight, down_weight):
    sequence_length = tokens.shape[0]
    group_size = QUERY_HEADS // KEY_VALUE_HEADS
    scale = 1.0 / math.sqrt(HEAD_DIM)
    cosine, sine = rope_tables(jnp.arange(sequence_length), HEAD_DIM)
    cosine_triple = cosine[:, None, :]
    sine_triple = sine[:, None, :]
    inv_one = lax.rsqrt(lax.optimization_barrier(jnp.mean(tokens * tokens, axis=-1, keepdims=True)) + norm_eps)
    normed_one = tokens * inv_one
    first_inputs = (normed_one * attention_gain).astype(jnp.bfloat16)
    query_projected = jnp.dot(first_inputs, query_weight, preferred_element_type=jnp.float32).reshape(sequence_length, QUERY_HEADS, HEAD_DIM)
    key_projected = jnp.dot(first_inputs, key_matrix, preferred_element_type=jnp.float32).reshape(sequence_length, KEY_VALUE_HEADS, HEAD_DIM)
    value_matrix_rows = jnp.dot(first_inputs, value_matrix, preferred_element_type=jnp.float32).astype(jnp.bfloat16)
    value_matrix_rows = value_matrix_rows.reshape(sequence_length, KEY_VALUE_HEADS, HEAD_DIM)
    query_rows = rotate_halves(query_projected, cosine_triple, sine_triple).astype(jnp.bfloat16).reshape(sequence_length, KEY_VALUE_HEADS, group_size, HEAD_DIM)
    key_rows = rotate_halves(key_projected, cosine_triple, sine_triple).astype(jnp.bfloat16)
    attended, log_total = attend_forward(query_rows, key_rows, value_matrix_rows, scale)
    attended_flat = attended.reshape(sequence_length, QUERY_HEADS * HEAD_DIM)
    hidden_one = tokens + jnp.dot(attended_flat, out_weight, preferred_element_type=jnp.float32)
    inv_two = lax.rsqrt(lax.optimization_barrier(jnp.mean(hidden_one * hidden_one, axis=-1, keepdims=True)) + norm_eps)
    normed_two = hidden_one * inv_two
    inputs_two = (normed_two * feedforward_gain).astype(jnp.bfloat16)
    gate_pre = jnp.dot(inputs_two, gate_weight, preferred_element_type=jnp.float32)
    up_pre = jnp.dot(inputs_two, up_weight, preferred_element_type=jnp.float32)
    sigmoid_gate = jax.nn.sigmoid(gate_pre)
    hidden_act = (gate_pre * sigmoid_gate * up_pre).astype(jnp.bfloat16)
    block_out = hidden_one + jnp.dot(hidden_act, down_weight, preferred_element_type=jnp.float32)
    grad_low = cotangent.astype(jnp.bfloat16)
    grad_down = jnp.dot(hidden_act.T, grad_low, preferred_element_type=jnp.float32)
    grad_hidden = jnp.dot(grad_low, down_weight.T, preferred_element_type=jnp.float32)
    grad_gate_pre = (grad_hidden * up_pre * sigmoid_gate * (1.0 + gate_pre * (1.0 - sigmoid_gate))).astype(jnp.bfloat16)
    grad_up_pre = (grad_hidden * gate_pre * sigmoid_gate).astype(jnp.bfloat16)
    grad_gate = jnp.dot(inputs_two.T, grad_gate_pre, preferred_element_type=jnp.float32)
    grad_up = jnp.dot(inputs_two.T, grad_up_pre, preferred_element_type=jnp.float32)
    grad_inputs_two = jnp.dot(grad_gate_pre, gate_weight.T, preferred_element_type=jnp.float32) + jnp.dot(grad_up_pre, up_weight.T, preferred_element_type=jnp.float32)
    grad_ffn_gain = lax.optimization_barrier(jnp.sum(grad_inputs_two * normed_two, axis=0))
    scaled_two = grad_inputs_two * feedforward_gain
    grad_hidden_one = cotangent + inv_two * (scaled_two - normed_two * lax.optimization_barrier(jnp.mean(scaled_two * normed_two, axis=-1, keepdims=True)))
    grad_low_one = grad_hidden_one.astype(jnp.bfloat16)
    grad_out = jnp.dot(attended_flat.T, grad_low_one, preferred_element_type=jnp.float32)
    attended_gradient = jnp.dot(grad_low_one, out_weight.T, preferred_element_type=jnp.float32).astype(jnp.bfloat16)
    attended_gradient = attended_gradient.reshape(sequence_length, KEY_VALUE_HEADS, group_size, HEAD_DIM)
    grad_queries, key_gradients, value_gradients = attend_backward(query_rows, key_rows, value_matrix_rows, attended, log_total, attended_gradient, scale)
    grad_queries = reverse_rotation(grad_queries.reshape(sequence_length, QUERY_HEADS, HEAD_DIM), cosine_triple, sine_triple)
    grad_queries = grad_queries.astype(jnp.bfloat16).reshape(sequence_length, QUERY_HEADS * HEAD_DIM)
    key_gradients = reverse_rotation(key_gradients, cosine_triple, sine_triple).astype(jnp.bfloat16).reshape(sequence_length, KEY_VALUE_HEADS * HEAD_DIM)
    value_gradients = value_gradients.astype(jnp.bfloat16).reshape(sequence_length, KEY_VALUE_HEADS * HEAD_DIM)
    grad_query = jnp.dot(first_inputs.T, grad_queries, preferred_element_type=jnp.float32)
    grad_key = jnp.dot(first_inputs.T, key_gradients, preferred_element_type=jnp.float32)
    grad_value = jnp.dot(first_inputs.T, value_gradients, preferred_element_type=jnp.float32)
    grad_inputs_one = jnp.dot(grad_queries, query_weight.T, preferred_element_type=jnp.float32) + jnp.dot(key_gradients, key_matrix.T, preferred_element_type=jnp.float32) + jnp.dot(value_gradients, value_matrix.T, preferred_element_type=jnp.float32)
    grad_attn_gain = lax.optimization_barrier(jnp.sum(grad_inputs_one * normed_one, axis=0))
    scaled_one = grad_inputs_one * attention_gain
    grad_tokens = grad_hidden_one + inv_one * (scaled_one - normed_one * lax.optimization_barrier(jnp.mean(scaled_one * normed_one, axis=-1, keepdims=True)))
    grads = (grad_attn_gain, grad_ffn_gain, grad_query, grad_key, grad_value, grad_out, grad_gate, grad_up, grad_down)
    return (block_out, grad_tokens, grads)

def reference(tokens, cotangent, attention_gain, feedforward_gain, query_weight, key_matrix, value_matrix, out_weight, gate_weight, up_weight, down_weight):
    attention_gain = attention_gain.astype(jnp.float32)
    feedforward_gain = feedforward_gain.astype(jnp.float32)
    shapes = (attention_gain.shape, feedforward_gain.shape, query_weight.shape, key_matrix.shape, value_matrix.shape, out_weight.shape, gate_weight.shape, up_weight.shape, down_weight.shape)
    initial = tuple((jnp.zeros(shape, jnp.float32) for shape in shapes))

    def advance(totals, inputs):
        block_out, grad_tokens, grads = one_sequence(inputs[0], inputs[1], attention_gain, feedforward_gain, query_weight, key_matrix, value_matrix, out_weight, gate_weight, up_weight, down_weight)
        summed = tuple((total + grad for total, grad in zip(totals, grads)))
        return (summed, (block_out, grad_tokens))
    totals, outputs = lax.scan(advance, initial, (tokens, cotangent))
    return (outputs[0], outputs[1], totals[0], totals[1], totals[2], totals[3], totals[4], totals[5], totals[6], totals[7], totals[8])
```

```python
import functools
import math

import jax
import jax.numpy as jnp
from jax import lax
from jax.experimental import pallas as pl
from jax.experimental.pallas import tpu as pltpu
from jax.sharding import PartitionSpec as P

QUERY_HEADS = 16
KEY_VALUE_HEADS = 8
HEAD_DIM = 96
GROUP = QUERY_HEADS // KEY_VALUE_HEADS
norm_eps = 1e-05
rope_base = 100000.0
masked_score = -1e30
F32, BF16 = jnp.float32, jnp.bfloat16
VMEM_LIMIT = 60 * 1024 * 1024


def nt_dot(left, right):
    return lax.dot_general(left, right, (((1,), (1,)), ((), ())), preferred_element_type=F32)


def tn_dot(left, right):
    return lax.dot_general(left, right, (((0,), (0,)), ((), ())), preferred_element_type=F32)


def nn_dot(left, right):
    return jnp.dot(left, right, preferred_element_type=F32)


def whole(shape):
    return pl.BlockSpec(shape, lambda *_: (0,) * len(shape))


def call(kernel, scalars, operands, outs, name, flops, moved, scratch=()):
    return pl.pallas_call(
        kernel,
        grid_spec=pltpu.PrefetchScalarGridSpec(
            num_scalar_prefetch=1,
            grid=(1,),
            in_specs=[whole(x.shape) for x in operands],
            out_specs=[whole(x.shape) for x in outs],
            scratch_shapes=scratch,
        ),
        out_shape=outs,
        compiler_params=pltpu.CompilerParams(vmem_limit_bytes=VMEM_LIMIT),
        cost_estimate=pl.CostEstimate(flops=flops, bytes_accessed=moved, transcendentals=0),
        name=name,
    )(scalars, *operands)


def rope_tables(positions, heads, plain):
    half = HEAD_DIM // 2
    freqs = rope_base ** (-(2.0 * jnp.arange(half, dtype=F32)) / HEAD_DIM)
    angles = positions.astype(F32)[:, None] * freqs[None, :]
    cosine, sine = jnp.cos(angles), jnp.sin(angles)
    rows = positions.shape[0]
    cosines = jnp.concatenate([jnp.tile(jnp.concatenate([cosine, cosine], 1), (1, heads)), jnp.ones((rows, plain), F32)], 1)
    sines = jnp.concatenate([jnp.tile(jnp.concatenate([-sine, sine], 1), (1, heads)), jnp.zeros((rows, plain), F32)], 1)
    return cosines, sines


def swap_halves(values):
    half = HEAD_DIM // 2
    width = values.shape[1]
    lane = lax.broadcasted_iota(jnp.int32, values.shape, 1)
    ahead = pltpu.roll(values, width - half, 1)
    behind = pltpu.roll(values, half, 1)
    return jnp.where(lane % HEAD_DIM < half, ahead, behind)


def project_kernel(scalars, x, w, cosines, sines, *outs):
    y = nn_dot(x[...], w[...])
    span = cosines.shape[0]
    for i, out in enumerate(outs):
        part = y[i * span : (i + 1) * span]
        out[...] = (part * cosines[...] + swap_halves(part) * sines[...]).astype(BF16)


def project(x, w, cosines, sines, me, shift, ns, count):
    rows, width = x.shape
    columns = w.shape[1] // ns
    span = rows // count
    target = lax.rem(me + shift, ns).reshape(1)
    return pl.pallas_call(
        project_kernel,
        grid_spec=pltpu.PrefetchScalarGridSpec(
            num_scalar_prefetch=1,
            grid=(1,),
            in_specs=[
                whole(x.shape),
                pl.BlockSpec((width, columns), lambda i, s: (0, s[0])),
                whole(cosines.shape),
                whole(sines.shape),
            ],
            out_specs=[whole((span, columns))] * count,
        ),
        out_shape=[jax.ShapeDtypeStruct((span, columns), BF16)] * count,
        compiler_params=pltpu.CompilerParams(vmem_limit_bytes=VMEM_LIMIT),
        cost_estimate=pl.CostEstimate(
            flops=2 * rows * width * columns,
            bytes_accessed=2 * (rows * width + width * columns + rows * columns),
            transcendentals=0,
        ),
        name="project",
    )(target, x, w, cosines, sines)


def load_heads(me, ns, packed, qs, ks, vs, kv):
    span = packed[0].shape[0]
    for d in range(ns):
        at = pl.ds(pl.multiple_of(lax.rem(me + ns - d, ns) * span, span), span)
        piece = packed[d][...]
        for h in range(kv * GROUP):
            qs[h, at, :] = piece[:, h * HEAD_DIM : (h + 1) * HEAD_DIM]
        for h in range(kv):
            k0 = (kv * GROUP + h) * HEAD_DIM
            v0 = (kv * GROUP + kv + h) * HEAD_DIM
            ks[h, at, :] = piece[:, k0 : k0 + HEAD_DIM]
            vs[h, at, :] = piece[:, v0 : v0 + HEAD_DIM]


def attend_kernel(ns, kv, scalars, *refs):
    packed, outs, logs = refs[:ns], refs[ns : 2 * ns], refs[2 * ns]
    qs, ks, vs, result = refs[2 * ns + 1 :]
    me = scalars[0]
    span = packed[0].shape[0]
    scale = 1.0 / math.sqrt(HEAD_DIM)
    load_heads(me, ns, packed, qs, ks, vs, kv)
    row = lax.broadcasted_iota(jnp.int32, (span, span), 0)
    column = lax.broadcasted_iota(jnp.int32, (span, span), 1)
    causal = row >= column
    lane = lax.broadcasted_iota(jnp.int32, (span, 128), 1)
    for s in range(ns):
        here = slice(s * span, (s + 1) * span)
        stats = jnp.zeros((span, 128), F32)
        for h in range(kv * GROUP):
            g = h // GROUP
            q = qs[h, here, :]
            near = jnp.where(causal, nt_dot(q, ks[g, here, :]) * scale, masked_score)
            top = jnp.max(near, axis=1, keepdims=True)
            if s > 0:
                far = nt_dot(q, ks[g, : s * span, :]) * scale
                top = jnp.maximum(top, jnp.max(far, axis=1, keepdims=True))
            near = jnp.exp(near - top)
            total = jnp.sum(near, axis=1, keepdims=True)
            if s > 0:
                far = jnp.exp(far - top)
                total = total + jnp.sum(far, axis=1, keepdims=True)
            inverse = 1.0 / total
            out = nn_dot((near * inverse).astype(BF16), vs[g, here, :])
            if s > 0:
                out = out + nn_dot((far * inverse).astype(BF16), vs[g, : s * span, :])
            stats = jnp.where(lane == h, top + jnp.log(total), stats)
            result[here, h * HEAD_DIM : (h + 1) * HEAD_DIM] = out.astype(BF16)
        logs[here, :] = stats
    for d in range(ns):
        at = pl.ds(pl.multiple_of(lax.rem(me + d, ns) * span, span), span)
        outs[d][...] = result[at, :]


def attend(packed, me, kv):
    ns = len(packed)
    span = packed[0].shape[0]
    length = ns * span
    heads = kv * GROUP
    outs = [jax.ShapeDtypeStruct((span, heads * HEAD_DIM), BF16)] * ns + [jax.ShapeDtypeStruct((length, 128), F32)]
    results = call(
        functools.partial(attend_kernel, ns, kv),
        me.reshape(1),
        packed,
        outs,
        "attend",
        2 * heads * length * length * 2 * 128,
        4 * length * heads * HEAD_DIM * 2,
        [
            pltpu.VMEM((heads, length, HEAD_DIM), BF16),
            pltpu.VMEM((kv, length, HEAD_DIM), BF16),
            pltpu.VMEM((kv, length, HEAD_DIM), BF16),
            pltpu.VMEM((length, heads * HEAD_DIM), BF16),
        ],
    )
    return results[:ns], results[ns]


def attend_back_kernel(ns, kv, scalars, *refs):
    packed, arrived, attended = refs[:ns], refs[ns : 2 * ns], refs[2 * ns : 3 * ns]
    logs, cosines, sines = refs[3 * ns : 3 * ns + 3]
    outs = refs[3 * ns + 3 : 4 * ns + 3]
    qs, ks, vs, gs, deltas, dk, dv, result = refs[4 * ns + 3 :]
    me = scalars[0]
    span = packed[0].shape[0]
    scale = 1.0 / math.sqrt(HEAD_DIM)
    heads = kv * GROUP
    load_heads(me, ns, packed, qs, ks, vs, kv)
    for d in range(ns):
        at = pl.ds(pl.multiple_of(lax.rem(me + ns - d, ns) * span, span), span)
        piece = arrived[d][...]
        for h in range(heads):
            gs[h, at, :] = piece[:, h * HEAD_DIM : (h + 1) * HEAD_DIM]
    lane = lax.broadcasted_iota(jnp.int32, (span, 128), 1)
    for d in range(ns):
        at = pl.ds(pl.multiple_of(lax.rem(me + d, ns) * span, span), span)
        piece = attended[d][...]
        stats = jnp.zeros((span, 128), F32)
        for h in range(heads):
            product = gs[h, at, :].astype(F32) * piece[:, h * HEAD_DIM : (h + 1) * HEAD_DIM].astype(F32)
            stats = jnp.where(lane == h, jnp.sum(product, axis=1, keepdims=True), stats)
        deltas[at, :] = stats
    row = lax.broadcasted_iota(jnp.int32, (span, span), 0)
    column = lax.broadcasted_iota(jnp.int32, (span, span), 1)
    causal = row >= column
    for s in range(ns):
        here = slice(s * span, (s + 1) * span)
        for g in range(kv):
            dk[g, here, :] = jnp.zeros((span, HEAD_DIM), F32)
            dv[g, here, :] = jnp.zeros((span, HEAD_DIM), F32)
    for s in range(ns):
        here = slice(s * span, (s + 1) * span)
        for h in range(heads):
            g = h // GROUP
            q, grad = qs[h, here, :], gs[h, here, :]
            log_total = logs[here, h : h + 1]
            delta = deltas[here, h : h + 1]
            k, v = ks[g, here, :], vs[g, here, :]
            near = jnp.where(causal, jnp.exp(nt_dot(q, k) * scale - log_total), 0.0)
            slope = (near * (nt_dot(grad, v) - delta) * scale).astype(BF16)
            dq = nn_dot(slope, k)
            dk[g, here, :] += tn_dot(slope, q)
            dv[g, here, :] += tn_dot(near.astype(BF16), grad)
            if s > 0:
                before = slice(0, s * span)
                k, v = ks[g, before, :], vs[g, before, :]
                far = jnp.exp(nt_dot(q, k) * scale - log_total)
                slope = (far * (nt_dot(grad, v) - delta) * scale).astype(BF16)
                dq = dq + nn_dot(slope, k)
                dk[g, before, :] += tn_dot(slope, q)
                dv[g, before, :] += tn_dot(far.astype(BF16), grad)
            result[here, h * HEAD_DIM : (h + 1) * HEAD_DIM] = dq
    for g in range(kv):
        k0 = (heads + g) * HEAD_DIM
        v0 = (heads + kv + g) * HEAD_DIM
        result[:, k0 : k0 + HEAD_DIM] = dk[g]
        result[:, v0 : v0 + HEAD_DIM] = dv[g]
    for d in range(ns):
        at = pl.ds(pl.multiple_of(lax.rem(me + d, ns) * span, span), span)
        part = result[at, :]
        outs[d][...] = (part * cosines[at, :] - swap_halves(part) * sines[at, :]).astype(BF16)


def attend_back(packed, arrived, attended, logs, cosines, sines, me, kv):
    ns = len(packed)
    span, width = packed[0].shape
    length = ns * span
    heads = kv * GROUP
    return call(
        functools.partial(attend_back_kernel, ns, kv),
        me.reshape(1),
        [*packed, *arrived, *attended, logs, cosines, sines],
        [jax.ShapeDtypeStruct((span, width), BF16)] * ns,
        "attend_back",
        5 * heads * length * length * 2 * 128,
        8 * length * heads * HEAD_DIM * 2,
        [
            pltpu.VMEM((heads, length, HEAD_DIM), BF16),
            pltpu.VMEM((kv, length, HEAD_DIM), BF16),
            pltpu.VMEM((kv, length, HEAD_DIM), BF16),
            pltpu.VMEM((heads, length, HEAD_DIM), BF16),
            pltpu.VMEM((length, 128), F32),
            pltpu.VMEM((kv, length, HEAD_DIM), F32),
            pltpu.VMEM((kv, length, HEAD_DIM), F32),
            pltpu.VMEM((length, width), F32),
        ],
    )


def out_kernel(ns, count, scalars, *refs):
    pieces = refs[: ns * count]
    tokens, w, gain, attended, hidden, inputs = refs[ns * count :]
    me = scalars[0]
    span, width = pieces[0].shape
    for d in range(ns):
        for j in range(ns):

            @pl.when(lax.rem(me + ns - d, ns) == j)
            def _():
                for i in range(count):
                    attended[i * span : (i + 1) * span, j * width : (j + 1) * width] = pieces[i * ns + d][...]

    rows = tokens[...] + nn_dot(attended[...], w[...])
    hidden[...] = rows
    inverse = lax.rsqrt(jnp.mean(rows * rows, axis=1, keepdims=True) + norm_eps)
    inputs[...] = (rows * inverse * gain[...]).astype(BF16)


def out_project(pieces, tokens, w, gain, me, ns, count):
    shape = tokens.shape
    return call(
        functools.partial(out_kernel, ns, count),
        me.reshape(1),
        [*pieces, tokens, w, gain],
        [jax.ShapeDtypeStruct(shape, BF16), jax.ShapeDtypeStruct(shape, F32), jax.ShapeDtypeStruct(shape, BF16)],
        "out_project",
        2 * shape[0] * w.shape[0] * w.shape[1],
        14 * shape[0] * shape[1],
    )


def ffn_kernel(tiles, scalars, x_own, x_other, g_own, g_other, wg, wu, wd, act, dgate, dup, out_own, out_other, dx_own, dx_other, acc_out, acc_dx):
    step = pl.program_id(0)

    @pl.when(step == 0)
    def _():
        out_own[...] = jnp.zeros_like(out_own)
        dx_own[...] = jnp.zeros_like(dx_own)
        acc_out[...] = jnp.zeros_like(acc_out)
        acc_dx[...] = jnp.zeros_like(acc_dx)

    for i, (x, g, out, dx) in enumerate(((x_own, g_own, out_own, dx_own), (x_other, g_other, acc_out, acc_dx))):
        gate = nn_dot(x[...], wg[...])
        up = nn_dot(x[...], wu[...])
        grad = nt_dot(g[...], wd[...])
        sigmoid = jax.nn.sigmoid(gate)
        silu = gate * sigmoid
        hidden = (silu * up).astype(BF16)
        act[i] = hidden
        gate_grad = (grad * up * sigmoid * (1.0 + gate * (1.0 - sigmoid))).astype(BF16)
        up_grad = (grad * silu).astype(BF16)
        dgate[i] = gate_grad
        dup[i] = up_grad
        out[...] += nn_dot(hidden, wd[...])
        dx[...] += nt_dot(gate_grad, wg[...]) + nt_dot(up_grad, wu[...])

    @pl.when(step == tiles - 1)
    def _():
        out_other[...] = acc_out[...].astype(BF16)
        dx_other[...] = acc_dx[...].astype(BF16)


def ffn(x_own, x_other, g_own, g_other, wg, wu, wd, order, core):
    rows, width = x_own.shape
    tiles = order.shape[0]
    cols = wg.shape[1] // (2 * tiles)
    scalars = jnp.concatenate([order, core.reshape(1)]).astype(jnp.int32)
    once = dict(pipeline_mode=pl.Buffered(1))
    keep = lambda: pl.BlockSpec((rows, width), lambda i, s: (0, 0), **once)
    last = lambda: pl.BlockSpec((rows, width), lambda i, s: (0, 0))
    by_chip = lambda: pl.BlockSpec((2, rows, cols), lambda i, s: (0, 0, s[i]))
    halves = jax.ShapeDtypeStruct((2, rows, cols * tiles), BF16)
    wide, low = jax.ShapeDtypeStruct((rows, width), F32), jax.ShapeDtypeStruct((rows, width), BF16)
    return pl.pallas_call(
        functools.partial(ffn_kernel, tiles),
        grid_spec=pltpu.PrefetchScalarGridSpec(
            num_scalar_prefetch=1,
            grid=(tiles,),
            in_specs=[keep(), keep(), keep(), keep()]
            + [pl.BlockSpec((width, cols), lambda i, s: (0, s[i] * 2 + s[tiles]))] * 2
            + [pl.BlockSpec((cols, width), lambda i, s: (s[i] * 2 + s[tiles], 0))],
            out_specs=[pl.BlockSpec((2, rows, cols), lambda i, s: (0, 0, i)), by_chip(), by_chip(), last(), last(), last(), last()],
            scratch_shapes=[pltpu.VMEM((rows, width), F32)] * 2,
        ),
        out_shape=[halves, halves, halves, wide, low, wide, low],
        compiler_params=pltpu.CompilerParams(vmem_limit_bytes=VMEM_LIMIT),
        cost_estimate=pl.CostEstimate(
            flops=24 * rows * width * cols * tiles,
            bytes_accessed=6 * width * cols * tiles + 12 * rows * cols * tiles + 20 * rows * width,
            transcendentals=0,
        ),
        name="ffn",
    )(scalars, x_own, x_other, g_own, g_other, wg, wu, wd)


def norm_back(grad, normed, inverse, gain):
    scaled = grad * gain
    return inverse * (scaled - normed * jnp.mean(scaled * normed, axis=1, keepdims=True))


def out_back_kernel(ns, count, scalars, dx_own, dx_other, hidden, cotangent, gain, w, high, low, gain_grad, *pieces):
    me = scalars[0]
    span, width = pieces[0].shape
    grad = dx_own[...] + dx_other[...].astype(F32)
    rows = hidden[...]
    inverse = lax.rsqrt(jnp.mean(rows * rows, axis=1, keepdims=True) + norm_eps)
    normed = rows * inverse
    gain_grad[...] = jnp.sum(grad * normed, axis=0, keepdims=True)
    total = cotangent[...] + norm_back(grad, normed, inverse, gain[...])
    high[...] = total
    low[...] = total.astype(BF16)
    for d in range(ns):
        at = pl.ds(pl.multiple_of(lax.rem(me + d, ns) * width, width), width)
        part = nt_dot(low[...], w[at, :]).astype(BF16)
        for i in range(count):
            pieces[i * ns + d][...] = part[i * span : (i + 1) * span]


def out_back(dx_own, dx_other, hidden, cotangent, gain, w, me, ns, count):
    rows, width = hidden.shape
    piece = jax.ShapeDtypeStruct((rows // count, w.shape[0] // ns), BF16)
    results = call(
        functools.partial(out_back_kernel, ns, count),
        me.reshape(1),
        [dx_own, dx_other, hidden, cotangent, gain, w],
        [
            jax.ShapeDtypeStruct((rows, width), F32),
            jax.ShapeDtypeStruct((rows, width), BF16),
            jax.ShapeDtypeStruct((1, width), F32),
        ]
        + [piece] * (ns * count),
        "out_back",
        2 * rows * width * w.shape[0],
        24 * rows * width,
    )
    return results[0], results[1], results[2], results[3:]


def sort_kernel(ns, count, scalars, *refs):
    pieces, out = refs[:-1], refs[-1]
    me = scalars[0]
    span, width = pieces[0].shape
    per = out.shape[2] // width
    for d in range(ns):
        source = lax.rem(me + ns - d, ns)
        half = source // per
        at = pl.ds(pl.multiple_of(lax.rem(source, per) * width, width), width)
        for i in range(count):
            out[half, i * span : (i + 1) * span, at] = pieces[i * ns + d][...]


def sort_pieces(pieces, me, ns, count):
    span, width = pieces[0].shape
    return call(
        functools.partial(sort_kernel, ns, count),
        me.reshape(1),
        pieces,
        [jax.ShapeDtypeStruct((2, span * count, width * ns // 2), BF16)],
        "sort_pieces",
        0,
        4 * span * count * width * ns,
    )[0]


def project_back_kernel(scalars, dqkv, w, tokens, high, gain, out, gain_grad):
    half = w.shape[1] // 2
    grad = nt_dot(dqkv[0], w[:, :half]) + nt_dot(dqkv[1], w[:, half:])
    rows = tokens[...]
    inverse = lax.rsqrt(jnp.mean(rows * rows, axis=1, keepdims=True) + norm_eps)
    normed = rows * inverse
    gain_grad[...] = jnp.sum(grad * normed, axis=0, keepdims=True)
    out[...] = high[...] + norm_back(grad, normed, inverse, gain[...])


def project_back(dqkv, w, tokens, high, gain):
    rows, width = tokens.shape
    return call(
        project_back_kernel,
        jnp.zeros((1,), jnp.int32),
        [dqkv, w, tokens, high, gain],
        [jax.ShapeDtypeStruct((rows, width), F32), jax.ShapeDtypeStruct((1, width), F32)],
        "project_back",
        2 * rows * width * w.shape[1],
        12 * rows * width + 2 * (rows + width) * w.shape[1],
    )


def solution(mesh):
    ns, nf = mesh.shape["seq"], mesh.shape["fsdp"]
    na = nf // 4
    chips = 2 * na
    kv = KEY_VALUE_HEADS // ns
    group_columns = kv * (GROUP + 2) * HEAD_DIM

    core_pairs = [(i, i ^ 1) for i in range(nf)]
    b_pairs = [(i, i ^ 2) for i in range(nf)]

    def a_pairs(d):
        return [(i, (i + 4 * d) % nf) for i in range(nf)]

    def z_shift(d):
        return [(i, (i + d) % ns) for i in range(ns)]

    def to_core(x):
        return lax.ppermute(x, "fsdp", core_pairs)

    def to_b(x):
        return lax.ppermute(x, "fsdp", b_pairs)

    def to_a(x, d):
        return lax.ppermute(x, "fsdp", a_pairs(d))

    def add(*parts):
        total = parts[0].astype(F32)
        for part in parts[1:]:
            total = total + part.astype(F32)
        return total.astype(BF16)

    def reduce_b_first(left, right):
        rows = left.shape[1] // chips

        def block(da, db):
            at = (da * 2 + db) * rows
            return tn_dot(left[:, at : at + rows], right)

        arrived = [to_b(block(da, 1).astype(BF16)) for da in range(na)]
        kept = [(block(da, 0) + arrived[da].astype(F32)).astype(BF16) for da in range(na)]
        return add(kept[0], *[to_a(kept[d], d) for d in range(1, na)])

    def reduce_a_first(left, right):
        rows = left.shape[1] // chips

        def block(da, db):
            at = (da * 2 + db) * rows
            return tn_dot(left[:, at : at + rows], right)

        kept = []
        for db in (1, 0):
            arrived = [to_a(block(d, db).astype(BF16), d) for d in range(1, na)]
            total = block(0, db)
            for part in arrived:
                total = total + part.astype(F32)
            kept.append(total.astype(BF16))
        return add(kept[1], to_b(kept[0]))

    def sum_seq(x, me):
        half = ns // 2
        total = x
        for i in range(half - 1):
            total = add(total, lax.ppermute(total, "seq", [(i, i + 1), (ns - 1 - i, ns - 2 - i)]))
        if ns > 1:
            total = add(total, lax.ppermute(total, "seq", [(half - 1, half), (half, half - 1)]))
        for i in reversed(range(half - 1)):
            back = lax.ppermute(total, "seq", [(i + 1, i), (ns - 2 - i, ns - 1 - i)])
            total = jnp.where((me == i) | (me == ns - 1 - i), back, total)
        return total

    def body(tokens, cotangent, attention_gain, feedforward_gain, query_weight, key_matrix, value_matrix, out_weight, gate_weight, up_weight, down_weight):
        count, span, width = tokens.shape
        rows = count * span
        length = ns * span
        me = lax.axis_index("seq")
        mine = lax.axis_index("fsdp")
        core = mine % 2
        my_b = (mine // 2) % 2
        my_a = mine // 4
        order = jnp.stack([((my_a + da) % na) * 2 + (my_b + db) % 2 for da in range(na) for db in range(2)]).astype(jnp.int32)

        def gather(x):
            return lax.all_gather(x, "fsdp", axis=0, tiled=True)

        def relative(x):
            block = x.shape[1] // chips
            return jnp.concatenate([lax.dynamic_slice(x, (0, order[i] * block), (x.shape[0], block)) for i in range(chips)], axis=1)

        local = query_weight.shape[0]
        packed_weight = jnp.concatenate(
            [
                query_weight.reshape(local, ns, kv * GROUP * HEAD_DIM),
                key_matrix.reshape(local, ns, kv * HEAD_DIM),
                value_matrix.reshape(local, ns, kv * HEAD_DIM),
            ],
            axis=2,
        ).reshape(local, ns * group_columns)
        gains = lax.all_gather(jnp.stack([attention_gain, feedforward_gain]).astype(F32), "fsdp", axis=1, tiled=True)
        gain_one, gain_two = gains[0:1], gains[1:2]
        w_qkv = gather(packed_weight)
        w_out = gather(out_weight)
        w_gate = gather(gate_weight)
        w_up = gather(up_weight)
        w_down = gather(down_weight)

        heads = kv * (GROUP + 1)
        plain = kv * HEAD_DIM
        cosines, sines = rope_tables(me * span + jnp.arange(span, dtype=jnp.int32), heads, plain)
        all_cosines, all_sines = rope_tables(jnp.arange(length, dtype=jnp.int32), heads, plain)

        flat = tokens.reshape(rows, width)
        grad_flat = cotangent.reshape(rows, width)
        grad_low = grad_flat.astype(BF16)
        grad_low_other = to_core(grad_low)
        inverse = lax.rsqrt(jnp.mean(flat * flat, axis=-1, keepdims=True) + norm_eps)
        first = (flat * inverse * gain_one).astype(BF16)
        first_other = to_core(first)

        projected = {}
        for d in [*range(1, ns), 0]:
            projected[d] = project(first, w_qkv, cosines, sines, me, d, ns, count)
        packed = []
        for i in range(count):
            packed.append([projected[0][i]] + [lax.ppermute(projected[d][i], "seq", z_shift(d)) for d in range(1, ns)])
        attended_parts, log_totals, pieces = [], [], []
        for i in range(count):
            parts, logs = attend(packed[i], me, kv)
            attended_parts.append(parts)
            log_totals.append(logs)
            pieces += [parts[0]] + [lax.ppermute(parts[d], "seq", z_shift(d)) for d in range(1, ns)]
        attended, hidden_one, second = out_project(pieces, flat, w_out, gain_two, me, ns, count)
        second_other = to_core(second)

        act, dgate, dup, out_own, out_other, dx_own, dx_other = ffn(
            second, second_other, grad_low, grad_low_other, w_gate, w_up, w_down, order, core
        )
        dx_arrived = to_core(dx_other)
        high, low, gain_grad_two, grad_pieces = out_back(dx_own, dx_arrived, hidden_one, grad_flat, gain_two, w_out, me, ns, count)
        block_out = hidden_one + out_own + to_core(out_other).astype(F32)

        def tall(x):
            return x.reshape(2 * rows, x.shape[-1])

        second_all = relative(jnp.concatenate([second, second_other], axis=0))
        low_all = jnp.concatenate([grad_low, grad_low_other], axis=0)
        gate_sum = reduce_b_first(second_all, tall(dgate))
        up_sum = reduce_a_first(second_all, tall(dup))
        middle = width // 2
        down_sum = jnp.concatenate(
            [sum_seq(reduce_b_first(tall(act), low_all[:, :middle]), me), sum_seq(reduce_a_first(tall(act), low_all[:, middle:]), me)],
            axis=1,
        )
        gate_sum = sum_seq(gate_sum, me)
        up_sum = sum_seq(up_sum, me)

        def own_rows(x, columns_of):
            half = x.shape[0] // 2
            kept = lax.dynamic_slice(x, (core * half, 0), (half, x.shape[1]))
            given = lax.dynamic_slice(x, ((1 - core) * half, 0), (half, x.shape[1]))
            arrived = to_core(given)
            parts = jnp.where(core == 0, jnp.stack([kept, arrived]), jnp.stack([arrived, kept]))
            return columns_of(parts.astype(F32))

        def interleaved(parts):
            _, r, n = parts.shape
            return parts.reshape(2, r, chips, n // chips).transpose(1, 2, 0, 3).reshape(r, 2 * n)

        def side_by_side(parts):
            return jnp.concatenate([parts[0], parts[1]], axis=1)

        grad_gate = own_rows(gate_sum, interleaved)
        grad_up = own_rows(up_sum, interleaved)

        arrived_grads, qkv_pieces = [], []
        for i in range(count):
            parts = grad_pieces[i * ns : (i + 1) * ns]
            arrived_grads.append([parts[0]] + [lax.ppermute(parts[d], "seq", z_shift(d)) for d in range(1, ns)])
        for i in range(count):
            parts = attend_back(packed[i], arrived_grads[i], attended_parts[i], log_totals[i], all_cosines, all_sines, me, kv)
            qkv_pieces += [parts[0]] + [lax.ppermute(parts[d], "seq", z_shift(d)) for d in range(1, ns)]
        dqkv = sort_pieces(qkv_pieces, me, ns, count)

        def pick(x, which):
            return lax.dynamic_index_in_dim(x, which, 0, keepdims=False)

        attended_all = relative(jnp.concatenate([attended, to_core(attended)], axis=0))
        low_halves = jnp.stack([low[:, :middle], low[:, middle:]])
        low_mine = jnp.concatenate([pick(low_halves, core), to_core(pick(low_halves, 1 - core))], axis=0)
        quarter = middle // 2
        out_sum = jnp.concatenate(
            [
                sum_seq(reduce_b_first(attended_all, low_mine[:, :quarter]), me),
                sum_seq(reduce_a_first(attended_all, low_mine[:, quarter:]), me),
            ],
            axis=1,
        )
        grad_out = own_rows(out_sum, side_by_side)

        dqkv_mine = jnp.concatenate([pick(dqkv, core), to_core(pick(dqkv, 1 - core))], axis=0)
        first_all = relative(jnp.concatenate([first, first_other], axis=0))
        middle_qkv = dqkv_mine.shape[1] // 2
        qkv_sum = jnp.concatenate(
            [
                sum_seq(reduce_b_first(first_all, dqkv_mine[:, :middle_qkv]), me),
                sum_seq(reduce_a_first(first_all, dqkv_mine[:, middle_qkv:]), me),
            ],
            axis=1,
        )
        grad_qkv = own_rows(qkv_sum, side_by_side).reshape(local, ns, group_columns)
        q_end, k_end = kv * GROUP * HEAD_DIM, kv * (GROUP + 1) * HEAD_DIM
        grad_query = grad_qkv[:, :, :q_end].reshape(local, -1)
        grad_key = grad_qkv[:, :, q_end:k_end].reshape(local, -1)
        grad_value = grad_qkv[:, :, k_end:].reshape(local, -1)

        grad_tokens, gain_grad_one = project_back(dqkv, w_qkv, flat, high, gain_one)
        gain_grads = lax.psum(jnp.concatenate([gain_grad_one, gain_grad_two], axis=0), ("seq", "fsdp"))
        gain_grads = lax.dynamic_slice(gain_grads, (0, mine * local), (2, local))

        return (
            block_out.reshape(count, span, width),
            grad_tokens.reshape(count, span, width),
            gain_grads[0],
            gain_grads[1],
            grad_query,
            grad_key,
            grad_value,
            grad_out,
            grad_gate,
            grad_up,
            down_sum.astype(F32),
        )

    tokens_spec, gain_spec, weight_spec = P("fsdp", "seq", None), P("fsdp"), P("fsdp", None)
    return jax.shard_map(
        body,
        mesh=mesh,
        in_specs=(tokens_spec, tokens_spec, gain_spec, gain_spec) + (weight_spec,) * 7,
        out_specs=(tokens_spec, tokens_spec, gain_spec, gain_spec) + (weight_spec,) * 7,
        check_vma=False,
    )
```

```python
import functools
import math

import jax
import jax.numpy as jnp
from jax import lax
from jax.experimental import pallas as pl
from jax.experimental.pallas import tpu as pltpu
from jax.sharding import PartitionSpec as P

QUERY_HEADS = 16
KEY_VALUE_HEADS = 8
HEAD_DIM = 96
GROUP = QUERY_HEADS // KEY_VALUE_HEADS
norm_eps = 1e-05
rope_base = 100000.0
masked_score = -1e30
F32, BF16 = jnp.float32, jnp.bfloat16
VMEM_LIMIT = 60 * 1024 * 1024
VMEM_MOST = 67043328


def nt_dot(left, right):
    return lax.dot_general(left, right, (((1,), (1,)), ((), ())), preferred_element_type=F32)


def tn_dot(left, right):
    return lax.dot_general(left, right, (((0,), (0,)), ((), ())), preferred_element_type=F32)


def nn_dot(left, right):
    return jnp.dot(left, right, preferred_element_type=F32)


def whole(shape):
    return pl.BlockSpec(shape, lambda *_: (0,) * len(shape))


def call(kernel, scalars, operands, outs, name, flops, moved, scratch=()):
    return pl.pallas_call(
        kernel,
        grid_spec=pltpu.PrefetchScalarGridSpec(
            num_scalar_prefetch=1,
            grid=(1,),
            in_specs=[whole(x.shape) for x in operands],
            out_specs=[whole(x.shape) for x in outs],
            scratch_shapes=scratch,
        ),
        out_shape=outs,
        compiler_params=pltpu.CompilerParams(vmem_limit_bytes=VMEM_LIMIT),
        cost_estimate=pl.CostEstimate(flops=flops, bytes_accessed=moved, transcendentals=0),
        name=name,
    )(scalars, *operands)


def rope_tables(positions, heads, plain):
    half = HEAD_DIM // 2
    freqs = rope_base ** (-(2.0 * jnp.arange(half, dtype=F32)) / HEAD_DIM)
    angles = positions.astype(F32)[:, None] * freqs[None, :]
    cosine, sine = jnp.cos(angles), jnp.sin(angles)
    rows = positions.shape[0]
    cosines = jnp.concatenate([jnp.tile(jnp.concatenate([cosine, cosine], 1), (1, heads)), jnp.ones((rows, plain), F32)], 1)
    sines = jnp.concatenate([jnp.tile(jnp.concatenate([-sine, sine], 1), (1, heads)), jnp.zeros((rows, plain), F32)], 1)
    return cosines, sines


def swap_halves(values):
    half = HEAD_DIM // 2
    width = values.shape[1]
    lane = lax.broadcasted_iota(jnp.int32, values.shape, 1)
    ahead = pltpu.roll(values, width - half, 1)
    behind = pltpu.roll(values, half, 1)
    return jnp.where(lane % HEAD_DIM < half, ahead, behind)


def project_kernel(scalars, x, w, cosines, sines, *outs):
    y = nn_dot(x[...], w[...])
    span = cosines.shape[0]
    for i, out in enumerate(outs):
        part = y[i * span : (i + 1) * span]
        out[...] = (part * cosines[...] + swap_halves(part) * sines[...]).astype(BF16)


def project(x, w, cosines, sines, me, shift, ns, count):
    rows, width = x.shape
    columns = w.shape[1] // ns
    span = rows // count
    target = lax.rem(me + shift, ns).reshape(1)
    return pl.pallas_call(
        project_kernel,
        grid_spec=pltpu.PrefetchScalarGridSpec(
            num_scalar_prefetch=1,
            grid=(1,),
            in_specs=[
                whole(x.shape),
                pl.BlockSpec((width, columns), lambda i, s: (0, s[0])),
                whole(cosines.shape),
                whole(sines.shape),
            ],
            out_specs=[whole((span, columns))] * count,
        ),
        out_shape=[jax.ShapeDtypeStruct((span, columns), BF16)] * count,
        compiler_params=pltpu.CompilerParams(vmem_limit_bytes=VMEM_LIMIT),
        cost_estimate=pl.CostEstimate(
            flops=2 * rows * width * columns,
            bytes_accessed=2 * (rows * width + width * columns + rows * columns),
            transcendentals=0,
        ),
        name="project",
    )(target, x, w, cosines, sines)


def load_heads(me, ns, packed, full, qs, ks, vs, kv):
    span = packed[0].shape[0]
    for d in range(ns):
        at = pl.ds(pl.multiple_of(lax.rem(me + ns - d, ns) * span, span), span)
        piece = packed[d][...]
        full[at, :] = piece
        for h in range(kv * GROUP):
            qs[h, at, :] = piece[:, h * HEAD_DIM : (h + 1) * HEAD_DIM]
        for h in range(kv):
            k0 = (kv * GROUP + h) * HEAD_DIM
            v0 = (kv * GROUP + kv + h) * HEAD_DIM
            ks[h, at, :] = piece[:, k0 : k0 + HEAD_DIM]
            vs[h, at, :] = piece[:, v0 : v0 + HEAD_DIM]


def attend_kernel(ns, kv, scalars, *refs):
    packed, outs = refs[:ns], refs[ns : 2 * ns]
    logs, result, full, qs, ks, vs = refs[2 * ns :]
    me = scalars[0]
    span = packed[0].shape[0]
    scale = 1.0 / math.sqrt(HEAD_DIM)
    load_heads(me, ns, packed, full, qs, ks, vs, kv)
    row = lax.broadcasted_iota(jnp.int32, (span, span), 0)
    column = lax.broadcasted_iota(jnp.int32, (span, span), 1)
    causal = row >= column
    lane = lax.broadcasted_iota(jnp.int32, (span, 128), 1)
    for s in range(ns):
        here = slice(s * span, (s + 1) * span)
        stats = jnp.zeros((span, 128), F32)
        for h in range(kv * GROUP):
            g = h // GROUP
            q = qs[h, here, :]
            near = jnp.where(causal, nt_dot(q, ks[g, here, :]) * scale, masked_score)
            top = jnp.max(near, axis=1, keepdims=True)
            if s > 0:
                far = nt_dot(q, ks[g, : s * span, :]) * scale
                top = jnp.maximum(top, jnp.max(far, axis=1, keepdims=True))
            near = jnp.exp(near - top)
            total = jnp.sum(near, axis=1, keepdims=True)
            if s > 0:
                far = jnp.exp(far - top)
                total = total + jnp.sum(far, axis=1, keepdims=True)
            inverse = 1.0 / total
            out = nn_dot((near * inverse).astype(BF16), vs[g, here, :])
            if s > 0:
                out = out + nn_dot((far * inverse).astype(BF16), vs[g, : s * span, :])
            stats = jnp.where(lane == h, top + jnp.log(total), stats)
            result[here, h * HEAD_DIM : (h + 1) * HEAD_DIM] = out.astype(BF16)
        logs[here, :] = stats
    for d in range(ns):
        at = pl.ds(pl.multiple_of(lax.rem(me + d, ns) * span, span), span)
        outs[d][...] = result[at, :]


def attend(packed, me, kv):
    ns = len(packed)
    span = packed[0].shape[0]
    length = ns * span
    heads = kv * GROUP
    outs = [jax.ShapeDtypeStruct((span, heads * HEAD_DIM), BF16)] * ns + [
        jax.ShapeDtypeStruct((length, 128), F32),
        jax.ShapeDtypeStruct((length, heads * HEAD_DIM), BF16),
        jax.ShapeDtypeStruct((length, packed[0].shape[1]), BF16),
    ]
    results = call(
        functools.partial(attend_kernel, ns, kv),
        me.reshape(1),
        packed,
        outs,
        "attend",
        2 * heads * length * length * 2 * 128,
        4 * length * heads * HEAD_DIM * 2,
        [
            pltpu.VMEM((heads, length, HEAD_DIM), BF16),
            pltpu.VMEM((kv, length, HEAD_DIM), BF16),
            pltpu.VMEM((kv, length, HEAD_DIM), BF16),
        ],
    )
    return results[:ns], results[ns], results[ns + 1], results[ns + 2]


def out_kernel(ns, count, scalars, *refs):
    pieces = refs[: ns * count]
    tokens, w, gain, attended, hidden, inputs = refs[ns * count :]
    me = scalars[0]
    span, width = pieces[0].shape
    for d in range(ns):
        for j in range(ns):

            @pl.when(lax.rem(me + ns - d, ns) == j)
            def _():
                for i in range(count):
                    attended[i * span : (i + 1) * span, j * width : (j + 1) * width] = pieces[i * ns + d][...]

    rows = tokens[...] + nn_dot(attended[...], w[...])
    hidden[...] = rows
    inverse = lax.rsqrt(jnp.mean(rows * rows, axis=1, keepdims=True) + norm_eps)
    inputs[...] = (rows * inverse * gain[...]).astype(BF16)


def out_project(pieces, tokens, w, gain, me, ns, count):
    shape = tokens.shape
    return call(
        functools.partial(out_kernel, ns, count),
        me.reshape(1),
        [*pieces, tokens, w, gain],
        [jax.ShapeDtypeStruct(shape, BF16), jax.ShapeDtypeStruct(shape, F32), jax.ShapeDtypeStruct(shape, BF16)],
        "out_project",
        2 * shape[0] * w.shape[0] * w.shape[1],
        14 * shape[0] * shape[1],
    )


def norm_back(grad, normed, inverse, gain):
    scaled = grad * gain
    return inverse * (scaled - normed * jnp.mean(scaled * normed, axis=1, keepdims=True))


MESH = pl.DeviceIdType.MESH


def ffn_kernel(tiles, scalars, x, g, wg, wu, wd, dwg, dwu, dwd, out_own, out_other, dx_own, dx_other, xt, acc_out, acc_dx, act, dgate, dup):
    step = pl.program_id(0)
    rows = x.shape[0] // 2

    @pl.when(step == 0)
    def _():
        out_own[...] = jnp.zeros_like(out_own)
        dx_own[...] = jnp.zeros_like(dx_own)
        acc_out[...] = jnp.zeros_like(acc_out)
        acc_dx[...] = jnp.zeros_like(acc_dx)
        xt[...] = x[...].T

    for i, (out, dx) in enumerate(((out_own, dx_own), (acc_out, acc_dx))):
        here = slice(i * rows, (i + 1) * rows)
        gate = nn_dot(x[here, :], wg[...])
        up = nn_dot(x[here, :], wu[...])
        grad = nt_dot(g[here, :], wd[...])
        sigmoid = jax.nn.sigmoid(gate)
        silu = gate * sigmoid
        hidden = (silu * up).astype(BF16)
        act[here, :] = hidden
        gate_grad = (grad * up * sigmoid * (1.0 + gate * (1.0 - sigmoid))).astype(BF16)
        up_grad = (grad * silu).astype(BF16)
        dgate[here, :] = gate_grad
        dup[here, :] = up_grad
        out[...] += nn_dot(hidden, wd[...])
        dx[...] += nt_dot(gate_grad, wg[...]) + nt_dot(up_grad, wu[...])
    dwg[...] = nn_dot(xt[...], dgate[...]).astype(BF16)
    dwu[...] = nn_dot(xt[...], dup[...]).astype(BF16)
    dwd[...] = tn_dot(act[...], g[...]).astype(BF16)

    @pl.when(step == tiles - 1)
    def _():
        out_other[...] = acc_out[...].astype(BF16)
        dx_other[...] = acc_dx[...].astype(BF16)


def ffn(x, g, wg, wu, wd, core, chips):
    rows, width = x.shape[0] // 2, x.shape[1]
    parts = 2
    tiles = chips * parts
    cols = wg.shape[1] // (2 * tiles)
    keep = lambda shape: pl.BlockSpec(shape, lambda i, s: (0, 0), pipeline_mode=pl.Buffered(1))
    last = lambda: pl.BlockSpec((rows, width), lambda i, s: (0, 0))

    def column(i, s):
        return ((i // parts) * 2 + s[0]) * parts + i % parts

    half = cols * tiles
    wide, low = jax.ShapeDtypeStruct((rows, width), F32), jax.ShapeDtypeStruct((rows, width), BF16)
    return pl.pallas_call(
        functools.partial(ffn_kernel, tiles),
        grid_spec=pltpu.PrefetchScalarGridSpec(
            num_scalar_prefetch=1,
            grid=(tiles,),
            in_specs=[keep(x.shape), keep(g.shape)]
            + [pl.BlockSpec((width, cols), lambda i, s: (0, column(i, s)))] * 2
            + [pl.BlockSpec((cols, width), lambda i, s: (column(i, s), 0))],
            out_specs=[pl.BlockSpec((width, cols), lambda i, s: (0, i))] * 2
            + [pl.BlockSpec((cols, width), lambda i, s: (i, 0)), last(), last(), last(), last()],
            scratch_shapes=[pltpu.VMEM((width, 2 * rows), BF16)]
            + [pltpu.VMEM((rows, width), F32)] * 2
            + [pltpu.VMEM((2 * rows, cols), BF16)] * 3,
        ),
        out_shape=[
            jax.ShapeDtypeStruct((width, half), BF16),
            jax.ShapeDtypeStruct((width, half), BF16),
            jax.ShapeDtypeStruct((half, width), BF16),
            wide,
            low,
            wide,
            low,
        ],
        compiler_params=pltpu.CompilerParams(vmem_limit_bytes=VMEM_LIMIT),
        cost_estimate=pl.CostEstimate(
            flops=36 * rows * width * half, bytes_accessed=12 * width * half + 20 * rows * width, transcendentals=0
        ),
        name="ffn",
    )(core.reshape(1).astype(jnp.int32), x, g, wg, wu, wd)


def part(x):
    return x[0].at[x[1:]] if isinstance(x, tuple) else x


def get(x):
    return x[0][x[1:]] if isinstance(x, tuple) else x[...]


def put(x, value):
    if isinstance(x, tuple):
        x[0][x[1:]] = value
    else:
        x[...] = value


class Copy:
    def __init__(self, src, dst, device, send_sem, recv_sem):
        self.src, self.dst, self.device, self.send_sem, self.recv_sem = src, dst, device, send_sem, recv_sem

    def made(self):
        if self.device is None:
            return pltpu.make_async_copy(part(self.src), part(self.dst), part(self.send_sem))
        return pltpu.make_async_remote_copy(
            src_ref=part(self.src),
            dst_ref=part(self.dst),
            send_sem=part(self.send_sem),
            recv_sem=part(self.recv_sem),
            device_id=self.device,
            device_id_type=MESH,
        )

    def start(self):
        self.made().start()

    def wait(self):
        self.made().wait()

    def wait_send(self):
        self.made().wait_send()

    def wait_recv(self):
        self.made().wait_recv()


class Links:
    def __init__(self, mesh, send_sems, recv_sems, local_sems):
        self.ns, self.nf = mesh
        self.na = self.nf // 4
        self.send_sems, self.recv_sems, self.local_sems = send_sems, recv_sems, local_sems
        self.count, self.local_count = 0, 0
        self.z, self.f = lax.axis_index("seq"), lax.axis_index("fsdp")
        self.core = lax.rem(self.f, 2)
        self.b = lax.rem(self.f // 2, 2)
        self.a = self.f // 4

    def chip(self, da, db):
        return lax.rem(self.a + da, self.na) * 2 + lax.rem(self.b + db, 2)

    def at_core(self):
        return (self.z, self.f + 1 - 2 * self.core)

    def at_b(self):
        return (self.z, self.f + 2 - 4 * self.b)

    def at_a(self, d):
        return (self.z, lax.rem(self.f + 4 * d, self.nf))

    def at_z(self, d):
        return (lax.rem(self.z + d, self.ns), self.f)

    def peers(self):
        return [self.at_core(), self.at_b()] + [self.at_a(d) for d in range(1, self.na)] + [self.at_z(d) for d in range(1, self.ns)]

    def barrier(self):
        barrier = pltpu.get_barrier_semaphore()
        peers = self.peers()
        for peer in peers:
            pl.semaphore_signal(barrier, inc=1, device_id=peer, device_id_type=MESH)
        pl.semaphore_wait(barrier, len(peers))

    def copy(self, src, dst, device):
        index = self.count
        self.count += 1
        return Copy(src, dst, device, (self.send_sems, index), (self.recv_sems, index))

    def again(self, src, dst, device):
        index = self.count - 1
        return Copy(src, dst, device, (self.send_sems, index), (self.recv_sems, index))

    def local(self, src, dst):
        index = self.local_count
        self.local_count += 1
        return Copy(src, dst, None, (self.local_sems, index), None)


def rows_at(start, size):
    return pl.ds(pl.multiple_of(start * size, size), size)


class ChipSum:
    def __init__(self, links, partial, b_first, arrived, passed, staging):
        self.links, self.partial, self.b_first = links, partial, b_first
        self.arrived, self.passed, self.staging = arrived, passed, staging
        na = links.na
        self.first, self.second = [], []
        if b_first:
            self.kept = [links.chip(da, 0) for da in range(na)]
            for da in range(na):
                self.first.append(links.copy(partial(links.chip(da, 1)), (arrived, da), links.at_b()))
            for d in range(1, na):
                self.second.append(links.copy((arrived, d), (passed, d - 1), links.at_a(d)))
        else:
            self.kept = [links.chip(0, db) for db in range(2)]
            for d in range(1, na):
                for db in range(2):
                    self.first.append(links.copy(partial(links.chip(d, db)), (arrived, (d - 1) * 2 + db), links.at_a(d)))
            self.second.append(links.copy((arrived, 1), (passed, 0), links.at_b()))
        self.loads = [] if staging is None else [links.local(partial(k), (staging, i)) for i, k in enumerate(self.kept)]

    def start(self):
        for copy in self.first:
            copy.start()

    def load(self):
        for load in self.loads:
            load.start()

    def turn(self):
        for load in self.loads:
            load.wait()
        for copy in self.first:
            copy.wait()
        count = len(self.kept)
        for i in [*range(1, count), 0]:
            own = self.partial(self.kept[i]) if self.staging is None else (self.staging, i)
            total = get(own).astype(F32)
            if self.b_first:
                total = total + self.arrived[i].astype(F32)
            else:
                for d in range(self.links.na - 1):
                    total = total + self.arrived[d * 2 + i].astype(F32)
            self.arrived[i] = total.astype(BF16)
            if i > 0 and self.b_first:
                self.second[i - 1].start()
            elif i > 0:
                self.second[0].start()

    def finish(self):
        for copy in self.second:
            copy.wait()
        total = self.arrived[0].astype(F32)
        for i in range(len(self.second)):
            total = total + self.passed[i].astype(F32)
        return total.astype(BF16)


def chip_sum_shapes(na, b_first, rows, columns):
    first = na if b_first else 2 * (na - 1)
    kept = na if b_first else 2
    return [
        pltpu.VMEM((max(first, kept), rows, columns), BF16),
        pltpu.VMEM((na - 1 if b_first else 1, rows, columns), BF16),
        pltpu.VMEM((kept, rows, columns), BF16),
    ]


def each(index, count, act):
    for j in range(count):
        pl.when(index == j)(functools.partial(act, j))


def attend_back_heads(ns, kv, span, qs, ks, vs, gs, attended, logs, dk, dv, result):
    scale = 1.0 / math.sqrt(HEAD_DIM)
    heads = kv * GROUP
    row = lax.broadcasted_iota(jnp.int32, (span, span), 0)
    column = lax.broadcasted_iota(jnp.int32, (span, span), 1)
    causal = row >= column
    dk[...] = jnp.zeros_like(dk)
    dv[...] = jnp.zeros_like(dv)
    for s in range(ns):
        here = slice(s * span, (s + 1) * span)
        for h in range(heads):
            g = h // GROUP
            q, grad = qs[h, here, :], gs[h, here, :]
            log_total = logs[here, h : h + 1]
            out = attended[here, h * HEAD_DIM : (h + 1) * HEAD_DIM]
            delta = jnp.sum(grad.astype(F32) * out.astype(F32), axis=1, keepdims=True)
            k, v = ks[g, here, :], vs[g, here, :]
            near = jnp.where(causal, jnp.exp(nt_dot(q, k) * scale - log_total), 0.0)
            slope = (near * (nt_dot(grad, v) - delta) * scale).astype(BF16)
            dq = nn_dot(slope, k)
            dk[g, here, :] += tn_dot(slope, q)
            dv[g, here, :] += tn_dot(near.astype(BF16), grad)
            if s > 0:
                before = slice(0, s * span)
                k, v = ks[g, before, :], vs[g, before, :]
                far = jnp.exp(nt_dot(q, k) * scale - log_total)
                slope = (far * (nt_dot(grad, v) - delta) * scale).astype(BF16)
                dq = dq + nn_dot(slope, k)
                dk[g, before, :] += tn_dot(slope, q)
                dv[g, before, :] += tn_dot(far.astype(BF16), grad)
            result[here, h * HEAD_DIM : (h + 1) * HEAD_DIM] = dq
    for g in range(kv):
        k0 = (heads + g) * HEAD_DIM
        v0 = (heads + kv + g) * HEAD_DIM
        result[:, k0 : k0 + HEAD_DIM] = dk[g]
        result[:, v0 : v0 + HEAD_DIM] = dv[g]


def back_kernel(
    mesh, count, kv,
    dx_own, dx_other, hidden, cotangent, gain_two, w_out, w_qkv, packed, attended, logs, cosines, sines, tokens, gain_one, dwg, dwu,
    high, low, out, gain_grads, dqkv, sum_gate, sum_up,
    dx_land, g_send, g_land, q_send, q_land, swap_send, swap_land, *rest,
):
    parts, (send_sems, recv_sems, local_sems) = rest[:-3], rest[-3:]
    links = Links(mesh, send_sems, recv_sems, local_sems)
    ns, na = links.ns, links.na
    chips = 2 * na
    z, core = links.z, links.core
    rows, width = hidden.shape
    span = rows // count
    length = ns * span
    heads = kv * GROUP
    g_width, q_width = heads * HEAD_DIM, (heads + 2 * kv) * HEAD_DIM
    half = dwg.shape[1]
    block = width // chips
    links.barrier()

    dx_copy = links.copy(dx_other, dx_land, links.at_core())
    dx_copy.start()
    sums = []
    for n, source in enumerate((dwg, dwu)):
        for b_first in (True, False):
            columns = slice(0, half // 2) if b_first else slice(half // 2, half)
            at = (n * 2 + (0 if b_first else 1)) * 3
            partial = lambda k, source=source, columns=columns: (source, rows_at(k, block), columns)
            sums.append(ChipSum(links, partial, b_first, *parts[at : at + 3]))
    for item in sums:
        item.start()
        item.load()

    g_copies, q_copies = [], []
    for i in range(count):
        g_copies.append([links.copy((g_send, i, lax.rem(z + d, ns)), (g_land, i, z), links.at_z(d)) for d in range(1, ns)])
        q_copies.append([links.copy((q_send, i, lax.rem(z + d, ns)), (q_land, z, i), links.at_z(d)) for d in range(1, ns)])

    def out_back(dx, old, grad, w):
        loads = [links.local(dx_own, dx), links.local(hidden, old), links.local(cotangent, grad), links.local(w_out, w)]
        for load in loads:
            load.start()
        dx_copy.wait()
        for load in loads[:3]:
            load.wait()
        step = dx[...] + dx_land[...].astype(F32)
        inverse = lax.rsqrt(jnp.mean(old[...] * old[...], axis=1, keepdims=True) + norm_eps)
        normed = old[...] * inverse
        gain_grads[1:2, :] = jnp.sum(step * normed, axis=0, keepdims=True)
        grad[...] = grad[...] + norm_back(step, normed, inverse, gain_two[...])
        low[...] = grad[...].astype(BF16)
        stores = [links.local(grad, high)]
        for store in stores:
            store.start()
        loads[3].wait()
        for i in range(count):
            here = slice(i * span, (i + 1) * span)
            part = nt_dot(low[here, :], w[...]).astype(BF16)
            for j in range(ns):
                g_send[i, j] = part[:, j * g_width : (j + 1) * g_width]
            for copies in g_copies[i]:
                copies.start()
            g_land[i, z] = g_send[i, z]
        for store in stores:
            store.wait()

    pl.run_scoped(
        out_back,
        pltpu.VMEM((rows, width), F32),
        pltpu.VMEM((rows, width), F32),
        pltpu.VMEM((rows, width), F32),
        pltpu.VMEM((width, width), BF16),
    )

    def attention(qkv, mid, log, qs, ks, vs, gs, dk, dv, result, cosine, sine):
        tables = [links.local(cosines, cosine), links.local(sines, sine)]
        for load in tables:
            load.start()
        for i in range(count):
            loads = [links.local((packed, i), qkv), links.local((attended, i), mid), links.local((logs, i), log)]
            for load in loads:
                load.start()
            for load in loads:
                load.wait()
            for h in range(heads):
                qs[h] = qkv[:, h * HEAD_DIM : (h + 1) * HEAD_DIM]
            for h in range(kv):
                k0, v0 = (heads + h) * HEAD_DIM, (heads + kv + h) * HEAD_DIM
                ks[h] = qkv[:, k0 : k0 + HEAD_DIM]
                vs[h] = qkv[:, v0 : v0 + HEAD_DIM]
            for copies in g_copies[i]:
                copies.wait()
            for j in range(ns):
                for h in range(heads):
                    gs[h, j * span : (j + 1) * span, :] = g_land[i, j, :, h * HEAD_DIM : (h + 1) * HEAD_DIM]
            attend_back_heads(ns, kv, span, qs, ks, vs, gs, mid, log, dk, dv, result)
            if i == 0:
                for load in tables:
                    load.wait()
            for j in range(ns):
                here = slice(j * span, (j + 1) * span)
                part = result[here, :]
                q_send[i, j] = (part * cosine[here, :] - swap_halves(part) * sine[here, :]).astype(BF16)
            for copies in q_copies[i]:
                copies.start()
            q_land[z, i] = q_send[i, z]
            if i < len(sums) // 2:
                for item in sums[2 * i : 2 * i + 2]:
                    item.turn()

    pl.run_scoped(
        attention,
        pltpu.VMEM((length, q_width), BF16),
        pltpu.VMEM((length, g_width), BF16),
        pltpu.VMEM((length, 128), F32),
        pltpu.VMEM((heads, length, HEAD_DIM), BF16),
        pltpu.VMEM((kv, length, HEAD_DIM), BF16),
        pltpu.VMEM((kv, length, HEAD_DIM), BF16),
        pltpu.VMEM((heads, length, HEAD_DIM), BF16),
        pltpu.VMEM((kv, length, HEAD_DIM), F32),
        pltpu.VMEM((kv, length, HEAD_DIM), F32),
        pltpu.VMEM((length, q_width), F32),
        pltpu.VMEM((length, q_width), F32),
        pltpu.VMEM((length, q_width), F32),
    )

    swaps = []
    local = block // 2
    for item in sums[2 * count :]:
        item.turn()

    def swap(n):
        for m in range(2):
            total = sums[2 * n + m].finish()
            swap_send[n, m, 0] = total[:local]
            swap_send[n, m, 1] = total[local:]
        for m in range(2):
            copies = links.copy((swap_send, n, m, 1 - core), (swap_land, n, m), links.at_core())
            copies.start()
            swaps.append(copies)

    swap(0)

    def project_back(w, old, base, grad):
        loads = [links.local(w_qkv, w), links.local(tokens, old), links.local(high, base)]
        for load in loads:
            load.start()
        for load in loads:
            load.wait()
        for i in range(count):
            here = slice(i * span, (i + 1) * span)
            for copies in q_copies[i]:
                copies.wait()
            total = nt_dot(q_land[0, i], w[:, :q_width])
            for j in range(1, ns):
                total = total + nt_dot(q_land[j, i], w[:, j * q_width : (j + 1) * q_width])
            grad[here, :] = total
        step = grad[...]
        inverse = lax.rsqrt(jnp.mean(old[...] * old[...], axis=1, keepdims=True) + norm_eps)
        normed = old[...] * inverse
        gain_grads[0:1, :] = jnp.sum(step * normed, axis=0, keepdims=True)
        base[...] = base[...] + norm_back(step, normed, inverse, gain_one[...])
        stores = [links.local(base, out), links.local(q_land, dqkv)]
        for store in stores:
            store.start()
        for store in stores:
            store.wait()

    pl.run_scoped(
        project_back,
        pltpu.VMEM((width, ns * q_width), BF16),
        pltpu.VMEM((rows, width), F32),
        pltpu.VMEM((rows, width), F32),
        pltpu.VMEM((rows, width), F32),
    )
    swap(1)
    tile = half // chips
    for n, total in enumerate((sum_gate, sum_up)):
        for m in range(2):
            swaps[2 * n + m].wait()
            kept, arrived = swap_send[n, m, core], swap_land[n, m]
            for t in range(chips // 2):
                here = slice(t * tile, (t + 1) * tile)
                k = m * (chips // 2) + t
                first, second = kept[:, here], arrived[:, here]
                total[:, 2 * k * tile : (2 * k + 1) * tile] = jnp.where(core == 0, first, second)
                total[:, (2 * k + 1) * tile : (2 * k + 2) * tile] = jnp.where(core == 0, second, first)


def back(mesh, count, kv, dx_own, dx_other, hidden, cotangent, gain_two, w_out, w_qkv, packed, attended, logs, cosines, sines, tokens, gain_one, dwg, dwu):
    ns, nf = mesh
    na = nf // 4
    rows, width = hidden.shape
    span = rows // count
    heads = kv * GROUP
    g_width, q_width = heads * HEAD_DIM, (heads + 2 * kv) * HEAD_DIM
    half = dwg.shape[1]
    block = width // (2 * na)
    local = block // 2
    anywhere = pl.BlockSpec(memory_space=pl.ANY)
    vmem = pl.BlockSpec(memory_space=pltpu.VMEM)
    operands = [dx_own, dx_other, hidden, cotangent, gain_two, w_out, w_qkv, packed, attended, logs, cosines, sines, tokens, gain_one, dwg, dwu]
    wide = jax.ShapeDtypeStruct((rows, width), F32)
    summed = jax.ShapeDtypeStruct((local, 2 * half), BF16)
    scratch = [
        pltpu.VMEM((rows, width), BF16),
        pltpu.VMEM((count, ns, span, g_width), BF16),
        pltpu.VMEM((count, ns, span, g_width), BF16),
        pltpu.VMEM((count, ns, span, q_width), BF16),
        pltpu.VMEM((ns, count, span, q_width), BF16),
        pltpu.VMEM((2, 2, 2, local, half // 2), BF16),
        pltpu.VMEM((2, 2, local, half // 2), BF16),
    ]
    for _ in range(2):
        for b_first in (True, False):
            scratch += chip_sum_shapes(na, b_first, block, half // 2)
    return pl.pallas_call(
        functools.partial(back_kernel, mesh, count, kv),
        in_specs=[vmem if x.shape[0] == 1 else anywhere for x in operands],
        out_specs=[anywhere, vmem, anywhere, vmem, anywhere, vmem, vmem],
        out_shape=[
            wide,
            jax.ShapeDtypeStruct((rows, width), BF16),
            wide,
            jax.ShapeDtypeStruct((2, width), F32),
            jax.ShapeDtypeStruct((ns, count, span, q_width), BF16),
            summed,
            summed,
        ],
        scratch_shapes=scratch
        + [pltpu.SemaphoreType.DMA((64,)), pltpu.SemaphoreType.DMA((64,)), pltpu.SemaphoreType.DMA((64,))],
        compiler_params=pltpu.CompilerParams(vmem_limit_bytes=VMEM_MOST, collective_id=1, has_side_effects=True),
        name="back",
    )(*operands)


class LineSum:
    def __init__(self, links, term, first, second, total):
        self.links, self.term, self.first, self.second, self.total = links, term, first, second, total
        z, ns = links.z, links.ns
        self.dtype = (term[0] if isinstance(term, tuple) else term).dtype
        middle = ns // 2
        self.deep = middle > 1
        lower = z < middle
        step = jnp.where(lower, 1, -1)
        self.end = (z == 0) | (z == ns - 1)
        self.inner = (z == middle - 1) | (z == middle)
        inward, outward = (z + step, links.f), (z - step, links.f)
        self.inward = links.copy(term, first, inward) if self.deep else None
        self.onward = links.again(first, first, inward) if self.deep else None
        self.across = links.copy(first if self.deep else term, second, inward)
        self.outward = links.copy(total, total, outward) if self.deep else None

    def add(self, target, one, two):
        put(target, (get(one).astype(F32) + get(two).astype(F32)).astype(self.dtype))

    def begin(self):
        if self.deep:
            pl.when(self.end)(self.inward.start)
        else:
            self.across.start()

    def relay(self):
        if not self.deep:
            return

        @pl.when(jnp.logical_not(self.end))
        def _():
            self.inward.wait_recv()
            self.add(self.first, self.term, self.first)
            pl.when(self.inner)(self.across.start)
            pl.when(jnp.logical_not(self.inner))(self.onward.start)

    def settle(self):
        @pl.when(self.inner)
        def _():
            self.across.wait()
            self.add(self.total, self.first if self.deep else self.term, self.second)
            if self.deep:
                self.outward.start()

        if self.deep:

            @pl.when(jnp.logical_not(self.inner | self.end))
            def _():
                self.outward.wait_recv()
                self.outward.start()

    def finish(self):
        if not self.deep:
            return
        pl.when(self.end)(self.outward.wait_recv)
        pl.when(jnp.logical_not(self.inner))(self.inward.wait_send)
        pl.when(jnp.logical_not(self.end))(self.outward.wait_send)


def finish_kernel(
    mesh, count, kv,
    term_gate, term_up, dwd, first, dqkv, attended, low, gains,
    out_gate, out_up, out_down, out_out, out_qkv, out_gains,
    term_down, term_out, term_qkv, in_gate, in_up, in_down, in_out, in_qkv,
    first_both, attended_both, low_both, dq_both, w_out_part, w_qkv_part,
    swap_out, land_out, swap_qkv, land_qkv, gain_terms, gain_lands, *rest,
):
    parts, (send_sems, recv_sems, local_sems) = rest[:-3], rest[-3:]
    links = Links(mesh, send_sems, recv_sems, local_sems)
    ns, na = links.ns, links.na
    chips, per = 2 * na, ns // 2
    core = links.core
    rows, width = first.shape
    q_width = dqkv.shape[3]
    middle = width // 2
    links.barrier()

    def lines(term, inbox, out, pieces):
        size = term.shape[1] // pieces
        every = slice(None)
        made = []
        for i in range(pieces):
            at = slice(i * size, (i + 1) * size)
            made.append(LineSum(links, (term, every, at), (inbox, 0, every, at), (inbox, 1, every, at), (out, every, at)))
        return made

    gate_lines = lines(term_gate, in_gate, out_gate, 2)
    up_lines = lines(term_up, in_up, out_up, 2)
    down_lines = lines(term_down, in_down, out_down, 2)
    out_lines = lines(term_out, in_out, out_out, 1)
    qkv_lines = lines(term_qkv, in_qkv, out_qkv, 2)
    for line in gate_lines + up_lines:
        line.begin()

    sends = [
        links.copy((dqkv, pl.ds((1 - core) * per, per)), (dq_both, 1), links.at_core()),
        links.copy((low, slice(None), rows_at(1 - core, middle)), (low_both, 1), links.at_core()),
        links.copy(first, (first_both, 1), links.at_core()),
        links.copy(attended, (attended_both, 1), links.at_core()),
    ]
    loads = [
        links.local((low, slice(None), rows_at(core, middle)), (low_both, 0)),
        links.local(attended, (attended_both, 0)),
        links.local(first, (first_both, 0)),
        links.local((dqkv, pl.ds(core * per, per)), (dq_both, 0)),
    ]
    for copies in loads + sends[1:2] + sends[3:4] + sends[2:3] + sends[:1]:
        copies.start()

    down_rows = dwd.shape[0] // chips
    block = width // chips

    def pair(source, row_count, at, staged):
        made = []
        cut = source.shape[1] // 2
        for n, b_first in enumerate((True, False)):
            columns = slice(0, cut) if b_first else slice(cut, 2 * cut)
            partial = lambda k, columns=columns: (source, rows_at(k, row_count), columns)
            refs = parts[at[n] : at[n + 1]]
            made.append(ChipSum(links, partial, b_first, *(refs if staged else (*refs[:2], None))))
        return made

    down = pair(dwd, down_rows, (0, 3, 6), True)
    for item in down:
        item.start()
        item.load()

    gain_copies = [links.copy((gain_terms, 0), (gain_lands, 0), links.at_core()), links.copy((gain_terms, 1), (gain_lands, 1), links.at_b())]
    gain_copies += [links.copy((gain_terms, 2), (gain_lands, 1 + d), links.at_a(d)) for d in range(1, na)]
    gain_line = LineSum(links, (gain_terms, 3), (gain_lands, na + 1), (gain_lands, na + 2), out_gains)
    gain_terms[0] = gains[...]
    gain_copies[0].start()

    for i in (1, 3):
        sends[i].wait()
    for i in (0, 1):
        loads[i].wait()
    for k in range(chips):
        at = slice(k * block, (k + 1) * block)
        total = tn_dot(attended_both[0, :, at], low_both[0]) + tn_dot(attended_both[1, :, at], low_both[1])
        w_out_part[at, :] = total.astype(BF16)
    out_sums = pair(w_out_part, block, (6, 8, 10), False)
    for item in out_sums:
        item.start()
    for i in (0, 2):
        sends[i].wait()
    for i in (2, 3):
        loads[i].wait()
    for p in range(per):
        columns = slice(p * q_width, (p + 1) * q_width)
        mine, other = dq_both[0, p].reshape(rows, q_width), dq_both[1, p].reshape(rows, q_width)
        for k in range(chips):
            at = slice(k * block, (k + 1) * block)
            total = tn_dot(first_both[0, :, at], mine) + tn_dot(first_both[1, :, at], other)
            w_qkv_part[at, columns] = total.astype(BF16)
    qkv_sums = pair(w_qkv_part, block, (10, 12, 14), False)
    for item in qkv_sums:
        item.start()

    def next_gain(i):
        gain_copies[i].wait()
        gain_terms[i + 1] = gain_terms[i] + gain_lands[i]
        if i == 0:
            gain_copies[1].start()
        else:
            for copies in gain_copies[2:]:
                copies.start()

    next_gain(0)
    for item in down:
        item.turn()
    for line in gate_lines:
        line.relay()
    next_gain(1)
    for item in out_sums:
        item.turn()
    cut = width // 2
    term_down[:, :cut] = down[0].finish()
    term_down[:, cut:] = down[1].finish()
    for line in down_lines:
        line.begin()
    for item in qkv_sums:
        item.turn()
    for copies in gain_copies[2:]:
        copies.wait()
    total = gain_terms[2]
    for d in range(1, na):
        total = total + gain_lands[1 + d]
    gain_terms[3] = total
    gain_line.begin()

    def swap(sums, send, land):
        local = block // 2
        for n, item in enumerate(sums):
            total = item.finish()
            size = total.shape[1]
            send[0, :, n * size : (n + 1) * size] = total[:local]
            send[1, :, n * size : (n + 1) * size] = total[local:]
        copies = links.copy((send, 1 - core), land, links.at_core())
        copies.start()
        return copies

    out_swap = swap(out_sums, swap_out, land_out)
    gate_lines[0].settle()
    up_lines[0].relay()
    gate_lines[1].settle()
    up_lines[1].relay()
    gain_line.relay()
    qkv_swap = swap(qkv_sums, swap_qkv, land_qkv)
    out_swap.wait()
    kept, arrived = swap_out[core], land_out[...]
    term_out[:, :cut] = jnp.where(core == 0, kept, arrived)
    term_out[:, cut:] = jnp.where(core == 0, arrived, kept)
    out_lines[0].begin()
    qkv_swap.wait()
    kept, arrived = swap_qkv[core], land_qkv[...]
    for n in range(2):
        group = jnp.where(core == n, kept, arrived)
        for p in range(per):
            taken, start = p * q_width, 0
            for size in (kv * GROUP * HEAD_DIM, kv * HEAD_DIM, kv * HEAD_DIM):
                at = start + (n * per + p) * size
                term_qkv[:, at : at + size] = group[:, taken : taken + size]
                taken, start = taken + size, start + ns * size
    for line in qkv_lines:
        line.begin()
    up_lines[0].settle()
    down_lines[0].relay()
    gain_line.settle()
    up_lines[1].settle()
    down_lines[1].relay()
    down_lines[0].settle()
    out_lines[0].relay()
    down_lines[1].settle()
    qkv_lines[0].relay()
    out_lines[0].settle()
    qkv_lines[1].relay()
    qkv_lines[0].settle()
    qkv_lines[1].settle()
    for line in [*gate_lines, *up_lines, gain_line, *down_lines, *out_lines, *qkv_lines]:
        line.finish()


def finish(mesh, count, kv, term_gate, term_up, dwd, first, dqkv, attended, low, gains):
    ns, nf = mesh
    na, per = nf // 4, ns // 2
    rows, width = first.shape
    q_width = dqkv.shape[3]
    local, half = term_gate.shape[0], width // 2
    block = 2 * local
    anywhere, vmem = pl.BlockSpec(memory_space=pl.ANY), pl.BlockSpec(memory_space=pltpu.VMEM)
    down = (dwd.shape[0] // (2 * na), dwd.shape[1])
    shapes = [term_gate.shape, term_up.shape, down, (local, width), (local, ns * q_width)]
    scratch = [pltpu.VMEM(s, BF16) for s in shapes[2:]]
    scratch += [pltpu.VMEM((2,) + tuple(s), BF16) for s in shapes]
    scratch += [
        pltpu.VMEM((2, rows, width), BF16),
        pltpu.VMEM((2, rows, width), BF16),
        pltpu.VMEM((2, rows, half), BF16),
        pltpu.VMEM((2, per, count, rows // count, q_width), BF16),
        pltpu.VMEM((width, half), BF16),
        pltpu.VMEM((width, per * q_width), BF16),
        pltpu.VMEM((2, local, half), BF16),
        pltpu.VMEM((local, half), BF16),
        pltpu.VMEM((2, local, per * q_width), BF16),
        pltpu.VMEM((local, per * q_width), BF16),
        pltpu.VMEM((4, 2, width), F32),
        pltpu.VMEM((na + 3, 2, width), F32),
    ]
    scratch += chip_sum_shapes(na, True, down[0], down[1] // 2) + chip_sum_shapes(na, False, down[0], down[1] // 2)
    for columns in (half // 2, per * q_width // 2):
        for b_first in (True, False):
            scratch += chip_sum_shapes(na, b_first, block, columns)[:2]
    return pl.pallas_call(
        functools.partial(finish_kernel, mesh, count, kv),
        in_specs=[vmem, vmem] + [anywhere] * 5 + [vmem],
        out_specs=[vmem] * 6,
        out_shape=[jax.ShapeDtypeStruct(s, BF16) for s in shapes] + [jax.ShapeDtypeStruct((2, width), F32)],
        scratch_shapes=scratch
        + [pltpu.SemaphoreType.DMA((64,)), pltpu.SemaphoreType.DMA((64,)), pltpu.SemaphoreType.DMA((64,))],
        compiler_params=pltpu.CompilerParams(vmem_limit_bytes=VMEM_MOST, collective_id=2, has_side_effects=True),
        name="finish",
    )(term_gate, term_up, dwd, first, dqkv, attended, low, gains)


def solution(mesh):
    ns, nf = mesh.shape["seq"], mesh.shape["fsdp"]
    na = nf // 4
    chips = 2 * na
    kv = KEY_VALUE_HEADS // ns
    group_columns = kv * (GROUP + 2) * HEAD_DIM

    core_pairs = [(i, i ^ 1) for i in range(nf)]
    def z_shift(d):
        return [(i, (i + d) % ns) for i in range(ns)]

    def to_core(x):
        return lax.ppermute(x, "fsdp", core_pairs)

    def body(tokens, cotangent, attention_gain, feedforward_gain, query_weight, key_matrix, value_matrix, out_weight, gate_weight, up_weight, down_weight):
        count, span, width = tokens.shape
        rows = count * span
        length = ns * span
        me = lax.axis_index("seq")
        mine = lax.axis_index("fsdp")
        core = mine % 2

        def gather(x):
            return lax.all_gather(x, "fsdp", axis=0, tiled=True)

        local = query_weight.shape[0]
        packed_weight = jnp.concatenate(
            [
                query_weight.reshape(local, ns, kv * GROUP * HEAD_DIM),
                key_matrix.reshape(local, ns, kv * HEAD_DIM),
                value_matrix.reshape(local, ns, kv * HEAD_DIM),
            ],
            axis=2,
        ).reshape(local, ns * group_columns)
        gains = lax.all_gather(jnp.stack([attention_gain, feedforward_gain]).astype(F32), "fsdp", axis=1, tiled=True)
        gain_one, gain_two = gains[0:1], gains[1:2]
        w_qkv = gather(packed_weight)
        w_out = gather(out_weight)
        w_gate = gather(gate_weight)
        w_up = gather(up_weight)
        w_down = gather(down_weight)

        heads = kv * (GROUP + 1)
        plain = kv * HEAD_DIM
        cosines, sines = rope_tables(me * span + jnp.arange(span, dtype=jnp.int32), heads, plain)
        all_cosines, all_sines = rope_tables(jnp.arange(length, dtype=jnp.int32), heads, plain)

        flat = tokens.reshape(rows, width)
        grad_flat = cotangent.reshape(rows, width)
        grad_low = grad_flat.astype(BF16)
        grad_low_other = to_core(grad_low)
        inverse = lax.rsqrt(jnp.mean(flat * flat, axis=-1, keepdims=True) + norm_eps)
        first = (flat * inverse * gain_one).astype(BF16)

        projected = {}
        for d in [*range(1, ns), 0]:
            projected[d] = project(first, w_qkv, cosines, sines, me, d, ns, count)
        pieces, logs, heads_attended, packed = [], [], [], []
        for i in range(count):
            arrived = [projected[0][i]] + [lax.ppermute(projected[d][i], "seq", z_shift(d)) for d in range(1, ns)]
            parts, *kept = attend(arrived, me, kv)
            for x, store in zip(kept, (logs, heads_attended, packed)):
                store.append(x)
            pieces += [parts[0]] + [lax.ppermute(parts[d], "seq", z_shift(d)) for d in range(1, ns)]
        attended, hidden_one, second = out_project(pieces, flat, w_out, gain_two, me, ns, count)
        second_both = jnp.concatenate([second, to_core(second)], axis=0)
        low_both = jnp.concatenate([grad_low, grad_low_other], axis=0)

        dwg, dwu, dwd, out_own, out_other, dx_own, dx_other = ffn(second_both, low_both, w_gate, w_up, w_down, core, chips)
        high, low, grad_tokens, gain_grads, dqkv, sum_gate, sum_up = back(
            (ns, nf), count, kv, dx_own, dx_other, hidden_one, grad_flat, gain_two, w_out, w_qkv,
            jnp.stack(packed), jnp.stack(heads_attended), jnp.stack(logs), all_cosines, all_sines, flat, gain_one, dwg, dwu,
        )
        block_out = hidden_one + out_own + to_core(out_other).astype(F32)
        grad_gate, grad_up, grad_down, grad_out, grad_qkv, gain_grads = finish(
            (ns, nf), count, kv, sum_gate, sum_up, dwd, first, dqkv, attended, low, gain_grads
        )
        q_end, k_end = ns * kv * GROUP * HEAD_DIM, ns * kv * (GROUP + 1) * HEAD_DIM
        gain_grads = lax.dynamic_slice(gain_grads, (0, mine * local), (2, local))

        return (
            block_out.reshape(count, span, width),
            grad_tokens.reshape(count, span, width),
            gain_grads[0],
            gain_grads[1],
            grad_qkv[:, :q_end].astype(F32),
            grad_qkv[:, q_end:k_end].astype(F32),
            grad_qkv[:, k_end:].astype(F32),
            grad_out.astype(F32),
            grad_gate.astype(F32),
            grad_up.astype(F32),
            grad_down.astype(F32),
        )

    tokens_spec, gain_spec, weight_spec = P("fsdp", "seq", None), P("fsdp"), P("fsdp", None)
    return jax.shard_map(
        body,
        mesh=mesh,
        in_specs=(tokens_spec, tokens_spec, gain_spec, gain_spec) + (weight_spec,) * 7,
        out_specs=(tokens_spec, tokens_spec, gain_spec, gain_spec) + (weight_spec,) * 7,
        check_vma=False,
    )
```

```python
import functools
import math

import jax
import jax.numpy as jnp
import numpy as np
from jax import lax
from jax.experimental import pallas as pl
from jax.experimental.pallas import tpu as pltpu
from jax.sharding import PartitionSpec as P

QUERY_HEADS = 16
KEY_VALUE_HEADS = 8
HEAD_DIM = 96
GROUP = QUERY_HEADS // KEY_VALUE_HEADS
norm_eps = 1e-05
rope_base = 100000.0
masked_score = -1e30
F32, BF16 = jnp.float32, jnp.bfloat16
VMEM_LIMIT = 60 * 1024 * 1024
VMEM_MOST = 67043328


def nt_dot(left, right):
    return lax.dot_general(left, right, (((1,), (1,)), ((), ())), preferred_element_type=F32)


def tn_dot(left, right):
    return lax.dot_general(left, right, (((0,), (0,)), ((), ())), preferred_element_type=F32)


def nn_dot(left, right):
    return jnp.dot(left, right, preferred_element_type=F32)


def whole(shape):
    return pl.BlockSpec(shape, lambda *_: (0,) * len(shape))


def call(kernel, scalars, operands, outs, name, flops, moved, scratch=()):
    return pl.pallas_call(
        kernel,
        grid_spec=pltpu.PrefetchScalarGridSpec(
            num_scalar_prefetch=1,
            grid=(1,),
            in_specs=[whole(x.shape) for x in operands],
            out_specs=[whole(x.shape) for x in outs],
            scratch_shapes=scratch,
        ),
        out_shape=outs,
        compiler_params=pltpu.CompilerParams(vmem_limit_bytes=VMEM_LIMIT),
        cost_estimate=pl.CostEstimate(flops=flops, bytes_accessed=moved, transcendentals=0),
        name=name,
    )(scalars, *operands)


def rope_tables(length):
    half = HEAD_DIM // 2
    freqs = np.float32(rope_base) ** (-(np.float32(2.0) * np.arange(half, dtype=np.float32)) / np.float32(HEAD_DIM))
    angles = np.arange(length, dtype=np.float32)[:, None] * freqs.astype(np.float32)[None, :]
    cosine, sine = np.cos(angles), np.sin(angles)
    return np.concatenate([cosine, cosine], 1), np.concatenate([-sine, sine], 1)


def swap_halves(values):
    half = HEAD_DIM // 2
    width = values.shape[1]
    lane = lax.broadcasted_iota(jnp.int32, values.shape, 1)
    ahead = pltpu.roll(values, width - half, 1)
    behind = pltpu.roll(values, half, 1)
    return jnp.where(lane % HEAD_DIM < half, ahead, behind)


def norm_back(grad, normed, inverse, gain):
    scaled = grad * gain
    return inverse * (scaled - normed * jnp.mean(scaled * normed, axis=1, keepdims=True))


MESH = pl.DeviceIdType.MESH


def ffn_kernel(tiles, scalars, x, g, wg, wu, wd, dwg, dwu, dwd, out_own, out_other, dx_own, dx_other, xt, acc_out, acc_dx, act, dgate, dup):
    step = pl.program_id(0)
    rows = x.shape[0] // 2

    @pl.when(step == 0)
    def _():
        out_own[...] = jnp.zeros_like(out_own)
        dx_own[...] = jnp.zeros_like(dx_own)
        acc_out[...] = jnp.zeros_like(acc_out)
        acc_dx[...] = jnp.zeros_like(acc_dx)
        xt[...] = x[...].T

    for i, (out, dx) in enumerate(((out_own, dx_own), (acc_out, acc_dx))):
        here = slice(i * rows, (i + 1) * rows)
        gate = nn_dot(x[here, :], wg[...])
        up = nn_dot(x[here, :], wu[...])
        grad = nt_dot(g[here, :], wd[...])
        sigmoid = jax.nn.sigmoid(gate)
        silu = gate * sigmoid
        hidden = (silu * up).astype(BF16)
        act[here, :] = hidden
        gate_grad = (grad * up * sigmoid * (1.0 + gate * (1.0 - sigmoid))).astype(BF16)
        up_grad = (grad * silu).astype(BF16)
        dgate[here, :] = gate_grad
        dup[here, :] = up_grad
        out[...] += nn_dot(hidden, wd[...])
        dx[...] += nt_dot(gate_grad, wg[...]) + nt_dot(up_grad, wu[...])
    dwg[...] = nn_dot(xt[...], dgate[...]).astype(BF16)
    dwu[...] = nn_dot(xt[...], dup[...]).astype(BF16)
    dwd[...] = tn_dot(act[...], g[...]).astype(BF16)

    @pl.when(step == tiles - 1)
    def _():
        out_other[...] = acc_out[...].astype(BF16)
        dx_other[...] = acc_dx[...].astype(BF16)


def ffn(x, g, wg, wu, wd, core, chips):
    rows, width = x.shape[0] // 2, x.shape[1]
    parts = 2
    tiles = chips * parts
    cols = wg.shape[2] // parts
    keep = lambda shape: pl.BlockSpec(shape, lambda i, s: (0, 0), pipeline_mode=pl.Buffered(1))
    last = lambda: pl.BlockSpec((rows, width), lambda i, s: (0, 0))

    half = cols * tiles
    wide, low = jax.ShapeDtypeStruct((rows, width), F32), jax.ShapeDtypeStruct((rows, width), BF16)
    return pl.pallas_call(
        functools.partial(ffn_kernel, tiles),
        grid_spec=pltpu.PrefetchScalarGridSpec(
            num_scalar_prefetch=1,
            grid=(tiles,),
            in_specs=[keep(x.shape), keep(g.shape)]
            + [pl.BlockSpec((None, width, cols), lambda i, s: (i // parts, 0, i % parts))] * 2
            + [pl.BlockSpec((cols, width), lambda i, s: (i, 0))],
            out_specs=[pl.BlockSpec((width, cols), lambda i, s: (0, i))] * 2
            + [pl.BlockSpec((cols, width), lambda i, s: (i, 0)), last(), last(), last(), last()],
            scratch_shapes=[pltpu.VMEM((width, 2 * rows), BF16)]
            + [pltpu.VMEM((rows, width), F32)] * 2
            + [pltpu.VMEM((2 * rows, cols), BF16)] * 3,
        ),
        out_shape=[
            jax.ShapeDtypeStruct((width, half), BF16),
            jax.ShapeDtypeStruct((width, half), BF16),
            jax.ShapeDtypeStruct((half, width), BF16),
            wide,
            low,
            wide,
            low,
        ],
        compiler_params=pltpu.CompilerParams(vmem_limit_bytes=VMEM_LIMIT),
        cost_estimate=pl.CostEstimate(
            flops=36 * rows * width * half, bytes_accessed=12 * width * half + 20 * rows * width, transcendentals=0
        ),
        name="ffn",
    )(core.reshape(1).astype(jnp.int32), x, g, wg, wu, wd)


def part(x):
    return x[0].at[x[1:]] if isinstance(x, tuple) else x


def get(x):
    return x[0][x[1:]] if isinstance(x, tuple) else x[...]


def put(x, value):
    if isinstance(x, tuple):
        x[0][x[1:]] = value
    else:
        x[...] = value


class Copy:
    def __init__(self, src, dst, device, send_sem, recv_sem):
        self.src, self.dst, self.device, self.send_sem, self.recv_sem = src, dst, device, send_sem, recv_sem

    def made(self):
        if self.device is None:
            return pltpu.make_async_copy(part(self.src), part(self.dst), part(self.send_sem))
        return pltpu.make_async_remote_copy(
            src_ref=part(self.src),
            dst_ref=part(self.dst),
            send_sem=part(self.send_sem),
            recv_sem=part(self.recv_sem),
            device_id=self.device,
            device_id_type=MESH,
        )

    def start(self):
        self.made().start()

    def wait(self):
        self.made().wait()

    def wait_send(self):
        self.made().wait_send()

    def wait_recv(self):
        self.made().wait_recv()


class Links:
    def __init__(self, mesh, send_sems, recv_sems, local_sems):
        self.ns, self.nf = mesh
        self.na = self.nf // 4
        self.send_sems, self.recv_sems, self.local_sems = send_sems, recv_sems, local_sems
        self.count, self.local_count = 0, 0
        self.z, self.f = lax.axis_index("seq"), lax.axis_index("fsdp")
        self.core = lax.rem(self.f, 2)
        self.b = lax.rem(self.f // 2, 2)
        self.a = self.f // 4

    def chip(self, da, db):
        return lax.rem(self.a + da, self.na) * 2 + lax.rem(self.b + db, 2)

    def at_core(self):
        return (self.z, self.f + 1 - 2 * self.core)

    def at_b(self):
        return (self.z, self.f + 2 - 4 * self.b)

    def at_a(self, d):
        return (self.z, lax.rem(self.f + 4 * d, self.nf))

    def at_z(self, d):
        return (lax.rem(self.z + d, self.ns), self.f)

    def peers(self):
        return [self.at_core(), self.at_b()] + [self.at_a(d) for d in range(1, self.na)] + [self.at_z(d) for d in range(1, self.ns)]

    def barrier(self):
        barrier = pltpu.get_barrier_semaphore()
        peers = self.peers()
        for peer in peers:
            pl.semaphore_signal(barrier, inc=1, device_id=peer, device_id_type=MESH)
        pl.semaphore_wait(barrier, len(peers))

    def copy(self, src, dst, device):
        index = self.count
        self.count += 1
        return Copy(src, dst, device, (self.send_sems, index), (self.recv_sems, index))

    def again(self, src, dst, device):
        index = self.count - 1
        return Copy(src, dst, device, (self.send_sems, index), (self.recv_sems, index))

    def local(self, src, dst):
        index = self.local_count
        self.local_count += 1
        return Copy(src, dst, None, (self.local_sems, index), None)


def rows_at(start, size):
    return pl.ds(pl.multiple_of(start * size, size), size)


class ChipSum:
    def __init__(self, links, partial, b_first, arrived, passed, staging):
        self.links, self.partial, self.b_first = links, partial, b_first
        self.arrived, self.passed, self.staging = arrived, passed, staging
        na = links.na
        self.first, self.second = [], []
        if b_first:
            self.kept = [links.chip(da, 0) for da in range(na)]
            for da in range(na):
                self.first.append(links.copy(partial(links.chip(da, 1)), (arrived, da), links.at_b()))
            for d in range(1, na):
                self.second.append(links.copy((arrived, d), (passed, d - 1), links.at_a(d)))
        else:
            self.kept = [links.chip(0, db) for db in range(2)]
            for d in range(1, na):
                for db in range(2):
                    self.first.append(links.copy(partial(links.chip(d, db)), (arrived, (d - 1) * 2 + db), links.at_a(d)))
            self.second.append(links.copy((arrived, 1), (passed, 0), links.at_b()))
        self.loads = [] if staging is None else [links.local(partial(k), (staging, i)) for i, k in enumerate(self.kept)]

    def start(self):
        for copy in self.first:
            copy.start()

    def load(self):
        for load in self.loads:
            load.start()

    def turn(self):
        for load in self.loads:
            load.wait()
        for copy in self.first:
            copy.wait()
        count = len(self.kept)
        for i in [*range(1, count), 0]:
            own = self.partial(self.kept[i]) if self.staging is None else (self.staging, i)
            total = get(own).astype(F32)
            if self.b_first:
                total = total + self.arrived[i].astype(F32)
            else:
                for d in range(self.links.na - 1):
                    total = total + self.arrived[d * 2 + i].astype(F32)
            self.arrived[i] = total.astype(BF16)
            if i > 0 and self.b_first:
                self.second[i - 1].start()
            elif i > 0:
                self.second[0].start()

    def finish(self):
        for copy in self.second:
            copy.wait()
        total = self.arrived[0].astype(F32)
        for i in range(len(self.second)):
            total = total + self.passed[i].astype(F32)
        return total.astype(BF16)


def chip_sum_shapes(na, b_first, rows, columns):
    first = na if b_first else 2 * (na - 1)
    kept = na if b_first else 2
    return [
        pltpu.VMEM((max(first, kept), rows, columns), BF16),
        pltpu.VMEM((na - 1 if b_first else 1, rows, columns), BF16),
        pltpu.VMEM((kept, rows, columns), BF16),
    ]


def flip_core(f):
    return f + 1 - 2 * lax.rem(f, 2)


def flip_b(f):
    return f + 2 - 4 * lax.rem(f // 2, 2)


class Gather:
    def __init__(self, links, own, land, both):
        self.links = links
        f, na, nf = links.f, links.na, links.nf
        to_core, to_b = links.at_core(), links.at_b()

        def move(origin, device, half=None):
            return links.copy(land(origin, half), land(origin, half), device)

        self.given = [links.copy(own, land(f, None), to_core)] if both else []
        self.own = [links.copy(own, land(f, None), to_b)]
        self.own += [links.copy(own, land(f, None), links.at_a(d)) for d in range(1, na)]
        from_b = flip_b(f)
        from_a = [lax.rem(f + nf - 4 * d, nf) for d in range(1, na)]
        if na == 2:
            self.relays = [move(from_b, links.at_a(1), 1), move(from_a[0], to_b, 0)]
            far = [(flip_b(from_a[0]), 0), (flip_b(from_a[0]), 1)]
        else:
            self.relays = [move(origin, to_b) for origin in from_a]
            far = [(flip_b(origin), None) for origin in from_a]
        near = [from_b, *from_a]
        self.near = [move(origin, to_core) for origin in near] if both else []
        self.far = [move(origin, to_core, half) for origin, half in far] if both else []

    def start(self):
        for copies in self.own + self.given:
            copies.start()

    def turn(self):
        for copies in self.own:
            copies.wait()
        for copies in self.relays + self.near:
            copies.start()

    def pass_on(self):
        for copies in self.relays:
            copies.wait()
        for copies in self.far:
            copies.start()

    def finish(self):
        for copies in self.given + self.near + self.far:
            copies.wait()


class GatherHalf:
    def __init__(self, links, stage, land):
        self.links = links
        f, na, nf, core = links.f, links.na, links.nf, links.core
        to_b = links.at_b()

        def move(origin, device):
            return links.copy(land(origin), land(origin), device)

        self.swap = links.copy((stage, 1 - core), land(f), links.at_core())
        self.kept = links.local((stage, core), land(f))
        targets = [to_b] + [links.at_a(d) for d in range(1, na)]
        self.own = [links.copy((stage, core), land(f), device) for device in targets]
        self.other = [move(flip_core(f), device) for device in targets]
        from_b = flip_b(f)
        from_a = [lax.rem(f + nf - 4 * d, nf) for d in range(1, na)]
        if na == 2:
            self.relays = [move(from_b, links.at_a(1))]
            self.late = [move(flip_core(from_a[0]), to_b)]
        else:
            self.relays = [move(origin, to_b) for origin in from_a]
            self.late = [move(flip_core(origin), to_b) for origin in from_a]

    def start(self):
        for copies in [self.swap, self.kept, *self.own]:
            copies.start()

    def other_start(self):
        self.swap.wait()
        for copies in self.other:
            copies.start()

    def turn(self):
        for copies in self.own:
            copies.wait()
        for copies in self.relays:
            copies.start()

    def turn_late(self):
        for copies in self.other:
            copies.wait()
        for copies in self.late:
            copies.start()

    def finish(self):
        for copies in [self.kept, *self.relays, *self.late]:
            copies.wait()


def attend_heads(ns, kv, span, qs, ks, vs, out, logs):
    scale = 1.0 / math.sqrt(HEAD_DIM)
    row = lax.broadcasted_iota(jnp.int32, (span, span), 0)
    column = lax.broadcasted_iota(jnp.int32, (span, span), 1)
    causal = row >= column
    lane = lax.broadcasted_iota(jnp.int32, (span, 128), 1)
    for s in range(ns):
        here = slice(s * span, (s + 1) * span)
        stats = jnp.zeros((span, 128), F32)
        for h in range(kv * GROUP):
            g = h // GROUP
            q = qs[h, here, :]
            near = jnp.where(causal, nt_dot(q, ks[g, here, :]) * scale, masked_score)
            top = jnp.max(near, axis=1, keepdims=True)
            if s > 0:
                far = nt_dot(q, ks[g, : s * span, :]) * scale
                top = jnp.maximum(top, jnp.max(far, axis=1, keepdims=True))
            near = jnp.exp(near - top)
            total = jnp.sum(near, axis=1, keepdims=True)
            if s > 0:
                far = jnp.exp(far - top)
                total = total + jnp.sum(far, axis=1, keepdims=True)
            inverse = 1.0 / total
            result = nn_dot((near * inverse).astype(BF16), vs[g, here, :])
            if s > 0:
                result = result + nn_dot((far * inverse).astype(BF16), vs[g, : s * span, :])
            stats = jnp.where(lane == h, top + jnp.log(total), stats)
            out[s, :, h * HEAD_DIM : (h + 1) * HEAD_DIM] = result.astype(BF16)
        logs[here, :] = stats


def fill_tables(cosines, sines, narrow_cosines, narrow_sines, heads):
    end = heads * HEAD_DIM
    cosines[:, end:] = jnp.ones((cosines.shape[0], cosines.shape[1] - end), F32)
    sines[:, end:] = jnp.zeros((cosines.shape[0], cosines.shape[1] - end), F32)
    for h in range(heads):
        at = slice(h * HEAD_DIM, (h + 1) * HEAD_DIM)
        cosines[:, at] = narrow_cosines
        sines[:, at] = narrow_sines


def fore_kernel(
    mesh, count, kv,
    tokens, cotangent, gain_one, gain_two, wq, wk, wv, wo, wg, wu, wd, narrow_cosines, narrow_sines,
    w_qkv, w_out, w_gate, w_up, w_down, first_out, packed, heads_attended, logs, attended_out, hidden_out, second_both, low_both, gains_out,
    rows_in, hidden, first, pack, w_land, wo_land, q_send, q_land, a_send, a_land, stage_gate, stage_up, gain_send, gain_land,
    qs, ks, vs, log, attended, second, second_abs, low, cosines, sines, send_sems, recv_sems, local_sems,
):
    links = Links(mesh, send_sems, recv_sems, local_sems)
    ns, na, nf = links.ns, links.na, links.nf
    chips = 2 * na
    z, f, core = links.z, links.f, links.core
    rows, width = rows_in.shape
    span = rows // count
    heads = kv * GROUP
    g_width, k_width = heads * HEAD_DIM, kv * HEAD_DIM
    q_width = g_width + 2 * k_width
    local = width // nf
    links.barrier()

    token_load = links.local(tokens, rows_in)
    token_load.start()
    gain_send[...] = jnp.zeros_like(gain_send)
    gain_send[0:1, :local] = gain_one[...].astype(F32)
    gain_send[1:2, :local] = gain_two[...].astype(F32)
    for j in range(ns):
        pack[j, :, :g_width] = wq[:, j * g_width : (j + 1) * g_width]
        pack[j, :, g_width : g_width + k_width] = wk[:, j * k_width : (j + 1) * k_width]
        pack[j, :, g_width + k_width :] = wv[:, j * k_width : (j + 1) * k_width]

    every = slice(None)

    def piece(start, size, half):
        if half is None:
            return rows_at(start, size)
        return rows_at(start * 2 + half, size // 2)

    units = []
    turns = [*range(1, ns), 0]
    for d in turns:
        g = lax.rem(z + d, ns)
        units.append(Gather(links, (pack, g), lambda o, half, g=g: (w_land, g, piece(o, local, half)), True))
    units.append(Gather(links, wo, lambda o, half: (wo_land, piece(o, local, half)), True))
    depth = wd.shape[0]
    units.append(Gather(links, wd, lambda o, half: (w_down, piece(o // 2, depth, half)), False))
    half_units = [
        GatherHalf(links, stage, lambda o, out=out: (out, every, rows_at(o, local)))
        for stage, out in ((stage_gate, w_gate), (stage_up, w_up))
    ]
    q_copies, a_copies = [], []
    for d in range(1, ns):
        g = lax.rem(z + d, ns)
        q_copies.append([links.copy((q_send, g, i), (q_land, i, z), links.at_z(d)) for i in range(count)])
    for i in range(count):
        a_copies.append([links.copy((a_send, i, lax.rem(z + d, ns)), (a_land, i, z), links.at_z(d)) for d in range(1, ns)])
    second_copy = links.copy(second_abs, (second_both, pl.ds(rows, rows)), links.at_core())
    low_copy = links.copy(low, (low_both, pl.ds(rows, rows)), links.at_core())

    def gain_at(start, size):
        return (gain_land, pl.ds(start, size))

    pair, chip_four = f // 2 * 2, f // 4 * 4
    gain_copies = [
        [links.copy(gain_at(f, 1), gain_at(f, 1), links.at_core())],
        [links.copy(gain_at(pair, 2), gain_at(pair, 2), links.at_b())],
        [links.copy(gain_at(chip_four, 4), gain_at(chip_four, 4), links.at_a(d)) for d in range(1, na)],
    ]
    stores = []

    def store(src, dst):
        copies = links.local(src, dst)
        copies.start()
        stores.append(copies)

    gain_land[f] = gain_send[...]
    for copies in gain_copies[0]:
        copies.start()
    units[0].start()
    units[1].start()
    for j in range(ns):
        w_land[j, rows_at(f, local), :] = pack[j]
    stage_loads = []
    tile = w_gate.shape[2]
    for source, stage in ((wg, stage_gate), (wu, stage_up)):
        for c in range(2):
            for k in range(chips):
                stage_loads.append(links.local((source, every, slice((k * 2 + c) * tile, (k * 2 + c + 1) * tile)), (stage, c, k)))
    for load in stage_loads:
        load.start()
    store_own = [links.local(wo, (wo_land, rows_at(f, local))), links.local(wd, (w_down, rows_at(f // 2, depth)))]
    for copies in store_own:
        copies.start()
    fill_tables(cosines, sines, narrow_cosines[rows_at(z, span), :], narrow_sines[rows_at(z, span), :], heads + kv)
    token_load.wait()
    old = rows_in[...]
    inverse = lax.rsqrt(jnp.mean(old * old, axis=1, keepdims=True) + norm_eps)
    for stage in range(3):
        for copies in gain_copies[stage]:
            copies.wait()
        if stage < 2:
            for copies in gain_copies[stage + 1]:
                copies.start()
    for j in range(nf):
        gains_out[:, j * local : (j + 1) * local] = gain_land[j, 0:2, :local]
    first[...] = (old * inverse * gains_out[0:1, :]).astype(BF16)
    store(first, first_out)

    def project(n):
        g = lax.rem(z + turns[n], ns)
        units[n].finish()
        y = nn_dot(first[...], w_land[g])
        for i in range(count):
            part = y[i * span : (i + 1) * span]
            part = (part * cosines[...] + swap_halves(part) * sines[...]).astype(BF16)
            if turns[n] == 0:
                q_land[i, z] = part
            else:
                q_send[g, i] = part
                q_copies[turns[n] - 1][i].start()
        store((w_land, g), (w_qkv, g))

    last = len(units)
    for n in range(ns):
        units[n].turn()
        if n + 2 < last:
            units[n + 2].start()
        if n > 0:
            units[n - 1].pass_on()
        if n > 1:
            project(n - 2)
    units[ns].turn()
    for load in stage_loads:
        load.wait()
    half_units[0].start()
    units[ns - 1].pass_on()
    project(ns - 2)
    half_units[0].other_start()
    project(ns - 1)
    units[ns].pass_on()

    def attend(i):
        for copies in q_copies:
            copies[i].wait()
        for j in range(ns):
            at = slice(j * span, (j + 1) * span)
            for h in range(heads):
                qs[h, at, :] = q_land[i, j, :, h * HEAD_DIM : (h + 1) * HEAD_DIM]
            for h in range(kv):
                k0, v0 = (heads + h) * HEAD_DIM, (heads + kv + h) * HEAD_DIM
                ks[h, at, :] = q_land[i, j, :, k0 : k0 + HEAD_DIM]
                vs[h, at, :] = q_land[i, j, :, v0 : v0 + HEAD_DIM]
        attend_heads(ns, kv, span, qs, ks, vs, a_send.at[i], log.at[i])
        for copies in a_copies[i]:
            copies.start()
        a_land[i, z] = a_send[i, z]

    for i in range(count):
        attend(i)
        if i == 0:
            units[ns + 1].turn()
            half_units[1].start()
            half_units[1].other_start()
            units[ns].finish()
            store_own[0].wait()
            store(wo_land, w_out)
    store(q_land, packed)
    store(a_send, heads_attended)
    store(log, logs)
    for i in range(count):
        for copies in a_copies[i]:
            copies.wait()
        for j in range(ns):
            attended[i * span : (i + 1) * span, j * g_width : (j + 1) * g_width] = a_land[i, j]
    new = rows_in[...] + nn_dot(attended[...], wo_land[...])
    hidden[...] = new
    inverse = lax.rsqrt(jnp.mean(new * new, axis=1, keepdims=True) + norm_eps)
    second_abs[...] = (new * inverse * gains_out[1:2, :]).astype(BF16)
    second_copy.start()
    store(second_abs, (second_both, pl.ds(0, rows)))
    store(attended, attended_out)
    store(hidden, hidden_out)
    units[ns + 1].pass_on()
    cot_load = links.local(cotangent, rows_in)
    cot_load.start()
    half_units[0].turn()
    cot_load.wait()
    low[...] = rows_in[...].astype(BF16)
    low_copy.start()
    store(low, (low_both, pl.ds(0, rows)))
    half_units[0].turn_late()
    half_units[1].turn()
    half_units[1].turn_late()
    for unit in half_units:
        unit.finish()
    second_copy.wait()
    low_copy.wait()
    store_own[1].wait()
    for copies in stores:
        copies.wait()


def fore(mesh, count, kv, tokens, cotangent, gain_one, gain_two, wq, wk, wv, wo, wg, wu, wd, narrow_cosines, narrow_sines):
    ns, nf = mesh
    na = nf // 4
    chips = 2 * na
    rows, width = tokens.shape
    span = rows // count
    length = ns * span
    heads = kv * GROUP
    g_width = heads * HEAD_DIM
    q_width = g_width + 2 * kv * HEAD_DIM
    local, depth = wq.shape[0], wd.shape[0]
    tile = wg.shape[1] // (2 * chips)
    anywhere, vmem = pl.BlockSpec(memory_space=pl.ANY), pl.BlockSpec(memory_space=pltpu.VMEM)
    low = lambda *shape: jax.ShapeDtypeStruct(shape, BF16)
    wide = lambda *shape: jax.ShapeDtypeStruct(shape, F32)
    outs = [
        low(ns, width, q_width),
        low(width, width),
        low(chips, width, tile),
        low(chips, width, tile),
        low(chips * depth, width),
        low(rows, width),
        low(count, ns, span, q_width),
        low(count, ns, span, g_width),
        wide(count, length, 128),
        low(rows, width),
        wide(rows, width),
        low(2 * rows, width),
        low(2 * rows, width),
        wide(2, width),
    ]
    scratch = [
        pltpu.VMEM((rows, width), F32),
        pltpu.VMEM((rows, width), F32),
        pltpu.VMEM((rows, width), BF16),
        pltpu.VMEM((ns, local, q_width), BF16),
        pltpu.VMEM((ns, width, q_width), BF16),
        pltpu.VMEM((width, width), BF16),
        pltpu.VMEM((ns, count, span, q_width), BF16),
        pltpu.VMEM((count, ns, span, q_width), BF16),
        pltpu.VMEM((count, ns, span, g_width), BF16),
        pltpu.VMEM((count, ns, span, g_width), BF16),
        pltpu.VMEM((2, chips, local, tile), BF16),
        pltpu.VMEM((2, chips, local, tile), BF16),
        pltpu.VMEM((8, 256), F32),
        pltpu.VMEM((nf, 8, 256), F32),
        pltpu.VMEM((heads, length, HEAD_DIM), BF16),
        pltpu.VMEM((kv, length, HEAD_DIM), BF16),
        pltpu.VMEM((kv, length, HEAD_DIM), BF16),
        pltpu.VMEM((count, length, 128), F32),
        pltpu.VMEM((rows, width), BF16),
        pltpu.VMEM((8, 128), BF16),
        pltpu.VMEM((rows, width), BF16),
        pltpu.VMEM((rows, width), BF16),
        pltpu.VMEM((span, q_width), F32),
        pltpu.VMEM((span, q_width), F32),
    ]
    return pl.pallas_call(
        functools.partial(fore_kernel, mesh, count, kv),
        in_specs=[anywhere] * 2 + [vmem] * 5 + [anywhere] * 4 + [vmem] * 2,
        out_specs=[anywhere] * 13 + [vmem],
        out_shape=outs,
        scratch_shapes=scratch
        + [pltpu.SemaphoreType.DMA((160,)), pltpu.SemaphoreType.DMA((160,)), pltpu.SemaphoreType.DMA((64,))],
        compiler_params=pltpu.CompilerParams(vmem_limit_bytes=VMEM_MOST, collective_id=0, has_side_effects=True),
        name="fore",
    )(tokens, cotangent, gain_one, gain_two, wq, wk, wv, wo, wg, wu, wd, narrow_cosines, narrow_sines)


def attend_back_heads(ns, kv, span, qs, ks, vs, gs, attended, logs, dk, dv, result):
    scale = 1.0 / math.sqrt(HEAD_DIM)
    heads = kv * GROUP
    row = lax.broadcasted_iota(jnp.int32, (span, span), 0)
    column = lax.broadcasted_iota(jnp.int32, (span, span), 1)
    causal = row >= column
    dk[...] = jnp.zeros_like(dk)
    dv[...] = jnp.zeros_like(dv)
    for s in range(ns):
        here = slice(s * span, (s + 1) * span)
        for h in range(heads):
            g = h // GROUP
            q, grad = qs[h, here, :], gs[h, here, :]
            log_total = logs[here, h : h + 1]
            out = attended[s, :, h * HEAD_DIM : (h + 1) * HEAD_DIM]
            delta = jnp.sum(grad.astype(F32) * out.astype(F32), axis=1, keepdims=True)
            k, v = ks[g, here, :], vs[g, here, :]
            near = jnp.where(causal, jnp.exp(nt_dot(q, k) * scale - log_total), 0.0)
            slope = (near * (nt_dot(grad, v) - delta) * scale).astype(BF16)
            dq = nn_dot(slope, k)
            dk[g, here, :] += tn_dot(slope, q)
            dv[g, here, :] += tn_dot(near.astype(BF16), grad)
            if s > 0:
                before = slice(0, s * span)
                k, v = ks[g, before, :], vs[g, before, :]
                far = jnp.exp(nt_dot(q, k) * scale - log_total)
                slope = (far * (nt_dot(grad, v) - delta) * scale).astype(BF16)
                dq = dq + nn_dot(slope, k)
                dk[g, before, :] += tn_dot(slope, q)
                dv[g, before, :] += tn_dot(far.astype(BF16), grad)
            result[here, h * HEAD_DIM : (h + 1) * HEAD_DIM] = dq
    for g in range(kv):
        k0 = (heads + g) * HEAD_DIM
        v0 = (heads + kv + g) * HEAD_DIM
        result[:, k0 : k0 + HEAD_DIM] = dk[g]
        result[:, v0 : v0 + HEAD_DIM] = dv[g]


def back_kernel(
    mesh, count, kv,
    dx_own, dx_other, hidden, cotangent, gain_two, w_out, w_qkv, packed, attended, logs, cosines, sines, tokens, gain_one, dwg, dwu,
    high, low, out, gain_grads, dqkv, sum_gate, sum_up,
    dx_land, g_send, g_land, q_send, q_land, swap_send, swap_land, *rest,
):
    parts, (send_sems, recv_sems, local_sems) = rest[:-3], rest[-3:]
    links = Links(mesh, send_sems, recv_sems, local_sems)
    ns, na = links.ns, links.na
    chips = 2 * na
    z, core = links.z, links.core
    rows, width = hidden.shape
    span = rows // count
    length = ns * span
    heads = kv * GROUP
    g_width, q_width = heads * HEAD_DIM, (heads + 2 * kv) * HEAD_DIM
    half = dwg.shape[1]
    block = width // chips
    links.barrier()

    dx_copy = links.copy(dx_other, dx_land, links.at_core())
    dx_copy.start()
    sums = []
    for n, source in enumerate((dwg, dwu)):
        for b_first in (True, False):
            columns = slice(0, half // 2) if b_first else slice(half // 2, half)
            at = (n * 2 + (0 if b_first else 1)) * 3
            partial = lambda k, source=source, columns=columns: (source, rows_at(k, block), columns)
            sums.append(ChipSum(links, partial, b_first, *parts[at : at + 3]))
    for item in sums:
        item.start()
        item.load()

    g_copies, q_copies = [], []
    for i in range(count):
        g_copies.append([links.copy((g_send, i, lax.rem(z + d, ns)), (g_land, i, z), links.at_z(d)) for d in range(1, ns)])
        q_copies.append([links.copy((q_send, i, lax.rem(z + d, ns)), (q_land, z, i), links.at_z(d)) for d in range(1, ns)])

    def out_back(dx, old, grad, w):
        loads = [links.local(dx_own, dx), links.local(hidden, old), links.local(cotangent, grad), links.local(w_out, w)]
        for load in loads:
            load.start()
        dx_copy.wait()
        for load in loads[:3]:
            load.wait()
        step = dx[...] + dx_land[...].astype(F32)
        inverse = lax.rsqrt(jnp.mean(old[...] * old[...], axis=1, keepdims=True) + norm_eps)
        normed = old[...] * inverse
        gain_grads[1:2, :] = jnp.sum(step * normed, axis=0, keepdims=True)
        grad[...] = grad[...] + norm_back(step, normed, inverse, gain_two[...])
        low[...] = grad[...].astype(BF16)
        stores = [links.local(grad, high)]
        for store in stores:
            store.start()
        loads[3].wait()
        for i in range(count):
            here = slice(i * span, (i + 1) * span)
            part = nt_dot(low[here, :], w[...]).astype(BF16)
            for j in range(ns):
                g_send[i, j] = part[:, j * g_width : (j + 1) * g_width]
            for copies in g_copies[i]:
                copies.start()
            g_land[i, z] = g_send[i, z]
        for store in stores:
            store.wait()

    pl.run_scoped(
        out_back,
        pltpu.VMEM((rows, width), F32),
        pltpu.VMEM((rows, width), F32),
        pltpu.VMEM((rows, width), F32),
        pltpu.VMEM((width, width), BF16),
    )

    def attention(qkv, mid, log, qs, ks, vs, gs, dk, dv, result, cosine, sine):
        fill_tables(cosine, sine, cosines[...], sines[...], heads + kv)
        for i in range(count):
            loads = [links.local((packed, i), qkv), links.local((attended, i), mid), links.local((logs, i), log)]
            for load in loads:
                load.start()
            for load in loads:
                load.wait()
            for j in range(ns):
                at = slice(j * span, (j + 1) * span)
                for h in range(heads):
                    qs[h, at, :] = qkv[j, :, h * HEAD_DIM : (h + 1) * HEAD_DIM]
                for h in range(kv):
                    k0, v0 = (heads + h) * HEAD_DIM, (heads + kv + h) * HEAD_DIM
                    ks[h, at, :] = qkv[j, :, k0 : k0 + HEAD_DIM]
                    vs[h, at, :] = qkv[j, :, v0 : v0 + HEAD_DIM]
            for copies in g_copies[i]:
                copies.wait()
            for j in range(ns):
                for h in range(heads):
                    gs[h, j * span : (j + 1) * span, :] = g_land[i, j, :, h * HEAD_DIM : (h + 1) * HEAD_DIM]
            attend_back_heads(ns, kv, span, qs, ks, vs, gs, mid, log, dk, dv, result)
            for j in range(ns):
                here = slice(j * span, (j + 1) * span)
                part = result[here, :]
                q_send[i, j] = (part * cosine[here, :] - swap_halves(part) * sine[here, :]).astype(BF16)
            for copies in q_copies[i]:
                copies.start()
            q_land[z, i] = q_send[i, z]
            if i < len(sums) // 2:
                for item in sums[2 * i : 2 * i + 2]:
                    item.turn()

    pl.run_scoped(
        attention,
        pltpu.VMEM((ns, span, q_width), BF16),
        pltpu.VMEM((ns, span, g_width), BF16),
        pltpu.VMEM((length, 128), F32),
        pltpu.VMEM((heads, length, HEAD_DIM), BF16),
        pltpu.VMEM((kv, length, HEAD_DIM), BF16),
        pltpu.VMEM((kv, length, HEAD_DIM), BF16),
        pltpu.VMEM((heads, length, HEAD_DIM), BF16),
        pltpu.VMEM((kv, length, HEAD_DIM), F32),
        pltpu.VMEM((kv, length, HEAD_DIM), F32),
        pltpu.VMEM((length, q_width), F32),
        pltpu.VMEM((length, q_width), F32),
        pltpu.VMEM((length, q_width), F32),
    )

    swaps = []
    local = block // 2
    for item in sums[2 * count :]:
        item.turn()

    def swap(n):
        for m in range(2):
            total = sums[2 * n + m].finish()
            swap_send[n, m, 0] = total[:local]
            swap_send[n, m, 1] = total[local:]
        for m in range(2):
            copies = links.copy((swap_send, n, m, 1 - core), (swap_land, n, m), links.at_core())
            copies.start()
            swaps.append(copies)

    swap(0)

    def project_back(w, old, base, grad):
        loads = [links.local(w_qkv, w), links.local(tokens, old), links.local(high, base)]
        for load in loads:
            load.start()
        for load in loads:
            load.wait()
        for i in range(count):
            here = slice(i * span, (i + 1) * span)
            for copies in q_copies[i]:
                copies.wait()
            total = nt_dot(q_land[0, i], w[0])
            for j in range(1, ns):
                total = total + nt_dot(q_land[j, i], w[j])
            grad[here, :] = total
        step = grad[...]
        inverse = lax.rsqrt(jnp.mean(old[...] * old[...], axis=1, keepdims=True) + norm_eps)
        normed = old[...] * inverse
        gain_grads[0:1, :] = jnp.sum(step * normed, axis=0, keepdims=True)
        base[...] = base[...] + norm_back(step, normed, inverse, gain_one[...])
        stores = [links.local(base, out), links.local(q_land, dqkv)]
        for store in stores:
            store.start()
        for store in stores:
            store.wait()

    pl.run_scoped(
        project_back,
        pltpu.VMEM((ns, width, q_width), BF16),
        pltpu.VMEM((rows, width), F32),
        pltpu.VMEM((rows, width), F32),
        pltpu.VMEM((rows, width), F32),
    )
    swap(1)
    tile = half // chips
    for n, total in enumerate((sum_gate, sum_up)):
        for m in range(2):
            swaps[2 * n + m].wait()
            kept, arrived = swap_send[n, m, core], swap_land[n, m]
            for t in range(chips // 2):
                here = slice(t * tile, (t + 1) * tile)
                k = m * (chips // 2) + t
                first, second = kept[:, here], arrived[:, here]
                total[:, 2 * k * tile : (2 * k + 1) * tile] = jnp.where(core == 0, first, second)
                total[:, (2 * k + 1) * tile : (2 * k + 2) * tile] = jnp.where(core == 0, second, first)


def back(mesh, count, kv, dx_own, dx_other, hidden, cotangent, gain_two, w_out, w_qkv, packed, attended, logs, cosines, sines, tokens, gain_one, dwg, dwu):
    ns, nf = mesh
    na = nf // 4
    rows, width = hidden.shape
    span = rows // count
    heads = kv * GROUP
    g_width, q_width = heads * HEAD_DIM, (heads + 2 * kv) * HEAD_DIM
    half = dwg.shape[1]
    block = width // (2 * na)
    local = block // 2
    anywhere = pl.BlockSpec(memory_space=pl.ANY)
    vmem = pl.BlockSpec(memory_space=pltpu.VMEM)
    operands = [dx_own, dx_other, hidden, cotangent, gain_two, w_out, w_qkv, packed, attended, logs, cosines, sines, tokens, gain_one, dwg, dwu]
    wide = jax.ShapeDtypeStruct((rows, width), F32)
    summed = jax.ShapeDtypeStruct((local, 2 * half), BF16)
    scratch = [
        pltpu.VMEM((rows, width), BF16),
        pltpu.VMEM((count, ns, span, g_width), BF16),
        pltpu.VMEM((count, ns, span, g_width), BF16),
        pltpu.VMEM((count, ns, span, q_width), BF16),
        pltpu.VMEM((ns, count, span, q_width), BF16),
        pltpu.VMEM((2, 2, 2, local, half // 2), BF16),
        pltpu.VMEM((2, 2, local, half // 2), BF16),
    ]
    for _ in range(2):
        for b_first in (True, False):
            scratch += chip_sum_shapes(na, b_first, block, half // 2)
    return pl.pallas_call(
        functools.partial(back_kernel, mesh, count, kv),
        in_specs=[vmem if x.shape[0] == 1 or x.shape[1] == HEAD_DIM else anywhere for x in operands],
        out_specs=[anywhere, vmem, anywhere, vmem, anywhere, vmem, vmem],
        out_shape=[
            wide,
            jax.ShapeDtypeStruct((rows, width), BF16),
            wide,
            jax.ShapeDtypeStruct((2, width), F32),
            jax.ShapeDtypeStruct((ns, count, span, q_width), BF16),
            summed,
            summed,
        ],
        scratch_shapes=scratch
        + [pltpu.SemaphoreType.DMA((64,)), pltpu.SemaphoreType.DMA((64,)), pltpu.SemaphoreType.DMA((64,))],
        compiler_params=pltpu.CompilerParams(vmem_limit_bytes=VMEM_MOST, collective_id=1, has_side_effects=True),
        name="back",
    )(*operands)


class LineSum:
    def __init__(self, links, term, first, second, total):
        self.links, self.term, self.first, self.second, self.total = links, term, first, second, total
        z, ns = links.z, links.ns
        self.dtype = (term[0] if isinstance(term, tuple) else term).dtype
        middle = ns // 2
        self.deep = middle > 1
        lower = z < middle
        step = jnp.where(lower, 1, -1)
        self.end = (z == 0) | (z == ns - 1)
        self.inner = (z == middle - 1) | (z == middle)
        inward, outward = (z + step, links.f), (z - step, links.f)
        self.inward = links.copy(term, first, inward) if self.deep else None
        self.onward = links.again(first, first, inward) if self.deep else None
        self.across = links.copy(first if self.deep else term, second, inward)
        self.outward = links.copy(total, total, outward) if self.deep else None

    def add(self, target, one, two):
        put(target, (get(one).astype(F32) + get(two).astype(F32)).astype(self.dtype))

    def begin(self):
        if self.deep:
            pl.when(self.end)(self.inward.start)
        else:
            self.across.start()

    def relay(self):
        if not self.deep:
            return

        @pl.when(jnp.logical_not(self.end))
        def _():
            self.inward.wait_recv()
            self.add(self.first, self.term, self.first)
            pl.when(self.inner)(self.across.start)
            pl.when(jnp.logical_not(self.inner))(self.onward.start)

    def settle(self):
        @pl.when(self.inner)
        def _():
            self.across.wait()
            self.add(self.total, self.first if self.deep else self.term, self.second)
            if self.deep:
                self.outward.start()

        if self.deep:

            @pl.when(jnp.logical_not(self.inner | self.end))
            def _():
                self.outward.wait_recv()
                self.outward.start()

    def finish(self):
        if not self.deep:
            return
        pl.when(self.end)(self.outward.wait_recv)
        pl.when(jnp.logical_not(self.inner))(self.inward.wait_send)
        pl.when(jnp.logical_not(self.end))(self.outward.wait_send)


def finish_kernel(
    mesh, count, kv,
    term_gate, term_up, dwd, first, dqkv, attended, low, gains,
    out_gate, out_up, out_down, out_out, out_qkv, out_gains,
    term_down, term_out, term_qkv, in_gate, in_up, in_down, in_out, in_qkv,
    first_both, attended_both, low_both, dq_both, w_out_part, w_qkv_part,
    swap_out, land_out, swap_qkv, land_qkv, gain_terms, gain_lands, *rest,
):
    parts, (send_sems, recv_sems, local_sems) = rest[:-3], rest[-3:]
    links = Links(mesh, send_sems, recv_sems, local_sems)
    ns, na = links.ns, links.na
    chips, per = 2 * na, ns // 2
    core = links.core
    rows, width = first.shape
    q_width = dqkv.shape[3]
    middle = width // 2
    links.barrier()

    def lines(term, inbox, out, pieces):
        size = term.shape[1] // pieces
        every = slice(None)
        made = []
        for i in range(pieces):
            at = slice(i * size, (i + 1) * size)
            made.append(LineSum(links, (term, every, at), (inbox, 0, every, at), (inbox, 1, every, at), (out, every, at)))
        return made

    gate_lines = lines(term_gate, in_gate, out_gate, 2)
    up_lines = lines(term_up, in_up, out_up, 2)
    down_lines = lines(term_down, in_down, out_down, 2)
    out_lines = lines(term_out, in_out, out_out, 1)
    qkv_lines = lines(term_qkv, in_qkv, out_qkv, 2)
    for line in gate_lines + up_lines:
        line.begin()

    sends = [
        links.copy((dqkv, pl.ds((1 - core) * per, per)), (dq_both, 1), links.at_core()),
        links.copy((low, slice(None), rows_at(1 - core, middle)), (low_both, 1), links.at_core()),
        links.copy(first, (first_both, 1), links.at_core()),
        links.copy(attended, (attended_both, 1), links.at_core()),
    ]
    loads = [
        links.local((low, slice(None), rows_at(core, middle)), (low_both, 0)),
        links.local(attended, (attended_both, 0)),
        links.local(first, (first_both, 0)),
        links.local((dqkv, pl.ds(core * per, per)), (dq_both, 0)),
    ]
    for copies in loads + sends[1:2] + sends[3:4] + sends[2:3] + sends[:1]:
        copies.start()

    down_rows = dwd.shape[0] // chips
    block = width // chips

    def pair(source, row_count, at, staged):
        made = []
        cut = source.shape[1] // 2
        for n, b_first in enumerate((True, False)):
            columns = slice(0, cut) if b_first else slice(cut, 2 * cut)
            partial = lambda k, columns=columns: (source, rows_at(k, row_count), columns)
            refs = parts[at[n] : at[n + 1]]
            made.append(ChipSum(links, partial, b_first, *(refs if staged else (*refs[:2], None))))
        return made

    down = pair(dwd, down_rows, (0, 3, 6), True)
    for item in down:
        item.start()
        item.load()

    gain_copies = [links.copy((gain_terms, 0), (gain_lands, 0), links.at_core()), links.copy((gain_terms, 1), (gain_lands, 1), links.at_b())]
    gain_copies += [links.copy((gain_terms, 2), (gain_lands, 1 + d), links.at_a(d)) for d in range(1, na)]
    gain_line = LineSum(links, (gain_terms, 3), (gain_lands, na + 1), (gain_lands, na + 2), out_gains)
    gain_terms[0] = gains[...]
    gain_copies[0].start()

    for i in (1, 3):
        sends[i].wait()
    for i in (0, 1):
        loads[i].wait()
    for k in range(chips):
        at = slice(k * block, (k + 1) * block)
        total = tn_dot(attended_both[0, :, at], low_both[0]) + tn_dot(attended_both[1, :, at], low_both[1])
        w_out_part[at, :] = total.astype(BF16)
    out_sums = pair(w_out_part, block, (6, 8, 10), False)
    for item in out_sums:
        item.start()
    for i in (0, 2):
        sends[i].wait()
    for i in (2, 3):
        loads[i].wait()
    for p in range(per):
        columns = slice(p * q_width, (p + 1) * q_width)
        mine, other = dq_both[0, p].reshape(rows, q_width), dq_both[1, p].reshape(rows, q_width)
        for k in range(chips):
            at = slice(k * block, (k + 1) * block)
            total = tn_dot(first_both[0, :, at], mine) + tn_dot(first_both[1, :, at], other)
            w_qkv_part[at, columns] = total.astype(BF16)
    qkv_sums = pair(w_qkv_part, block, (10, 12, 14), False)
    for item in qkv_sums:
        item.start()

    def next_gain(i):
        gain_copies[i].wait()
        gain_terms[i + 1] = gain_terms[i] + gain_lands[i]
        if i == 0:
            gain_copies[1].start()
        else:
            for copies in gain_copies[2:]:
                copies.start()

    next_gain(0)
    for item in down:
        item.turn()
    for line in gate_lines:
        line.relay()
    next_gain(1)
    for item in out_sums:
        item.turn()
    cut = width // 2
    term_down[:, :cut] = down[0].finish()
    term_down[:, cut:] = down[1].finish()
    for line in down_lines:
        line.begin()
    for item in qkv_sums:
        item.turn()
    for copies in gain_copies[2:]:
        copies.wait()
    total = gain_terms[2]
    for d in range(1, na):
        total = total + gain_lands[1 + d]
    gain_terms[3] = total
    gain_line.begin()

    def swap(sums, send, land):
        local = block // 2
        for n, item in enumerate(sums):
            total = item.finish()
            size = total.shape[1]
            send[0, :, n * size : (n + 1) * size] = total[:local]
            send[1, :, n * size : (n + 1) * size] = total[local:]
        copies = links.copy((send, 1 - core), land, links.at_core())
        copies.start()
        return copies

    out_swap = swap(out_sums, swap_out, land_out)
    gate_lines[0].settle()
    up_lines[0].relay()
    gate_lines[1].settle()
    up_lines[1].relay()
    gain_line.relay()
    qkv_swap = swap(qkv_sums, swap_qkv, land_qkv)
    out_swap.wait()
    kept, arrived = swap_out[core], land_out[...]
    term_out[:, :cut] = jnp.where(core == 0, kept, arrived)
    term_out[:, cut:] = jnp.where(core == 0, arrived, kept)
    out_lines[0].begin()
    qkv_swap.wait()
    kept, arrived = swap_qkv[core], land_qkv[...]
    for n in range(2):
        group = jnp.where(core == n, kept, arrived)
        for p in range(per):
            taken, start = p * q_width, 0
            for size in (kv * GROUP * HEAD_DIM, kv * HEAD_DIM, kv * HEAD_DIM):
                at = start + (n * per + p) * size
                term_qkv[:, at : at + size] = group[:, taken : taken + size]
                taken, start = taken + size, start + ns * size
    for line in qkv_lines:
        line.begin()
    up_lines[0].settle()
    down_lines[0].relay()
    gain_line.settle()
    up_lines[1].settle()
    down_lines[1].relay()
    down_lines[0].settle()
    out_lines[0].relay()
    down_lines[1].settle()
    qkv_lines[0].relay()
    out_lines[0].settle()
    qkv_lines[1].relay()
    qkv_lines[0].settle()
    qkv_lines[1].settle()
    for line in [*gate_lines, *up_lines, gain_line, *down_lines, *out_lines, *qkv_lines]:
        line.finish()


def finish(mesh, count, kv, term_gate, term_up, dwd, first, dqkv, attended, low, gains):
    ns, nf = mesh
    na, per = nf // 4, ns // 2
    rows, width = first.shape
    q_width = dqkv.shape[3]
    local, half = term_gate.shape[0], width // 2
    block = 2 * local
    anywhere, vmem = pl.BlockSpec(memory_space=pl.ANY), pl.BlockSpec(memory_space=pltpu.VMEM)
    down = (dwd.shape[0] // (2 * na), dwd.shape[1])
    shapes = [term_gate.shape, term_up.shape, down, (local, width), (local, ns * q_width)]
    scratch = [pltpu.VMEM(s, BF16) for s in shapes[2:]]
    scratch += [pltpu.VMEM((2,) + tuple(s), BF16) for s in shapes]
    scratch += [
        pltpu.VMEM((2, rows, width), BF16),
        pltpu.VMEM((2, rows, width), BF16),
        pltpu.VMEM((2, rows, half), BF16),
        pltpu.VMEM((2, per, count, rows // count, q_width), BF16),
        pltpu.VMEM((width, half), BF16),
        pltpu.VMEM((width, per * q_width), BF16),
        pltpu.VMEM((2, local, half), BF16),
        pltpu.VMEM((local, half), BF16),
        pltpu.VMEM((2, local, per * q_width), BF16),
        pltpu.VMEM((local, per * q_width), BF16),
        pltpu.VMEM((4, 2, width), F32),
        pltpu.VMEM((na + 3, 2, width), F32),
    ]
    scratch += chip_sum_shapes(na, True, down[0], down[1] // 2) + chip_sum_shapes(na, False, down[0], down[1] // 2)
    for columns in (half // 2, per * q_width // 2):
        for b_first in (True, False):
            scratch += chip_sum_shapes(na, b_first, block, columns)[:2]
    return pl.pallas_call(
        functools.partial(finish_kernel, mesh, count, kv),
        in_specs=[vmem, vmem] + [anywhere] * 5 + [vmem],
        out_specs=[vmem] * 6,
        out_shape=[jax.ShapeDtypeStruct(s, BF16) for s in shapes] + [jax.ShapeDtypeStruct((2, width), F32)],
        scratch_shapes=scratch
        + [pltpu.SemaphoreType.DMA((64,)), pltpu.SemaphoreType.DMA((64,)), pltpu.SemaphoreType.DMA((64,))],
        compiler_params=pltpu.CompilerParams(vmem_limit_bytes=VMEM_MOST, collective_id=2, has_side_effects=True),
        name="finish",
    )(term_gate, term_up, dwd, first, dqkv, attended, low, gains)


def solution(mesh):
    ns, nf = mesh.shape["seq"], mesh.shape["fsdp"]
    na = nf // 4
    chips = 2 * na
    kv = KEY_VALUE_HEADS // ns

    def body(tokens, cotangent, attention_gain, feedforward_gain, query_weight, key_matrix, value_matrix, out_weight, gate_weight, up_weight, down_weight):
        count, span, width = tokens.shape
        rows = count * span
        local = query_weight.shape[0]
        sizes = (ns, nf)
        mine = lax.axis_index("fsdp")
        cosines, sines = (jnp.asarray(x) for x in rope_tables(ns * span))
        flat = tokens.reshape(rows, width)
        grad_flat = cotangent.reshape(rows, width)
        (w_qkv, w_out, w_gate, w_up, w_down, first, packed, heads_attended, logs, attended, hidden_one, second_both, low_both, gains) = fore(
            sizes, count, kv, flat, grad_flat, attention_gain.reshape(1, local), feedforward_gain.reshape(1, local),
            query_weight, key_matrix, value_matrix, out_weight, gate_weight, up_weight, down_weight, cosines, sines,
        )
        dwg, dwu, dwd, out_own, out_other, dx_own, dx_other = ffn(second_both, low_both, w_gate, w_up, w_down, mine % 2, chips)
        high, low, grad_tokens, gain_grads, dqkv, sum_gate, sum_up = back(
            sizes, count, kv, dx_own, dx_other, hidden_one, grad_flat, gains[1:2], w_out, w_qkv,
            packed, heads_attended, logs, cosines, sines, flat, gains[0:1], dwg, dwu,
        )
        out_arrived = lax.ppermute(out_other, "fsdp", [(i, i ^ 1) for i in range(nf)])
        block_out = hidden_one + out_own + out_arrived.astype(F32)
        grad_gate, grad_up, grad_down, grad_out, grad_qkv, gain_grads = finish(
            sizes, count, kv, sum_gate, sum_up, dwd, first, dqkv, attended, low, gain_grads
        )
        q_end, k_end = ns * kv * GROUP * HEAD_DIM, ns * kv * (GROUP + 1) * HEAD_DIM
        gain_grads = lax.dynamic_slice(gain_grads, (0, mine * local), (2, local))

        return (
            block_out.reshape(count, span, width),
            grad_tokens.reshape(count, span, width),
            gain_grads[0],
            gain_grads[1],
            grad_qkv[:, :q_end].astype(F32),
            grad_qkv[:, q_end:k_end].astype(F32),
            grad_qkv[:, k_end:].astype(F32),
            grad_out.astype(F32),
            grad_gate.astype(F32),
            grad_up.astype(F32),
            grad_down.astype(F32),
        )

    tokens_spec, gain_spec, weight_spec = P("fsdp", "seq", None), P("fsdp"), P("fsdp", None)
    return jax.shard_map(
        body,
        mesh=mesh,
        in_specs=(tokens_spec, tokens_spec, gain_spec, gain_spec) + (weight_spec,) * 7,
        out_specs=(tokens_spec, tokens_spec, gain_spec, gain_spec) + (weight_spec,) * 7,
        check_vma=False,
    )
```

```python
import functools
import math

import jax
import jax.numpy as jnp
import numpy as np
from jax import lax
from jax.experimental import pallas as pl
from jax.experimental.pallas import tpu as pltpu
from jax.sharding import PartitionSpec as P

QUERY_HEADS = 16
KEY_VALUE_HEADS = 8
HEAD_DIM = 96
GROUP = QUERY_HEADS // KEY_VALUE_HEADS
norm_eps = 1e-05
rope_base = 100000.0
masked_score = -1e30
F32, BF16 = jnp.float32, jnp.bfloat16
VMEM_LIMIT = 60 * 1024 * 1024
VMEM_MOST = 67043328


def nt_dot(left, right):
    return lax.dot_general(left, right, (((1,), (1,)), ((), ())), preferred_element_type=F32)


def tn_dot(left, right):
    return lax.dot_general(left, right, (((0,), (0,)), ((), ())), preferred_element_type=F32)


def nn_dot(left, right):
    return jnp.dot(left, right, preferred_element_type=F32)


def whole(shape):
    return pl.BlockSpec(shape, lambda *_: (0,) * len(shape))


def call(kernel, scalars, operands, outs, name, flops, moved, scratch=()):
    return pl.pallas_call(
        kernel,
        grid_spec=pltpu.PrefetchScalarGridSpec(
            num_scalar_prefetch=1,
            grid=(1,),
            in_specs=[whole(x.shape) for x in operands],
            out_specs=[whole(x.shape) for x in outs],
            scratch_shapes=scratch,
        ),
        out_shape=outs,
        compiler_params=pltpu.CompilerParams(vmem_limit_bytes=VMEM_LIMIT),
        cost_estimate=pl.CostEstimate(flops=flops, bytes_accessed=moved, transcendentals=0),
        name=name,
    )(scalars, *operands)


def rope_tables(length):
    half = HEAD_DIM // 2
    freqs = np.float32(rope_base) ** (-(np.float32(2.0) * np.arange(half, dtype=np.float32)) / np.float32(HEAD_DIM))
    angles = np.arange(length, dtype=np.float32)[:, None] * freqs.astype(np.float32)[None, :]
    cosine, sine = np.cos(angles), np.sin(angles)
    return np.concatenate([cosine, cosine], 1), np.concatenate([-sine, sine], 1)


def swap_halves(values):
    half = HEAD_DIM // 2
    width = values.shape[1]
    lane = lax.broadcasted_iota(jnp.int32, values.shape, 1)
    ahead = pltpu.roll(values, width - half, 1)
    behind = pltpu.roll(values, half, 1)
    return jnp.where(lane % HEAD_DIM < half, ahead, behind)


def norm_back(grad, normed, inverse, gain):
    scaled = grad * gain
    return inverse * (scaled - normed * jnp.mean(scaled * normed, axis=1, keepdims=True))


MESH = pl.DeviceIdType.MESH


def ffn_kernel(tiles, scalars, x, g, wg, wu, wd, dwg, dwu, dwd, out_own, out_other, dx_own, dx_other, xt, acc_out, acc_dx, act, dgate, dup):
    step = pl.program_id(0)
    rows = x.shape[0] // 2

    @pl.when(step == 0)
    def _():
        out_own[...] = jnp.zeros_like(out_own)
        dx_own[...] = jnp.zeros_like(dx_own)
        acc_out[...] = jnp.zeros_like(acc_out)
        acc_dx[...] = jnp.zeros_like(acc_dx)
        xt[...] = x[...].T

    for i, (out, dx) in enumerate(((out_own, dx_own), (acc_out, acc_dx))):
        here = slice(i * rows, (i + 1) * rows)
        gate = nn_dot(x[here, :], wg[...])
        up = nn_dot(x[here, :], wu[...])
        grad = nt_dot(g[here, :], wd[...])
        sigmoid = jax.nn.sigmoid(gate)
        silu = gate * sigmoid
        hidden = (silu * up).astype(BF16)
        act[here, :] = hidden
        gate_grad = (grad * up * sigmoid * (1.0 + gate * (1.0 - sigmoid))).astype(BF16)
        up_grad = (grad * silu).astype(BF16)
        dgate[here, :] = gate_grad
        dup[here, :] = up_grad
        out[...] += nn_dot(hidden, wd[...])
        dx[...] += nt_dot(gate_grad, wg[...]) + nt_dot(up_grad, wu[...])
    dwg[...] = nn_dot(xt[...], dgate[...]).astype(BF16)
    dwu[...] = nn_dot(xt[...], dup[...]).astype(BF16)
    dwd[...] = tn_dot(act[...], g[...]).astype(BF16)

    @pl.when(step == tiles - 1)
    def _():
        out_other[...] = acc_out[...].astype(BF16)
        dx_other[...] = acc_dx[...].astype(BF16)


def ffn(x, g, wg, wu, wd, core, chips):
    rows, width = x.shape[0] // 2, x.shape[1]
    parts = 2
    tiles = chips * parts
    cols = wg.shape[2] // parts
    keep = lambda shape: pl.BlockSpec(shape, lambda i, s: (0, 0), pipeline_mode=pl.Buffered(1))
    last = lambda: pl.BlockSpec((rows, width), lambda i, s: (0, 0))

    half = cols * tiles
    wide, low = jax.ShapeDtypeStruct((rows, width), F32), jax.ShapeDtypeStruct((rows, width), BF16)
    return pl.pallas_call(
        functools.partial(ffn_kernel, tiles),
        grid_spec=pltpu.PrefetchScalarGridSpec(
            num_scalar_prefetch=1,
            grid=(tiles,),
            in_specs=[keep(x.shape), keep(g.shape)]
            + [pl.BlockSpec((None, width, cols), lambda i, s: (i // parts, 0, i % parts))] * 2
            + [pl.BlockSpec((cols, width), lambda i, s: (i, 0))],
            out_specs=[pl.BlockSpec((width, cols), lambda i, s: (0, i))] * 2
            + [pl.BlockSpec((cols, width), lambda i, s: (i, 0)), last(), last(), last(), last()],
            scratch_shapes=[pltpu.VMEM((width, 2 * rows), BF16)]
            + [pltpu.VMEM((rows, width), F32)] * 2
            + [pltpu.VMEM((2 * rows, cols), BF16)] * 3,
        ),
        out_shape=[
            jax.ShapeDtypeStruct((width, half), BF16),
            jax.ShapeDtypeStruct((width, half), BF16),
            jax.ShapeDtypeStruct((half, width), BF16),
            wide,
            low,
            wide,
            low,
        ],
        compiler_params=pltpu.CompilerParams(vmem_limit_bytes=VMEM_LIMIT),
        cost_estimate=pl.CostEstimate(
            flops=36 * rows * width * half, bytes_accessed=12 * width * half + 20 * rows * width, transcendentals=0
        ),
        name="ffn",
    )(core.reshape(1).astype(jnp.int32), x, g, wg, wu, wd)


def part(x):
    return x[0].at[x[1:]] if isinstance(x, tuple) else x


def get(x):
    return x[0][x[1:]] if isinstance(x, tuple) else x[...]


def put(x, value):
    if isinstance(x, tuple):
        x[0][x[1:]] = value
    else:
        x[...] = value


class Copy:
    def __init__(self, src, dst, device, send_sem, recv_sem):
        self.src, self.dst, self.device, self.send_sem, self.recv_sem = src, dst, device, send_sem, recv_sem

    def made(self):
        if self.device is None:
            return pltpu.make_async_copy(part(self.src), part(self.dst), part(self.send_sem))
        return pltpu.make_async_remote_copy(
            src_ref=part(self.src),
            dst_ref=part(self.dst),
            send_sem=part(self.send_sem),
            recv_sem=part(self.recv_sem),
            device_id=self.device,
            device_id_type=MESH,
        )

    def start(self):
        self.made().start()

    def wait(self):
        self.made().wait()

    def wait_send(self):
        self.made().wait_send()

    def wait_recv(self):
        self.made().wait_recv()


class Links:
    def __init__(self, mesh, send_sems, recv_sems, local_sems):
        self.ns, self.nf = mesh
        self.na = self.nf // 4
        self.send_sems, self.recv_sems, self.local_sems = send_sems, recv_sems, local_sems
        self.count, self.local_count = 0, 0
        self.z, self.f = lax.axis_index("seq"), lax.axis_index("fsdp")
        self.core = lax.rem(self.f, 2)
        self.b = lax.rem(self.f // 2, 2)
        self.a = self.f // 4

    def chip(self, da, db):
        return lax.rem(self.a + da, self.na) * 2 + lax.rem(self.b + db, 2)

    def at_core(self):
        return (self.z, self.f + 1 - 2 * self.core)

    def at_b(self):
        return (self.z, self.f + 2 - 4 * self.b)

    def at_a(self, d):
        return (self.z, lax.rem(self.f + 4 * d, self.nf))

    def at_z(self, d):
        return (lax.rem(self.z + d, self.ns), self.f)

    def peers(self):
        return [self.at_core(), self.at_b()] + [self.at_a(d) for d in range(1, self.na)] + [self.at_z(d) for d in range(1, self.ns)]

    def barrier(self):
        barrier = pltpu.get_barrier_semaphore()
        peers = self.peers()
        for peer in peers:
            pl.semaphore_signal(barrier, inc=1, device_id=peer, device_id_type=MESH)
        pl.semaphore_wait(barrier, len(peers))

    def copy(self, src, dst, device):
        index = self.count
        self.count += 1
        return Copy(src, dst, device, (self.send_sems, index), (self.recv_sems, index))

    def again(self, src, dst, device):
        index = self.count - 1
        return Copy(src, dst, device, (self.send_sems, index), (self.recv_sems, index))

    def local(self, src, dst):
        index = self.local_count
        self.local_count += 1
        return Copy(src, dst, None, (self.local_sems, index), None)


def rows_at(start, size):
    return pl.ds(pl.multiple_of(start * size, size), size)


class ChipSum:
    def __init__(self, links, partial, b_first, arrived, passed, staging):
        self.links, self.partial, self.b_first = links, partial, b_first
        self.arrived, self.passed, self.staging = arrived, passed, staging
        na = links.na
        self.first, self.second = [], []
        if b_first:
            self.kept = [links.chip(da, 0) for da in range(na)]
            for da in range(na):
                self.first.append(links.copy(partial(links.chip(da, 1)), (arrived, da), links.at_b()))
            for d in range(1, na):
                self.second.append(links.copy((arrived, d), (passed, d - 1), links.at_a(d)))
        else:
            self.kept = [links.chip(0, db) for db in range(2)]
            for d in range(1, na):
                for db in range(2):
                    self.first.append(links.copy(partial(links.chip(d, db)), (arrived, (d - 1) * 2 + db), links.at_a(d)))
            self.second.append(links.copy((arrived, 1), (passed, 0), links.at_b()))
        self.loads = [] if staging is None else [links.local(partial(k), (staging, i)) for i, k in enumerate(self.kept)]

    def start(self):
        for copy in self.first:
            copy.start()

    def load(self):
        for load in self.loads:
            load.start()

    def turn(self):
        for load in self.loads:
            load.wait()
        for copy in self.first:
            copy.wait()
        count = len(self.kept)
        for i in [*range(1, count), 0]:
            own = self.partial(self.kept[i]) if self.staging is None else (self.staging, i)
            total = get(own).astype(F32)
            if self.b_first:
                total = total + self.arrived[i].astype(F32)
            else:
                for d in range(self.links.na - 1):
                    total = total + self.arrived[d * 2 + i].astype(F32)
            self.arrived[i] = total.astype(BF16)
            if i > 0 and self.b_first:
                self.second[i - 1].start()
            elif i > 0:
                self.second[0].start()

    def finish(self):
        for copy in self.second:
            copy.wait()
        total = self.arrived[0].astype(F32)
        for i in range(len(self.second)):
            total = total + self.passed[i].astype(F32)
        return total.astype(BF16)


def chip_sum_shapes(na, b_first, rows, columns):
    first = na if b_first else 2 * (na - 1)
    kept = na if b_first else 2
    return [
        pltpu.VMEM((max(first, kept), rows, columns), BF16),
        pltpu.VMEM((na - 1 if b_first else 1, rows, columns), BF16),
        pltpu.VMEM((kept, rows, columns), BF16),
    ]


def flip_core(f):
    return f + 1 - 2 * lax.rem(f, 2)


def flip_b(f):
    return f + 2 - 4 * lax.rem(f // 2, 2)


class Gather:
    def __init__(self, links, own, land, both):
        self.links = links
        f, na, nf = links.f, links.na, links.nf
        to_core, to_b = links.at_core(), links.at_b()

        def move(origin, device, half=None):
            return links.copy(land(origin, half), land(origin, half), device)

        self.given = [links.copy(own, land(f, None), to_core)] if both else []
        self.own = [links.copy(own, land(f, None), to_b)]
        self.own += [links.copy(own, land(f, None), links.at_a(d)) for d in range(1, na)]
        from_b = flip_b(f)
        from_a = [lax.rem(f + nf - 4 * d, nf) for d in range(1, na)]
        if na == 2:
            self.relays = [move(from_b, links.at_a(1), 1), move(from_a[0], to_b, 0)]
            far = [(flip_b(from_a[0]), 0), (flip_b(from_a[0]), 1)]
        else:
            self.relays = [move(origin, to_b) for origin in from_a]
            far = [(flip_b(origin), None) for origin in from_a]
        near = [from_b, *from_a]
        self.near = [move(origin, to_core) for origin in near] if both else []
        self.far = [move(origin, to_core, half) for origin, half in far] if both else []

    def start(self):
        for copies in self.own + self.given:
            copies.start()

    def turn(self):
        for copies in self.own:
            copies.wait()
        for copies in self.relays + self.near:
            copies.start()

    def pass_on(self):
        for copies in self.relays:
            copies.wait()
        for copies in self.far:
            copies.start()

    def finish(self):
        for copies in self.given + self.near + self.far:
            copies.wait()


class GatherHalf:
    def __init__(self, links, stage, land):
        self.links = links
        f, na, nf, core = links.f, links.na, links.nf, links.core
        to_b = links.at_b()

        def move(origin, device):
            return links.copy(land(origin), land(origin), device)

        self.swap = links.copy((stage, 1 - core), land(f), links.at_core())
        self.kept = links.local((stage, core), land(f))
        targets = [to_b] + [links.at_a(d) for d in range(1, na)]
        self.own = [links.copy((stage, core), land(f), device) for device in targets]
        self.other = [move(flip_core(f), device) for device in targets]
        from_b = flip_b(f)
        from_a = [lax.rem(f + nf - 4 * d, nf) for d in range(1, na)]
        if na == 2:
            self.relays = [move(from_b, links.at_a(1))]
            self.late = [move(flip_core(from_a[0]), to_b)]
        else:
            self.relays = [move(origin, to_b) for origin in from_a]
            self.late = [move(flip_core(origin), to_b) for origin in from_a]

    def start(self):
        for copies in [self.swap, self.kept, *self.own]:
            copies.start()

    def other_start(self):
        self.swap.wait()
        for copies in self.other:
            copies.start()

    def turn(self):
        for copies in self.own:
            copies.wait()
        for copies in self.relays:
            copies.start()

    def turn_late(self):
        for copies in self.other:
            copies.wait()
        for copies in self.late:
            copies.start()

    def finish(self):
        for copies in [self.kept, *self.relays, *self.late]:
            copies.wait()


def attend_heads(ns, kv, span, qs, ks, vs, out, logs):
    scale = 1.0 / math.sqrt(HEAD_DIM)
    row = lax.broadcasted_iota(jnp.int32, (span, span), 0)
    column = lax.broadcasted_iota(jnp.int32, (span, span), 1)
    causal = row >= column
    lane = lax.broadcasted_iota(jnp.int32, (span, 128), 1)
    for s in range(ns):
        here = slice(s * span, (s + 1) * span)
        stats = jnp.zeros((span, 128), F32)
        for h in range(kv * GROUP):
            g = h // GROUP
            q = qs[h, here, :]
            near = jnp.where(causal, nt_dot(q, ks[g, here, :]) * scale, masked_score)
            top = jnp.max(near, axis=1, keepdims=True)
            if s > 0:
                far = nt_dot(q, ks[g, : s * span, :]) * scale
                top = jnp.maximum(top, jnp.max(far, axis=1, keepdims=True))
            near = jnp.exp(near - top)
            total = jnp.sum(near, axis=1, keepdims=True)
            if s > 0:
                far = jnp.exp(far - top)
                total = total + jnp.sum(far, axis=1, keepdims=True)
            inverse = 1.0 / total
            result = nn_dot((near * inverse).astype(BF16), vs[g, here, :])
            if s > 0:
                result = result + nn_dot((far * inverse).astype(BF16), vs[g, : s * span, :])
            stats = jnp.where(lane == h, top + jnp.log(total), stats)
            out[s, :, h * HEAD_DIM : (h + 1) * HEAD_DIM] = result.astype(BF16)
        logs[here, :] = stats


def fill_tables(cosines, sines, narrow_cosines, narrow_sines, heads):
    end = heads * HEAD_DIM
    cosines[:, end:] = jnp.ones((cosines.shape[0], cosines.shape[1] - end), F32)
    sines[:, end:] = jnp.zeros((cosines.shape[0], cosines.shape[1] - end), F32)
    for h in range(heads):
        at = slice(h * HEAD_DIM, (h + 1) * HEAD_DIM)
        cosines[:, at] = narrow_cosines
        sines[:, at] = narrow_sines


def fore_kernel(
    mesh, count, kv,
    tokens, cotangent, gain_one, gain_two, wq, wk, wv, wo, wg, wu, wd, narrow_cosines, narrow_sines,
    w_qkv, w_out, w_gate, w_up, w_down, first_out, packed, heads_attended, logs, attended_out, hidden_out, second_both, low_both, gains_out,
    rows_in, hidden, first, pack, w_land, wo_land, q_send, q_land, a_send, a_land, stage_gate, stage_up, gain_send, gain_land,
    qs, ks, vs, log, attended, second, second_abs, low, cosines, sines, send_sems, recv_sems, local_sems,
):
    links = Links(mesh, send_sems, recv_sems, local_sems)
    ns, na, nf = links.ns, links.na, links.nf
    chips = 2 * na
    z, f, core = links.z, links.f, links.core
    rows, width = rows_in.shape
    span = rows // count
    heads = kv * GROUP
    g_width, k_width = heads * HEAD_DIM, kv * HEAD_DIM
    q_width = g_width + 2 * k_width
    local = width // nf
    links.barrier()

    token_load = links.local(tokens, rows_in)
    token_load.start()
    gain_send[...] = jnp.zeros_like(gain_send)
    gain_send[0:1, :local] = gain_one[...].astype(F32)
    gain_send[1:2, :local] = gain_two[...].astype(F32)
    for j in range(ns):
        pack[j, :, :g_width] = wq[:, j * g_width : (j + 1) * g_width]
        pack[j, :, g_width : g_width + k_width] = wk[:, j * k_width : (j + 1) * k_width]
        pack[j, :, g_width + k_width :] = wv[:, j * k_width : (j + 1) * k_width]

    every = slice(None)

    def piece(start, size, half):
        if half is None:
            return rows_at(start, size)
        return rows_at(start * 2 + half, size // 2)

    units = []
    turns = [*range(1, ns), 0]
    for d in turns:
        g = lax.rem(z + d, ns)
        units.append(Gather(links, (pack, g), lambda o, half, g=g: (w_land, g, piece(o, local, half)), True))
    units.append(Gather(links, wo, lambda o, half: (wo_land, piece(o, local, half)), True))
    depth = wd.shape[0]
    units.append(Gather(links, wd, lambda o, half: (w_down, piece(o // 2, depth, half)), False))
    half_units = [
        GatherHalf(links, stage, lambda o, out=out: (out, every, rows_at(o, local)))
        for stage, out in ((stage_gate, w_gate), (stage_up, w_up))
    ]
    q_copies, a_copies = [], []
    for d in range(1, ns):
        g = lax.rem(z + d, ns)
        q_copies.append([links.copy((q_send, g, i), (q_land, i, z), links.at_z(d)) for i in range(count)])
    for i in range(count):
        a_copies.append([links.copy((a_send, i, lax.rem(z + d, ns)), (a_land, i, z), links.at_z(d)) for d in range(1, ns)])
    second_copy = links.copy(second_abs, (second_both, pl.ds(rows, rows)), links.at_core())
    low_copy = links.copy(low, (low_both, pl.ds(rows, rows)), links.at_core())

    def gain_at(start, size):
        return (gain_land, pl.ds(start, size))

    pair, chip_four = f // 2 * 2, f // 4 * 4
    gain_copies = [
        [links.copy(gain_at(f, 1), gain_at(f, 1), links.at_core())],
        [links.copy(gain_at(pair, 2), gain_at(pair, 2), links.at_b())],
        [links.copy(gain_at(chip_four, 4), gain_at(chip_four, 4), links.at_a(d)) for d in range(1, na)],
    ]
    stores = []

    def store(src, dst):
        copies = links.local(src, dst)
        copies.start()
        stores.append(copies)

    gain_land[f] = gain_send[...]
    for copies in gain_copies[0]:
        copies.start()
    units[0].start()
    units[1].start()
    for j in range(ns):
        w_land[j, rows_at(f, local), :] = pack[j]
    stage_loads = []
    tile = w_gate.shape[2]
    for source, stage in ((wg, stage_gate), (wu, stage_up)):
        for c in range(2):
            for k in range(chips):
                stage_loads.append(links.local((source, every, slice((k * 2 + c) * tile, (k * 2 + c + 1) * tile)), (stage, c, k)))
    for load in stage_loads:
        load.start()
    store_own = [links.local(wo, (wo_land, rows_at(f, local))), links.local(wd, (w_down, rows_at(f // 2, depth)))]
    for copies in store_own:
        copies.start()
    fill_tables(cosines, sines, narrow_cosines[rows_at(z, span), :], narrow_sines[rows_at(z, span), :], heads + kv)
    token_load.wait()
    old = rows_in[...]
    inverse = lax.rsqrt(jnp.mean(old * old, axis=1, keepdims=True) + norm_eps)
    for stage in range(3):
        for copies in gain_copies[stage]:
            copies.wait()
        if stage < 2:
            for copies in gain_copies[stage + 1]:
                copies.start()
    for j in range(nf):
        gains_out[:, j * local : (j + 1) * local] = gain_land[j, 0:2, :local]
    first[...] = (old * inverse * gains_out[0:1, :]).astype(BF16)
    store(first, first_out)

    def project(n):
        g = lax.rem(z + turns[n], ns)
        units[n].finish()
        y = nn_dot(first[...], w_land[g])
        for i in range(count):
            part = y[i * span : (i + 1) * span]
            part = (part * cosines[...] + swap_halves(part) * sines[...]).astype(BF16)
            if turns[n] == 0:
                q_land[i, z] = part
            else:
                q_send[g, i] = part
                q_copies[turns[n] - 1][i].start()
        store((w_land, g), (w_qkv, g))

    last = len(units)
    for n in range(ns):
        units[n].turn()
        if n + 2 < last:
            units[n + 2].start()
        if n > 0:
            units[n - 1].pass_on()
        if n > 1:
            project(n - 2)
    units[ns].turn()
    for load in stage_loads:
        load.wait()
    half_units[0].start()
    units[ns - 1].pass_on()
    project(ns - 2)
    half_units[0].other_start()
    project(ns - 1)
    units[ns].pass_on()

    def attend(i):
        for copies in q_copies:
            copies[i].wait()
        for j in range(ns):
            at = slice(j * span, (j + 1) * span)
            for h in range(heads):
                qs[h, at, :] = q_land[i, j, :, h * HEAD_DIM : (h + 1) * HEAD_DIM]
            for h in range(kv):
                k0, v0 = (heads + h) * HEAD_DIM, (heads + kv + h) * HEAD_DIM
                ks[h, at, :] = q_land[i, j, :, k0 : k0 + HEAD_DIM]
                vs[h, at, :] = q_land[i, j, :, v0 : v0 + HEAD_DIM]
        attend_heads(ns, kv, span, qs, ks, vs, a_send.at[i], log.at[i])
        for copies in a_copies[i]:
            copies.start()
        a_land[i, z] = a_send[i, z]

    for i in range(count):
        attend(i)
        if i == 0:
            units[ns + 1].turn()
            half_units[1].start()
            half_units[1].other_start()
            units[ns].finish()
            store_own[0].wait()
            store(wo_land, w_out)
    store(q_land, packed)
    store(a_send, heads_attended)
    store(log, logs)
    for i in range(count):
        for copies in a_copies[i]:
            copies.wait()
        for j in range(ns):
            attended[i * span : (i + 1) * span, j * g_width : (j + 1) * g_width] = a_land[i, j]
    new = rows_in[...] + nn_dot(attended[...], wo_land[...])
    hidden[...] = new
    inverse = lax.rsqrt(jnp.mean(new * new, axis=1, keepdims=True) + norm_eps)
    second_abs[...] = (new * inverse * gains_out[1:2, :]).astype(BF16)
    second_copy.start()
    store(second_abs, (second_both, pl.ds(0, rows)))
    store(attended, attended_out)
    store(hidden, hidden_out)
    units[ns + 1].pass_on()
    cot_load = links.local(cotangent, rows_in)
    cot_load.start()
    half_units[0].turn()
    cot_load.wait()
    low[...] = rows_in[...].astype(BF16)
    low_copy.start()
    store(low, (low_both, pl.ds(0, rows)))
    half_units[0].turn_late()
    half_units[1].turn()
    half_units[1].turn_late()
    for unit in half_units:
        unit.finish()
    second_copy.wait()
    low_copy.wait()
    store_own[1].wait()
    for copies in stores:
        copies.wait()


def fore(mesh, count, kv, tokens, cotangent, gain_one, gain_two, wq, wk, wv, wo, wg, wu, wd, narrow_cosines, narrow_sines):
    ns, nf = mesh
    na = nf // 4
    chips = 2 * na
    rows, width = tokens.shape
    span = rows // count
    length = ns * span
    heads = kv * GROUP
    g_width = heads * HEAD_DIM
    q_width = g_width + 2 * kv * HEAD_DIM
    local, depth = wq.shape[0], wd.shape[0]
    tile = wg.shape[1] // (2 * chips)
    anywhere, vmem = pl.BlockSpec(memory_space=pl.ANY), pl.BlockSpec(memory_space=pltpu.VMEM)
    low = lambda *shape: jax.ShapeDtypeStruct(shape, BF16)
    wide = lambda *shape: jax.ShapeDtypeStruct(shape, F32)
    outs = [
        low(ns, width, q_width),
        low(width, width),
        low(chips, width, tile),
        low(chips, width, tile),
        low(chips * depth, width),
        low(rows, width),
        low(count, ns, span, q_width),
        low(count, ns, span, g_width),
        wide(count, length, 128),
        low(rows, width),
        wide(rows, width),
        low(2 * rows, width),
        low(2 * rows, width),
        wide(2, width),
    ]
    scratch = [
        pltpu.VMEM((rows, width), F32),
        pltpu.VMEM((rows, width), F32),
        pltpu.VMEM((rows, width), BF16),
        pltpu.VMEM((ns, local, q_width), BF16),
        pltpu.VMEM((ns, width, q_width), BF16),
        pltpu.VMEM((width, width), BF16),
        pltpu.VMEM((ns, count, span, q_width), BF16),
        pltpu.VMEM((count, ns, span, q_width), BF16),
        pltpu.VMEM((count, ns, span, g_width), BF16),
        pltpu.VMEM((count, ns, span, g_width), BF16),
        pltpu.VMEM((2, chips, local, tile), BF16),
        pltpu.VMEM((2, chips, local, tile), BF16),
        pltpu.VMEM((8, 256), F32),
        pltpu.VMEM((nf, 8, 256), F32),
        pltpu.VMEM((heads, length, HEAD_DIM), BF16),
        pltpu.VMEM((kv, length, HEAD_DIM), BF16),
        pltpu.VMEM((kv, length, HEAD_DIM), BF16),
        pltpu.VMEM((count, length, 128), F32),
        pltpu.VMEM((rows, width), BF16),
        pltpu.VMEM((8, 128), BF16),
        pltpu.VMEM((rows, width), BF16),
        pltpu.VMEM((rows, width), BF16),
        pltpu.VMEM((span, q_width), F32),
        pltpu.VMEM((span, q_width), F32),
    ]
    return pl.pallas_call(
        functools.partial(fore_kernel, mesh, count, kv),
        in_specs=[anywhere] * 2 + [vmem] * 5 + [anywhere] * 4 + [vmem] * 2,
        out_specs=[anywhere] * 13 + [vmem],
        out_shape=outs,
        scratch_shapes=scratch
        + [pltpu.SemaphoreType.DMA((160,)), pltpu.SemaphoreType.DMA((160,)), pltpu.SemaphoreType.DMA((64,))],
        compiler_params=pltpu.CompilerParams(vmem_limit_bytes=VMEM_MOST, collective_id=0, has_side_effects=True),
        name="fore",
    )(tokens, cotangent, gain_one, gain_two, wq, wk, wv, wo, wg, wu, wd, narrow_cosines, narrow_sines)


def attend_back_heads(ns, kv, span, qs, ks, vs, gs, attended, logs, dk, dv, result):
    scale = 1.0 / math.sqrt(HEAD_DIM)
    heads = kv * GROUP
    row = lax.broadcasted_iota(jnp.int32, (span, span), 0)
    column = lax.broadcasted_iota(jnp.int32, (span, span), 1)
    causal = row >= column
    dk[...] = jnp.zeros_like(dk)
    dv[...] = jnp.zeros_like(dv)
    for s in range(ns):
        here = slice(s * span, (s + 1) * span)
        for h in range(heads):
            g = h // GROUP
            q, grad = qs[h, here, :], gs[h, here, :]
            log_total = logs[here, h : h + 1]
            out = attended[s, :, h * HEAD_DIM : (h + 1) * HEAD_DIM]
            delta = jnp.sum(grad.astype(F32) * out.astype(F32), axis=1, keepdims=True)
            k, v = ks[g, here, :], vs[g, here, :]
            near = jnp.where(causal, jnp.exp(nt_dot(q, k) * scale - log_total), 0.0)
            slope = (near * (nt_dot(grad, v) - delta) * scale).astype(BF16)
            dq = nn_dot(slope, k)
            dk[g, here, :] += tn_dot(slope, q)
            dv[g, here, :] += tn_dot(near.astype(BF16), grad)
            if s > 0:
                before = slice(0, s * span)
                k, v = ks[g, before, :], vs[g, before, :]
                far = jnp.exp(nt_dot(q, k) * scale - log_total)
                slope = (far * (nt_dot(grad, v) - delta) * scale).astype(BF16)
                dq = dq + nn_dot(slope, k)
                dk[g, before, :] += tn_dot(slope, q)
                dv[g, before, :] += tn_dot(far.astype(BF16), grad)
            result[here, h * HEAD_DIM : (h + 1) * HEAD_DIM] = dq
    for g in range(kv):
        k0 = (heads + g) * HEAD_DIM
        v0 = (heads + kv + g) * HEAD_DIM
        result[:, k0 : k0 + HEAD_DIM] = dk[g]
        result[:, v0 : v0 + HEAD_DIM] = dv[g]


def back_kernel(
    mesh, count, kv,
    dx_own, dx_other, hidden, cotangent, gain_two, w_out, w_qkv, packed, attended, logs, cosines, sines, tokens, gain_one, dwg, dwu,
    high, low, out, gain_grads, dqkv, sum_gate, sum_up,
    dx_land, g_send, g_land, q_send, q_land, swap_send, swap_land, *rest,
):
    parts, (send_sems, recv_sems, local_sems) = rest[:-3], rest[-3:]
    links = Links(mesh, send_sems, recv_sems, local_sems)
    ns, na = links.ns, links.na
    chips = 2 * na
    z, core = links.z, links.core
    rows, width = hidden.shape
    span = rows // count
    length = ns * span
    heads = kv * GROUP
    g_width, q_width = heads * HEAD_DIM, (heads + 2 * kv) * HEAD_DIM
    half = dwg.shape[1]
    block = width // chips
    links.barrier()

    dx_copy = links.copy(dx_other, dx_land, links.at_core())
    dx_copy.start()
    sums = []
    for n, source in enumerate((dwg, dwu)):
        for b_first in (True, False):
            columns = slice(0, half // 2) if b_first else slice(half // 2, half)
            at = (n * 2 + (0 if b_first else 1)) * 3
            partial = lambda k, source=source, columns=columns: (source, rows_at(k, block), columns)
            sums.append(ChipSum(links, partial, b_first, *parts[at : at + 3]))
    for item in sums:
        item.start()
        item.load()

    g_copies, q_copies = [], []
    for i in range(count):
        g_copies.append([links.copy((g_send, i, lax.rem(z + d, ns)), (g_land, i, z), links.at_z(d)) for d in range(1, ns)])
        q_copies.append([links.copy((q_send, i, lax.rem(z + d, ns)), (q_land, z, i), links.at_z(d)) for d in range(1, ns)])

    def out_back(dx, old, grad, w):
        loads = [links.local(dx_own, dx), links.local(hidden, old), links.local(cotangent, grad), links.local(w_out, w)]
        for load in loads:
            load.start()
        dx_copy.wait()
        for load in loads[:3]:
            load.wait()
        step = dx[...] + dx_land[...].astype(F32)
        inverse = lax.rsqrt(jnp.mean(old[...] * old[...], axis=1, keepdims=True) + norm_eps)
        normed = old[...] * inverse
        gain_grads[1:2, :] = jnp.sum(step * normed, axis=0, keepdims=True)
        grad[...] = grad[...] + norm_back(step, normed, inverse, gain_two[...])
        low[...] = grad[...].astype(BF16)
        stores = [links.local(grad, high)]
        for store in stores:
            store.start()
        loads[3].wait()
        for i in range(count):
            here = slice(i * span, (i + 1) * span)
            part = nt_dot(low[here, :], w[...]).astype(BF16)
            for j in range(ns):
                g_send[i, j] = part[:, j * g_width : (j + 1) * g_width]
            for copies in g_copies[i]:
                copies.start()
            g_land[i, z] = g_send[i, z]
        for store in stores:
            store.wait()

    pl.run_scoped(
        out_back,
        pltpu.VMEM((rows, width), F32),
        pltpu.VMEM((rows, width), F32),
        pltpu.VMEM((rows, width), F32),
        pltpu.VMEM((width, width), BF16),
    )

    def attention(qkv, mid, log, qs, ks, vs, gs, dk, dv, result, cosine, sine):
        fill_tables(cosine, sine, cosines[...], sines[...], heads + kv)
        for i in range(count):
            loads = [links.local((packed, i), qkv), links.local((attended, i), mid), links.local((logs, i), log)]
            for load in loads:
                load.start()
            for load in loads:
                load.wait()
            for j in range(ns):
                at = slice(j * span, (j + 1) * span)
                for h in range(heads):
                    qs[h, at, :] = qkv[j, :, h * HEAD_DIM : (h + 1) * HEAD_DIM]
                for h in range(kv):
                    k0, v0 = (heads + h) * HEAD_DIM, (heads + kv + h) * HEAD_DIM
                    ks[h, at, :] = qkv[j, :, k0 : k0 + HEAD_DIM]
                    vs[h, at, :] = qkv[j, :, v0 : v0 + HEAD_DIM]
            for copies in g_copies[i]:
                copies.wait()
            for j in range(ns):
                for h in range(heads):
                    gs[h, j * span : (j + 1) * span, :] = g_land[i, j, :, h * HEAD_DIM : (h + 1) * HEAD_DIM]
            attend_back_heads(ns, kv, span, qs, ks, vs, gs, mid, log, dk, dv, result)
            for j in range(ns):
                here = slice(j * span, (j + 1) * span)
                part = result[here, :]
                q_send[i, j] = (part * cosine[here, :] - swap_halves(part) * sine[here, :]).astype(BF16)
            for copies in q_copies[i]:
                copies.start()
            q_land[z, i] = q_send[i, z]
            if i < len(sums) // 2:
                for item in sums[2 * i : 2 * i + 2]:
                    item.turn()

    pl.run_scoped(
        attention,
        pltpu.VMEM((ns, span, q_width), BF16),
        pltpu.VMEM((ns, span, g_width), BF16),
        pltpu.VMEM((length, 128), F32),
        pltpu.VMEM((heads, length, HEAD_DIM), BF16),
        pltpu.VMEM((kv, length, HEAD_DIM), BF16),
        pltpu.VMEM((kv, length, HEAD_DIM), BF16),
        pltpu.VMEM((heads, length, HEAD_DIM), BF16),
        pltpu.VMEM((kv, length, HEAD_DIM), F32),
        pltpu.VMEM((kv, length, HEAD_DIM), F32),
        pltpu.VMEM((length, q_width), F32),
        pltpu.VMEM((length, q_width), F32),
        pltpu.VMEM((length, q_width), F32),
    )

    swaps = []
    local = block // 2
    for item in sums[2 * count :]:
        item.turn()

    def swap(n):
        for m in range(2):
            total = sums[2 * n + m].finish()
            swap_send[n, m, 0] = total[:local]
            swap_send[n, m, 1] = total[local:]
        for m in range(2):
            copies = links.copy((swap_send, n, m, 1 - core), (swap_land, n, m), links.at_core())
            copies.start()
            swaps.append(copies)

    swap(0)

    def project_back(w, old, base, grad):
        loads = [links.local(w_qkv, w), links.local(tokens, old), links.local(high, base)]
        for load in loads:
            load.start()
        for load in loads:
            load.wait()
        for i in range(count):
            here = slice(i * span, (i + 1) * span)
            for copies in q_copies[i]:
                copies.wait()
            total = nt_dot(q_land[0, i], w[0])
            for j in range(1, ns):
                total = total + nt_dot(q_land[j, i], w[j])
            grad[here, :] = total
        step = grad[...]
        inverse = lax.rsqrt(jnp.mean(old[...] * old[...], axis=1, keepdims=True) + norm_eps)
        normed = old[...] * inverse
        gain_grads[0:1, :] = jnp.sum(step * normed, axis=0, keepdims=True)
        base[...] = base[...] + norm_back(step, normed, inverse, gain_one[...])
        stores = [links.local(base, out), links.local(q_land, dqkv)]
        for store in stores:
            store.start()
        for store in stores:
            store.wait()

    pl.run_scoped(
        project_back,
        pltpu.VMEM((ns, width, q_width), BF16),
        pltpu.VMEM((rows, width), F32),
        pltpu.VMEM((rows, width), F32),
        pltpu.VMEM((rows, width), F32),
    )
    swap(1)
    tile = half // chips
    for n, total in enumerate((sum_gate, sum_up)):
        for m in range(2):
            swaps[2 * n + m].wait()
            kept, arrived = swap_send[n, m, core], swap_land[n, m]
            for t in range(chips // 2):
                here = slice(t * tile, (t + 1) * tile)
                k = m * (chips // 2) + t
                first, second = kept[:, here], arrived[:, here]
                total[:, 2 * k * tile : (2 * k + 1) * tile] = jnp.where(core == 0, first, second)
                total[:, (2 * k + 1) * tile : (2 * k + 2) * tile] = jnp.where(core == 0, second, first)


def back(mesh, count, kv, dx_own, dx_other, hidden, cotangent, gain_two, w_out, w_qkv, packed, attended, logs, cosines, sines, tokens, gain_one, dwg, dwu):
    ns, nf = mesh
    na = nf // 4
    rows, width = hidden.shape
    span = rows // count
    heads = kv * GROUP
    g_width, q_width = heads * HEAD_DIM, (heads + 2 * kv) * HEAD_DIM
    half = dwg.shape[1]
    block = width // (2 * na)
    local = block // 2
    anywhere = pl.BlockSpec(memory_space=pl.ANY)
    vmem = pl.BlockSpec(memory_space=pltpu.VMEM)
    operands = [dx_own, dx_other, hidden, cotangent, gain_two, w_out, w_qkv, packed, attended, logs, cosines, sines, tokens, gain_one, dwg, dwu]
    wide = jax.ShapeDtypeStruct((rows, width), F32)
    summed = jax.ShapeDtypeStruct((local, 2 * half), BF16)
    scratch = [
        pltpu.VMEM((rows, width), BF16),
        pltpu.VMEM((count, ns, span, g_width), BF16),
        pltpu.VMEM((count, ns, span, g_width), BF16),
        pltpu.VMEM((count, ns, span, q_width), BF16),
        pltpu.VMEM((ns, count, span, q_width), BF16),
        pltpu.VMEM((2, 2, 2, local, half // 2), BF16),
        pltpu.VMEM((2, 2, local, half // 2), BF16),
    ]
    for _ in range(2):
        for b_first in (True, False):
            scratch += chip_sum_shapes(na, b_first, block, half // 2)
    return pl.pallas_call(
        functools.partial(back_kernel, mesh, count, kv),
        in_specs=[vmem if x.shape[0] == 1 or x.shape[1] == HEAD_DIM else anywhere for x in operands],
        out_specs=[anywhere, vmem, anywhere, vmem, anywhere, vmem, vmem],
        out_shape=[
            wide,
            jax.ShapeDtypeStruct((rows, width), BF16),
            wide,
            jax.ShapeDtypeStruct((2, width), F32),
            jax.ShapeDtypeStruct((ns, count, span, q_width), BF16),
            summed,
            summed,
        ],
        scratch_shapes=scratch
        + [pltpu.SemaphoreType.DMA((64,)), pltpu.SemaphoreType.DMA((64,)), pltpu.SemaphoreType.DMA((64,))],
        compiler_params=pltpu.CompilerParams(vmem_limit_bytes=VMEM_MOST, collective_id=1, has_side_effects=True),
        name="back",
    )(*operands)


class LineSum:
    def __init__(self, links, term, first, second, total):
        self.links, self.term, self.first, self.second, self.total = links, term, first, second, total
        z, ns = links.z, links.ns
        self.dtype = (term[0] if isinstance(term, tuple) else term).dtype
        middle = ns // 2
        self.deep = middle > 1
        lower = z < middle
        step = jnp.where(lower, 1, -1)
        self.end = (z == 0) | (z == ns - 1)
        self.inner = (z == middle - 1) | (z == middle)
        inward, outward = (z + step, links.f), (z - step, links.f)
        self.inward = links.copy(term, first, inward) if self.deep else None
        self.onward = links.again(first, first, inward) if self.deep else None
        self.across = links.copy(first if self.deep else term, second, inward)
        self.outward = links.copy(total, total, outward) if self.deep else None

    def add(self, target, one, two):
        put(target, (get(one).astype(F32) + get(two).astype(F32)).astype(self.dtype))

    def begin(self):
        if self.deep:
            pl.when(self.end)(self.inward.start)
        else:
            self.across.start()

    def relay(self):
        if not self.deep:
            return

        @pl.when(jnp.logical_not(self.end))
        def _():
            self.inward.wait_recv()
            self.add(self.first, self.term, self.first)
            pl.when(self.inner)(self.across.start)
            pl.when(jnp.logical_not(self.inner))(self.onward.start)

    def settle(self):
        @pl.when(self.inner)
        def _():
            self.across.wait()
            self.add(self.total, self.first if self.deep else self.term, self.second)
            if self.deep:
                self.outward.start()

        if self.deep:

            @pl.when(jnp.logical_not(self.inner | self.end))
            def _():
                self.outward.wait_recv()
                self.outward.start()

    def finish(self):
        if not self.deep:
            return
        pl.when(self.end)(self.outward.wait_recv)
        pl.when(jnp.logical_not(self.inner))(self.inward.wait_send)
        pl.when(jnp.logical_not(self.end))(self.outward.wait_send)


def finish_kernel(
    mesh, count, kv,
    term_gate, term_up, dwd, first, dqkv, attended, low, gains,
    out_gate, out_up, out_down, out_out, out_qkv, out_gains,
    term_down, term_out, term_qkv, in_gate, in_up, in_down, in_out, in_qkv,
    first_both, attended_both, low_both, dq_both, w_out_part, w_qkv_part,
    swap_out, land_out, swap_qkv, land_qkv, gain_terms, gain_lands, *rest,
):
    parts, (send_sems, recv_sems, local_sems) = rest[:-3], rest[-3:]
    links = Links(mesh, send_sems, recv_sems, local_sems)
    ns, na = links.ns, links.na
    chips, per = 2 * na, ns // 2
    core = links.core
    rows, width = first.shape
    q_width = dqkv.shape[3]
    middle = width // 2
    links.barrier()

    def lines(term, inbox, out, pieces):
        size = term.shape[1] // pieces
        every = slice(None)
        made = []
        for i in range(pieces):
            at = slice(i * size, (i + 1) * size)
            made.append(LineSum(links, (term, every, at), (inbox, 0, every, at), (inbox, 1, every, at), (out, every, at)))
        return made

    gate_lines = lines(term_gate, in_gate, out_gate, 4)
    up_lines = lines(term_up, in_up, out_up, 4)
    down_lines = lines(term_down, in_down, out_down, 4)
    out_lines = lines(term_out, in_out, out_out, 2)
    qkv_lines = lines(term_qkv, in_qkv, out_qkv, 4)
    for line in gate_lines + up_lines:
        line.begin()

    sends = [
        links.copy((dqkv, pl.ds((1 - core) * per, per)), (dq_both, 1), links.at_core()),
        links.copy((low, slice(None), rows_at(1 - core, middle)), (low_both, 1), links.at_core()),
        links.copy(first, (first_both, 1), links.at_core()),
        links.copy(attended, (attended_both, 1), links.at_core()),
    ]
    loads = [
        links.local((low, slice(None), rows_at(core, middle)), (low_both, 0)),
        links.local(attended, (attended_both, 0)),
        links.local(first, (first_both, 0)),
        links.local((dqkv, pl.ds(core * per, per)), (dq_both, 0)),
    ]
    for copies in loads + sends[1:2] + sends[3:4] + sends[2:3] + sends[:1]:
        copies.start()

    down_rows = dwd.shape[0] // chips
    block = width // chips

    def pair(source, row_count, at, staged):
        made = []
        cut = source.shape[1] // 2
        for n, b_first in enumerate((True, False)):
            columns = slice(0, cut) if b_first else slice(cut, 2 * cut)
            partial = lambda k, columns=columns: (source, rows_at(k, row_count), columns)
            refs = parts[at[n] : at[n + 1]]
            made.append(ChipSum(links, partial, b_first, *(refs if staged else (*refs[:2], None))))
        return made

    down = pair(dwd, down_rows, (0, 3, 6), True)
    for item in down:
        item.start()
        item.load()

    gain_copies = [links.copy((gain_terms, 0), (gain_lands, 0), links.at_core()), links.copy((gain_terms, 1), (gain_lands, 1), links.at_b())]
    gain_copies += [links.copy((gain_terms, 2), (gain_lands, 1 + d), links.at_a(d)) for d in range(1, na)]
    gain_line = LineSum(links, (gain_terms, 3), (gain_lands, na + 1), (gain_lands, na + 2), out_gains)
    gain_terms[0] = gains[...]
    gain_copies[0].start()

    def next_gain(i):
        for copies in gain_copies[i : i + 1] if i < 2 else gain_copies[2:]:
            copies.wait()
        if i < 2:
            gain_terms[i + 1] = gain_terms[i] + gain_lands[i]
            for copies in gain_copies[1:2] if i == 0 else gain_copies[2:]:
                copies.start()
        else:
            total = gain_terms[2]
            for d in range(1, na):
                total = total + gain_lands[1 + d]
            gain_terms[3] = total
            gain_line.begin()

    def qkv_part(p):
        columns = slice(p * q_width, (p + 1) * q_width)
        mine, other = dq_both[0, p].reshape(rows, q_width), dq_both[1, p].reshape(rows, q_width)
        for k in range(chips):
            at = slice(k * block, (k + 1) * block)
            total = tn_dot(first_both[0, :, at], mine) + tn_dot(first_both[1, :, at], other)
            w_qkv_part[at, columns] = total.astype(BF16)

    def swap(sums, send, land):
        local = block // 2
        for n, item in enumerate(sums):
            total = item.finish()
            size = total.shape[1]
            send[0, :, n * size : (n + 1) * size] = total[:local]
            send[1, :, n * size : (n + 1) * size] = total[local:]
        copies = links.copy((send, 1 - core), land, links.at_core())
        copies.start()
        return copies

    out_sums = pair(w_out_part, block, (6, 8, 10), False)
    qkv_sums = pair(w_qkv_part, block, (10, 12, 14), False)
    cut = width // 2
    next_gain(0)
    for i in (1, 3):
        sends[i].wait()
    for i in (0, 1):
        loads[i].wait()
    gate_lines[0].relay()
    for k in range(chips):
        at = slice(k * block, (k + 1) * block)
        total = tn_dot(attended_both[0, :, at], low_both[0]) + tn_dot(attended_both[1, :, at], low_both[1])
        w_out_part[at, :] = total.astype(BF16)
    for item in out_sums:
        item.start()
    gate_lines[1].relay()
    next_gain(1)
    for i in (0, 2):
        sends[i].wait()
    for i in (2, 3):
        loads[i].wait()
    gate_lines[0].settle()
    for p in range(per // 2):
        qkv_part(p)
    gate_lines[2].relay()
    next_gain(2)
    gate_lines[1].settle()
    for p in range(per // 2, per):
        qkv_part(p)
    gate_lines[3].relay()
    for item in down:
        item.turn()
    for item in qkv_sums:
        item.start()
    gate_lines[2].settle()
    gain_line.relay()
    gate_lines[3].settle()
    for item in out_sums:
        item.turn()
    up_lines[0].relay()
    gain_line.settle()
    up_lines[1].relay()
    up_lines[0].settle()
    term_down[:, :cut] = down[0].finish()
    term_down[:, cut:] = down[1].finish()
    for line in down_lines:
        line.begin()
    up_lines[2].relay()
    up_lines[1].settle()
    up_lines[3].relay()
    up_lines[2].settle()
    down_lines[0].relay()
    up_lines[3].settle()
    for item in qkv_sums:
        item.turn()
    down_lines[1].relay()
    down_lines[0].settle()
    out_swap = swap(out_sums, swap_out, land_out)
    down_lines[2].relay()
    down_lines[1].settle()
    out_swap.wait()
    kept, arrived = swap_out[core], land_out[...]
    term_out[:, :cut] = jnp.where(core == 0, kept, arrived)
    term_out[:, cut:] = jnp.where(core == 0, arrived, kept)
    for line in out_lines:
        line.begin()
    down_lines[3].relay()
    down_lines[2].settle()
    qkv_swap = swap(qkv_sums, swap_qkv, land_qkv)
    out_lines[0].relay()
    down_lines[3].settle()
    qkv_swap.wait()
    kept, arrived = swap_qkv[core], land_qkv[...]
    for n in range(2):
        group = jnp.where(core == n, kept, arrived)
        for p in range(per):
            taken, start = p * q_width, 0
            for size in (kv * GROUP * HEAD_DIM, kv * HEAD_DIM, kv * HEAD_DIM):
                at = start + (n * per + p) * size
                term_qkv[:, at : at + size] = group[:, taken : taken + size]
                taken, start = taken + size, start + ns * size
    for line in qkv_lines:
        line.begin()
    out_lines[1].relay()
    out_lines[0].settle()
    qkv_lines[0].relay()
    out_lines[1].settle()
    for n in range(1, len(qkv_lines)):
        qkv_lines[n].relay()
        qkv_lines[n - 1].settle()
    qkv_lines[-1].settle()
    for line in [*gate_lines, *up_lines, gain_line, *down_lines, *out_lines, *qkv_lines]:
        line.finish()


def finish(mesh, count, kv, term_gate, term_up, dwd, first, dqkv, attended, low, gains):
    ns, nf = mesh
    na, per = nf // 4, ns // 2
    rows, width = first.shape
    q_width = dqkv.shape[3]
    local, half = term_gate.shape[0], width // 2
    block = 2 * local
    anywhere, vmem = pl.BlockSpec(memory_space=pl.ANY), pl.BlockSpec(memory_space=pltpu.VMEM)
    down = (dwd.shape[0] // (2 * na), dwd.shape[1])
    shapes = [term_gate.shape, term_up.shape, down, (local, width), (local, ns * q_width)]
    scratch = [pltpu.VMEM(s, BF16) for s in shapes[2:]]
    scratch += [pltpu.VMEM((2,) + tuple(s), BF16) for s in shapes]
    scratch += [
        pltpu.VMEM((2, rows, width), BF16),
        pltpu.VMEM((2, rows, width), BF16),
        pltpu.VMEM((2, rows, half), BF16),
        pltpu.VMEM((2, per, count, rows // count, q_width), BF16),
        pltpu.VMEM((width, half), BF16),
        pltpu.VMEM((width, per * q_width), BF16),
        pltpu.VMEM((2, local, half), BF16),
        pltpu.VMEM((local, half), BF16),
        pltpu.VMEM((2, local, per * q_width), BF16),
        pltpu.VMEM((local, per * q_width), BF16),
        pltpu.VMEM((4, 2, width), F32),
        pltpu.VMEM((na + 3, 2, width), F32),
    ]
    scratch += chip_sum_shapes(na, True, down[0], down[1] // 2) + chip_sum_shapes(na, False, down[0], down[1] // 2)
    for columns in (half // 2, per * q_width // 2):
        for b_first in (True, False):
            scratch += chip_sum_shapes(na, b_first, block, columns)[:2]
    return pl.pallas_call(
        functools.partial(finish_kernel, mesh, count, kv),
        in_specs=[vmem, vmem] + [anywhere] * 5 + [vmem],
        out_specs=[vmem] * 6,
        out_shape=[jax.ShapeDtypeStruct(s, BF16) for s in shapes] + [jax.ShapeDtypeStruct((2, width), F32)],
        scratch_shapes=scratch
        + [pltpu.SemaphoreType.DMA((128,)), pltpu.SemaphoreType.DMA((128,)), pltpu.SemaphoreType.DMA((64,))],
        compiler_params=pltpu.CompilerParams(vmem_limit_bytes=VMEM_MOST, collective_id=2, has_side_effects=True),
        name="finish",
    )(term_gate, term_up, dwd, first, dqkv, attended, low, gains)


def solution(mesh):
    ns, nf = mesh.shape["seq"], mesh.shape["fsdp"]
    na = nf // 4
    chips = 2 * na
    kv = KEY_VALUE_HEADS // ns

    def body(tokens, cotangent, attention_gain, feedforward_gain, query_weight, key_matrix, value_matrix, out_weight, gate_weight, up_weight, down_weight):
        count, span, width = tokens.shape
        rows = count * span
        local = query_weight.shape[0]
        sizes = (ns, nf)
        mine = lax.axis_index("fsdp")
        cosines, sines = (jnp.asarray(x) for x in rope_tables(ns * span))
        flat = tokens.reshape(rows, width)
        grad_flat = cotangent.reshape(rows, width)
        (w_qkv, w_out, w_gate, w_up, w_down, first, packed, heads_attended, logs, attended, hidden_one, second_both, low_both, gains) = fore(
            sizes, count, kv, flat, grad_flat, attention_gain.reshape(1, local), feedforward_gain.reshape(1, local),
            query_weight, key_matrix, value_matrix, out_weight, gate_weight, up_weight, down_weight, cosines, sines,
        )
        dwg, dwu, dwd, out_own, out_other, dx_own, dx_other = ffn(second_both, low_both, w_gate, w_up, w_down, mine % 2, chips)
        high, low, grad_tokens, gain_grads, dqkv, sum_gate, sum_up = back(
            sizes, count, kv, dx_own, dx_other, hidden_one, grad_flat, gains[1:2], w_out, w_qkv,
            packed, heads_attended, logs, cosines, sines, flat, gains[0:1], dwg, dwu,
        )
        out_arrived = lax.ppermute(out_other, "fsdp", [(i, i ^ 1) for i in range(nf)])
        block_out = hidden_one + out_own + out_arrived.astype(F32)
        grad_gate, grad_up, grad_down, grad_out, grad_qkv, gain_grads = finish(
            sizes, count, kv, sum_gate, sum_up, dwd, first, dqkv, attended, low, gain_grads
        )
        q_end, k_end = ns * kv * GROUP * HEAD_DIM, ns * kv * (GROUP + 1) * HEAD_DIM
        gain_grads = lax.dynamic_slice(gain_grads, (0, mine * local), (2, local))

        return (
            block_out.reshape(count, span, width),
            grad_tokens.reshape(count, span, width),
            gain_grads[0],
            gain_grads[1],
            grad_qkv[:, :q_end].astype(F32),
            grad_qkv[:, q_end:k_end].astype(F32),
            grad_qkv[:, k_end:].astype(F32),
            grad_out.astype(F32),
            grad_gate.astype(F32),
            grad_up.astype(F32),
            grad_down.astype(F32),
        )

    tokens_spec, gain_spec, weight_spec = P("fsdp", "seq", None), P("fsdp"), P("fsdp", None)
    return jax.shard_map(
        body,
        mesh=mesh,
        in_specs=(tokens_spec, tokens_spec, gain_spec, gain_spec) + (weight_spec,) * 7,
        out_specs=(tokens_spec, tokens_spec, gain_spec, gain_spec) + (weight_spec,) * 7,
        check_vma=False,
    )
```

```python
import functools
import math

import jax
import jax.numpy as jnp
import numpy as np
from jax import lax
from jax.experimental import pallas as pl
from jax.experimental.pallas import tpu as pltpu
from jax.sharding import PartitionSpec as P

QUERY_HEADS = 16
KEY_VALUE_HEADS = 8
HEAD_DIM = 96
GROUP = QUERY_HEADS // KEY_VALUE_HEADS
norm_eps = 1e-05
rope_base = 100000.0
masked_score = -1e30
F32, BF16 = jnp.float32, jnp.bfloat16
VMEM_LIMIT = 60 * 1024 * 1024
VMEM_MOST = 67043328
MESH = pl.DeviceIdType.MESH


def nt_dot(left, right):
    return lax.dot_general(left, right, (((1,), (1,)), ((), ())), preferred_element_type=F32)


def tn_dot(left, right):
    return lax.dot_general(left, right, (((0,), (0,)), ((), ())), preferred_element_type=F32)


def nn_dot(left, right):
    return jnp.dot(left, right, preferred_element_type=F32)


def whole(shape):
    return pl.BlockSpec(shape, lambda *_: (0,) * len(shape))


def call(kernel, scalars, operands, outs, name, flops, moved, scratch=()):
    return pl.pallas_call(
        kernel,
        grid_spec=pltpu.PrefetchScalarGridSpec(
            num_scalar_prefetch=1,
            grid=(1,),
            in_specs=[whole(x.shape) for x in operands],
            out_specs=[whole(x.shape) for x in outs],
            scratch_shapes=scratch,
        ),
        out_shape=outs,
        compiler_params=pltpu.CompilerParams(vmem_limit_bytes=VMEM_LIMIT),
        cost_estimate=pl.CostEstimate(flops=flops, bytes_accessed=moved, transcendentals=0),
        name=name,
    )(scalars, *operands)


def rope_tables(length):
    half = HEAD_DIM // 2
    freqs = np.float32(rope_base) ** (-(np.float32(2.0) * np.arange(half, dtype=np.float32)) / np.float32(HEAD_DIM))
    angles = np.arange(length, dtype=np.float32)[:, None] * freqs.astype(np.float32)[None, :]
    cosine, sine = np.cos(angles), np.sin(angles)
    return np.concatenate([cosine, cosine], 1), np.concatenate([-sine, sine], 1)


def swap_halves(values):
    half = HEAD_DIM // 2
    width = values.shape[1]
    lane = lax.broadcasted_iota(jnp.int32, values.shape, 1)
    ahead = pltpu.roll(values, width - half, 1)
    behind = pltpu.roll(values, half, 1)
    return jnp.where(lane % HEAD_DIM < half, ahead, behind)


def norm_back(grad, normed, inverse, gain):
    scaled = grad * gain
    return inverse * (scaled - normed * jnp.mean(scaled * normed, axis=1, keepdims=True))


def ffn_kernel(
    mesh, tiles, parts, x, g, wg, wd, wu, dwg, dwu, dwd, out_own, out_other, dx_own, dx_other,
    xt, acc_out, acc_dx, act, dgate, dup, stage, land, send_sems, recv_sems, local_sems,
):
    step = pl.program_id(0)
    rows = x.shape[0] // 2
    links = Links(mesh, send_sems, recv_sems, local_sems)
    chips, local, tile = tiles // parts, wu.shape[0], land.shape[2]
    cols = tile // parts
    gathers, loads = [], []
    for k in range(chips):
        gathers.append(GatherHalf(links, lambda c, k=k: (stage, c, k), lambda o, k=k: (land, k, rows_at(o, local))))
        for c in range(2):
            source = (wu, slice(None), slice((k * 2 + c) * tile, (k * 2 + c + 1) * tile))
            loads.append(links.local(source, (stage, c, k)))

    @pl.when(step == 0)
    def _():
        for load in loads:
            load.start()
        links.barrier()
        for load in loads:
            load.wait()
        gathers[0].start()

    @pl.when(step == 0)
    def _():
        out_own[...] = jnp.zeros_like(out_own)
        dx_own[...] = jnp.zeros_like(dx_own)
        acc_out[...] = jnp.zeros_like(acc_out)
        acc_dx[...] = jnp.zeros_like(acc_dx)
        xt[...] = x[...].T
        gathers[0].other_start()

    for k in range(1, chips):

        @pl.when(step == (k - 1) * parts + 1)
        def _():
            gathers[k].turn()
            gathers[k].turn_late()
            if k + 1 < chips:
                gathers[k + 1].start()
                gathers[k + 1].other_start()

    def first_part():
        gathers[0].turn()
        gathers[0].turn_late()
        if chips > 1:
            gathers[1].start()
            gathers[1].other_start()
        gathers[0].finish()

    pl.when(step == 0)(first_part)
    for k in range(1, chips):
        pl.when(step == k * parts)(gathers[k].finish)
    at = pl.ds(pl.multiple_of(lax.rem(step, parts) * cols, cols), cols)
    chip = step // parts
    for i, (out, dx) in enumerate(((out_own, dx_own), (acc_out, acc_dx))):
        here = slice(i * rows, (i + 1) * rows)
        gate = nn_dot(x[here, :], wg[...])
        up = nn_dot(x[here, :], land[chip, :, at])
        grad = nt_dot(g[here, :], wd[...])
        sigmoid = jax.nn.sigmoid(gate)
        silu = gate * sigmoid
        hidden = (silu * up).astype(BF16)
        act[here, :] = hidden
        gate_grad = (grad * up * sigmoid * (1.0 + gate * (1.0 - sigmoid))).astype(BF16)
        up_grad = (grad * silu).astype(BF16)
        dgate[here, :] = gate_grad
        dup[here, :] = up_grad
        out[...] += nn_dot(hidden, wd[...])
        dx[...] += nt_dot(gate_grad, wg[...]) + nt_dot(up_grad, land[chip, :, at])
    dwg[...] = nn_dot(xt[...], dgate[...]).astype(BF16)
    dwu[...] = nn_dot(xt[...], dup[...]).astype(BF16)
    dwd[...] = tn_dot(act[...], g[...]).astype(BF16)

    @pl.when(step == tiles - 1)
    def _():
        out_other[...] = acc_out[...].astype(BF16)
        dx_other[...] = acc_dx[...].astype(BF16)


def ffn(mesh, x, g, wg, wd, wu):
    rows, width = x.shape[0] // 2, x.shape[1]
    chips, _, tile = wg.shape
    parts = 2
    tiles, cols = chips * parts, tile // parts
    local = wu.shape[0]
    keep = lambda shape: pl.BlockSpec(shape, lambda i: (0, 0), pipeline_mode=pl.Buffered(1))
    last = lambda: pl.BlockSpec((rows, width), lambda i: (0, 0))
    half = tile * chips
    wide, low = jax.ShapeDtypeStruct((rows, width), F32), jax.ShapeDtypeStruct((rows, width), BF16)
    return pl.pallas_call(
        functools.partial(ffn_kernel, mesh, tiles, parts),
        grid=(tiles,),
        in_specs=[
            keep(x.shape),
            keep(g.shape),
            pl.BlockSpec((None, width, cols), lambda i: (i // parts, 0, i % parts)),
            pl.BlockSpec((cols, width), lambda i: (i, 0)),
            pl.BlockSpec(memory_space=pl.ANY),
        ],
        out_specs=[pl.BlockSpec((width, cols), lambda i: (0, i))] * 2
        + [pl.BlockSpec((cols, width), lambda i: (i, 0)), last(), last(), last(), last()],
        scratch_shapes=[pltpu.VMEM((width, 2 * rows), BF16)]
        + [pltpu.VMEM((rows, width), F32)] * 2
        + [pltpu.VMEM((2 * rows, cols), BF16)] * 3
        + [pltpu.VMEM((2, chips, local, tile), BF16), pltpu.VMEM((chips, width, tile), BF16)]
        + [pltpu.SemaphoreType.DMA((96,)), pltpu.SemaphoreType.DMA((96,)), pltpu.SemaphoreType.DMA((64,))],
        out_shape=[
            jax.ShapeDtypeStruct((width, half), BF16),
            jax.ShapeDtypeStruct((width, half), BF16),
            jax.ShapeDtypeStruct((half, width), BF16),
            wide,
            low,
            wide,
            low,
        ],
        compiler_params=pltpu.CompilerParams(vmem_limit_bytes=VMEM_MOST, collective_id=3, has_side_effects=True),
        cost_estimate=pl.CostEstimate(
            flops=36 * rows * width * half, bytes_accessed=12 * width * half + 20 * rows * width, transcendentals=0
        ),
        name="ffn",
    )(x, g, wg, wd, wu)


def part(x):
    return x[0].at[x[1:]] if isinstance(x, tuple) else x


def get(x):
    return x[0][x[1:]] if isinstance(x, tuple) else x[...]


def put(x, value):
    if isinstance(x, tuple):
        x[0][x[1:]] = value
    else:
        x[...] = value


class Copy:
    def __init__(self, src, dst, device, send_sem, recv_sem):
        self.src, self.dst, self.device, self.send_sem, self.recv_sem = src, dst, device, send_sem, recv_sem

    def made(self):
        if self.device is None:
            return pltpu.make_async_copy(part(self.src), part(self.dst), part(self.send_sem))
        return pltpu.make_async_remote_copy(
            src_ref=part(self.src),
            dst_ref=part(self.dst),
            send_sem=part(self.send_sem),
            recv_sem=part(self.recv_sem),
            device_id=self.device,
            device_id_type=MESH,
        )

    def start(self):
        self.made().start()

    def wait(self):
        self.made().wait()

    def wait_send(self):
        self.made().wait_send()

    def wait_recv(self):
        self.made().wait_recv()


class Links:
    def __init__(self, mesh, send_sems, recv_sems, local_sems):
        self.ns, self.nf = mesh
        self.na = self.nf // 4
        self.send_sems, self.recv_sems, self.local_sems = send_sems, recv_sems, local_sems
        self.count, self.local_count = 0, 0
        self.z, self.f = lax.axis_index("seq"), lax.axis_index("fsdp")
        self.core = lax.rem(self.f, 2)
        self.b = lax.rem(self.f // 2, 2)
        self.a = self.f // 4

    def chip(self, da, db):
        return lax.rem(self.a + da, self.na) * 2 + lax.rem(self.b + db, 2)

    def at_core(self):
        return (self.z, self.f + 1 - 2 * self.core)

    def at_b(self):
        return (self.z, self.f + 2 - 4 * self.b)

    def at_a(self, d):
        return (self.z, lax.rem(self.f + 4 * d, self.nf))

    def at_z(self, d):
        return (lax.rem(self.z + d, self.ns), self.f)

    def peers(self):
        return [self.at_core(), self.at_b()] + [self.at_a(d) for d in range(1, self.na)] + [self.at_z(d) for d in range(1, self.ns)]

    def barrier(self):
        barrier = pltpu.get_barrier_semaphore()
        peers = self.peers()
        for peer in peers:
            pl.semaphore_signal(barrier, inc=1, device_id=peer, device_id_type=MESH)
        pl.semaphore_wait(barrier, len(peers))

    def copy(self, src, dst, device):
        index = self.count
        self.count += 1
        return Copy(src, dst, device, (self.send_sems, index), (self.recv_sems, index))

    def again(self, src, dst, device):
        index = self.count - 1
        return Copy(src, dst, device, (self.send_sems, index), (self.recv_sems, index))

    def local(self, src, dst):
        index = self.local_count
        self.local_count += 1
        return Copy(src, dst, None, (self.local_sems, index), None)


def rows_at(start, size):
    return pl.ds(pl.multiple_of(start * size, size), size)


class ChipSum:
    def __init__(self, links, partial, b_first, arrived, passed, staging):
        self.links, self.partial, self.b_first = links, partial, b_first
        self.arrived, self.passed, self.staging = arrived, passed, staging
        na = links.na
        self.first, self.second = [], []
        if b_first:
            self.kept = [links.chip(da, 0) for da in range(na)]
            for da in range(na):
                self.first.append(links.copy(partial(links.chip(da, 1)), (arrived, da), links.at_b()))
            for d in range(1, na):
                self.second.append(links.copy((arrived, d), (passed, d - 1), links.at_a(d)))
        else:
            self.kept = [links.chip(0, db) for db in range(2)]
            for d in range(1, na):
                for db in range(2):
                    self.first.append(links.copy(partial(links.chip(d, db)), (arrived, (d - 1) * 2 + db), links.at_a(d)))
            self.second.append(links.copy((arrived, 1), (passed, 0), links.at_b()))
        self.loads = [] if staging is None else [links.local(partial(k), (staging, i)) for i, k in enumerate(self.kept)]

    def start(self):
        for copy in self.first:
            copy.start()

    def load(self):
        for load in self.loads:
            load.start()

    def turn(self):
        for load in self.loads:
            load.wait()
        for copy in self.first:
            copy.wait()
        count = len(self.kept)
        for i in [*range(1, count), 0]:
            own = self.partial(self.kept[i]) if self.staging is None else (self.staging, i)
            total = get(own).astype(F32)
            if self.b_first:
                total = total + self.arrived[i].astype(F32)
            else:
                for d in range(self.links.na - 1):
                    total = total + self.arrived[d * 2 + i].astype(F32)
            self.arrived[i] = total.astype(BF16)
            if i > 0 and self.b_first:
                self.second[i - 1].start()
            elif i > 0:
                self.second[0].start()

    def finish(self):
        for copy in self.second:
            copy.wait()
        total = self.arrived[0].astype(F32)
        for i in range(len(self.second)):
            total = total + self.passed[i].astype(F32)
        return total.astype(BF16)


def chip_sum_shapes(na, b_first, rows, columns):
    first = na if b_first else 2 * (na - 1)
    kept = na if b_first else 2
    return [
        pltpu.VMEM((max(first, kept), rows, columns), BF16),
        pltpu.VMEM((na - 1 if b_first else 1, rows, columns), BF16),
        pltpu.VMEM((kept, rows, columns), BF16),
    ]


def flip_core(f):
    return f + 1 - 2 * lax.rem(f, 2)


def flip_b(f):
    return f + 2 - 4 * lax.rem(f // 2, 2)


class Gather:
    def __init__(self, links, own, land, both):
        self.links = links
        f, na, nf = links.f, links.na, links.nf
        to_core, to_b = links.at_core(), links.at_b()

        def move(origin, device, half=None):
            return links.copy(land(origin, half), land(origin, half), device)

        self.given = [links.copy(own, land(f, None), to_core)] if both else []
        self.own = [links.copy(own, land(f, None), to_b)]
        self.own += [links.copy(own, land(f, None), links.at_a(d)) for d in range(1, na)]
        from_b = flip_b(f)
        from_a = [lax.rem(f + nf - 4 * d, nf) for d in range(1, na)]
        if na == 2:
            self.relays = [move(from_b, links.at_a(1), 1), move(from_a[0], to_b, 0)]
            far = [(flip_b(from_a[0]), 0), (flip_b(from_a[0]), 1)]
        else:
            self.relays = [move(origin, to_b) for origin in from_a]
            far = [(flip_b(origin), None) for origin in from_a]
        near = [from_b, *from_a]
        self.near = [move(origin, to_core) for origin in near] if both else []
        self.far = [move(origin, to_core, half) for origin, half in far] if both else []

    def start(self):
        for copies in self.own + self.given:
            copies.start()

    def turn(self):
        for copies in self.own:
            copies.wait()
        for copies in self.relays + self.near:
            copies.start()

    def pass_on(self):
        for copies in self.relays:
            copies.wait()
        for copies in self.far:
            copies.start()

    def finish(self):
        for copies in self.given + self.near + self.far:
            copies.wait()


class GatherHalf:
    def __init__(self, links, stage, land):
        self.links = links
        f, na, nf, core = links.f, links.na, links.nf, links.core
        to_b = links.at_b()

        def move(origin, device):
            return links.copy(land(origin), land(origin), device)

        self.swap = links.copy(stage(1 - core), land(f), links.at_core())
        self.kept = links.local(stage(core), land(f))
        targets = [to_b] + [links.at_a(d) for d in range(1, na)]
        self.own = [links.copy(stage(core), land(f), device) for device in targets]
        self.other = [move(flip_core(f), device) for device in targets]
        from_b = flip_b(f)
        from_a = [lax.rem(f + nf - 4 * d, nf) for d in range(1, na)]
        if na == 2:
            self.relays = [move(from_b, links.at_a(1))]
            self.late = [move(flip_core(from_a[0]), to_b)]
        else:
            self.relays = [move(origin, to_b) for origin in from_a]
            self.late = [move(flip_core(origin), to_b) for origin in from_a]

    def start(self):
        for copies in [self.swap, self.kept, *self.own]:
            copies.start()

    def other_start(self):
        self.swap.wait()
        for copies in self.other:
            copies.start()

    def turn(self):
        for copies in self.own:
            copies.wait()
        for copies in self.relays:
            copies.start()

    def turn_late(self):
        for copies in self.other:
            copies.wait()
        for copies in self.late:
            copies.start()

    def finish(self):
        for copies in [self.kept, *self.relays, *self.late]:
            copies.wait()


def attend_heads(ns, kv, span, qs, ks, vs, out, logs):
    scale = 1.0 / math.sqrt(HEAD_DIM)
    row = lax.broadcasted_iota(jnp.int32, (span, span), 0)
    column = lax.broadcasted_iota(jnp.int32, (span, span), 1)
    causal = row >= column
    lane = lax.broadcasted_iota(jnp.int32, (span, 128), 1)
    for s in range(ns):
        here = slice(s * span, (s + 1) * span)
        stats = jnp.zeros((span, 128), F32)
        for h in range(kv * GROUP):
            g = h // GROUP
            q = qs[h, here, :]
            near = jnp.where(causal, nt_dot(q, ks[g, here, :]) * scale, masked_score)
            top = jnp.max(near, axis=1, keepdims=True)
            if s > 0:
                far = nt_dot(q, ks[g, : s * span, :]) * scale
                top = jnp.maximum(top, jnp.max(far, axis=1, keepdims=True))
            near = jnp.exp(near - top)
            total = jnp.sum(near, axis=1, keepdims=True)
            if s > 0:
                far = jnp.exp(far - top)
                total = total + jnp.sum(far, axis=1, keepdims=True)
            inverse = 1.0 / total
            result = nn_dot((near * inverse).astype(BF16), vs[g, here, :])
            if s > 0:
                result = result + nn_dot((far * inverse).astype(BF16), vs[g, : s * span, :])
            stats = jnp.where(lane == h, top + jnp.log(total), stats)
            out[s, :, h * HEAD_DIM : (h + 1) * HEAD_DIM] = result.astype(BF16)
        logs[here, :] = stats


def fill_tables(cosines, sines, narrow_cosines, narrow_sines, heads):
    end = heads * HEAD_DIM
    cosines[:, end:] = jnp.ones((cosines.shape[0], cosines.shape[1] - end), F32)
    sines[:, end:] = jnp.zeros((cosines.shape[0], cosines.shape[1] - end), F32)
    for h in range(heads):
        at = slice(h * HEAD_DIM, (h + 1) * HEAD_DIM)
        cosines[:, at] = narrow_cosines
        sines[:, at] = narrow_sines


def fore_kernel(
    mesh, count, kv,
    tokens, cotangent, gain_one, gain_two, wq, wk, wv, wo, wg, wd, narrow_cosines, narrow_sines,
    w_qkv, w_out, w_gate, w_down, first_out, packed, heads_attended, logs, attended_out, hidden_out, second_both, low_both, gains_out,
    rows_in, hidden, first, pack, w_land, wo_land, q_send, q_land, a_send, a_land, stage_gate, gain_send, gain_land,
    qs, ks, vs, log, attended, second, second_abs, low, cosines, sines, send_sems, recv_sems, local_sems,
):
    links = Links(mesh, send_sems, recv_sems, local_sems)
    ns, na, nf = links.ns, links.na, links.nf
    chips = 2 * na
    z, f, core = links.z, links.f, links.core
    rows, width = rows_in.shape
    span = rows // count
    heads = kv * GROUP
    g_width, k_width = heads * HEAD_DIM, kv * HEAD_DIM
    q_width = g_width + 2 * k_width
    local = width // nf
    links.barrier()

    token_load = links.local(tokens, rows_in)
    token_load.start()
    gain_send[...] = jnp.zeros_like(gain_send)
    gain_send[0:1, :local] = gain_one[...].astype(F32)
    gain_send[1:2, :local] = gain_two[...].astype(F32)
    for j in range(ns):
        pack[j, :, :g_width] = wq[:, j * g_width : (j + 1) * g_width]
        pack[j, :, g_width : g_width + k_width] = wk[:, j * k_width : (j + 1) * k_width]
        pack[j, :, g_width + k_width :] = wv[:, j * k_width : (j + 1) * k_width]

    every = slice(None)

    def piece(start, size, half):
        if half is None:
            return rows_at(start, size)
        return rows_at(start * 2 + half, size // 2)

    units = []
    turns = [*range(1, ns), 0]
    for d in turns:
        g = lax.rem(z + d, ns)
        units.append(Gather(links, (pack, g), lambda o, half, g=g: (w_land, g, piece(o, local, half)), True))
    units.append(Gather(links, wo, lambda o, half: (wo_land, piece(o, local, half)), True))
    depth = wd.shape[0]
    units.append(Gather(links, wd, lambda o, half: (w_down, piece(o // 2, depth, half)), False))
    gate_unit = GatherHalf(links, lambda c: (stage_gate, c), lambda o: (w_gate, every, rows_at(o, local)))
    q_copies, a_copies = [], []
    for d in range(1, ns):
        g = lax.rem(z + d, ns)
        q_copies.append([links.copy((q_send, g, i), (q_land, i, z), links.at_z(d)) for i in range(count)])
    for i in range(count):
        a_copies.append([links.copy((a_send, i, lax.rem(z + d, ns)), (a_land, i, z), links.at_z(d)) for d in range(1, ns)])
    second_copy = links.copy(second_abs, (second_both, pl.ds(rows, rows)), links.at_core())
    low_copy = links.copy(low, (low_both, pl.ds(rows, rows)), links.at_core())

    def gain_at(start, size):
        return (gain_land, pl.ds(start, size))

    pair, chip_four = f // 2 * 2, f // 4 * 4
    gain_copies = [
        [links.copy(gain_at(f, 1), gain_at(f, 1), links.at_core())],
        [links.copy(gain_at(pair, 2), gain_at(pair, 2), links.at_b())],
        [links.copy(gain_at(chip_four, 4), gain_at(chip_four, 4), links.at_a(d)) for d in range(1, na)],
    ]
    stores = []

    def store(src, dst):
        copies = links.local(src, dst)
        copies.start()
        stores.append(copies)

    gain_land[f] = gain_send[...]
    for copies in gain_copies[0]:
        copies.start()
    units[0].start()
    units[1].start()
    for j in range(ns):
        w_land[j, rows_at(f, local), :] = pack[j]
    stage_loads = []
    tile = w_gate.shape[2]
    for c in range(2):
        for k in range(chips):
            source = (wg, every, slice((k * 2 + c) * tile, (k * 2 + c + 1) * tile))
            stage_loads.append(links.local(source, (stage_gate, c, k)))
    for load in stage_loads:
        load.start()
    store_own = [links.local(wo, (wo_land, rows_at(f, local))), links.local(wd, (w_down, rows_at(f // 2, depth)))]
    for copies in store_own:
        copies.start()
    fill_tables(cosines, sines, narrow_cosines[rows_at(z, span), :], narrow_sines[rows_at(z, span), :], heads + kv)
    token_load.wait()
    old = rows_in[...]
    inverse = lax.rsqrt(jnp.mean(old * old, axis=1, keepdims=True) + norm_eps)
    for stage in range(3):
        for copies in gain_copies[stage]:
            copies.wait()
        if stage < 2:
            for copies in gain_copies[stage + 1]:
                copies.start()
    for j in range(nf):
        gains_out[:, j * local : (j + 1) * local] = gain_land[j, 0:2, :local]
    first[...] = (old * inverse * gains_out[0:1, :]).astype(BF16)
    store(first, first_out)

    def project(n):
        g = lax.rem(z + turns[n], ns)
        units[n].finish()
        y = nn_dot(first[...], w_land[g])
        for i in range(count):
            part = y[i * span : (i + 1) * span]
            part = (part * cosines[...] + swap_halves(part) * sines[...]).astype(BF16)
            if turns[n] == 0:
                q_land[i, z] = part
            else:
                q_send[g, i] = part
                q_copies[turns[n] - 1][i].start()
        store((w_land, g), (w_qkv, g))

    last = len(units)
    for n in range(ns):
        units[n].turn()
        if n + 2 < last:
            units[n + 2].start()
        if n > 0:
            units[n - 1].pass_on()
        if n > 1:
            project(n - 2)
    units[ns].turn()
    for load in stage_loads:
        load.wait()
    gate_unit.start()
    units[ns - 1].pass_on()
    project(ns - 2)
    gate_unit.other_start()
    project(ns - 1)
    units[ns].pass_on()

    def attend(i):
        for copies in q_copies:
            copies[i].wait()
        for j in range(ns):
            at = slice(j * span, (j + 1) * span)
            for h in range(heads):
                qs[h, at, :] = q_land[i, j, :, h * HEAD_DIM : (h + 1) * HEAD_DIM]
            for h in range(kv):
                k0, v0 = (heads + h) * HEAD_DIM, (heads + kv + h) * HEAD_DIM
                ks[h, at, :] = q_land[i, j, :, k0 : k0 + HEAD_DIM]
                vs[h, at, :] = q_land[i, j, :, v0 : v0 + HEAD_DIM]
        attend_heads(ns, kv, span, qs, ks, vs, a_send.at[i], log.at[i])
        for copies in a_copies[i]:
            copies.start()
        a_land[i, z] = a_send[i, z]

    for i in range(count):
        attend(i)
        if i == 0:
            units[ns + 1].turn()
            units[ns].finish()
            store_own[0].wait()
            store(wo_land, w_out)
    store(q_land, packed)
    store(a_send, heads_attended)
    store(log, logs)
    for i in range(count):
        for copies in a_copies[i]:
            copies.wait()
        for j in range(ns):
            attended[i * span : (i + 1) * span, j * g_width : (j + 1) * g_width] = a_land[i, j]
    new = rows_in[...] + nn_dot(attended[...], wo_land[...])
    hidden[...] = new
    inverse = lax.rsqrt(jnp.mean(new * new, axis=1, keepdims=True) + norm_eps)
    second_abs[...] = (new * inverse * gains_out[1:2, :]).astype(BF16)
    second_copy.start()
    store(second_abs, (second_both, pl.ds(0, rows)))
    store(attended, attended_out)
    store(hidden, hidden_out)
    units[ns + 1].pass_on()
    cot_load = links.local(cotangent, rows_in)
    cot_load.start()
    gate_unit.turn()
    cot_load.wait()
    low[...] = rows_in[...].astype(BF16)
    low_copy.start()
    store(low, (low_both, pl.ds(0, rows)))
    gate_unit.turn_late()
    gate_unit.finish()
    second_copy.wait()
    low_copy.wait()
    store_own[1].wait()
    for copies in stores:
        copies.wait()


def fore(mesh, count, kv, tokens, cotangent, gain_one, gain_two, wq, wk, wv, wo, wg, wd, narrow_cosines, narrow_sines):
    ns, nf = mesh
    na = nf // 4
    chips = 2 * na
    rows, width = tokens.shape
    span = rows // count
    length = ns * span
    heads = kv * GROUP
    g_width = heads * HEAD_DIM
    q_width = g_width + 2 * kv * HEAD_DIM
    local, depth = wq.shape[0], wd.shape[0]
    tile = wg.shape[1] // (2 * chips)
    anywhere, vmem = pl.BlockSpec(memory_space=pl.ANY), pl.BlockSpec(memory_space=pltpu.VMEM)
    low = lambda *shape: jax.ShapeDtypeStruct(shape, BF16)
    wide = lambda *shape: jax.ShapeDtypeStruct(shape, F32)
    outs = [
        low(ns, width, q_width),
        low(width, width),
        low(chips, width, tile),
        low(chips * depth, width),
        low(rows, width),
        low(count, ns, span, q_width),
        low(count, ns, span, g_width),
        wide(count, length, 128),
        low(rows, width),
        wide(rows, width),
        low(2 * rows, width),
        low(2 * rows, width),
        wide(2, width),
    ]
    scratch = [
        pltpu.VMEM((rows, width), F32),
        pltpu.VMEM((rows, width), F32),
        pltpu.VMEM((rows, width), BF16),
        pltpu.VMEM((ns, local, q_width), BF16),
        pltpu.VMEM((ns, width, q_width), BF16),
        pltpu.VMEM((width, width), BF16),
        pltpu.VMEM((ns, count, span, q_width), BF16),
        pltpu.VMEM((count, ns, span, q_width), BF16),
        pltpu.VMEM((count, ns, span, g_width), BF16),
        pltpu.VMEM((count, ns, span, g_width), BF16),
        pltpu.VMEM((2, chips, local, tile), BF16),
        pltpu.VMEM((8, 256), F32),
        pltpu.VMEM((nf, 8, 256), F32),
        pltpu.VMEM((heads, length, HEAD_DIM), BF16),
        pltpu.VMEM((kv, length, HEAD_DIM), BF16),
        pltpu.VMEM((kv, length, HEAD_DIM), BF16),
        pltpu.VMEM((count, length, 128), F32),
        pltpu.VMEM((rows, width), BF16),
        pltpu.VMEM((8, 128), BF16),
        pltpu.VMEM((rows, width), BF16),
        pltpu.VMEM((rows, width), BF16),
        pltpu.VMEM((span, q_width), F32),
        pltpu.VMEM((span, q_width), F32),
    ]
    return pl.pallas_call(
        functools.partial(fore_kernel, mesh, count, kv),
        in_specs=[anywhere] * 2 + [vmem] * 5 + [anywhere] * 3 + [vmem] * 2,
        out_specs=[anywhere] * 12 + [vmem],
        out_shape=outs,
        scratch_shapes=scratch
        + [pltpu.SemaphoreType.DMA((160,)), pltpu.SemaphoreType.DMA((160,)), pltpu.SemaphoreType.DMA((64,))],
        compiler_params=pltpu.CompilerParams(vmem_limit_bytes=VMEM_MOST, collective_id=0, has_side_effects=True),
        name="fore",
    )(tokens, cotangent, gain_one, gain_two, wq, wk, wv, wo, wg, wd, narrow_cosines, narrow_sines)


def attend_back_heads(ns, kv, span, qs, ks, vs, gs, attended, logs, dk, dv, result):
    scale = 1.0 / math.sqrt(HEAD_DIM)
    heads = kv * GROUP
    row = lax.broadcasted_iota(jnp.int32, (span, span), 0)
    column = lax.broadcasted_iota(jnp.int32, (span, span), 1)
    causal = row >= column
    dk[...] = jnp.zeros_like(dk)
    dv[...] = jnp.zeros_like(dv)
    for s in range(ns):
        here = slice(s * span, (s + 1) * span)
        for h in range(heads):
            g = h // GROUP
            q, grad = qs[h, here, :], gs[h, here, :]
            log_total = logs[here, h : h + 1]
            out = attended[s, :, h * HEAD_DIM : (h + 1) * HEAD_DIM]
            delta = jnp.sum(grad.astype(F32) * out.astype(F32), axis=1, keepdims=True)
            k, v = ks[g, here, :], vs[g, here, :]
            near = jnp.where(causal, jnp.exp(nt_dot(q, k) * scale - log_total), 0.0)
            slope = (near * (nt_dot(grad, v) - delta) * scale).astype(BF16)
            dq = nn_dot(slope, k)
            dk[g, here, :] += tn_dot(slope, q)
            dv[g, here, :] += tn_dot(near.astype(BF16), grad)
            if s > 0:
                before = slice(0, s * span)
                k, v = ks[g, before, :], vs[g, before, :]
                far = jnp.exp(nt_dot(q, k) * scale - log_total)
                slope = (far * (nt_dot(grad, v) - delta) * scale).astype(BF16)
                dq = dq + nn_dot(slope, k)
                dk[g, before, :] += tn_dot(slope, q)
                dv[g, before, :] += tn_dot(far.astype(BF16), grad)
            result[here, h * HEAD_DIM : (h + 1) * HEAD_DIM] = dq
    for g in range(kv):
        k0 = (heads + g) * HEAD_DIM
        v0 = (heads + kv + g) * HEAD_DIM
        result[:, k0 : k0 + HEAD_DIM] = dk[g]
        result[:, v0 : v0 + HEAD_DIM] = dv[g]


def back_kernel(
    mesh, count, kv,
    dx_own, dx_other, hidden, cotangent, gain_two, w_out, w_qkv, packed, attended, logs, cosines, sines, tokens, gain_one, dwg, dwu,
    high, low, out, gain_grads, dqkv, sum_gate, sum_up,
    dx_land, g_send, g_land, q_send, q_land, swap_send, swap_land, *rest,
):
    parts, (send_sems, recv_sems, local_sems) = rest[:-3], rest[-3:]
    links = Links(mesh, send_sems, recv_sems, local_sems)
    ns, na = links.ns, links.na
    chips = 2 * na
    z, core = links.z, links.core
    rows, width = hidden.shape
    span = rows // count
    length = ns * span
    heads = kv * GROUP
    g_width, q_width = heads * HEAD_DIM, (heads + 2 * kv) * HEAD_DIM
    half = dwg.shape[1]
    block = width // chips
    links.barrier()

    dx_copy = links.copy(dx_other, dx_land, links.at_core())
    dx_copy.start()
    sums = []
    for n, source in enumerate((dwg, dwu)):
        for b_first in (True, False):
            columns = slice(0, half // 2) if b_first else slice(half // 2, half)
            at = (n * 2 + (0 if b_first else 1)) * 3
            partial = lambda k, source=source, columns=columns: (source, rows_at(k, block), columns)
            sums.append(ChipSum(links, partial, b_first, *parts[at : at + 3]))
    for item in sums:
        item.start()
        item.load()

    g_copies, q_copies = [], []
    for i in range(count):
        g_copies.append([links.copy((g_send, i, lax.rem(z + d, ns)), (g_land, i, z), links.at_z(d)) for d in range(1, ns)])
        q_copies.append([links.copy((q_send, i, lax.rem(z + d, ns)), (q_land, z, i), links.at_z(d)) for d in range(1, ns)])

    def out_back(dx, old, grad, w):
        loads = [links.local(dx_own, dx), links.local(hidden, old), links.local(cotangent, grad), links.local(w_out, w)]
        for load in loads:
            load.start()
        dx_copy.wait()
        for load in loads[:3]:
            load.wait()
        step = dx[...] + dx_land[...].astype(F32)
        inverse = lax.rsqrt(jnp.mean(old[...] * old[...], axis=1, keepdims=True) + norm_eps)
        normed = old[...] * inverse
        gain_grads[1:2, :] = jnp.sum(step * normed, axis=0, keepdims=True)
        grad[...] = grad[...] + norm_back(step, normed, inverse, gain_two[...])
        low[...] = grad[...].astype(BF16)
        stores = [links.local(grad, high)]
        for store in stores:
            store.start()
        loads[3].wait()
        for i in range(count):
            here = slice(i * span, (i + 1) * span)
            part = nt_dot(low[here, :], w[...]).astype(BF16)
            for j in range(ns):
                g_send[i, j] = part[:, j * g_width : (j + 1) * g_width]
            for copies in g_copies[i]:
                copies.start()
            g_land[i, z] = g_send[i, z]
        for store in stores:
            store.wait()

    pl.run_scoped(
        out_back,
        pltpu.VMEM((rows, width), F32),
        pltpu.VMEM((rows, width), F32),
        pltpu.VMEM((rows, width), F32),
        pltpu.VMEM((width, width), BF16),
    )

    def attention(qkv, mid, log, qs, ks, vs, gs, dk, dv, result, cosine, sine):
        fill_tables(cosine, sine, cosines[...], sines[...], heads + kv)
        for i in range(count):
            loads = [links.local((packed, i), qkv), links.local((attended, i), mid), links.local((logs, i), log)]
            for load in loads:
                load.start()
            for load in loads:
                load.wait()
            for j in range(ns):
                at = slice(j * span, (j + 1) * span)
                for h in range(heads):
                    qs[h, at, :] = qkv[j, :, h * HEAD_DIM : (h + 1) * HEAD_DIM]
                for h in range(kv):
                    k0, v0 = (heads + h) * HEAD_DIM, (heads + kv + h) * HEAD_DIM
                    ks[h, at, :] = qkv[j, :, k0 : k0 + HEAD_DIM]
                    vs[h, at, :] = qkv[j, :, v0 : v0 + HEAD_DIM]
            for copies in g_copies[i]:
                copies.wait()
            for j in range(ns):
                for h in range(heads):
                    gs[h, j * span : (j + 1) * span, :] = g_land[i, j, :, h * HEAD_DIM : (h + 1) * HEAD_DIM]
            attend_back_heads(ns, kv, span, qs, ks, vs, gs, mid, log, dk, dv, result)
            for j in range(ns):
                here = slice(j * span, (j + 1) * span)
                part = result[here, :]
                q_send[i, j] = (part * cosine[here, :] - swap_halves(part) * sine[here, :]).astype(BF16)
            for copies in q_copies[i]:
                copies.start()
            q_land[z, i] = q_send[i, z]
            if i < len(sums) // 2:
                for item in sums[2 * i : 2 * i + 2]:
                    item.turn()

    pl.run_scoped(
        attention,
        pltpu.VMEM((ns, span, q_width), BF16),
        pltpu.VMEM((ns, span, g_width), BF16),
        pltpu.VMEM((length, 128), F32),
        pltpu.VMEM((heads, length, HEAD_DIM), BF16),
        pltpu.VMEM((kv, length, HEAD_DIM), BF16),
        pltpu.VMEM((kv, length, HEAD_DIM), BF16),
        pltpu.VMEM((heads, length, HEAD_DIM), BF16),
        pltpu.VMEM((kv, length, HEAD_DIM), F32),
        pltpu.VMEM((kv, length, HEAD_DIM), F32),
        pltpu.VMEM((length, q_width), F32),
        pltpu.VMEM((length, q_width), F32),
        pltpu.VMEM((length, q_width), F32),
    )

    swaps = []
    local = block // 2
    for item in sums[2 * count :]:
        item.turn()

    def swap(n):
        for m in range(2):
            total = sums[2 * n + m].finish()
            swap_send[n, m, 0] = total[:local]
            swap_send[n, m, 1] = total[local:]
        for m in range(2):
            copies = links.copy((swap_send, n, m, 1 - core), (swap_land, n, m), links.at_core())
            copies.start()
            swaps.append(copies)

    swap(0)

    def project_back(w, old, base, grad):
        loads = [links.local(w_qkv, w), links.local(tokens, old), links.local(high, base)]
        for load in loads:
            load.start()
        for load in loads:
            load.wait()
        for i in range(count):
            here = slice(i * span, (i + 1) * span)
            for copies in q_copies[i]:
                copies.wait()
            total = nt_dot(q_land[0, i], w[0])
            for j in range(1, ns):
                total = total + nt_dot(q_land[j, i], w[j])
            grad[here, :] = total
        step = grad[...]
        inverse = lax.rsqrt(jnp.mean(old[...] * old[...], axis=1, keepdims=True) + norm_eps)
        normed = old[...] * inverse
        gain_grads[0:1, :] = jnp.sum(step * normed, axis=0, keepdims=True)
        base[...] = base[...] + norm_back(step, normed, inverse, gain_one[...])
        stores = [links.local(base, out), links.local(q_land, dqkv)]
        for store in stores:
            store.start()
        for store in stores:
            store.wait()

    pl.run_scoped(
        project_back,
        pltpu.VMEM((ns, width, q_width), BF16),
        pltpu.VMEM((rows, width), F32),
        pltpu.VMEM((rows, width), F32),
        pltpu.VMEM((rows, width), F32),
    )
    swap(1)
    tile = half // chips
    for n, total in enumerate((sum_gate, sum_up)):
        for m in range(2):
            swaps[2 * n + m].wait()
            kept, arrived = swap_send[n, m, core], swap_land[n, m]
            for t in range(chips // 2):
                here = slice(t * tile, (t + 1) * tile)
                k = m * (chips // 2) + t
                first, second = kept[:, here], arrived[:, here]
                total[:, 2 * k * tile : (2 * k + 1) * tile] = jnp.where(core == 0, first, second)
                total[:, (2 * k + 1) * tile : (2 * k + 2) * tile] = jnp.where(core == 0, second, first)


def back(mesh, count, kv, dx_own, dx_other, hidden, cotangent, gain_two, w_out, w_qkv, packed, attended, logs, cosines, sines, tokens, gain_one, dwg, dwu):
    ns, nf = mesh
    na = nf // 4
    rows, width = hidden.shape
    span = rows // count
    heads = kv * GROUP
    g_width, q_width = heads * HEAD_DIM, (heads + 2 * kv) * HEAD_DIM
    half = dwg.shape[1]
    block = width // (2 * na)
    local = block // 2
    anywhere = pl.BlockSpec(memory_space=pl.ANY)
    vmem = pl.BlockSpec(memory_space=pltpu.VMEM)
    operands = [dx_own, dx_other, hidden, cotangent, gain_two, w_out, w_qkv, packed, attended, logs, cosines, sines, tokens, gain_one, dwg, dwu]
    wide = jax.ShapeDtypeStruct((rows, width), F32)
    summed = jax.ShapeDtypeStruct((local, 2 * half), BF16)
    scratch = [
        pltpu.VMEM((rows, width), BF16),
        pltpu.VMEM((count, ns, span, g_width), BF16),
        pltpu.VMEM((count, ns, span, g_width), BF16),
        pltpu.VMEM((count, ns, span, q_width), BF16),
        pltpu.VMEM((ns, count, span, q_width), BF16),
        pltpu.VMEM((2, 2, 2, local, half // 2), BF16),
        pltpu.VMEM((2, 2, local, half // 2), BF16),
    ]
    for _ in range(2):
        for b_first in (True, False):
            scratch += chip_sum_shapes(na, b_first, block, half // 2)
    return pl.pallas_call(
        functools.partial(back_kernel, mesh, count, kv),
        in_specs=[vmem if x.shape[0] == 1 or x.shape[1] == HEAD_DIM else anywhere for x in operands],
        out_specs=[anywhere, vmem, anywhere, vmem, anywhere, vmem, vmem],
        out_shape=[
            wide,
            jax.ShapeDtypeStruct((rows, width), BF16),
            wide,
            jax.ShapeDtypeStruct((2, width), F32),
            jax.ShapeDtypeStruct((ns, count, span, q_width), BF16),
            summed,
            summed,
        ],
        scratch_shapes=scratch
        + [pltpu.SemaphoreType.DMA((64,)), pltpu.SemaphoreType.DMA((64,)), pltpu.SemaphoreType.DMA((64,))],
        compiler_params=pltpu.CompilerParams(vmem_limit_bytes=VMEM_MOST, collective_id=1, has_side_effects=True),
        name="back",
    )(*operands)


class LineSum:
    def __init__(self, links, term, first, second, total):
        self.links, self.term, self.first, self.second, self.total = links, term, first, second, total
        z, ns = links.z, links.ns
        self.dtype = (term[0] if isinstance(term, tuple) else term).dtype
        middle = ns // 2
        self.deep = middle > 1
        lower = z < middle
        step = jnp.where(lower, 1, -1)
        self.end = (z == 0) | (z == ns - 1)
        self.inner = (z == middle - 1) | (z == middle)
        inward, outward = (z + step, links.f), (z - step, links.f)
        self.inward = links.copy(term, first, inward) if self.deep else None
        self.onward = links.again(first, first, inward) if self.deep else None
        self.across = links.copy(first if self.deep else term, second, inward)
        self.outward = links.copy(total, total, outward) if self.deep else None

    def add(self, target, one, two):
        put(target, (get(one).astype(F32) + get(two).astype(F32)).astype(self.dtype))

    def begin(self):
        if self.deep:
            pl.when(self.end)(self.inward.start)
        else:
            self.across.start()

    def relay(self):
        if not self.deep:
            return

        @pl.when(jnp.logical_not(self.end))
        def _():
            self.inward.wait_recv()
            self.add(self.first, self.term, self.first)
            pl.when(self.inner)(self.across.start)
            pl.when(jnp.logical_not(self.inner))(self.onward.start)

    def settle(self):
        @pl.when(self.inner)
        def _():
            self.across.wait()
            self.add(self.total, self.first if self.deep else self.term, self.second)
            if self.deep:
                self.outward.start()

        if self.deep:

            @pl.when(jnp.logical_not(self.inner | self.end))
            def _():
                self.outward.wait_recv()
                self.outward.start()

    def finish(self):
        if not self.deep:
            return
        pl.when(self.end)(self.outward.wait_recv)
        pl.when(jnp.logical_not(self.inner))(self.inward.wait_send)
        pl.when(jnp.logical_not(self.end))(self.outward.wait_send)


def finish_kernel(
    mesh, count, kv,
    term_gate, term_up, dwd, first, dqkv, attended, low, gains,
    out_gate, out_up, out_down, out_out, out_qkv, out_gains,
    term_down, term_out, term_qkv, in_gate, in_up, in_down, in_out, in_qkv,
    first_both, attended_both, low_both, dq_both, w_out_part, w_qkv_part,
    swap_out, land_out, swap_qkv, land_qkv, gain_terms, gain_lands, *rest,
):
    parts, (send_sems, recv_sems, local_sems) = rest[:-3], rest[-3:]
    links = Links(mesh, send_sems, recv_sems, local_sems)
    ns, na = links.ns, links.na
    chips, per = 2 * na, ns // 2
    core = links.core
    rows, width = first.shape
    q_width = dqkv.shape[3]
    middle = width // 2
    links.barrier()

    def lines(term, inbox, out, pieces):
        size = term.shape[1] // pieces
        every = slice(None)
        made = []
        for i in range(pieces):
            at = slice(i * size, (i + 1) * size)
            made.append(LineSum(links, (term, every, at), (inbox, 0, every, at), (inbox, 1, every, at), (out, every, at)))
        return made

    gate_lines = lines(term_gate, in_gate, out_gate, 4)
    up_lines = lines(term_up, in_up, out_up, 4)
    down_lines = lines(term_down, in_down, out_down, 4)
    out_lines = lines(term_out, in_out, out_out, 2)
    qkv_lines = lines(term_qkv, in_qkv, out_qkv, 4)
    for line in gate_lines + up_lines:
        line.begin()

    sends = [
        links.copy((dqkv, pl.ds((1 - core) * per, per)), (dq_both, 1), links.at_core()),
        links.copy((low, slice(None), rows_at(1 - core, middle)), (low_both, 1), links.at_core()),
        links.copy(first, (first_both, 1), links.at_core()),
        links.copy(attended, (attended_both, 1), links.at_core()),
    ]
    loads = [
        links.local((low, slice(None), rows_at(core, middle)), (low_both, 0)),
        links.local(attended, (attended_both, 0)),
        links.local(first, (first_both, 0)),
        links.local((dqkv, pl.ds(core * per, per)), (dq_both, 0)),
    ]
    for copies in loads + sends[1:2] + sends[3:4] + sends[2:3] + sends[:1]:
        copies.start()

    down_rows = dwd.shape[0] // chips
    block = width // chips

    def pair(source, row_count, at, staged):
        made = []
        cut = source.shape[1] // 2
        for n, b_first in enumerate((True, False)):
            columns = slice(0, cut) if b_first else slice(cut, 2 * cut)
            partial = lambda k, columns=columns: (source, rows_at(k, row_count), columns)
            refs = parts[at[n] : at[n + 1]]
            made.append(ChipSum(links, partial, b_first, *(refs if staged else (*refs[:2], None))))
        return made

    down = pair(dwd, down_rows, (0, 3, 6), True)
    for item in down:
        item.start()
        item.load()

    gain_copies = [links.copy((gain_terms, 0), (gain_lands, 0), links.at_core()), links.copy((gain_terms, 1), (gain_lands, 1), links.at_b())]
    gain_copies += [links.copy((gain_terms, 2), (gain_lands, 1 + d), links.at_a(d)) for d in range(1, na)]
    gain_line = LineSum(links, (gain_terms, 3), (gain_lands, na + 1), (gain_lands, na + 2), out_gains)
    gain_terms[0] = gains[...]
    gain_copies[0].start()

    def next_gain(i):
        for copies in gain_copies[i : i + 1] if i < 2 else gain_copies[2:]:
            copies.wait()
        if i < 2:
            gain_terms[i + 1] = gain_terms[i] + gain_lands[i]
            for copies in gain_copies[1:2] if i == 0 else gain_copies[2:]:
                copies.start()
        else:
            total = gain_terms[2]
            for d in range(1, na):
                total = total + gain_lands[1 + d]
            gain_terms[3] = total
            gain_line.begin()

    def qkv_part(p):
        columns = slice(p * q_width, (p + 1) * q_width)
        mine, other = dq_both[0, p].reshape(rows, q_width), dq_both[1, p].reshape(rows, q_width)
        for k in range(chips):
            at = slice(k * block, (k + 1) * block)
            total = tn_dot(first_both[0, :, at], mine) + tn_dot(first_both[1, :, at], other)
            w_qkv_part[at, columns] = total.astype(BF16)

    def swap(sums, send, land):
        local = block // 2
        for n, item in enumerate(sums):
            total = item.finish()
            size = total.shape[1]
            send[0, :, n * size : (n + 1) * size] = total[:local]
            send[1, :, n * size : (n + 1) * size] = total[local:]
        copies = links.copy((send, 1 - core), land, links.at_core())
        copies.start()
        return copies

    out_sums = pair(w_out_part, block, (6, 8, 10), False)
    qkv_sums = pair(w_qkv_part, block, (10, 12, 14), False)
    cut = width // 2
    next_gain(0)
    for i in (1, 3):
        sends[i].wait()
    for i in (0, 1):
        loads[i].wait()
    gate_lines[0].relay()
    for k in range(chips):
        at = slice(k * block, (k + 1) * block)
        total = tn_dot(attended_both[0, :, at], low_both[0]) + tn_dot(attended_both[1, :, at], low_both[1])
        w_out_part[at, :] = total.astype(BF16)
    for item in out_sums:
        item.start()
    gate_lines[1].relay()
    next_gain(1)
    for i in (0, 2):
        sends[i].wait()
    for i in (2, 3):
        loads[i].wait()
    gate_lines[0].settle()
    for p in range(per // 2):
        qkv_part(p)
    gate_lines[2].relay()
    next_gain(2)
    gate_lines[1].settle()
    for p in range(per // 2, per):
        qkv_part(p)
    gate_lines[3].relay()
    for item in down:
        item.turn()
    for item in qkv_sums:
        item.start()
    gate_lines[2].settle()
    gain_line.relay()
    gate_lines[3].settle()
    for item in out_sums:
        item.turn()
    up_lines[0].relay()
    gain_line.settle()
    up_lines[1].relay()
    up_lines[0].settle()
    term_down[:, :cut] = down[0].finish()
    term_down[:, cut:] = down[1].finish()
    for line in down_lines:
        line.begin()
    up_lines[2].relay()
    up_lines[1].settle()
    up_lines[3].relay()
    up_lines[2].settle()
    down_lines[0].relay()
    up_lines[3].settle()
    for item in qkv_sums:
        item.turn()
    down_lines[1].relay()
    down_lines[0].settle()
    out_swap = swap(out_sums, swap_out, land_out)
    down_lines[2].relay()
    down_lines[1].settle()
    out_swap.wait()
    kept, arrived = swap_out[core], land_out[...]
    term_out[:, :cut] = jnp.where(core == 0, kept, arrived)
    term_out[:, cut:] = jnp.where(core == 0, arrived, kept)
    for line in out_lines:
        line.begin()
    down_lines[3].relay()
    down_lines[2].settle()
    qkv_swap = swap(qkv_sums, swap_qkv, land_qkv)
    out_lines[0].relay()
    down_lines[3].settle()
    qkv_swap.wait()
    kept, arrived = swap_qkv[core], land_qkv[...]
    for n in range(2):
        group = jnp.where(core == n, kept, arrived)
        for p in range(per):
            taken, start = p * q_width, 0
            for size in (kv * GROUP * HEAD_DIM, kv * HEAD_DIM, kv * HEAD_DIM):
                at = start + (n * per + p) * size
                term_qkv[:, at : at + size] = group[:, taken : taken + size]
                taken, start = taken + size, start + ns * size
    for line in qkv_lines:
        line.begin()
    out_lines[1].relay()
    out_lines[0].settle()
    qkv_lines[0].relay()
    out_lines[1].settle()
    for n in range(1, len(qkv_lines)):
        qkv_lines[n].relay()
        qkv_lines[n - 1].settle()
    qkv_lines[-1].settle()
    for line in [*gate_lines, *up_lines, gain_line, *down_lines, *out_lines, *qkv_lines]:
        line.finish()


def finish(mesh, count, kv, term_gate, term_up, dwd, first, dqkv, attended, low, gains):
    ns, nf = mesh
    na, per = nf // 4, ns // 2
    rows, width = first.shape
    q_width = dqkv.shape[3]
    local, half = term_gate.shape[0], width // 2
    block = 2 * local
    anywhere, vmem = pl.BlockSpec(memory_space=pl.ANY), pl.BlockSpec(memory_space=pltpu.VMEM)
    down = (dwd.shape[0] // (2 * na), dwd.shape[1])
    shapes = [term_gate.shape, term_up.shape, down, (local, width), (local, ns * q_width)]
    scratch = [pltpu.VMEM(s, BF16) for s in shapes[2:]]
    scratch += [pltpu.VMEM((2,) + tuple(s), BF16) for s in shapes]
    scratch += [
        pltpu.VMEM((2, rows, width), BF16),
        pltpu.VMEM((2, rows, width), BF16),
        pltpu.VMEM((2, rows, half), BF16),
        pltpu.VMEM((2, per, count, rows // count, q_width), BF16),
        pltpu.VMEM((width, half), BF16),
        pltpu.VMEM((width, per * q_width), BF16),
        pltpu.VMEM((2, local, half), BF16),
        pltpu.VMEM((local, half), BF16),
        pltpu.VMEM((2, local, per * q_width), BF16),
        pltpu.VMEM((local, per * q_width), BF16),
        pltpu.VMEM((4, 2, width), F32),
        pltpu.VMEM((na + 3, 2, width), F32),
    ]
    scratch += chip_sum_shapes(na, True, down[0], down[1] // 2) + chip_sum_shapes(na, False, down[0], down[1] // 2)
    for columns in (half // 2, per * q_width // 2):
        for b_first in (True, False):
            scratch += chip_sum_shapes(na, b_first, block, columns)[:2]
    return pl.pallas_call(
        functools.partial(finish_kernel, mesh, count, kv),
        in_specs=[vmem, vmem] + [anywhere] * 5 + [vmem],
        out_specs=[vmem] * 6,
        out_shape=[jax.ShapeDtypeStruct(s, BF16) for s in shapes] + [jax.ShapeDtypeStruct((2, width), F32)],
        scratch_shapes=scratch
        + [pltpu.SemaphoreType.DMA((128,)), pltpu.SemaphoreType.DMA((128,)), pltpu.SemaphoreType.DMA((64,))],
        compiler_params=pltpu.CompilerParams(vmem_limit_bytes=VMEM_MOST, collective_id=2, has_side_effects=True),
        name="finish",
    )(term_gate, term_up, dwd, first, dqkv, attended, low, gains)


def solution(mesh):
    ns, nf = mesh.shape["seq"], mesh.shape["fsdp"]
    na = nf // 4
    chips = 2 * na
    kv = KEY_VALUE_HEADS // ns

    def body(tokens, cotangent, attention_gain, feedforward_gain, query_weight, key_matrix, value_matrix, out_weight, gate_weight, up_weight, down_weight):
        count, span, width = tokens.shape
        rows = count * span
        local = query_weight.shape[0]
        sizes = (ns, nf)
        mine = lax.axis_index("fsdp")
        cosines, sines = (jnp.asarray(x) for x in rope_tables(ns * span))
        flat = tokens.reshape(rows, width)
        grad_flat = cotangent.reshape(rows, width)
        (w_qkv, w_out, w_gate, w_down, first, packed, heads_attended, logs, attended, hidden_one, second_both, low_both, gains) = fore(
            sizes, count, kv, flat, grad_flat, attention_gain.reshape(1, local), feedforward_gain.reshape(1, local),
            query_weight, key_matrix, value_matrix, out_weight, gate_weight, down_weight, cosines, sines,
        )
        dwg, dwu, dwd, out_own, out_other, dx_own, dx_other = ffn(sizes, second_both, low_both, w_gate, w_down, up_weight)
        high, low, grad_tokens, gain_grads, dqkv, sum_gate, sum_up = back(
            sizes, count, kv, dx_own, dx_other, hidden_one, grad_flat, gains[1:2], w_out, w_qkv,
            packed, heads_attended, logs, cosines, sines, flat, gains[0:1], dwg, dwu,
        )
        out_arrived = lax.ppermute(out_other, "fsdp", [(i, i ^ 1) for i in range(nf)])
        block_out = hidden_one + out_own + out_arrived.astype(F32)
        grad_gate, grad_up, grad_down, grad_out, grad_qkv, gain_grads = finish(
            sizes, count, kv, sum_gate, sum_up, dwd, first, dqkv, attended, low, gain_grads
        )
        q_end, k_end = ns * kv * GROUP * HEAD_DIM, ns * kv * (GROUP + 1) * HEAD_DIM
        gain_grads = lax.dynamic_slice(gain_grads, (0, mine * local), (2, local))

        return (
            block_out.reshape(count, span, width),
            grad_tokens.reshape(count, span, width),
            gain_grads[0],
            gain_grads[1],
            grad_qkv[:, :q_end].astype(F32),
            grad_qkv[:, q_end:k_end].astype(F32),
            grad_qkv[:, k_end:].astype(F32),
            grad_out.astype(F32),
            grad_gate.astype(F32),
            grad_up.astype(F32),
            grad_down.astype(F32),
        )

    tokens_spec, gain_spec, weight_spec = P("fsdp", "seq", None), P("fsdp"), P("fsdp", None)
    return jax.shard_map(
        body,
        mesh=mesh,
        in_specs=(tokens_spec, tokens_spec, gain_spec, gain_spec) + (weight_spec,) * 7,
        out_specs=(tokens_spec, tokens_spec, gain_spec, gain_spec) + (weight_spec,) * 7,
        check_vma=False,
    )
```

```python
import functools
import math

import jax
import jax.numpy as jnp
import numpy as np
from jax import lax
from jax.experimental import pallas as pl
from jax.experimental.pallas import tpu as pltpu
from jax.sharding import PartitionSpec as P

QUERY_HEADS = 16
KEY_VALUE_HEADS = 8
HEAD_DIM = 96
GROUP = QUERY_HEADS // KEY_VALUE_HEADS
norm_eps = 1e-05
rope_base = 100000.0
masked_score = -1e30
F32, BF16 = jnp.float32, jnp.bfloat16
VMEM_LIMIT = 60 * 1024 * 1024
VMEM_MOST = 67043328
MESH = pl.DeviceIdType.MESH


def nt_dot(left, right):
    return lax.dot_general(left, right, (((1,), (1,)), ((), ())), preferred_element_type=F32)


def tn_dot(left, right):
    return lax.dot_general(left, right, (((0,), (0,)), ((), ())), preferred_element_type=F32)


def nn_dot(left, right):
    return jnp.dot(left, right, preferred_element_type=F32)


def whole(shape):
    return pl.BlockSpec(shape, lambda *_: (0,) * len(shape))


def call(kernel, scalars, operands, outs, name, flops, moved, scratch=()):
    return pl.pallas_call(
        kernel,
        grid_spec=pltpu.PrefetchScalarGridSpec(
            num_scalar_prefetch=1,
            grid=(1,),
            in_specs=[whole(x.shape) for x in operands],
            out_specs=[whole(x.shape) for x in outs],
            scratch_shapes=scratch,
        ),
        out_shape=outs,
        compiler_params=pltpu.CompilerParams(vmem_limit_bytes=VMEM_LIMIT),
        cost_estimate=pl.CostEstimate(flops=flops, bytes_accessed=moved, transcendentals=0),
        name=name,
    )(scalars, *operands)


def rope_tables(length):
    half = HEAD_DIM // 2
    freqs = np.float32(rope_base) ** (-(np.float32(2.0) * np.arange(half, dtype=np.float32)) / np.float32(HEAD_DIM))
    angles = np.arange(length, dtype=np.float32)[:, None] * freqs.astype(np.float32)[None, :]
    cosine, sine = np.cos(angles), np.sin(angles)
    return np.concatenate([cosine, cosine], 1), np.concatenate([-sine, sine], 1)


def swap_halves(values):
    half = HEAD_DIM // 2
    width = values.shape[1]
    lane = lax.broadcasted_iota(jnp.int32, values.shape, 1)
    ahead = pltpu.roll(values, width - half, 1)
    behind = pltpu.roll(values, half, 1)
    return jnp.where(lane % HEAD_DIM < half, ahead, behind)


def norm_back(grad, normed, inverse, gain):
    scaled = grad * gain
    return inverse * (scaled - normed * jnp.mean(scaled * normed, axis=1, keepdims=True))


def ffn_kernel(
    mesh, tiles, parts, x, g, wg, wd, wu, w_last, dwg, dwu, dwd, out_own, out_other, dx_own, dx_other,
    xt, acc_out, acc_dx, act, dgate, dup, stage, land, gate, send_sems, recv_sems, local_sems,
):
    step = pl.program_id(0)
    rows = x.shape[0] // 2
    links = Links(mesh, send_sems, recv_sems, local_sems)
    chips, local, tile = tiles // parts, wu.shape[0], land.shape[2]
    cols = tile // parts
    gathers, loads = [], []
    for k in range(chips + 1):
        gathers.append(GatherHalf(links, lambda c, k=k: (stage, c, k), lambda o, k=k: (land, k, rows_at(o, local))))
        weight, tile_at = (wu, k) if k < chips else (w_last, chips - 1)
        for c in range(2):
            source = (weight, slice(None), slice((tile_at * 2 + c) * tile, (tile_at * 2 + c + 1) * tile))
            loads.append(links.local(source, (stage, c, k)))

    def begin(k):
        gathers[k].start()
        gathers[k].other_start()

    def turn(k):
        gathers[k].turn()
        gathers[k].turn_late()

    @pl.when(step == 0)
    def _():
        for load in loads:
            load.start()
        links.barrier()
        for load in loads:
            load.wait()
        gathers[0].start()

    @pl.when(step == 0)
    def _():
        out_own[...] = jnp.zeros_like(out_own)
        dx_own[...] = jnp.zeros_like(dx_own)
        acc_out[...] = jnp.zeros_like(acc_out)
        acc_dx[...] = jnp.zeros_like(acc_dx)
        xt[...] = x[...].T
        gathers[0].other_start()

    def first_part():
        turn(0)
        begin(1)
        gathers[0].finish()

    def later_part(k):
        turn(k)
        for n in (2, 3) if k == 1 else (k + 2,):
            if n <= chips:
                begin(n)
        if k == chips - 1:
            turn(chips)

    pl.when(step == 0)(first_part)
    for k in range(1, chips):
        pl.when(step == (k - 1) * parts + 1)(functools.partial(later_part, k))
        pl.when(step == k * parts)(gathers[k].finish)
    pl.when(step == (chips - 1) * parts)(gathers[chips].finish)
    at = pl.ds(pl.multiple_of(lax.rem(step, parts) * cols, cols), cols)
    chip = step // parts

    @pl.when(chip < chips - 1)
    def _():
        gate[...] = wg[...]

    @pl.when(chip == chips - 1)
    def _():
        gate[...] = land[chips, :, at]

    for i, (out, dx) in enumerate(((out_own, dx_own), (acc_out, acc_dx))):
        here = slice(i * rows, (i + 1) * rows)
        gate_pre = nn_dot(x[here, :], gate[...])
        up = nn_dot(x[here, :], land[chip, :, at])
        grad = nt_dot(g[here, :], wd[...])
        sigmoid = jax.nn.sigmoid(gate_pre)
        silu = gate_pre * sigmoid
        hidden = (silu * up).astype(BF16)
        act[here, :] = hidden
        gate_grad = (grad * up * sigmoid * (1.0 + gate_pre * (1.0 - sigmoid))).astype(BF16)
        up_grad = (grad * silu).astype(BF16)
        dgate[here, :] = gate_grad
        dup[here, :] = up_grad
        out[...] += nn_dot(hidden, wd[...])
        dx[...] += nt_dot(gate_grad, gate[...]) + nt_dot(up_grad, land[chip, :, at])
    dwg[...] = nn_dot(xt[...], dgate[...]).astype(BF16)
    dwu[...] = nn_dot(xt[...], dup[...]).astype(BF16)
    dwd[...] = tn_dot(act[...], g[...]).astype(BF16)

    @pl.when(step == tiles - 1)
    def _():
        out_other[...] = acc_out[...].astype(BF16)
        dx_other[...] = acc_dx[...].astype(BF16)


def ffn(mesh, x, g, wg, wd, wu, w_last):
    rows, width = x.shape[0] // 2, x.shape[1]
    chips, tile = wg.shape[0] + 1, wg.shape[2]
    parts = 2
    tiles, cols = chips * parts, tile // parts
    local = wu.shape[0]
    keep = lambda shape: pl.BlockSpec(shape, lambda i: (0, 0), pipeline_mode=pl.Buffered(1))
    last = lambda: pl.BlockSpec((rows, width), lambda i: (0, 0))
    half = tile * chips
    wide, low = jax.ShapeDtypeStruct((rows, width), F32), jax.ShapeDtypeStruct((rows, width), BF16)
    return pl.pallas_call(
        functools.partial(ffn_kernel, mesh, tiles, parts),
        grid=(tiles,),
        in_specs=[
            keep(x.shape),
            keep(g.shape),
            pl.BlockSpec((None, width, cols), lambda i: (jnp.minimum(i // parts, chips - 2), 0, i % parts)),
            pl.BlockSpec((cols, width), lambda i: (i, 0)),
            pl.BlockSpec(memory_space=pl.ANY),
            pl.BlockSpec(memory_space=pl.ANY),
        ],
        out_specs=[pl.BlockSpec((width, cols), lambda i: (0, i))] * 2
        + [pl.BlockSpec((cols, width), lambda i: (i, 0)), last(), last(), last(), last()],
        scratch_shapes=[pltpu.VMEM((width, 2 * rows), BF16)]
        + [pltpu.VMEM((rows, width), F32)] * 2
        + [pltpu.VMEM((2 * rows, cols), BF16)] * 3
        + [pltpu.VMEM((2, chips + 1, local, tile), BF16), pltpu.VMEM((chips + 1, width, tile), BF16), pltpu.VMEM((width, cols), BF16)]
        + [pltpu.SemaphoreType.DMA((96,)), pltpu.SemaphoreType.DMA((96,)), pltpu.SemaphoreType.DMA((64,))],
        out_shape=[
            jax.ShapeDtypeStruct((width, half), BF16),
            jax.ShapeDtypeStruct((width, half), BF16),
            jax.ShapeDtypeStruct((half, width), BF16),
            wide,
            low,
            wide,
            low,
        ],
        compiler_params=pltpu.CompilerParams(vmem_limit_bytes=VMEM_MOST, collective_id=3, has_side_effects=True),
        cost_estimate=pl.CostEstimate(
            flops=36 * rows * width * half, bytes_accessed=12 * width * half + 20 * rows * width, transcendentals=0
        ),
        name="ffn",
    )(x, g, wg, wd, wu, w_last)


def part(x):
    return x[0].at[x[1:]] if isinstance(x, tuple) else x


def get(x):
    return x[0][x[1:]] if isinstance(x, tuple) else x[...]


def put(x, value):
    if isinstance(x, tuple):
        x[0][x[1:]] = value
    else:
        x[...] = value


class Copy:
    def __init__(self, src, dst, device, send_sem, recv_sem):
        self.src, self.dst, self.device, self.send_sem, self.recv_sem = src, dst, device, send_sem, recv_sem

    def made(self):
        if self.device is None:
            return pltpu.make_async_copy(part(self.src), part(self.dst), part(self.send_sem))
        return pltpu.make_async_remote_copy(
            src_ref=part(self.src),
            dst_ref=part(self.dst),
            send_sem=part(self.send_sem),
            recv_sem=part(self.recv_sem),
            device_id=self.device,
            device_id_type=MESH,
        )

    def start(self):
        self.made().start()

    def wait(self):
        self.made().wait()

    def wait_send(self):
        self.made().wait_send()

    def wait_recv(self):
        self.made().wait_recv()


class Links:
    def __init__(self, mesh, send_sems, recv_sems, local_sems):
        self.ns, self.nf = mesh
        self.na = self.nf // 4
        self.send_sems, self.recv_sems, self.local_sems = send_sems, recv_sems, local_sems
        self.count, self.local_count = 0, 0
        self.z, self.f = lax.axis_index("seq"), lax.axis_index("fsdp")
        self.core = lax.rem(self.f, 2)
        self.b = lax.rem(self.f // 2, 2)
        self.a = self.f // 4

    def chip(self, da, db):
        return lax.rem(self.a + da, self.na) * 2 + lax.rem(self.b + db, 2)

    def at_core(self):
        return (self.z, self.f + 1 - 2 * self.core)

    def at_b(self):
        return (self.z, self.f + 2 - 4 * self.b)

    def at_a(self, d):
        return (self.z, lax.rem(self.f + 4 * d, self.nf))

    def at_z(self, d):
        return (lax.rem(self.z + d, self.ns), self.f)

    def peers(self):
        return [self.at_core(), self.at_b()] + [self.at_a(d) for d in range(1, self.na)] + [self.at_z(d) for d in range(1, self.ns)]

    def barrier(self):
        barrier = pltpu.get_barrier_semaphore()
        peers = self.peers()
        for peer in peers:
            pl.semaphore_signal(barrier, inc=1, device_id=peer, device_id_type=MESH)
        pl.semaphore_wait(barrier, len(peers))

    def copy(self, src, dst, device):
        index = self.count
        self.count += 1
        return Copy(src, dst, device, (self.send_sems, index), (self.recv_sems, index))

    def again(self, src, dst, device):
        index = self.count - 1
        return Copy(src, dst, device, (self.send_sems, index), (self.recv_sems, index))

    def local(self, src, dst):
        index = self.local_count
        self.local_count += 1
        return Copy(src, dst, None, (self.local_sems, index), None)


def rows_at(start, size):
    return pl.ds(pl.multiple_of(start * size, size), size)


class ChipSum:
    def __init__(self, links, partial, b_first, arrived, passed, staging):
        self.links, self.partial, self.b_first = links, partial, b_first
        self.arrived, self.passed, self.staging = arrived, passed, staging
        na = links.na
        self.first, self.second = [], []
        if b_first:
            self.kept = [links.chip(da, 0) for da in range(na)]
            for da in range(na):
                self.first.append(links.copy(partial(links.chip(da, 1)), (arrived, da), links.at_b()))
            for d in range(1, na):
                self.second.append(links.copy((arrived, d), (passed, d - 1), links.at_a(d)))
        else:
            self.kept = [links.chip(0, db) for db in range(2)]
            for d in range(1, na):
                for db in range(2):
                    self.first.append(links.copy(partial(links.chip(d, db)), (arrived, (d - 1) * 2 + db), links.at_a(d)))
            self.second.append(links.copy((arrived, 1), (passed, 0), links.at_b()))
        self.loads = [] if staging is None else [links.local(partial(k), (staging, i)) for i, k in enumerate(self.kept)]

    def start(self):
        for copy in self.first:
            copy.start()

    def load(self):
        for load in self.loads:
            load.start()

    def turn(self):
        for load in self.loads:
            load.wait()
        for copy in self.first:
            copy.wait()
        count = len(self.kept)
        for i in [*range(1, count), 0]:
            own = self.partial(self.kept[i]) if self.staging is None else (self.staging, i)
            total = get(own).astype(F32)
            if self.b_first:
                total = total + self.arrived[i].astype(F32)
            else:
                for d in range(self.links.na - 1):
                    total = total + self.arrived[d * 2 + i].astype(F32)
            self.arrived[i] = total.astype(BF16)
            if i > 0 and self.b_first:
                self.second[i - 1].start()
            elif i > 0:
                self.second[0].start()

    def finish(self):
        for copy in self.second:
            copy.wait()
        total = self.arrived[0].astype(F32)
        for i in range(len(self.second)):
            total = total + self.passed[i].astype(F32)
        return total.astype(BF16)


def chip_sum_shapes(na, b_first, rows, columns):
    first = na if b_first else 2 * (na - 1)
    kept = na if b_first else 2
    return [
        pltpu.VMEM((max(first, kept), rows, columns), BF16),
        pltpu.VMEM((na - 1 if b_first else 1, rows, columns), BF16),
        pltpu.VMEM((kept, rows, columns), BF16),
    ]


def flip_core(f):
    return f + 1 - 2 * lax.rem(f, 2)


def flip_b(f):
    return f + 2 - 4 * lax.rem(f // 2, 2)


class Gather:
    def __init__(self, links, own, land, both):
        self.links = links
        f, na, nf = links.f, links.na, links.nf
        to_core, to_b = links.at_core(), links.at_b()

        def move(origin, device, half=None):
            return links.copy(land(origin, half), land(origin, half), device)

        self.given = [links.copy(own, land(f, None), to_core)] if both else []
        self.own = [links.copy(own, land(f, None), to_b)]
        self.own += [links.copy(own, land(f, None), links.at_a(d)) for d in range(1, na)]
        from_b = flip_b(f)
        from_a = [lax.rem(f + nf - 4 * d, nf) for d in range(1, na)]
        if na == 2:
            self.relays = [move(from_b, links.at_a(1), 1), move(from_a[0], to_b, 0)]
            far = [(flip_b(from_a[0]), 0), (flip_b(from_a[0]), 1)]
        else:
            self.relays = [move(origin, to_b) for origin in from_a]
            far = [(flip_b(origin), None) for origin in from_a]
        near = [from_b, *from_a]
        self.near = [move(origin, to_core) for origin in near] if both else []
        self.far = [move(origin, to_core, half) for origin, half in far] if both else []

    def start(self):
        for copies in self.own + self.given:
            copies.start()

    def turn(self):
        for copies in self.own:
            copies.wait()
        for copies in self.relays + self.near:
            copies.start()

    def pass_on(self):
        for copies in self.relays:
            copies.wait()
        for copies in self.far:
            copies.start()

    def finish(self):
        for copies in self.given + self.near + self.far:
            copies.wait()


class GatherHalf:
    def __init__(self, links, stage, land):
        self.links = links
        f, na, nf, core = links.f, links.na, links.nf, links.core
        to_b = links.at_b()

        def move(origin, device):
            return links.copy(land(origin), land(origin), device)

        self.swap = links.copy(stage(1 - core), land(f), links.at_core())
        self.kept = links.local(stage(core), land(f))
        targets = [to_b] + [links.at_a(d) for d in range(1, na)]
        self.own = [links.copy(stage(core), land(f), device) for device in targets]
        self.other = [move(flip_core(f), device) for device in targets]
        from_b = flip_b(f)
        from_a = [lax.rem(f + nf - 4 * d, nf) for d in range(1, na)]
        if na == 2:
            self.relays = [move(from_b, links.at_a(1))]
            self.late = [move(flip_core(from_a[0]), to_b)]
        else:
            self.relays = [move(origin, to_b) for origin in from_a]
            self.late = [move(flip_core(origin), to_b) for origin in from_a]

    def start(self):
        for copies in [self.swap, self.kept, *self.own]:
            copies.start()

    def other_start(self):
        self.swap.wait()
        for copies in self.other:
            copies.start()

    def turn(self):
        for copies in self.own:
            copies.wait()
        for copies in self.relays:
            copies.start()

    def turn_late(self):
        for copies in self.other:
            copies.wait()
        for copies in self.late:
            copies.start()

    def finish(self):
        for copies in [self.kept, *self.relays, *self.late]:
            copies.wait()


def attend_heads(ns, kv, span, qs, ks, vs, out, logs):
    scale = 1.0 / math.sqrt(HEAD_DIM)
    row = lax.broadcasted_iota(jnp.int32, (span, span), 0)
    column = lax.broadcasted_iota(jnp.int32, (span, span), 1)
    causal = row >= column
    lane = lax.broadcasted_iota(jnp.int32, (span, 128), 1)
    for s in range(ns):
        here = slice(s * span, (s + 1) * span)
        stats = jnp.zeros((span, 128), F32)
        for h in range(kv * GROUP):
            g = h // GROUP
            q = qs[h, here, :]
            near = jnp.where(causal, nt_dot(q, ks[g, here, :]) * scale, masked_score)
            top = jnp.max(near, axis=1, keepdims=True)
            if s > 0:
                far = nt_dot(q, ks[g, : s * span, :]) * scale
                top = jnp.maximum(top, jnp.max(far, axis=1, keepdims=True))
            near = jnp.exp(near - top)
            total = jnp.sum(near, axis=1, keepdims=True)
            if s > 0:
                far = jnp.exp(far - top)
                total = total + jnp.sum(far, axis=1, keepdims=True)
            inverse = 1.0 / total
            result = nn_dot((near * inverse).astype(BF16), vs[g, here, :])
            if s > 0:
                result = result + nn_dot((far * inverse).astype(BF16), vs[g, : s * span, :])
            stats = jnp.where(lane == h, top + jnp.log(total), stats)
            out[s, :, h * HEAD_DIM : (h + 1) * HEAD_DIM] = result.astype(BF16)
        logs[here, :] = stats


def fill_tables(cosines, sines, narrow_cosines, narrow_sines, heads):
    end = heads * HEAD_DIM
    cosines[:, end:] = jnp.ones((cosines.shape[0], cosines.shape[1] - end), F32)
    sines[:, end:] = jnp.zeros((cosines.shape[0], cosines.shape[1] - end), F32)
    for h in range(heads):
        at = slice(h * HEAD_DIM, (h + 1) * HEAD_DIM)
        cosines[:, at] = narrow_cosines
        sines[:, at] = narrow_sines


def fore_kernel(
    mesh, count, kv,
    tokens, cotangent, gain_one, gain_two, wq, wk, wv, wo, wg, wd, narrow_cosines, narrow_sines,
    w_qkv, w_out, w_gate, w_down, first_out, packed, heads_attended, logs, attended_out, hidden_out, second_both, low_both, gains_out,
    rows_in, hidden, first, pack, w_land, wo_land, q_send, q_land, a_send, a_land, stage_gate, gain_send, gain_land,
    qs, ks, vs, log, attended, second, second_abs, low, cosines, sines, send_sems, recv_sems, local_sems,
):
    links = Links(mesh, send_sems, recv_sems, local_sems)
    ns, na, nf = links.ns, links.na, links.nf
    chips = 2 * na
    z, f, core = links.z, links.f, links.core
    rows, width = rows_in.shape
    span = rows // count
    heads = kv * GROUP
    g_width, k_width = heads * HEAD_DIM, kv * HEAD_DIM
    q_width = g_width + 2 * k_width
    local = width // nf
    links.barrier()

    token_load = links.local(tokens, rows_in)
    token_load.start()
    gain_send[...] = jnp.zeros_like(gain_send)
    gain_send[0:1, :local] = gain_one[...].astype(F32)
    gain_send[1:2, :local] = gain_two[...].astype(F32)
    for j in range(ns):
        pack[j, :, :g_width] = wq[:, j * g_width : (j + 1) * g_width]
        pack[j, :, g_width : g_width + k_width] = wk[:, j * k_width : (j + 1) * k_width]
        pack[j, :, g_width + k_width :] = wv[:, j * k_width : (j + 1) * k_width]

    every = slice(None)

    def piece(start, size, half):
        if half is None:
            return rows_at(start, size)
        return rows_at(start * 2 + half, size // 2)

    units = []
    turns = [*range(1, ns), 0]
    for d in turns:
        g = lax.rem(z + d, ns)
        units.append(Gather(links, (pack, g), lambda o, half, g=g: (w_land, g, piece(o, local, half)), True))
    units.append(Gather(links, wo, lambda o, half: (wo_land, piece(o, local, half)), True))
    depth = wd.shape[0]
    units.append(Gather(links, wd, lambda o, half: (w_down, piece(o // 2, depth, half)), False))
    gate_unit = GatherHalf(links, lambda c: (stage_gate, c), lambda o: (w_gate, every, rows_at(o, local)))
    q_copies, a_copies = [], []
    for d in range(1, ns):
        g = lax.rem(z + d, ns)
        q_copies.append([links.copy((q_send, g, i), (q_land, i, z), links.at_z(d)) for i in range(count)])
    for i in range(count):
        a_copies.append([links.copy((a_send, i, lax.rem(z + d, ns)), (a_land, i, z), links.at_z(d)) for d in range(1, ns)])
    second_copy = links.copy(second_abs, (second_both, pl.ds(rows, rows)), links.at_core())
    low_copy = links.copy(low, (low_both, pl.ds(rows, rows)), links.at_core())

    def gain_at(start, size):
        return (gain_land, pl.ds(start, size))

    pair, chip_four = f // 2 * 2, f // 4 * 4
    gain_copies = [
        [links.copy(gain_at(f, 1), gain_at(f, 1), links.at_core())],
        [links.copy(gain_at(pair, 2), gain_at(pair, 2), links.at_b())],
        [links.copy(gain_at(chip_four, 4), gain_at(chip_four, 4), links.at_a(d)) for d in range(1, na)],
    ]
    stores = []

    def store(src, dst):
        copies = links.local(src, dst)
        copies.start()
        stores.append(copies)

    gain_land[f] = gain_send[...]
    for copies in gain_copies[0]:
        copies.start()
    units[0].start()
    units[1].start()
    for j in range(ns):
        w_land[j, rows_at(f, local), :] = pack[j]
    stage_loads = []
    tile = w_gate.shape[2]
    for c in range(2):
        for k in range(chips - 1):
            source = (wg, every, slice((k * 2 + c) * tile, (k * 2 + c + 1) * tile))
            stage_loads.append(links.local(source, (stage_gate, c, k)))
    for load in stage_loads:
        load.start()
    store_own = [links.local(wo, (wo_land, rows_at(f, local))), links.local(wd, (w_down, rows_at(f // 2, depth)))]
    for copies in store_own:
        copies.start()
    fill_tables(cosines, sines, narrow_cosines[rows_at(z, span), :], narrow_sines[rows_at(z, span), :], heads + kv)
    token_load.wait()
    old = rows_in[...]
    inverse = lax.rsqrt(jnp.mean(old * old, axis=1, keepdims=True) + norm_eps)
    for stage in range(3):
        for copies in gain_copies[stage]:
            copies.wait()
        if stage < 2:
            for copies in gain_copies[stage + 1]:
                copies.start()
    for j in range(nf):
        gains_out[:, j * local : (j + 1) * local] = gain_land[j, 0:2, :local]
    first[...] = (old * inverse * gains_out[0:1, :]).astype(BF16)
    store(first, first_out)

    def project(n):
        g = lax.rem(z + turns[n], ns)
        units[n].finish()
        y = nn_dot(first[...], w_land[g])
        for i in range(count):
            part = y[i * span : (i + 1) * span]
            part = (part * cosines[...] + swap_halves(part) * sines[...]).astype(BF16)
            if turns[n] == 0:
                q_land[i, z] = part
            else:
                q_send[g, i] = part
                q_copies[turns[n] - 1][i].start()
        store((w_land, g), (w_qkv, g))

    last = len(units)
    for n in range(ns):
        units[n].turn()
        if n + 2 < last:
            units[n + 2].start()
        if n > 0:
            units[n - 1].pass_on()
        if n > 1:
            project(n - 2)
    units[ns].turn()
    for load in stage_loads:
        load.wait()
    gate_unit.start()
    units[ns - 1].pass_on()
    project(ns - 2)
    gate_unit.other_start()
    project(ns - 1)
    units[ns].pass_on()

    def attend(i):
        for copies in q_copies:
            copies[i].wait()
        for j in range(ns):
            at = slice(j * span, (j + 1) * span)
            for h in range(heads):
                qs[h, at, :] = q_land[i, j, :, h * HEAD_DIM : (h + 1) * HEAD_DIM]
            for h in range(kv):
                k0, v0 = (heads + h) * HEAD_DIM, (heads + kv + h) * HEAD_DIM
                ks[h, at, :] = q_land[i, j, :, k0 : k0 + HEAD_DIM]
                vs[h, at, :] = q_land[i, j, :, v0 : v0 + HEAD_DIM]
        attend_heads(ns, kv, span, qs, ks, vs, a_send.at[i], log.at[i])
        for copies in a_copies[i]:
            copies.start()
        a_land[i, z] = a_send[i, z]

    for i in range(count):
        attend(i)
        if i == 0:
            units[ns + 1].turn()
            units[ns].finish()
            store_own[0].wait()
            store(wo_land, w_out)
    store(q_land, packed)
    store(a_send, heads_attended)
    store(log, logs)
    for i in range(count):
        for copies in a_copies[i]:
            copies.wait()
        for j in range(ns):
            attended[i * span : (i + 1) * span, j * g_width : (j + 1) * g_width] = a_land[i, j]
    new = rows_in[...] + nn_dot(attended[...], wo_land[...])
    hidden[...] = new
    inverse = lax.rsqrt(jnp.mean(new * new, axis=1, keepdims=True) + norm_eps)
    second_abs[...] = (new * inverse * gains_out[1:2, :]).astype(BF16)
    second_copy.start()
    store(second_abs, (second_both, pl.ds(0, rows)))
    store(attended, attended_out)
    store(hidden, hidden_out)
    units[ns + 1].pass_on()
    cot_load = links.local(cotangent, rows_in)
    cot_load.start()
    gate_unit.turn()
    cot_load.wait()
    low[...] = rows_in[...].astype(BF16)
    low_copy.start()
    store(low, (low_both, pl.ds(0, rows)))
    gate_unit.turn_late()
    gate_unit.finish()
    second_copy.wait()
    low_copy.wait()
    store_own[1].wait()
    for copies in stores:
        copies.wait()


def fore(mesh, count, kv, tokens, cotangent, gain_one, gain_two, wq, wk, wv, wo, wg, wd, narrow_cosines, narrow_sines):
    ns, nf = mesh
    na = nf // 4
    chips = 2 * na
    rows, width = tokens.shape
    span = rows // count
    length = ns * span
    heads = kv * GROUP
    g_width = heads * HEAD_DIM
    q_width = g_width + 2 * kv * HEAD_DIM
    local, depth = wq.shape[0], wd.shape[0]
    tile = wg.shape[1] // (2 * chips)
    anywhere, vmem = pl.BlockSpec(memory_space=pl.ANY), pl.BlockSpec(memory_space=pltpu.VMEM)
    low = lambda *shape: jax.ShapeDtypeStruct(shape, BF16)
    wide = lambda *shape: jax.ShapeDtypeStruct(shape, F32)
    outs = [
        low(ns, width, q_width),
        low(width, width),
        low(chips - 1, width, tile),
        low(chips * depth, width),
        low(rows, width),
        low(count, ns, span, q_width),
        low(count, ns, span, g_width),
        wide(count, length, 128),
        low(rows, width),
        wide(rows, width),
        low(2 * rows, width),
        low(2 * rows, width),
        wide(2, width),
    ]
    scratch = [
        pltpu.VMEM((rows, width), F32),
        pltpu.VMEM((rows, width), F32),
        pltpu.VMEM((rows, width), BF16),
        pltpu.VMEM((ns, local, q_width), BF16),
        pltpu.VMEM((ns, width, q_width), BF16),
        pltpu.VMEM((width, width), BF16),
        pltpu.VMEM((ns, count, span, q_width), BF16),
        pltpu.VMEM((count, ns, span, q_width), BF16),
        pltpu.VMEM((count, ns, span, g_width), BF16),
        pltpu.VMEM((count, ns, span, g_width), BF16),
        pltpu.VMEM((2, chips - 1, local, tile), BF16),
        pltpu.VMEM((8, 256), F32),
        pltpu.VMEM((nf, 8, 256), F32),
        pltpu.VMEM((heads, length, HEAD_DIM), BF16),
        pltpu.VMEM((kv, length, HEAD_DIM), BF16),
        pltpu.VMEM((kv, length, HEAD_DIM), BF16),
        pltpu.VMEM((count, length, 128), F32),
        pltpu.VMEM((rows, width), BF16),
        pltpu.VMEM((8, 128), BF16),
        pltpu.VMEM((rows, width), BF16),
        pltpu.VMEM((rows, width), BF16),
        pltpu.VMEM((span, q_width), F32),
        pltpu.VMEM((span, q_width), F32),
    ]
    return pl.pallas_call(
        functools.partial(fore_kernel, mesh, count, kv),
        in_specs=[anywhere] * 2 + [vmem] * 5 + [anywhere] * 3 + [vmem] * 2,
        out_specs=[anywhere] * 12 + [vmem],
        out_shape=outs,
        scratch_shapes=scratch
        + [pltpu.SemaphoreType.DMA((160,)), pltpu.SemaphoreType.DMA((160,)), pltpu.SemaphoreType.DMA((64,))],
        compiler_params=pltpu.CompilerParams(vmem_limit_bytes=VMEM_MOST, collective_id=0, has_side_effects=True),
        name="fore",
    )(tokens, cotangent, gain_one, gain_two, wq, wk, wv, wo, wg, wd, narrow_cosines, narrow_sines)


def attend_back_heads(ns, kv, span, qs, ks, vs, gs, attended, logs, dk, dv, result):
    scale = 1.0 / math.sqrt(HEAD_DIM)
    heads = kv * GROUP
    row = lax.broadcasted_iota(jnp.int32, (span, span), 0)
    column = lax.broadcasted_iota(jnp.int32, (span, span), 1)
    causal = row >= column
    dk[...] = jnp.zeros_like(dk)
    dv[...] = jnp.zeros_like(dv)
    for s in range(ns):
        here = slice(s * span, (s + 1) * span)
        for h in range(heads):
            g = h // GROUP
            q, grad = qs[h, here, :], gs[h, here, :]
            log_total = logs[here, h : h + 1]
            out = attended[s, :, h * HEAD_DIM : (h + 1) * HEAD_DIM]
            delta = jnp.sum(grad.astype(F32) * out.astype(F32), axis=1, keepdims=True)
            k, v = ks[g, here, :], vs[g, here, :]
            near = jnp.where(causal, jnp.exp(nt_dot(q, k) * scale - log_total), 0.0)
            slope = (near * (nt_dot(grad, v) - delta) * scale).astype(BF16)
            dq = nn_dot(slope, k)
            dk[g, here, :] += tn_dot(slope, q)
            dv[g, here, :] += tn_dot(near.astype(BF16), grad)
            if s > 0:
                before = slice(0, s * span)
                k, v = ks[g, before, :], vs[g, before, :]
                far = jnp.exp(nt_dot(q, k) * scale - log_total)
                slope = (far * (nt_dot(grad, v) - delta) * scale).astype(BF16)
                dq = dq + nn_dot(slope, k)
                dk[g, before, :] += tn_dot(slope, q)
                dv[g, before, :] += tn_dot(far.astype(BF16), grad)
            result[here, h * HEAD_DIM : (h + 1) * HEAD_DIM] = dq
    for g in range(kv):
        k0 = (heads + g) * HEAD_DIM
        v0 = (heads + kv + g) * HEAD_DIM
        result[:, k0 : k0 + HEAD_DIM] = dk[g]
        result[:, v0 : v0 + HEAD_DIM] = dv[g]


def back_kernel(
    mesh, count, kv,
    dx_own, dx_other, hidden, cotangent, gain_two, w_out, w_qkv, packed, attended, logs, cosines, sines, tokens, gain_one, dwg, dwu,
    high, low_out, out, gain_grads, dqkv, sum_gate, sum_up,
    low, sum_rows, dx_land, g_send, g_land, q_send, q_land, swap_send, swap_land, *rest,
):
    parts, (send_sems, recv_sems, local_sems) = rest[:-3], rest[-3:]
    links = Links(mesh, send_sems, recv_sems, local_sems)
    ns, na = links.ns, links.na
    chips = 2 * na
    z, core = links.z, links.core
    rows, width = hidden.shape
    span = rows // count
    length = ns * span
    heads = kv * GROUP
    g_width, q_width = heads * HEAD_DIM, (heads + 2 * kv) * HEAD_DIM
    half = dwg.shape[1]
    block = width // chips
    links.barrier()

    dx_copy = links.copy(dx_other, dx_land, links.at_core())
    dx_copy.start()
    sums = []
    for n, source in enumerate((dwg, dwu)):
        for b_first in (True, False):
            columns = slice(0, half // 2) if b_first else slice(half // 2, half)
            at = (n * 2 + (0 if b_first else 1)) * 3
            partial = lambda k, source=source, columns=columns: (source, rows_at(k, block), columns)
            sums.append(ChipSum(links, partial, b_first, *parts[at : at + 3]))
    for item in sums:
        item.start()
        item.load()

    g_copies, q_copies = [], []
    for i in range(count):
        g_copies.append([links.copy((g_send, i, lax.rem(z + d, ns)), (g_land, i, z), links.at_z(d)) for d in range(1, ns)])
        q_copies.append([links.copy((q_send, i, lax.rem(z + d, ns)), (q_land, z, i), links.at_z(d)) for d in range(1, ns)])

    def out_back(dx, old, grad, w):
        loads = [links.local(dx_own, dx), links.local(hidden, old), links.local(cotangent, grad), links.local(w_out, w)]
        for load in loads:
            load.start()
        dx_copy.wait()
        for load in loads[:3]:
            load.wait()
        step = dx[...] + dx_land[...].astype(F32)
        inverse = lax.rsqrt(jnp.mean(old[...] * old[...], axis=1, keepdims=True) + norm_eps)
        normed = old[...] * inverse
        gain_grads[1:2, :] = jnp.sum(step * normed, axis=0, keepdims=True)
        grad[...] = grad[...] + norm_back(step, normed, inverse, gain_two[...])
        low[...] = grad[...].astype(BF16)
        stores = [links.local(grad, high), links.local(low, low_out)]
        for store in stores:
            store.start()
        loads[3].wait()
        for i in range(count):
            here = slice(i * span, (i + 1) * span)
            part = nt_dot(low[here, :], w[...]).astype(BF16)
            for j in range(ns):
                g_send[i, j] = part[:, j * g_width : (j + 1) * g_width]
            for copies in g_copies[i]:
                copies.start()
            g_land[i, z] = g_send[i, z]
        for store in stores:
            store.wait()

    pl.run_scoped(
        out_back,
        pltpu.VMEM((rows, width), F32),
        pltpu.VMEM((rows, width), F32),
        pltpu.VMEM((rows, width), F32),
        pltpu.VMEM((width, width), BF16),
    )

    def attention(qkv, mid, log, qs, ks, vs, gs, dk, dv, result, cosine, sine):
        fill_tables(cosine, sine, cosines[...], sines[...], heads + kv)
        for i in range(count):
            loads = [links.local((packed, i), qkv), links.local((attended, i), mid), links.local((logs, i), log)]
            for load in loads:
                load.start()
            for load in loads:
                load.wait()
            for j in range(ns):
                at = slice(j * span, (j + 1) * span)
                for h in range(heads):
                    qs[h, at, :] = qkv[j, :, h * HEAD_DIM : (h + 1) * HEAD_DIM]
                for h in range(kv):
                    k0, v0 = (heads + h) * HEAD_DIM, (heads + kv + h) * HEAD_DIM
                    ks[h, at, :] = qkv[j, :, k0 : k0 + HEAD_DIM]
                    vs[h, at, :] = qkv[j, :, v0 : v0 + HEAD_DIM]
            for copies in g_copies[i]:
                copies.wait()
            for j in range(ns):
                for h in range(heads):
                    gs[h, j * span : (j + 1) * span, :] = g_land[i, j, :, h * HEAD_DIM : (h + 1) * HEAD_DIM]
            attend_back_heads(ns, kv, span, qs, ks, vs, gs, mid, log, dk, dv, result)
            for j in range(ns):
                here = slice(j * span, (j + 1) * span)
                part = result[here, :]
                q_send[i, j] = (part * cosine[here, :] - swap_halves(part) * sine[here, :]).astype(BF16)
            for copies in q_copies[i]:
                copies.start()
            q_land[z, i] = q_send[i, z]
            if i < len(sums) // 2:
                for item in sums[2 * i : 2 * i + 2]:
                    item.turn()

    pl.run_scoped(
        attention,
        pltpu.VMEM((ns, span, q_width), BF16),
        pltpu.VMEM((ns, span, g_width), BF16),
        pltpu.VMEM((length, 128), F32),
        pltpu.VMEM((heads, length, HEAD_DIM), BF16),
        pltpu.VMEM((kv, length, HEAD_DIM), BF16),
        pltpu.VMEM((kv, length, HEAD_DIM), BF16),
        pltpu.VMEM((heads, length, HEAD_DIM), BF16),
        pltpu.VMEM((kv, length, HEAD_DIM), F32),
        pltpu.VMEM((kv, length, HEAD_DIM), F32),
        pltpu.VMEM((length, q_width), F32),
        pltpu.VMEM((length, q_width), F32),
        pltpu.VMEM((length, q_width), F32),
    )

    swaps = []
    local = block // 2
    for item in sums[2 * count :]:
        item.turn()

    def swap(n):
        for m in range(2):
            total = sums[2 * n + m].finish()
            swap_send[n, m, 0] = total[:local]
            swap_send[n, m, 1] = total[local:]
        for m in range(2):
            copies = links.copy((swap_send, n, m, 1 - core), (swap_land, n, m), links.at_core())
            copies.start()
            swaps.append(copies)

    tile = half // chips
    stores = []

    def combine(n, total):
        for m in range(2):
            swaps[2 * n + m].wait()
            kept, arrived = swap_send[n, m, core], swap_land[n, m]
            for t in range(chips // 2):
                here = slice(t * tile, (t + 1) * tile)
                k = m * (chips // 2) + t
                one, two = kept[:, here], arrived[:, here]
                sum_rows[n, :, 2 * k * tile : (2 * k + 1) * tile] = jnp.where(core == 0, one, two)
                sum_rows[n, :, (2 * k + 1) * tile : (2 * k + 2) * tile] = jnp.where(core == 0, two, one)
        copies = links.local((sum_rows, n), total)
        copies.start()
        stores.append(copies)

    def project_back(w, old, base, grad):
        loads = [links.local(tokens, old), links.local(high, base), links.local(w_qkv, w)]
        for load in loads:
            load.start()
        swap(0)
        for load in loads:
            load.wait()
        for i in range(count):
            here = slice(i * span, (i + 1) * span)
            if i == count - 1:
                combine(0, sum_gate)
                swap(1)
                combine(1, sum_up)
            for copies in q_copies[i]:
                copies.wait()
            total = nt_dot(q_land[0, i], w[0])
            for j in range(1, ns):
                total = total + nt_dot(q_land[j, i], w[j])
            grad[here, :] = total
            copies = links.local((q_land, slice(None), i), (dqkv, slice(None), i))
            copies.start()
            stores.append(copies)
            step, rows_old = grad[here, :], old[here, :]
            inverse = lax.rsqrt(jnp.mean(rows_old * rows_old, axis=1, keepdims=True) + norm_eps)
            normed = rows_old * inverse
            part_sum = jnp.sum(step * normed, axis=0, keepdims=True)
            gain_grads[0:1, :] = part_sum if i == 0 else gain_grads[0:1, :] + part_sum
            base[here, :] = base[here, :] + norm_back(step, normed, inverse, gain_one[...])
            copies = links.local((base, here), (out, here))
            copies.start()
            stores.append(copies)
        for copies in stores:
            copies.wait()

    pl.run_scoped(
        project_back,
        pltpu.VMEM((ns, width, q_width), BF16),
        pltpu.VMEM((rows, width), F32),
        pltpu.VMEM((rows, width), F32),
        pltpu.VMEM((rows, width), F32),
    )


def back(mesh, count, kv, dx_own, dx_other, hidden, cotangent, gain_two, w_out, w_qkv, packed, attended, logs, cosines, sines, tokens, gain_one, dwg, dwu):
    ns, nf = mesh
    na = nf // 4
    rows, width = hidden.shape
    span = rows // count
    heads = kv * GROUP
    g_width, q_width = heads * HEAD_DIM, (heads + 2 * kv) * HEAD_DIM
    half = dwg.shape[1]
    block = width // (2 * na)
    local = block // 2
    anywhere = pl.BlockSpec(memory_space=pl.ANY)
    vmem = pl.BlockSpec(memory_space=pltpu.VMEM)
    operands = [dx_own, dx_other, hidden, cotangent, gain_two, w_out, w_qkv, packed, attended, logs, cosines, sines, tokens, gain_one, dwg, dwu]
    wide = jax.ShapeDtypeStruct((rows, width), F32)
    summed = jax.ShapeDtypeStruct((local, 2 * half), BF16)
    scratch = [
        pltpu.VMEM((rows, width), BF16),
        pltpu.VMEM((2, local, 2 * half), BF16),
        pltpu.VMEM((rows, width), BF16),
        pltpu.VMEM((count, ns, span, g_width), BF16),
        pltpu.VMEM((count, ns, span, g_width), BF16),
        pltpu.VMEM((count, ns, span, q_width), BF16),
        pltpu.VMEM((ns, count, span, q_width), BF16),
        pltpu.VMEM((2, 2, 2, local, half // 2), BF16),
        pltpu.VMEM((2, 2, local, half // 2), BF16),
    ]
    for _ in range(2):
        for b_first in (True, False):
            scratch += chip_sum_shapes(na, b_first, block, half // 2)
    return pl.pallas_call(
        functools.partial(back_kernel, mesh, count, kv),
        in_specs=[vmem if x.shape[0] == 1 or x.shape[1] == HEAD_DIM else anywhere for x in operands],
        out_specs=[anywhere, anywhere, anywhere, vmem, anywhere, anywhere, anywhere],
        out_shape=[
            wide,
            jax.ShapeDtypeStruct((rows, width), BF16),
            wide,
            jax.ShapeDtypeStruct((2, width), F32),
            jax.ShapeDtypeStruct((ns, count, span, q_width), BF16),
            summed,
            summed,
        ],
        scratch_shapes=scratch
        + [pltpu.SemaphoreType.DMA((64,)), pltpu.SemaphoreType.DMA((64,)), pltpu.SemaphoreType.DMA((64,))],
        compiler_params=pltpu.CompilerParams(vmem_limit_bytes=VMEM_MOST, collective_id=1, has_side_effects=True),
        name="back",
    )(*operands)


class LineSum:
    def __init__(self, links, term, first, second, total):
        self.links, self.term, self.first, self.second, self.total = links, term, first, second, total
        z, ns = links.z, links.ns
        self.dtype = (term[0] if isinstance(term, tuple) else term).dtype
        middle = ns // 2
        self.deep = middle > 1
        lower = z < middle
        step = jnp.where(lower, 1, -1)
        self.end = (z == 0) | (z == ns - 1)
        self.inner = (z == middle - 1) | (z == middle)
        inward, outward = (z + step, links.f), (z - step, links.f)
        self.inward = links.copy(term, first, inward) if self.deep else None
        self.onward = links.again(first, first, inward) if self.deep else None
        self.across = links.copy(first if self.deep else term, second, inward)
        self.outward = links.copy(total, total, outward) if self.deep else None

    def add(self, target, one, two):
        put(target, (get(one).astype(F32) + get(two).astype(F32)).astype(self.dtype))

    def begin(self):
        if self.deep:
            pl.when(self.end)(self.inward.start)
        else:
            self.across.start()

    def relay(self):
        if not self.deep:
            return

        @pl.when(jnp.logical_not(self.end))
        def _():
            self.inward.wait_recv()
            self.add(self.first, self.term, self.first)
            pl.when(self.inner)(self.across.start)
            pl.when(jnp.logical_not(self.inner))(self.onward.start)

    def settle(self):
        @pl.when(self.inner)
        def _():
            self.across.wait()
            self.add(self.total, self.first if self.deep else self.term, self.second)
            if self.deep:
                self.outward.start()

        if self.deep:

            @pl.when(jnp.logical_not(self.inner | self.end))
            def _():
                self.outward.wait_recv()
                self.outward.start()

    def finish(self):
        if not self.deep:
            return
        pl.when(self.end)(self.outward.wait_recv)
        pl.when(jnp.logical_not(self.inner))(self.inward.wait_send)
        pl.when(jnp.logical_not(self.end))(self.outward.wait_send)


def finish_kernel(
    mesh, count, kv,
    term_gate, term_up, dwd, first, dqkv, attended, low, gains,
    out_gate, out_up, out_down, out_out, out_qkv, out_gains,
    term_down, term_out, term_qkv, in_gate, in_up, in_down, in_out, in_qkv,
    first_both, attended_both, low_both, dq_both, w_out_part, w_qkv_part,
    swap_out, land_out, swap_qkv, land_qkv, gain_terms, gain_lands, *rest,
):
    parts, (send_sems, recv_sems, local_sems) = rest[:-3], rest[-3:]
    links = Links(mesh, send_sems, recv_sems, local_sems)
    ns, na = links.ns, links.na
    chips, per = 2 * na, ns // 2
    core = links.core
    rows, width = first.shape
    q_width = dqkv.shape[3]
    middle = width // 2
    links.barrier()

    def lines(term, inbox, out, pieces):
        size = term.shape[1] // pieces
        every = slice(None)
        made = []
        for i in range(pieces):
            at = slice(i * size, (i + 1) * size)
            made.append(LineSum(links, (term, every, at), (inbox, 0, every, at), (inbox, 1, every, at), (out, every, at)))
        return made

    gate_lines = lines(term_gate, in_gate, out_gate, 4)
    up_lines = lines(term_up, in_up, out_up, 4)
    down_lines = lines(term_down, in_down, out_down, 4)
    out_lines = lines(term_out, in_out, out_out, 2)
    qkv_lines = lines(term_qkv, in_qkv, out_qkv, 4)
    for line in gate_lines + up_lines:
        line.begin()

    sends = [
        links.copy((dqkv, pl.ds((1 - core) * per, per)), (dq_both, 1), links.at_core()),
        links.copy((low, slice(None), rows_at(1 - core, middle)), (low_both, 1), links.at_core()),
        links.copy(first, (first_both, 1), links.at_core()),
        links.copy(attended, (attended_both, 1), links.at_core()),
    ]
    loads = [
        links.local((low, slice(None), rows_at(core, middle)), (low_both, 0)),
        links.local(attended, (attended_both, 0)),
        links.local(first, (first_both, 0)),
        links.local((dqkv, pl.ds(core * per, per)), (dq_both, 0)),
    ]
    for copies in loads + sends[1:2] + sends[3:4] + sends[2:3] + sends[:1]:
        copies.start()

    down_rows = dwd.shape[0] // chips
    block = width // chips

    def pair(source, row_count, at, staged):
        made = []
        cut = source.shape[1] // 2
        for n, b_first in enumerate((True, False)):
            columns = slice(0, cut) if b_first else slice(cut, 2 * cut)
            partial = lambda k, columns=columns: (source, rows_at(k, row_count), columns)
            refs = parts[at[n] : at[n + 1]]
            made.append(ChipSum(links, partial, b_first, *(refs if staged else (*refs[:2], None))))
        return made

    down = pair(dwd, down_rows, (0, 3, 6), True)
    for item in down:
        item.start()
        item.load()

    gain_copies = [links.copy((gain_terms, 0), (gain_lands, 0), links.at_core()), links.copy((gain_terms, 1), (gain_lands, 1), links.at_b())]
    gain_copies += [links.copy((gain_terms, 2), (gain_lands, 1 + d), links.at_a(d)) for d in range(1, na)]
    gain_line = LineSum(links, (gain_terms, 3), (gain_lands, na + 1), (gain_lands, na + 2), out_gains)
    gain_terms[0] = gains[...]
    gain_copies[0].start()

    def next_gain(i):
        for copies in gain_copies[i : i + 1] if i < 2 else gain_copies[2:]:
            copies.wait()
        if i < 2:
            gain_terms[i + 1] = gain_terms[i] + gain_lands[i]
            for copies in gain_copies[1:2] if i == 0 else gain_copies[2:]:
                copies.start()
        else:
            total = gain_terms[2]
            for d in range(1, na):
                total = total + gain_lands[1 + d]
            gain_terms[3] = total
            gain_line.begin()

    def qkv_part(p):
        columns = slice(p * q_width, (p + 1) * q_width)
        mine, other = dq_both[0, p].reshape(rows, q_width), dq_both[1, p].reshape(rows, q_width)
        for k in range(chips):
            at = slice(k * block, (k + 1) * block)
            total = tn_dot(first_both[0, :, at], mine) + tn_dot(first_both[1, :, at], other)
            w_qkv_part[at, columns] = total.astype(BF16)

    def swap(sums, send, land):
        local = block // 2
        for n, item in enumerate(sums):
            total = item.finish()
            size = total.shape[1]
            send[0, :, n * size : (n + 1) * size] = total[:local]
            send[1, :, n * size : (n + 1) * size] = total[local:]
        copies = links.copy((send, 1 - core), land, links.at_core())
        copies.start()
        return copies

    out_sums = pair(w_out_part, block, (6, 8, 10), False)
    qkv_sums = pair(w_qkv_part, block, (10, 12, 14), False)
    cut = width // 2
    next_gain(0)
    for i in (1, 3):
        sends[i].wait()
    for i in (0, 1):
        loads[i].wait()
    gate_lines[0].relay()
    for k in range(chips):
        at = slice(k * block, (k + 1) * block)
        total = tn_dot(attended_both[0, :, at], low_both[0]) + tn_dot(attended_both[1, :, at], low_both[1])
        w_out_part[at, :] = total.astype(BF16)
    for item in out_sums:
        item.start()
    gate_lines[1].relay()
    next_gain(1)
    for i in (0, 2):
        sends[i].wait()
    for i in (2, 3):
        loads[i].wait()
    gate_lines[0].settle()
    for p in range(per // 2):
        qkv_part(p)
    gate_lines[2].relay()
    next_gain(2)
    gate_lines[1].settle()
    for p in range(per // 2, per):
        qkv_part(p)
    gate_lines[3].relay()
    for item in down:
        item.turn()
    for item in qkv_sums:
        item.start()
    gate_lines[2].settle()
    gain_line.relay()
    gate_lines[3].settle()
    for item in out_sums:
        item.turn()
    up_lines[0].relay()
    gain_line.settle()
    up_lines[1].relay()
    up_lines[0].settle()
    term_down[:, :cut] = down[0].finish()
    term_down[:, cut:] = down[1].finish()
    for line in down_lines:
        line.begin()
    up_lines[2].relay()
    up_lines[1].settle()
    up_lines[3].relay()
    up_lines[2].settle()
    down_lines[0].relay()
    up_lines[3].settle()
    for item in qkv_sums:
        item.turn()
    down_lines[1].relay()
    down_lines[0].settle()
    out_swap = swap(out_sums, swap_out, land_out)
    down_lines[2].relay()
    down_lines[1].settle()
    out_swap.wait()
    kept, arrived = swap_out[core], land_out[...]
    term_out[:, :cut] = jnp.where(core == 0, kept, arrived)
    term_out[:, cut:] = jnp.where(core == 0, arrived, kept)
    for line in out_lines:
        line.begin()
    down_lines[3].relay()
    down_lines[2].settle()
    qkv_swap = swap(qkv_sums, swap_qkv, land_qkv)
    out_lines[0].relay()
    down_lines[3].settle()
    qkv_swap.wait()
    kept, arrived = swap_qkv[core], land_qkv[...]
    for n in range(2):
        group = jnp.where(core == n, kept, arrived)
        for p in range(per):
            taken, start = p * q_width, 0
            for size in (kv * GROUP * HEAD_DIM, kv * HEAD_DIM, kv * HEAD_DIM):
                at = start + (n * per + p) * size
                term_qkv[:, at : at + size] = group[:, taken : taken + size]
                taken, start = taken + size, start + ns * size
    for line in qkv_lines:
        line.begin()
    out_lines[1].relay()
    out_lines[0].settle()
    qkv_lines[0].relay()
    out_lines[1].settle()
    for n in range(1, len(qkv_lines)):
        qkv_lines[n].relay()
        qkv_lines[n - 1].settle()
    qkv_lines[-1].settle()
    for line in [*gate_lines, *up_lines, gain_line, *down_lines, *out_lines, *qkv_lines]:
        line.finish()


def finish(mesh, count, kv, term_gate, term_up, dwd, first, dqkv, attended, low, gains):
    ns, nf = mesh
    na, per = nf // 4, ns // 2
    rows, width = first.shape
    q_width = dqkv.shape[3]
    local, half = term_gate.shape[0], width // 2
    block = 2 * local
    anywhere, vmem = pl.BlockSpec(memory_space=pl.ANY), pl.BlockSpec(memory_space=pltpu.VMEM)
    down = (dwd.shape[0] // (2 * na), dwd.shape[1])
    shapes = [term_gate.shape, term_up.shape, down, (local, width), (local, ns * q_width)]
    scratch = [pltpu.VMEM(s, BF16) for s in shapes[2:]]
    scratch += [pltpu.VMEM((2,) + tuple(s), BF16) for s in shapes]
    scratch += [
        pltpu.VMEM((2, rows, width), BF16),
        pltpu.VMEM((2, rows, width), BF16),
        pltpu.VMEM((2, rows, half), BF16),
        pltpu.VMEM((2, per, count, rows // count, q_width), BF16),
        pltpu.VMEM((width, half), BF16),
        pltpu.VMEM((width, per * q_width), BF16),
        pltpu.VMEM((2, local, half), BF16),
        pltpu.VMEM((local, half), BF16),
        pltpu.VMEM((2, local, per * q_width), BF16),
        pltpu.VMEM((local, per * q_width), BF16),
        pltpu.VMEM((4, 2, width), F32),
        pltpu.VMEM((na + 3, 2, width), F32),
    ]
    scratch += chip_sum_shapes(na, True, down[0], down[1] // 2) + chip_sum_shapes(na, False, down[0], down[1] // 2)
    for columns in (half // 2, per * q_width // 2):
        for b_first in (True, False):
            scratch += chip_sum_shapes(na, b_first, block, columns)[:2]
    return pl.pallas_call(
        functools.partial(finish_kernel, mesh, count, kv),
        in_specs=[vmem, vmem] + [anywhere] * 5 + [vmem],
        out_specs=[vmem] * 6,
        out_shape=[jax.ShapeDtypeStruct(s, BF16) for s in shapes] + [jax.ShapeDtypeStruct((2, width), F32)],
        scratch_shapes=scratch
        + [pltpu.SemaphoreType.DMA((128,)), pltpu.SemaphoreType.DMA((128,)), pltpu.SemaphoreType.DMA((64,))],
        compiler_params=pltpu.CompilerParams(vmem_limit_bytes=VMEM_MOST, collective_id=2, has_side_effects=True),
        name="finish",
    )(term_gate, term_up, dwd, first, dqkv, attended, low, gains)


def widen_kernel(cuts, *refs):
    gate, up, down, out, qkv, hidden, own, other = refs[:8]
    o_gate, o_up, o_down, o_out, o_q, o_k, o_v, o_block = refs[8:]
    for source, target in ((gate, o_gate), (up, o_up), (down, o_down), (out, o_out)):
        target[...] = source[...].astype(F32)
    for (start, end), target in zip(cuts, (o_q, o_k, o_v)):
        target[...] = qkv[:, start:end].astype(F32)
    o_block[...] = hidden[...] + own[...] + other[...].astype(F32)


def widen(gate, up, down, out, qkv, hidden, own, other, cuts):
    steps = 4
    operands = [gate, up, down, out, qkv, hidden, own, other]
    rows = out.shape[0]
    shapes = [gate.shape, up.shape, down.shape, out.shape] + [(rows, end - start) for start, end in cuts] + [hidden.shape]
    block = lambda shape: pl.BlockSpec((shape[0] // steps, shape[1]), lambda i: (i, 0))
    return pl.pallas_call(
        functools.partial(widen_kernel, cuts),
        grid=(steps,),
        in_specs=[block(x.shape) for x in operands],
        out_specs=[block(shape) for shape in shapes],
        out_shape=[jax.ShapeDtypeStruct(shape, F32) for shape in shapes],
        compiler_params=pltpu.CompilerParams(vmem_limit_bytes=VMEM_LIMIT),
        cost_estimate=pl.CostEstimate(flops=0, bytes_accessed=40 * rows * gate.shape[1], transcendentals=0),
        name="widen",
    )(*operands)


def solution(mesh):
    ns, nf = mesh.shape["seq"], mesh.shape["fsdp"]
    na = nf // 4
    chips = 2 * na
    kv = KEY_VALUE_HEADS // ns

    def body(tokens, cotangent, attention_gain, feedforward_gain, query_weight, key_matrix, value_matrix, out_weight, gate_weight, up_weight, down_weight):
        count, span, width = tokens.shape
        rows = count * span
        local = query_weight.shape[0]
        sizes = (ns, nf)
        mine = lax.axis_index("fsdp")
        cosines, sines = (jnp.asarray(x) for x in rope_tables(ns * span))
        flat = tokens.reshape(rows, width)
        grad_flat = cotangent.reshape(rows, width)
        (w_qkv, w_out, w_gate, w_down, first, packed, heads_attended, logs, attended, hidden_one, second_both, low_both, gains) = fore(
            sizes, count, kv, flat, grad_flat, attention_gain.reshape(1, local), feedforward_gain.reshape(1, local),
            query_weight, key_matrix, value_matrix, out_weight, gate_weight, down_weight, cosines, sines,
        )
        dwg, dwu, dwd, out_own, out_other, dx_own, dx_other = ffn(sizes, second_both, low_both, w_gate, w_down, up_weight, gate_weight)
        high, low, grad_tokens, gain_grads, dqkv, sum_gate, sum_up = back(
            sizes, count, kv, dx_own, dx_other, hidden_one, grad_flat, gains[1:2], w_out, w_qkv,
            packed, heads_attended, logs, cosines, sines, flat, gains[0:1], dwg, dwu,
        )
        out_arrived = lax.ppermute(out_other, "fsdp", [(i, i ^ 1) for i in range(nf)])
        *sums, gain_grads = finish(
            sizes, count, kv, sum_gate, sum_up, dwd, first, dqkv, attended, low, gain_grads
        )
        q_end, k_end = ns * kv * GROUP * HEAD_DIM, ns * kv * (GROUP + 1) * HEAD_DIM
        cuts = ((0, q_end), (q_end, k_end), (k_end, sums[4].shape[1]))
        grad_gate, grad_up, grad_down, grad_out, grad_query, grad_key, grad_value, block_out = widen(
            *sums, hidden_one, out_own, out_arrived, cuts
        )
        gain_grads = lax.dynamic_slice(gain_grads, (0, mine * local), (2, local))

        return (
            block_out.reshape(count, span, width),
            grad_tokens.reshape(count, span, width),
            gain_grads[0],
            gain_grads[1],
            grad_query,
            grad_key,
            grad_value,
            grad_out,
            grad_gate,
            grad_up,
            grad_down,
        )

    tokens_spec, gain_spec, weight_spec = P("fsdp", "seq", None), P("fsdp"), P("fsdp", None)
    return jax.shard_map(
        body,
        mesh=mesh,
        in_specs=(tokens_spec, tokens_spec, gain_spec, gain_spec) + (weight_spec,) * 7,
        out_specs=(tokens_spec, tokens_spec, gain_spec, gain_spec) + (weight_spec,) * 7,
        check_vma=False,
    )
```

```python
import functools
import math

import jax
import jax.numpy as jnp
import numpy as np
from jax import lax
from jax.experimental import pallas as pl
from jax.experimental.pallas import tpu as pltpu
from jax.sharding import PartitionSpec as P

QUERY_HEADS = 16
KEY_VALUE_HEADS = 8
HEAD_DIM = 96
GROUP = QUERY_HEADS // KEY_VALUE_HEADS
norm_eps = 1e-05
rope_base = 100000.0
masked_score = -1e30
F32, BF16 = jnp.float32, jnp.bfloat16
VMEM_LIMIT = 60 * 1024 * 1024
VMEM_MOST = 67043328
MESH = pl.DeviceIdType.MESH


def nt_dot(left, right):
    return lax.dot_general(left, right, (((1,), (1,)), ((), ())), preferred_element_type=F32)


def tn_dot(left, right):
    return lax.dot_general(left, right, (((0,), (0,)), ((), ())), preferred_element_type=F32)


def nn_dot(left, right):
    return jnp.dot(left, right, preferred_element_type=F32)


def whole(shape):
    return pl.BlockSpec(shape, lambda *_: (0,) * len(shape))


def call(kernel, scalars, operands, outs, name, flops, moved, scratch=()):
    return pl.pallas_call(
        kernel,
        grid_spec=pltpu.PrefetchScalarGridSpec(
            num_scalar_prefetch=1,
            grid=(1,),
            in_specs=[whole(x.shape) for x in operands],
            out_specs=[whole(x.shape) for x in outs],
            scratch_shapes=scratch,
        ),
        out_shape=outs,
        compiler_params=pltpu.CompilerParams(vmem_limit_bytes=VMEM_LIMIT),
        cost_estimate=pl.CostEstimate(flops=flops, bytes_accessed=moved, transcendentals=0),
        name=name,
    )(scalars, *operands)


def rope_tables(length):
    half = HEAD_DIM // 2
    freqs = np.float32(rope_base) ** (-(np.float32(2.0) * np.arange(half, dtype=np.float32)) / np.float32(HEAD_DIM))
    angles = np.arange(length, dtype=np.float32)[:, None] * freqs.astype(np.float32)[None, :]
    cosine, sine = np.cos(angles), np.sin(angles)
    return np.concatenate([cosine, cosine], 1), np.concatenate([-sine, sine], 1)


def swap_halves(values):
    half = HEAD_DIM // 2
    width = values.shape[1]
    lane = lax.broadcasted_iota(jnp.int32, values.shape, 1)
    ahead = pltpu.roll(values, width - half, 1)
    behind = pltpu.roll(values, half, 1)
    return jnp.where(lane % HEAD_DIM < half, ahead, behind)


def norm_back(grad, normed, inverse, gain):
    scaled = grad * gain
    return inverse * (scaled - normed * jnp.mean(scaled * normed, axis=1, keepdims=True))


def ffn_kernel(
    mesh, tiles, parts, x, g, wg, wd, wu, w_last, dwg, dwu, dwd, out_own, out_other, dx_own, dx_other,
    xt, acc_out, acc_dx, act, dgate, dup, stage, land, gate, send_sems, recv_sems, local_sems,
):
    step = pl.program_id(0)
    rows = x.shape[0] // 2
    links = Links(mesh, send_sems, recv_sems, local_sems)
    chips, local, tile = tiles // parts, wu.shape[0], land.shape[2]
    cols = tile // parts
    gathers, loads = [], []
    for k in range(chips + 1):
        gathers.append(GatherHalf(links, lambda c, k=k: (stage, c, k), lambda o, k=k: (land, k, rows_at(o, local))))
        weight, tile_at = (wu, k) if k < chips else (w_last, chips - 1)
        for c in range(2):
            source = (weight, slice(None), slice((tile_at * 2 + c) * tile, (tile_at * 2 + c + 1) * tile))
            loads.append(links.local(source, (stage, c, k)))

    def begin(k):
        gathers[k].start()
        gathers[k].other_start()

    def turn(k):
        gathers[k].turn()
        gathers[k].turn_late()

    @pl.when(step == 0)
    def _():
        for load in loads:
            load.start()
        links.barrier()
        for load in loads:
            load.wait()
        gathers[0].start()

    @pl.when(step == 0)
    def _():
        out_own[...] = jnp.zeros_like(out_own)
        dx_own[...] = jnp.zeros_like(dx_own)
        acc_out[...] = jnp.zeros_like(acc_out)
        acc_dx[...] = jnp.zeros_like(acc_dx)
        xt[...] = x[...].T
        gathers[0].other_start()

    def first_part():
        turn(0)
        begin(1)
        gathers[0].finish()

    def later_part(k):
        turn(k)
        for n in (2, 3) if k == 1 else (k + 2,):
            if n <= chips:
                begin(n)
        if k == chips - 1:
            turn(chips)

    for k in range(1, chips):
        pl.when(step == (k - 1) * parts + 1)(functools.partial(later_part, k))
    pl.when(step == (chips - 1) * parts)(gathers[chips].finish)
    at = pl.ds(pl.multiple_of(lax.rem(step, parts) * cols, cols), cols)
    chip = step // parts

    @pl.when(chip < chips - 1)
    def _():
        gate[...] = wg[...]

    @pl.when(chip == chips - 1)
    def _():
        gate[...] = land[chips, :, at]

    before = []
    for i in range(2):
        here = slice(i * rows, (i + 1) * rows)
        before.append((nn_dot(x[here, :], gate[...]), nt_dot(g[here, :], wd[...])))
    pl.when(step == 0)(first_part)
    for k in range(1, chips):
        pl.when(step == k * parts)(gathers[k].finish)
    for i, (out, dx) in enumerate(((out_own, dx_own), (acc_out, acc_dx))):
        here = slice(i * rows, (i + 1) * rows)
        gate_pre, grad = before[i]
        up = nn_dot(x[here, :], land[chip, :, at])
        sigmoid = jax.nn.sigmoid(gate_pre)
        silu = gate_pre * sigmoid
        hidden = (silu * up).astype(BF16)
        act[here, :] = hidden
        gate_grad = (grad * up * sigmoid * (1.0 + gate_pre * (1.0 - sigmoid))).astype(BF16)
        up_grad = (grad * silu).astype(BF16)
        dgate[here, :] = gate_grad
        dup[here, :] = up_grad
        out[...] += nn_dot(hidden, wd[...])
        dx[...] += nt_dot(gate_grad, gate[...]) + nt_dot(up_grad, land[chip, :, at])
    dwg[...] = nn_dot(xt[...], dgate[...]).astype(BF16)
    dwu[...] = nn_dot(xt[...], dup[...]).astype(BF16)
    dwd[...] = tn_dot(act[...], g[...]).astype(BF16)

    @pl.when(step == tiles - 1)
    def _():
        out_other[...] = acc_out[...].astype(BF16)
        dx_other[...] = acc_dx[...].astype(BF16)


def ffn(mesh, x, g, wg, wd, wu, w_last):
    rows, width = x.shape[0] // 2, x.shape[1]
    chips, tile = wg.shape[0] + 1, wg.shape[2]
    parts = 2
    tiles, cols = chips * parts, tile // parts
    local = wu.shape[0]
    keep = lambda shape: pl.BlockSpec(shape, lambda i: (0, 0), pipeline_mode=pl.Buffered(1))
    last = lambda: pl.BlockSpec((rows, width), lambda i: (0, 0))
    half = tile * chips
    wide, low = jax.ShapeDtypeStruct((rows, width), F32), jax.ShapeDtypeStruct((rows, width), BF16)
    return pl.pallas_call(
        functools.partial(ffn_kernel, mesh, tiles, parts),
        grid=(tiles,),
        in_specs=[
            keep(x.shape),
            keep(g.shape),
            pl.BlockSpec((None, width, cols), lambda i: (jnp.minimum(i // parts, chips - 2), 0, i % parts)),
            pl.BlockSpec((cols, width), lambda i: (i, 0)),
            pl.BlockSpec(memory_space=pl.ANY),
            pl.BlockSpec(memory_space=pl.ANY),
        ],
        out_specs=[pl.BlockSpec((width, cols), lambda i: (0, i))] * 2
        + [pl.BlockSpec((cols, width), lambda i: (i, 0)), last(), last(), last(), last()],
        scratch_shapes=[pltpu.VMEM((width, 2 * rows), BF16)]
        + [pltpu.VMEM((rows, width), F32)] * 2
        + [pltpu.VMEM((2 * rows, cols), BF16)] * 3
        + [pltpu.VMEM((2, chips + 1, local, tile), BF16), pltpu.VMEM((chips + 1, width, tile), BF16), pltpu.VMEM((width, cols), BF16)]
        + [pltpu.SemaphoreType.DMA((96,)), pltpu.SemaphoreType.DMA((96,)), pltpu.SemaphoreType.DMA((64,))],
        out_shape=[
            jax.ShapeDtypeStruct((width, half), BF16),
            jax.ShapeDtypeStruct((width, half), BF16),
            jax.ShapeDtypeStruct((half, width), BF16),
            wide,
            low,
            wide,
            low,
        ],
        compiler_params=pltpu.CompilerParams(vmem_limit_bytes=VMEM_MOST, collective_id=3, has_side_effects=True),
        cost_estimate=pl.CostEstimate(
            flops=36 * rows * width * half, bytes_accessed=12 * width * half + 20 * rows * width, transcendentals=0
        ),
        name="ffn",
    )(x, g, wg, wd, wu, w_last)


def part(x):
    return x[0].at[x[1:]] if isinstance(x, tuple) else x


def get(x):
    return x[0][x[1:]] if isinstance(x, tuple) else x[...]


def put(x, value):
    if isinstance(x, tuple):
        x[0][x[1:]] = value
    else:
        x[...] = value


class Copy:
    def __init__(self, src, dst, device, send_sem, recv_sem):
        self.src, self.dst, self.device, self.send_sem, self.recv_sem = src, dst, device, send_sem, recv_sem

    def made(self):
        if self.device is None:
            return pltpu.make_async_copy(part(self.src), part(self.dst), part(self.send_sem))
        return pltpu.make_async_remote_copy(
            src_ref=part(self.src),
            dst_ref=part(self.dst),
            send_sem=part(self.send_sem),
            recv_sem=part(self.recv_sem),
            device_id=self.device,
            device_id_type=MESH,
        )

    def start(self):
        self.made().start()

    def wait(self):
        self.made().wait()

    def wait_send(self):
        self.made().wait_send()

    def wait_recv(self):
        self.made().wait_recv()


class Links:
    def __init__(self, mesh, send_sems, recv_sems, local_sems):
        self.ns, self.nf = mesh
        self.na = self.nf // 4
        self.send_sems, self.recv_sems, self.local_sems = send_sems, recv_sems, local_sems
        self.count, self.local_count = 0, 0
        self.z, self.f = lax.axis_index("seq"), lax.axis_index("fsdp")
        self.core = lax.rem(self.f, 2)
        self.b = lax.rem(self.f // 2, 2)
        self.a = self.f // 4

    def chip(self, da, db):
        return lax.rem(self.a + da, self.na) * 2 + lax.rem(self.b + db, 2)

    def at_core(self):
        return (self.z, self.f + 1 - 2 * self.core)

    def at_b(self):
        return (self.z, self.f + 2 - 4 * self.b)

    def at_a(self, d):
        return (self.z, lax.rem(self.f + 4 * d, self.nf))

    def at_z(self, d):
        return (lax.rem(self.z + d, self.ns), self.f)

    def peers(self):
        return [self.at_core(), self.at_b()] + [self.at_a(d) for d in range(1, self.na)] + [self.at_z(d) for d in range(1, self.ns)]

    def barrier(self):
        barrier = pltpu.get_barrier_semaphore()
        peers = self.peers()
        for peer in peers:
            pl.semaphore_signal(barrier, inc=1, device_id=peer, device_id_type=MESH)
        pl.semaphore_wait(barrier, len(peers))

    def copy(self, src, dst, device):
        index = self.count
        self.count += 1
        return Copy(src, dst, device, (self.send_sems, index), (self.recv_sems, index))

    def again(self, src, dst, device):
        index = self.count - 1
        return Copy(src, dst, device, (self.send_sems, index), (self.recv_sems, index))

    def local(self, src, dst):
        index = self.local_count
        self.local_count += 1
        return Copy(src, dst, None, (self.local_sems, index), None)


def line_place(links):
    z, ns = links.z, links.ns
    middle = ns // 2
    step = jnp.where(z < middle, 1, -1)
    end = (z == 0) | (z == ns - 1)
    inner = (z == middle - 1) | (z == middle)
    return end, inner, (z + step, links.f), (z - step, links.f)


GATE_PIECES = 4


def first_piece(ns, columns):
    return columns // GATE_PIECES if ns == 4 else 0


def rows_at(start, size):
    return pl.ds(pl.multiple_of(start * size, size), size)


class ChipSum:
    def __init__(self, links, partial, b_first, arrived, passed, staging):
        self.links, self.partial, self.b_first = links, partial, b_first
        self.arrived, self.passed, self.staging = arrived, passed, staging
        na = links.na
        self.first, self.second = [], []
        if b_first:
            self.kept = [links.chip(da, 0) for da in range(na)]
            for da in range(na):
                self.first.append(links.copy(partial(links.chip(da, 1)), (arrived, da), links.at_b()))
            for d in range(1, na):
                self.second.append(links.copy((arrived, d), (passed, d - 1), links.at_a(d)))
        else:
            self.kept = [links.chip(0, db) for db in range(2)]
            for d in range(1, na):
                for db in range(2):
                    self.first.append(links.copy(partial(links.chip(d, db)), (arrived, (d - 1) * 2 + db), links.at_a(d)))
            self.second.append(links.copy((arrived, 1), (passed, 0), links.at_b()))
        self.loads = [] if staging is None else [links.local(partial(k), (staging, i)) for i, k in enumerate(self.kept)]

    def start(self):
        for copy in self.first:
            copy.start()

    def load(self):
        for load in self.loads:
            load.start()

    def turn(self):
        for load in self.loads:
            load.wait()
        for copy in self.first:
            copy.wait()
        count = len(self.kept)
        for i in [*range(1, count), 0]:
            own = self.partial(self.kept[i]) if self.staging is None else (self.staging, i)
            total = get(own).astype(F32)
            if self.b_first:
                total = total + self.arrived[i].astype(F32)
            else:
                for d in range(self.links.na - 1):
                    total = total + self.arrived[d * 2 + i].astype(F32)
            self.arrived[i] = total.astype(BF16)
            if i > 0 and self.b_first:
                self.second[i - 1].start()
            elif i > 0:
                self.second[0].start()

    def finish(self):
        for copy in self.second:
            copy.wait()
        total = self.arrived[0].astype(F32)
        for i in range(len(self.second)):
            total = total + self.passed[i].astype(F32)
        return total.astype(BF16)


def chip_sum_shapes(na, b_first, rows, columns):
    first = na if b_first else 2 * (na - 1)
    kept = na if b_first else 2
    return [
        pltpu.VMEM((max(first, kept), rows, columns), BF16),
        pltpu.VMEM((na - 1 if b_first else 1, rows, columns), BF16),
        pltpu.VMEM((kept, rows, columns), BF16),
    ]


def flip_core(f):
    return f + 1 - 2 * lax.rem(f, 2)


def flip_b(f):
    return f + 2 - 4 * lax.rem(f // 2, 2)


class Gather:
    def __init__(self, links, own, land, both):
        self.links = links
        f, na, nf = links.f, links.na, links.nf
        to_core, to_b = links.at_core(), links.at_b()

        def move(origin, device, half=None):
            return links.copy(land(origin, half), land(origin, half), device)

        self.given = [links.copy(own, land(f, None), to_core)] if both else []
        self.own = [links.copy(own, land(f, None), to_b)]
        self.own += [links.copy(own, land(f, None), links.at_a(d)) for d in range(1, na)]
        from_b = flip_b(f)
        from_a = [lax.rem(f + nf - 4 * d, nf) for d in range(1, na)]
        if na == 2:
            self.relays = [move(from_b, links.at_a(1), 1), move(from_a[0], to_b, 0)]
            far = [(flip_b(from_a[0]), 0), (flip_b(from_a[0]), 1)]
        else:
            self.relays = [move(origin, to_b) for origin in from_a]
            far = [(flip_b(origin), None) for origin in from_a]
        near = [from_b, *from_a]
        self.near = [move(origin, to_core) for origin in near] if both else []
        self.far = [move(origin, to_core, half) for origin, half in far] if both else []

    def start(self):
        for copies in self.own + self.given:
            copies.start()

    def turn(self):
        for copies in self.own:
            copies.wait()
        for copies in self.relays + self.near:
            copies.start()

    def pass_on(self):
        for copies in self.relays:
            copies.wait()
        for copies in self.far:
            copies.start()

    def finish(self):
        for copies in self.given + self.near + self.far:
            copies.wait()


class GatherHalf:
    def __init__(self, links, stage, land):
        self.links = links
        f, na, nf, core = links.f, links.na, links.nf, links.core
        to_b = links.at_b()

        def move(origin, device):
            return links.copy(land(origin), land(origin), device)

        self.swap = links.copy(stage(1 - core), land(f), links.at_core())
        self.kept = links.local(stage(core), land(f))
        targets = [to_b] + [links.at_a(d) for d in range(1, na)]
        self.own = [links.copy(stage(core), land(f), device) for device in targets]
        self.other = [move(flip_core(f), device) for device in targets]
        from_b = flip_b(f)
        from_a = [lax.rem(f + nf - 4 * d, nf) for d in range(1, na)]
        if na == 2:
            self.relays = [move(from_b, links.at_a(1))]
            self.late = [move(flip_core(from_a[0]), to_b)]
        else:
            self.relays = [move(origin, to_b) for origin in from_a]
            self.late = [move(flip_core(origin), to_b) for origin in from_a]

    def start(self):
        for copies in [self.swap, self.kept, *self.own]:
            copies.start()

    def other_start(self):
        self.swap.wait()
        for copies in self.other:
            copies.start()

    def turn(self):
        for copies in self.own:
            copies.wait()
        for copies in self.relays:
            copies.start()

    def turn_late(self):
        for copies in self.other:
            copies.wait()
        for copies in self.late:
            copies.start()

    def finish(self):
        for copies in [self.kept, *self.relays, *self.late]:
            copies.wait()


def attend_heads(ns, kv, span, qs, ks, vs, out, logs):
    scale = 1.0 / math.sqrt(HEAD_DIM)
    row = lax.broadcasted_iota(jnp.int32, (span, span), 0)
    column = lax.broadcasted_iota(jnp.int32, (span, span), 1)
    causal = row >= column
    lane = lax.broadcasted_iota(jnp.int32, (span, 128), 1)
    for s in range(ns):
        here = slice(s * span, (s + 1) * span)
        stats = jnp.zeros((span, 128), F32)
        for h in range(kv * GROUP):
            g = h // GROUP
            q = qs[h, here, :]
            near = jnp.where(causal, nt_dot(q, ks[g, here, :]) * scale, masked_score)
            top = jnp.max(near, axis=1, keepdims=True)
            if s > 0:
                far = nt_dot(q, ks[g, : s * span, :]) * scale
                top = jnp.maximum(top, jnp.max(far, axis=1, keepdims=True))
            near = jnp.exp(near - top)
            total = jnp.sum(near, axis=1, keepdims=True)
            if s > 0:
                far = jnp.exp(far - top)
                total = total + jnp.sum(far, axis=1, keepdims=True)
            inverse = 1.0 / total
            result = nn_dot((near * inverse).astype(BF16), vs[g, here, :])
            if s > 0:
                result = result + nn_dot((far * inverse).astype(BF16), vs[g, : s * span, :])
            stats = jnp.where(lane == h, top + jnp.log(total), stats)
            out[s, :, h * HEAD_DIM : (h + 1) * HEAD_DIM] = result.astype(BF16)
        logs[here, :] = stats


def fill_tables(cosines, sines, narrow_cosines, narrow_sines, heads):
    end = heads * HEAD_DIM
    cosines[:, end:] = jnp.ones((cosines.shape[0], cosines.shape[1] - end), F32)
    sines[:, end:] = jnp.zeros((cosines.shape[0], cosines.shape[1] - end), F32)
    for h in range(heads):
        at = slice(h * HEAD_DIM, (h + 1) * HEAD_DIM)
        cosines[:, at] = narrow_cosines
        sines[:, at] = narrow_sines


def fore_kernel(
    mesh, count, kv,
    tokens, cotangent, gain_one, gain_two, wq, wk, wv, wo, wg, wd, narrow_cosines, narrow_sines,
    w_qkv, w_out, w_gate, w_down, first_out, packed, heads_attended, logs, attended_out, hidden_out, second_both, low_both, gains_out,
    rows_in, hidden, first, pack, w_land, wo_land, q_send, q_land, a_send, a_land, stage_gate, gain_send, gain_land,
    qs, ks, vs, log, attended, second, second_abs, low, cosines, sines, send_sems, recv_sems, local_sems,
):
    links = Links(mesh, send_sems, recv_sems, local_sems)
    ns, na, nf = links.ns, links.na, links.nf
    chips = 2 * na
    z, f, core = links.z, links.f, links.core
    rows, width = rows_in.shape
    span = rows // count
    heads = kv * GROUP
    g_width, k_width = heads * HEAD_DIM, kv * HEAD_DIM
    q_width = g_width + 2 * k_width
    local = width // nf
    links.barrier()

    token_load = links.local(tokens, rows_in)
    token_load.start()
    cot_load = links.local(cotangent, hidden)
    cot_load.start()
    gain_send[...] = jnp.zeros_like(gain_send)
    gain_send[0:1, :local] = gain_one[...].astype(F32)
    gain_send[1:2, :local] = gain_two[...].astype(F32)
    for j in range(ns):
        pack[j, :, :g_width] = wq[:, j * g_width : (j + 1) * g_width]
        pack[j, :, g_width : g_width + k_width] = wk[:, j * k_width : (j + 1) * k_width]
        pack[j, :, g_width + k_width :] = wv[:, j * k_width : (j + 1) * k_width]

    every = slice(None)

    def piece(start, size, half):
        if half is None:
            return rows_at(start, size)
        return rows_at(start * 2 + half, size // 2)

    units = []
    turns = [*range(1, ns), 0]
    for d in turns:
        g = lax.rem(z + d, ns)
        units.append(Gather(links, (pack, g), lambda o, half, g=g: (w_land, g, piece(o, local, half)), True))
    units.append(Gather(links, wo, lambda o, half: (wo_land, piece(o, local, half)), True))
    depth = wd.shape[0]
    units.append(Gather(links, wd, lambda o, half: (w_down, piece(o // 2, depth, half)), False))
    gate_unit = GatherHalf(links, lambda c: (stage_gate, c), lambda o: (w_gate, every, rows_at(o, local)))
    q_copies, a_copies = [], []
    for d in range(1, ns):
        g = lax.rem(z + d, ns)
        q_copies.append([links.copy((q_send, g, i), (q_land, i, z), links.at_z(d)) for i in range(count)])
    for i in range(count):
        a_copies.append([links.copy((a_send, i, lax.rem(z + d, ns)), (a_land, i, z), links.at_z(d)) for d in range(1, ns)])
    second_copy = links.copy(second_abs, (second_both, pl.ds(rows, rows)), links.at_core())
    low_copy = links.copy(low, (low_both, pl.ds(rows, rows)), links.at_core())

    def gain_at(start, size):
        return (gain_land, pl.ds(start, size))

    pair, chip_four = f // 2 * 2, f // 4 * 4
    gain_copies = [
        [links.copy(gain_at(f, 1), gain_at(f, 1), links.at_core())],
        [links.copy(gain_at(pair, 2), gain_at(pair, 2), links.at_b())],
        [links.copy(gain_at(chip_four, 4), gain_at(chip_four, 4), links.at_a(d)) for d in range(1, na)],
    ]
    stores = []

    def store(src, dst):
        copies = links.local(src, dst)
        copies.start()
        stores.append(copies)

    gain_land[f] = gain_send[...]
    for copies in gain_copies[0]:
        copies.start()
    units[0].start()
    units[1].start()
    for j in range(ns):
        w_land[j, rows_at(f, local), :] = pack[j]
    stage_loads = []
    tile = w_gate.shape[2]
    for c in range(2):
        for k in range(chips - 1):
            source = (wg, every, slice((k * 2 + c) * tile, (k * 2 + c + 1) * tile))
            stage_loads.append(links.local(source, (stage_gate, c, k)))
    for load in stage_loads:
        load.start()
    store_own = [links.local(wo, (wo_land, rows_at(f, local))), links.local(wd, (w_down, rows_at(f // 2, depth)))]
    for copies in store_own:
        copies.start()
    fill_tables(cosines, sines, narrow_cosines[rows_at(z, span), :], narrow_sines[rows_at(z, span), :], heads + kv)
    token_load.wait()
    old = rows_in[...]
    inverse = lax.rsqrt(jnp.mean(old * old, axis=1, keepdims=True) + norm_eps)
    for stage in range(3):
        for copies in gain_copies[stage]:
            copies.wait()
        if stage < 2:
            for copies in gain_copies[stage + 1]:
                copies.start()
    for j in range(nf):
        gains_out[:, j * local : (j + 1) * local] = gain_land[j, 0:2, :local]
    first[...] = (old * inverse * gains_out[0:1, :]).astype(BF16)
    store(first, first_out)

    def project(n):
        g = lax.rem(z + turns[n], ns)
        units[n].finish()
        y = nn_dot(first[...], w_land[g])
        for i in range(count):
            part = y[i * span : (i + 1) * span]
            part = (part * cosines[...] + swap_halves(part) * sines[...]).astype(BF16)
            if turns[n] == 0:
                q_land[i, z] = part
            else:
                q_send[g, i] = part
        if turns[n] > 0:
            q_copies[turns[n] - 1][0].start()
        if n > 0 and turns[n - 1] > 0:
            for copies in q_copies[turns[n - 1] - 1][1:]:
                copies.start()
        store((w_land, g), (w_qkv, g))

    last = len(units)
    for n in range(ns):
        units[n].turn()
        if n + 2 < last:
            units[n + 2].start()
        if n > 0:
            units[n - 1].pass_on()
        if n > 1:
            project(n - 2)
    units[ns].turn()
    for load in stage_loads:
        load.wait()
    gate_unit.start()
    units[ns - 1].pass_on()
    project(ns - 2)
    gate_unit.other_start()
    project(ns - 1)
    units[ns].pass_on()
    cot_load.wait()
    low[...] = hidden[...].astype(BF16)
    low_copy.start()
    store(low, (low_both, pl.ds(0, rows)))

    def attend(i):
        for copies in q_copies:
            copies[i].wait()
        for j in range(ns):
            at = slice(j * span, (j + 1) * span)
            for h in range(heads):
                qs[h, at, :] = q_land[i, j, :, h * HEAD_DIM : (h + 1) * HEAD_DIM]
            for h in range(kv):
                k0, v0 = (heads + h) * HEAD_DIM, (heads + kv + h) * HEAD_DIM
                ks[h, at, :] = q_land[i, j, :, k0 : k0 + HEAD_DIM]
                vs[h, at, :] = q_land[i, j, :, v0 : v0 + HEAD_DIM]
        attend_heads(ns, kv, span, qs, ks, vs, a_send.at[i], log.at[i])
        for copies in a_copies[i]:
            copies.start()
        a_land[i, z] = a_send[i, z]

    for i in range(count):
        attend(i)
        if i == 0:
            units[ns + 1].turn()
            units[ns].finish()
            store_own[0].wait()
            store(wo_land, w_out)
    store(q_land, packed)
    store(a_send, heads_attended)
    store(log, logs)
    for i in range(count):
        for copies in a_copies[i]:
            copies.wait()
        for j in range(ns):
            attended[i * span : (i + 1) * span, j * g_width : (j + 1) * g_width] = a_land[i, j]
    new = rows_in[...] + nn_dot(attended[...], wo_land[...])
    hidden[...] = new
    inverse = lax.rsqrt(jnp.mean(new * new, axis=1, keepdims=True) + norm_eps)
    second_abs[...] = (new * inverse * gains_out[1:2, :]).astype(BF16)
    second_copy.start()
    store(second_abs, (second_both, pl.ds(0, rows)))
    store(attended, attended_out)
    store(hidden, hidden_out)
    units[ns + 1].pass_on()
    gate_unit.turn()
    gate_unit.turn_late()
    gate_unit.finish()
    second_copy.wait()
    low_copy.wait()
    store_own[1].wait()
    for copies in stores:
        copies.wait()


def fore(mesh, count, kv, tokens, cotangent, gain_one, gain_two, wq, wk, wv, wo, wg, wd, narrow_cosines, narrow_sines):
    ns, nf = mesh
    na = nf // 4
    chips = 2 * na
    rows, width = tokens.shape
    span = rows // count
    length = ns * span
    heads = kv * GROUP
    g_width = heads * HEAD_DIM
    q_width = g_width + 2 * kv * HEAD_DIM
    local, depth = wq.shape[0], wd.shape[0]
    tile = wg.shape[1] // (2 * chips)
    anywhere, vmem = pl.BlockSpec(memory_space=pl.ANY), pl.BlockSpec(memory_space=pltpu.VMEM)
    low = lambda *shape: jax.ShapeDtypeStruct(shape, BF16)
    wide = lambda *shape: jax.ShapeDtypeStruct(shape, F32)
    outs = [
        low(ns, width, q_width),
        low(width, width),
        low(chips - 1, width, tile),
        low(chips * depth, width),
        low(rows, width),
        low(count, ns, span, q_width),
        low(count, ns, span, g_width),
        wide(count, length, 128),
        low(rows, width),
        wide(rows, width),
        low(2 * rows, width),
        low(2 * rows, width),
        wide(2, width),
    ]
    scratch = [
        pltpu.VMEM((rows, width), F32),
        pltpu.VMEM((rows, width), F32),
        pltpu.VMEM((rows, width), BF16),
        pltpu.VMEM((ns, local, q_width), BF16),
        pltpu.VMEM((ns, width, q_width), BF16),
        pltpu.VMEM((width, width), BF16),
        pltpu.VMEM((ns, count, span, q_width), BF16),
        pltpu.VMEM((count, ns, span, q_width), BF16),
        pltpu.VMEM((count, ns, span, g_width), BF16),
        pltpu.VMEM((count, ns, span, g_width), BF16),
        pltpu.VMEM((2, chips - 1, local, tile), BF16),
        pltpu.VMEM((8, 256), F32),
        pltpu.VMEM((nf, 8, 256), F32),
        pltpu.VMEM((heads, length, HEAD_DIM), BF16),
        pltpu.VMEM((kv, length, HEAD_DIM), BF16),
        pltpu.VMEM((kv, length, HEAD_DIM), BF16),
        pltpu.VMEM((count, length, 128), F32),
        pltpu.VMEM((rows, width), BF16),
        pltpu.VMEM((8, 128), BF16),
        pltpu.VMEM((rows, width), BF16),
        pltpu.VMEM((rows, width), BF16),
        pltpu.VMEM((span, q_width), F32),
        pltpu.VMEM((span, q_width), F32),
    ]
    return pl.pallas_call(
        functools.partial(fore_kernel, mesh, count, kv),
        in_specs=[anywhere] * 2 + [vmem] * 5 + [anywhere] * 3 + [vmem] * 2,
        out_specs=[anywhere] * 12 + [vmem],
        out_shape=outs,
        scratch_shapes=scratch
        + [pltpu.SemaphoreType.DMA((160,)), pltpu.SemaphoreType.DMA((160,)), pltpu.SemaphoreType.DMA((64,))],
        compiler_params=pltpu.CompilerParams(vmem_limit_bytes=VMEM_MOST, collective_id=0, has_side_effects=True),
        name="fore",
    )(tokens, cotangent, gain_one, gain_two, wq, wk, wv, wo, wg, wd, narrow_cosines, narrow_sines)


def attend_back_heads(ns, kv, span, qs, ks, vs, gs, attended, logs, dk, dv, result):
    scale = 1.0 / math.sqrt(HEAD_DIM)
    heads = kv * GROUP
    row = lax.broadcasted_iota(jnp.int32, (span, span), 0)
    column = lax.broadcasted_iota(jnp.int32, (span, span), 1)
    causal = row >= column
    dk[...] = jnp.zeros_like(dk)
    dv[...] = jnp.zeros_like(dv)
    for s in range(ns):
        here = slice(s * span, (s + 1) * span)
        for h in range(heads):
            g = h // GROUP
            q, grad = qs[h, here, :], gs[h, here, :]
            log_total = logs[here, h : h + 1]
            out = attended[s, :, h * HEAD_DIM : (h + 1) * HEAD_DIM]
            delta = jnp.sum(grad.astype(F32) * out.astype(F32), axis=1, keepdims=True)
            k, v = ks[g, here, :], vs[g, here, :]
            near = jnp.where(causal, jnp.exp(nt_dot(q, k) * scale - log_total), 0.0)
            slope = (near * (nt_dot(grad, v) - delta) * scale).astype(BF16)
            dq = nn_dot(slope, k)
            dk[g, here, :] += tn_dot(slope, q)
            dv[g, here, :] += tn_dot(near.astype(BF16), grad)
            if s > 0:
                before = slice(0, s * span)
                k, v = ks[g, before, :], vs[g, before, :]
                far = jnp.exp(nt_dot(q, k) * scale - log_total)
                slope = (far * (nt_dot(grad, v) - delta) * scale).astype(BF16)
                dq = dq + nn_dot(slope, k)
                dk[g, before, :] += tn_dot(slope, q)
                dv[g, before, :] += tn_dot(far.astype(BF16), grad)
            result[here, h * HEAD_DIM : (h + 1) * HEAD_DIM] = dq
    for g in range(kv):
        k0 = (heads + g) * HEAD_DIM
        v0 = (heads + kv + g) * HEAD_DIM
        result[:, k0 : k0 + HEAD_DIM] = dk[g]
        result[:, v0 : v0 + HEAD_DIM] = dv[g]


def back_kernel(
    mesh, count, kv,
    dx_own, dx_other, hidden, cotangent, gain_two, w_out, w_qkv, packed, attended, logs, cosines, sines, tokens, gain_one, dwg, dwu,
    high, low_out, out, gain_grads, dqkv, sum_gate, sum_up,
    low, sum_rows, sum_land, dx_land, g_send, g_land, q_send, q_land, swap_send, swap_land, *rest,
):
    parts, (send_sems, recv_sems, local_sems) = rest[:-3], rest[-3:]
    links = Links(mesh, send_sems, recv_sems, local_sems)
    ns, na = links.ns, links.na
    chips = 2 * na
    z, core = links.z, links.core
    rows, width = hidden.shape
    span = rows // count
    length = ns * span
    heads = kv * GROUP
    g_width, q_width = heads * HEAD_DIM, (heads + 2 * kv) * HEAD_DIM
    half = dwg.shape[1]
    block = width // chips
    links.barrier()

    dx_copy = links.copy(dx_other, dx_land, links.at_core())
    dx_copy.start()
    sums = []
    for n, source in enumerate((dwg, dwu)):
        for b_first in (True, False):
            columns = slice(0, half // 2) if b_first else slice(half // 2, half)
            at = (n * 2 + (0 if b_first else 1)) * 3
            partial = lambda k, source=source, columns=columns: (source, rows_at(k, block), columns)
            sums.append(ChipSum(links, partial, b_first, *parts[at : at + 3]))
    for item in sums:
        item.start()
        item.load()

    g_copies, q_copies = [], []
    for i in range(count):
        g_copies.append([links.copy((g_send, i, lax.rem(z + d, ns)), (g_land, i, z), links.at_z(d)) for d in range(1, ns)])
        q_copies.append([links.copy((q_send, i, lax.rem(z + d, ns)), (q_land, z, i), links.at_z(d)) for d in range(1, ns)])

    def out_back(dx, old, grad, w):
        loads = [links.local(dx_own, dx), links.local(hidden, old), links.local(cotangent, grad), links.local(w_out, w)]
        for load in loads:
            load.start()
        dx_copy.wait()
        for load in loads[:3]:
            load.wait()
        step = dx[...] + dx_land[...].astype(F32)
        inverse = lax.rsqrt(jnp.mean(old[...] * old[...], axis=1, keepdims=True) + norm_eps)
        normed = old[...] * inverse
        gain_grads[1:2, :] = jnp.sum(step * normed, axis=0, keepdims=True)
        grad[...] = grad[...] + norm_back(step, normed, inverse, gain_two[...])
        low[...] = grad[...].astype(BF16)
        stores = [links.local(grad, high), links.local(low, low_out)]
        for store in stores:
            store.start()
        loads[3].wait()
        for i in range(count):
            here = slice(i * span, (i + 1) * span)
            part = nt_dot(low[here, :], w[...]).astype(BF16)
            for j in range(ns):
                g_send[i, j] = part[:, j * g_width : (j + 1) * g_width]
            for copies in g_copies[i]:
                copies.start()
            g_land[i, z] = g_send[i, z]
        for store in stores:
            store.wait()

    pl.run_scoped(
        out_back,
        pltpu.VMEM((rows, width), F32),
        pltpu.VMEM((rows, width), F32),
        pltpu.VMEM((rows, width), F32),
        pltpu.VMEM((width, width), BF16),
    )

    def attention(qkv, mid, log, qs, ks, vs, gs, dk, dv, result, cosine, sine):
        fill_tables(cosine, sine, cosines[...], sines[...], heads + kv)
        for i in range(count):
            loads = [links.local((packed, i), qkv), links.local((attended, i), mid), links.local((logs, i), log)]
            for load in loads:
                load.start()
            for load in loads:
                load.wait()
            for j in range(ns):
                at = slice(j * span, (j + 1) * span)
                for h in range(heads):
                    qs[h, at, :] = qkv[j, :, h * HEAD_DIM : (h + 1) * HEAD_DIM]
                for h in range(kv):
                    k0, v0 = (heads + h) * HEAD_DIM, (heads + kv + h) * HEAD_DIM
                    ks[h, at, :] = qkv[j, :, k0 : k0 + HEAD_DIM]
                    vs[h, at, :] = qkv[j, :, v0 : v0 + HEAD_DIM]
            for copies in g_copies[i]:
                copies.wait()
            for j in range(ns):
                for h in range(heads):
                    gs[h, j * span : (j + 1) * span, :] = g_land[i, j, :, h * HEAD_DIM : (h + 1) * HEAD_DIM]
            attend_back_heads(ns, kv, span, qs, ks, vs, gs, mid, log, dk, dv, result)
            for j in range(ns):
                here = slice(j * span, (j + 1) * span)
                part = result[here, :]
                q_send[i, j] = (part * cosine[here, :] - swap_halves(part) * sine[here, :]).astype(BF16)
            for copies in q_copies[i]:
                copies.start()
            q_land[z, i] = q_send[i, z]
            if i < len(sums) // 2:
                for item in sums[2 * i : 2 * i + 2]:
                    item.turn()

    pl.run_scoped(
        attention,
        pltpu.VMEM((ns, span, q_width), BF16),
        pltpu.VMEM((ns, span, g_width), BF16),
        pltpu.VMEM((length, 128), F32),
        pltpu.VMEM((heads, length, HEAD_DIM), BF16),
        pltpu.VMEM((kv, length, HEAD_DIM), BF16),
        pltpu.VMEM((kv, length, HEAD_DIM), BF16),
        pltpu.VMEM((heads, length, HEAD_DIM), BF16),
        pltpu.VMEM((kv, length, HEAD_DIM), F32),
        pltpu.VMEM((kv, length, HEAD_DIM), F32),
        pltpu.VMEM((length, q_width), F32),
        pltpu.VMEM((length, q_width), F32),
        pltpu.VMEM((length, q_width), F32),
    )

    swaps = []
    local = block // 2
    for item in sums[2 * count :]:
        item.turn()

    def swap(n):
        for m in range(2):
            total = sums[2 * n + m].finish()
            swap_send[n, m, 0] = total[:local]
            swap_send[n, m, 1] = total[local:]
        for m in range(2):
            copies = links.copy((swap_send, n, m, 1 - core), (swap_land, n, m), links.at_core())
            copies.start()
            swaps.append(copies)

    tile = half // chips
    stores = []
    early = first_piece(ns, 2 * half)
    piece = (sum_rows, 0, slice(None), slice(0, max(early, 1)))
    end, inner, inward = line_place(links)[:3]
    early_copy = links.copy(piece, sum_land, inward)

    def combine(n, total):
        for m in range(2):
            swaps[2 * n + m].wait()
            kept, arrived = swap_send[n, m, core], swap_land[n, m]
            for t in range(chips // 2):
                here = slice(t * tile, (t + 1) * tile)
                k = m * (chips // 2) + t
                one, two = kept[:, here], arrived[:, here]
                sum_rows[n, :, 2 * k * tile : (2 * k + 1) * tile] = jnp.where(core == 0, one, two)
                sum_rows[n, :, (2 * k + 1) * tile : (2 * k + 2) * tile] = jnp.where(core == 0, two, one)
        if n == 0 and early:
            pl.when(end)(early_copy.start)
        else:
            copies = links.local((sum_rows, n), total)
            copies.start()
            stores.append(copies)

    def project_back(w, old, base, grad):
        loads = [links.local(tokens, old), links.local(high, base), links.local(w_qkv, w)]
        for load in loads:
            load.start()
        swap(0)
        for load in loads:
            load.wait()
        for i in range(count):
            here = slice(i * span, (i + 1) * span)
            if i == count - 1:
                combine(0, sum_gate)
                swap(1)
                combine(1, sum_up)
            for copies in q_copies[i]:
                copies.wait()
            total = nt_dot(q_land[0, i], w[0])
            for j in range(1, ns):
                total = total + nt_dot(q_land[j, i], w[j])
            grad[here, :] = total
            copies = links.local((q_land, slice(None), i), (dqkv, slice(None), i))
            copies.start()
            stores.append(copies)
            step, rows_old = grad[here, :], old[here, :]
            inverse = lax.rsqrt(jnp.mean(rows_old * rows_old, axis=1, keepdims=True) + norm_eps)
            normed = rows_old * inverse
            part_sum = jnp.sum(step * normed, axis=0, keepdims=True)
            gain_grads[0:1, :] = part_sum if i == 0 else gain_grads[0:1, :] + part_sum
            base[here, :] = base[here, :] + norm_back(step, normed, inverse, gain_one[...])
            copies = links.local((base, here), (out, here))
            copies.start()
            stores.append(copies)
        if early:

            @pl.when(inner)
            def _():
                early_copy.wait_recv()
                put(piece, (get(piece).astype(F32) + sum_land[...].astype(F32)).astype(BF16))

            pl.when(end)(early_copy.wait_send)
            copies = links.local((sum_rows, 0), sum_gate)
            copies.start()
            stores.append(copies)
        for copies in stores:
            copies.wait()

    pl.run_scoped(
        project_back,
        pltpu.VMEM((ns, width, q_width), BF16),
        pltpu.VMEM((rows, width), F32),
        pltpu.VMEM((rows, width), F32),
        pltpu.VMEM((rows, width), F32),
    )


def back(mesh, count, kv, dx_own, dx_other, hidden, cotangent, gain_two, w_out, w_qkv, packed, attended, logs, cosines, sines, tokens, gain_one, dwg, dwu):
    ns, nf = mesh
    na = nf // 4
    rows, width = hidden.shape
    span = rows // count
    heads = kv * GROUP
    g_width, q_width = heads * HEAD_DIM, (heads + 2 * kv) * HEAD_DIM
    half = dwg.shape[1]
    block = width // (2 * na)
    local = block // 2
    anywhere = pl.BlockSpec(memory_space=pl.ANY)
    vmem = pl.BlockSpec(memory_space=pltpu.VMEM)
    operands = [dx_own, dx_other, hidden, cotangent, gain_two, w_out, w_qkv, packed, attended, logs, cosines, sines, tokens, gain_one, dwg, dwu]
    wide = jax.ShapeDtypeStruct((rows, width), F32)
    summed = jax.ShapeDtypeStruct((local, 2 * half), BF16)
    scratch = [
        pltpu.VMEM((rows, width), BF16),
        pltpu.VMEM((2, local, 2 * half), BF16),
        pltpu.VMEM((local, max(first_piece(ns, 2 * half), 128)), BF16),
        pltpu.VMEM((rows, width), BF16),
        pltpu.VMEM((count, ns, span, g_width), BF16),
        pltpu.VMEM((count, ns, span, g_width), BF16),
        pltpu.VMEM((count, ns, span, q_width), BF16),
        pltpu.VMEM((ns, count, span, q_width), BF16),
        pltpu.VMEM((2, 2, 2, local, half // 2), BF16),
        pltpu.VMEM((2, 2, local, half // 2), BF16),
    ]
    for _ in range(2):
        for b_first in (True, False):
            scratch += chip_sum_shapes(na, b_first, block, half // 2)
    return pl.pallas_call(
        functools.partial(back_kernel, mesh, count, kv),
        in_specs=[vmem if x.shape[0] == 1 or x.shape[1] == HEAD_DIM else anywhere for x in operands],
        out_specs=[anywhere, anywhere, anywhere, vmem, anywhere, anywhere, anywhere],
        out_shape=[
            wide,
            jax.ShapeDtypeStruct((rows, width), BF16),
            wide,
            jax.ShapeDtypeStruct((2, width), F32),
            jax.ShapeDtypeStruct((ns, count, span, q_width), BF16),
            summed,
            summed,
        ],
        scratch_shapes=scratch
        + [pltpu.SemaphoreType.DMA((64,)), pltpu.SemaphoreType.DMA((64,)), pltpu.SemaphoreType.DMA((64,))],
        compiler_params=pltpu.CompilerParams(vmem_limit_bytes=VMEM_MOST, collective_id=1, has_side_effects=True),
        name="back",
    )(*operands)


class LineSum:
    def __init__(self, links, term, first, second, total, out=None, begun=False):
        self.links, self.term, self.first, self.second, self.total = links, term, first, second, total
        self.dtype = (term[0] if isinstance(term, tuple) else term).dtype
        self.deep = links.ns // 2 > 1
        self.begun = begun
        self.end, self.inner, inward, outward = line_place(links)
        moved = self.deep and not begun
        self.inward = links.copy(term, first, inward) if moved else None
        self.onward = links.again(first, first, inward) if moved else None
        self.sum = first if moved else term
        self.across = links.copy(self.sum, second, inward)
        self.outward = links.copy(total, total, outward) if self.deep else None
        self.store = links.local(total, out) if out is not None else None

    def keep(self):
        if self.store is not None:
            self.store.start()

    def add(self, target, one, two):
        put(target, (get(one).astype(F32) + get(two).astype(F32)).astype(self.dtype))

    def begin(self):
        if self.begun:
            pl.when(self.inner)(self.across.start)
        elif self.deep:
            pl.when(self.end)(self.inward.start)
        else:
            self.across.start()

    def relay(self):
        if not self.deep or self.begun:
            return

        @pl.when(jnp.logical_not(self.end))
        def _():
            self.inward.wait_recv()
            self.add(self.first, self.term, self.first)
            pl.when(self.inner)(self.across.start)
            pl.when(jnp.logical_not(self.inner))(self.onward.start)

    def settle(self):
        @pl.when(self.inner)
        def _():
            self.across.wait()
            self.add(self.total, self.sum, self.second)
            if self.deep:
                self.outward.start()
            self.keep()

        if self.deep:

            @pl.when(jnp.logical_not(self.inner | self.end))
            def _():
                self.outward.wait_recv()
                self.outward.start()
                self.keep()

    def finish(self):
        if self.deep:

            @pl.when(self.end)
            def _():
                self.outward.wait_recv()
                self.keep()

            if not self.begun:
                pl.when(jnp.logical_not(self.inner))(self.inward.wait_send)
            pl.when(jnp.logical_not(self.end))(self.outward.wait_send)


def finish_kernel(
    mesh, count, kv,
    term_gate, term_up, dwd, first, dqkv, attended, low, gains,
    out_gate, out_up, out_down, out_out, out_qkv, out_gains,
    tot_gate, tot_up, tot_down, tot_out, tot_qkv, term_down, term_out, term_qkv, in_gate, in_up, in_down, in_out, in_qkv,
    first_both, attended_both, low_both, dq_both, w_out_part, w_qkv_part,
    swap_out, land_out, swap_qkv, land_qkv, gain_terms, gain_lands, *rest,
):
    parts, (send_sems, recv_sems, local_sems) = rest[:-3], rest[-3:]
    links = Links(mesh, send_sems, recv_sems, local_sems)
    ns, na = links.ns, links.na
    chips, per = 2 * na, ns // 2
    core = links.core
    rows, width = first.shape
    q_width = dqkv.shape[3]
    middle = width // 2
    links.barrier()

    def lines(term, inbox, total, out, pieces, begun=False):
        size = term.shape[1] // pieces
        every = slice(None)
        made = []
        for i in range(pieces):
            at = slice(i * size, (i + 1) * size)
            refs = [(ref, *where, every, at) for ref, *where in ((term,), (inbox, 0), (inbox, 1), (total,), (out,))]
            made.append(LineSum(links, *refs, begun and i == 0))
        return made

    gate_lines = lines(term_gate, in_gate, tot_gate, out_gate, GATE_PIECES, first_piece(ns, term_gate.shape[1]) > 0)
    up_lines = lines(term_up, in_up, tot_up, out_up, 4)
    down_lines = lines(term_down, in_down, tot_down, out_down, 4)
    out_lines = lines(term_out, in_out, tot_out, out_out, 2)
    qkv_lines = lines(term_qkv, in_qkv, tot_qkv, out_qkv, 4)
    for line in gate_lines + up_lines:
        line.begin()

    sends = [
        links.copy((dqkv, pl.ds((1 - core) * per, per)), (dq_both, 1), links.at_core()),
        links.copy((low, slice(None), rows_at(1 - core, middle)), (low_both, 1), links.at_core()),
        links.copy(first, (first_both, 1), links.at_core()),
        links.copy(attended, (attended_both, 1), links.at_core()),
    ]
    loads = [
        links.local((low, slice(None), rows_at(core, middle)), (low_both, 0)),
        links.local(attended, (attended_both, 0)),
        links.local(first, (first_both, 0)),
        links.local((dqkv, pl.ds(core * per, per)), (dq_both, 0)),
    ]
    for copies in loads + sends[1:2] + sends[3:4] + sends[2:3] + sends[:1]:
        copies.start()

    down_rows = dwd.shape[0] // chips
    block = width // chips

    def pair(source, row_count, at, staged):
        made = []
        cut = source.shape[1] // 2
        for n, b_first in enumerate((True, False)):
            columns = slice(0, cut) if b_first else slice(cut, 2 * cut)
            partial = lambda k, columns=columns: (source, rows_at(k, row_count), columns)
            refs = parts[at[n] : at[n + 1]]
            made.append(ChipSum(links, partial, b_first, *(refs if staged else (*refs[:2], None))))
        return made

    down = pair(dwd, down_rows, (0, 3, 6), True)
    for item in down:
        item.start()
        item.load()

    gain_copies = [links.copy((gain_terms, 0), (gain_lands, 0), links.at_core()), links.copy((gain_terms, 1), (gain_lands, 1), links.at_b())]
    gain_copies += [links.copy((gain_terms, 2), (gain_lands, 1 + d), links.at_a(d)) for d in range(1, na)]
    gain_line = LineSum(links, (gain_terms, 3), (gain_lands, na + 1), (gain_lands, na + 2), out_gains)
    gain_terms[0] = gains[...]
    gain_copies[0].start()

    def next_gain(i):
        for copies in gain_copies[i : i + 1] if i < 2 else gain_copies[2:]:
            copies.wait()
        if i < 2:
            gain_terms[i + 1] = gain_terms[i] + gain_lands[i]
            for copies in gain_copies[1:2] if i == 0 else gain_copies[2:]:
                copies.start()
        else:
            total = gain_terms[2]
            for d in range(1, na):
                total = total + gain_lands[1 + d]
            gain_terms[3] = total
            gain_line.begin()

    def qkv_part(p):
        columns = slice(p * q_width, (p + 1) * q_width)
        mine, other = dq_both[0, p].reshape(rows, q_width), dq_both[1, p].reshape(rows, q_width)
        for k in range(chips):
            at = slice(k * block, (k + 1) * block)
            total = tn_dot(first_both[0, :, at], mine) + tn_dot(first_both[1, :, at], other)
            w_qkv_part[at, columns] = total.astype(BF16)

    def swap(sums, send, land):
        local = block // 2
        for n, item in enumerate(sums):
            total = item.finish()
            size = total.shape[1]
            send[0, :, n * size : (n + 1) * size] = total[:local]
            send[1, :, n * size : (n + 1) * size] = total[local:]
        copies = links.copy((send, 1 - core), land, links.at_core())
        copies.start()
        return copies

    out_sums = pair(w_out_part, block, (6, 8, 10), False)
    qkv_sums = pair(w_qkv_part, block, (10, 12, 14), False)
    cut = width // 2
    next_gain(0)
    for i in (1, 3):
        sends[i].wait()
    for i in (0, 1):
        loads[i].wait()
    gate_lines[0].relay()
    for k in range(chips):
        at = slice(k * block, (k + 1) * block)
        total = tn_dot(attended_both[0, :, at], low_both[0]) + tn_dot(attended_both[1, :, at], low_both[1])
        w_out_part[at, :] = total.astype(BF16)
    for item in out_sums:
        item.start()
    gate_lines[1].relay()
    next_gain(1)
    for i in (0, 2):
        sends[i].wait()
    for i in (2, 3):
        loads[i].wait()
    gate_lines[0].settle()
    for p in range(per // 2):
        qkv_part(p)
    gate_lines[2].relay()
    next_gain(2)
    gate_lines[1].settle()
    for p in range(per // 2, per):
        qkv_part(p)
    gate_lines[3].relay()
    for item in down:
        item.turn()
    for item in qkv_sums:
        item.start()
    gate_lines[2].settle()
    gain_line.relay()
    gate_lines[3].settle()
    for item in out_sums:
        item.turn()
    up_lines[0].relay()
    gain_line.settle()
    up_lines[1].relay()
    up_lines[0].settle()
    term_down[:, :cut] = down[0].finish()
    term_down[:, cut:] = down[1].finish()
    for line in down_lines:
        line.begin()
    up_lines[2].relay()
    up_lines[1].settle()
    up_lines[3].relay()
    up_lines[2].settle()
    down_lines[0].relay()
    up_lines[3].settle()
    for item in qkv_sums:
        item.turn()
    down_lines[1].relay()
    down_lines[0].settle()
    out_swap = swap(out_sums, swap_out, land_out)
    down_lines[2].relay()
    down_lines[1].settle()
    out_swap.wait()
    kept, arrived = swap_out[core], land_out[...]
    term_out[:, :cut] = jnp.where(core == 0, kept, arrived)
    term_out[:, cut:] = jnp.where(core == 0, arrived, kept)
    for line in out_lines:
        line.begin()
    down_lines[3].relay()
    down_lines[2].settle()
    qkv_swap = swap(qkv_sums, swap_qkv, land_qkv)
    out_lines[0].relay()
    down_lines[3].settle()
    qkv_swap.wait()
    kept, arrived = swap_qkv[core], land_qkv[...]
    for n in range(2):
        group = jnp.where(core == n, kept, arrived)
        for p in range(per):
            taken, start = p * q_width, 0
            for size in (kv * GROUP * HEAD_DIM, kv * HEAD_DIM, kv * HEAD_DIM):
                at = start + (n * per + p) * size
                term_qkv[:, at : at + size] = group[:, taken : taken + size]
                taken, start = taken + size, start + ns * size
    for line in qkv_lines:
        line.begin()
    out_lines[1].relay()
    out_lines[0].settle()
    qkv_lines[0].relay()
    out_lines[1].settle()
    for n in range(1, len(qkv_lines)):
        qkv_lines[n].relay()
        qkv_lines[n - 1].settle()
    qkv_lines[-1].settle()
    every_line = [*gate_lines, *up_lines, gain_line, *down_lines, *out_lines, *qkv_lines]
    for line in every_line:
        line.finish()
    for line in every_line:
        if line.store is not None:
            line.store.wait()


def finish(mesh, count, kv, term_gate, term_up, dwd, first, dqkv, attended, low, gains):
    ns, nf = mesh
    na, per = nf // 4, ns // 2
    rows, width = first.shape
    q_width = dqkv.shape[3]
    local, half = term_gate.shape[0], width // 2
    block = 2 * local
    anywhere, vmem = pl.BlockSpec(memory_space=pl.ANY), pl.BlockSpec(memory_space=pltpu.VMEM)
    down = (dwd.shape[0] // (2 * na), dwd.shape[1])
    shapes = [term_gate.shape, term_up.shape, down, (local, width), (local, ns * q_width)]
    scratch = [pltpu.VMEM(s, BF16) for s in shapes]
    scratch += [pltpu.VMEM(s, BF16) for s in shapes[2:]]
    scratch += [pltpu.VMEM((2,) + tuple(s), BF16) for s in shapes]
    scratch += [
        pltpu.VMEM((2, rows, width), BF16),
        pltpu.VMEM((2, rows, width), BF16),
        pltpu.VMEM((2, rows, half), BF16),
        pltpu.VMEM((2, per, count, rows // count, q_width), BF16),
        pltpu.VMEM((width, half), BF16),
        pltpu.VMEM((width, per * q_width), BF16),
        pltpu.VMEM((2, local, half), BF16),
        pltpu.VMEM((local, half), BF16),
        pltpu.VMEM((2, local, per * q_width), BF16),
        pltpu.VMEM((local, per * q_width), BF16),
        pltpu.VMEM((4, 2, width), F32),
        pltpu.VMEM((na + 3, 2, width), F32),
    ]
    scratch += chip_sum_shapes(na, True, down[0], down[1] // 2) + chip_sum_shapes(na, False, down[0], down[1] // 2)
    for columns in (half // 2, per * q_width // 2):
        for b_first in (True, False):
            scratch += chip_sum_shapes(na, b_first, block, columns)[:2]
    return pl.pallas_call(
        functools.partial(finish_kernel, mesh, count, kv),
        in_specs=[vmem, vmem] + [anywhere] * 5 + [vmem],
        out_specs=[anywhere] * 5 + [vmem],
        out_shape=[jax.ShapeDtypeStruct(s, BF16) for s in shapes] + [jax.ShapeDtypeStruct((2, width), F32)],
        scratch_shapes=scratch
        + [pltpu.SemaphoreType.DMA((128,)), pltpu.SemaphoreType.DMA((128,)), pltpu.SemaphoreType.DMA((64,))],
        compiler_params=pltpu.CompilerParams(vmem_limit_bytes=VMEM_MOST, collective_id=2, has_side_effects=True),
        name="finish",
    )(term_gate, term_up, dwd, first, dqkv, attended, low, gains)


def widen_kernel(cuts, *refs):
    gate, up, down, out, qkv, hidden, own, other = refs[:8]
    o_gate, o_up, o_down, o_out, o_q, o_k, o_v, o_block = refs[8:]
    for source, target in ((gate, o_gate), (up, o_up), (down, o_down), (out, o_out)):
        target[...] = source[...].astype(F32)
    for (start, end), target in zip(cuts, (o_q, o_k, o_v)):
        target[...] = qkv[:, start:end].astype(F32)
    o_block[...] = hidden[...] + own[...] + other[...].astype(F32)


def widen(gate, up, down, out, qkv, hidden, own, other, cuts):
    steps = 4
    operands = [gate, up, down, out, qkv, hidden, own, other]
    rows = out.shape[0]
    shapes = [gate.shape, up.shape, down.shape, out.shape] + [(rows, end - start) for start, end in cuts] + [hidden.shape]
    block = lambda shape: pl.BlockSpec((shape[0] // steps, shape[1]), lambda i: (i, 0))
    return pl.pallas_call(
        functools.partial(widen_kernel, cuts),
        grid=(steps,),
        in_specs=[block(x.shape) for x in operands],
        out_specs=[block(shape) for shape in shapes],
        out_shape=[jax.ShapeDtypeStruct(shape, F32) for shape in shapes],
        compiler_params=pltpu.CompilerParams(vmem_limit_bytes=VMEM_LIMIT),
        cost_estimate=pl.CostEstimate(flops=0, bytes_accessed=40 * rows * gate.shape[1], transcendentals=0),
        name="widen",
    )(*operands)


def solution(mesh):
    ns, nf = mesh.shape["seq"], mesh.shape["fsdp"]
    na = nf // 4
    chips = 2 * na
    kv = KEY_VALUE_HEADS // ns

    def body(tokens, cotangent, attention_gain, feedforward_gain, query_weight, key_matrix, value_matrix, out_weight, gate_weight, up_weight, down_weight):
        count, span, width = tokens.shape
        rows = count * span
        local = query_weight.shape[0]
        sizes = (ns, nf)
        mine = lax.axis_index("fsdp")
        cosines, sines = (jnp.asarray(x) for x in rope_tables(ns * span))
        flat = tokens.reshape(rows, width)
        grad_flat = cotangent.reshape(rows, width)
        (w_qkv, w_out, w_gate, w_down, first, packed, heads_attended, logs, attended, hidden_one, second_both, low_both, gains) = fore(
            sizes, count, kv, flat, grad_flat, attention_gain.reshape(1, local), feedforward_gain.reshape(1, local),
            query_weight, key_matrix, value_matrix, out_weight, gate_weight, down_weight, cosines, sines,
        )
        dwg, dwu, dwd, out_own, out_other, dx_own, dx_other = ffn(sizes, second_both, low_both, w_gate, w_down, up_weight, gate_weight)
        high, low, grad_tokens, gain_grads, dqkv, sum_gate, sum_up = back(
            sizes, count, kv, dx_own, dx_other, hidden_one, grad_flat, gains[1:2], w_out, w_qkv,
            packed, heads_attended, logs, cosines, sines, flat, gains[0:1], dwg, dwu,
        )
        out_arrived = lax.ppermute(out_other, "fsdp", [(i, i ^ 1) for i in range(nf)])
        *sums, gain_grads = finish(
            sizes, count, kv, sum_gate, sum_up, dwd, first, dqkv, attended, low, gain_grads
        )
        q_end, k_end = ns * kv * GROUP * HEAD_DIM, ns * kv * (GROUP + 1) * HEAD_DIM
        cuts = ((0, q_end), (q_end, k_end), (k_end, sums[4].shape[1]))
        grad_gate, grad_up, grad_down, grad_out, grad_query, grad_key, grad_value, block_out = widen(
            *sums, hidden_one, out_own, out_arrived, cuts
        )
        gain_grads = lax.dynamic_slice(gain_grads, (0, mine * local), (2, local))

        return (
            block_out.reshape(count, span, width),
            grad_tokens.reshape(count, span, width),
            gain_grads[0],
            gain_grads[1],
            grad_query,
            grad_key,
            grad_value,
            grad_out,
            grad_gate,
            grad_up,
            grad_down,
        )

    tokens_spec, gain_spec, weight_spec = P("fsdp", "seq", None), P("fsdp"), P("fsdp", None)
    return jax.shard_map(
        body,
        mesh=mesh,
        in_specs=(tokens_spec, tokens_spec, gain_spec, gain_spec) + (weight_spec,) * 7,
        out_specs=(tokens_spec, tokens_spec, gain_spec, gain_spec) + (weight_spec,) * 7,
        check_vma=False,
    )
```

```python
import functools
import math

import jax
import jax.numpy as jnp
import numpy as np
from jax import lax
from jax.experimental import pallas as pl
from jax.experimental.pallas import tpu as pltpu
from jax.sharding import PartitionSpec as P

QUERY_HEADS = 16
KEY_VALUE_HEADS = 8
HEAD_DIM = 96
GROUP = QUERY_HEADS // KEY_VALUE_HEADS
norm_eps = 1e-05
rope_base = 100000.0
masked_score = -1e30
F32, BF16 = jnp.float32, jnp.bfloat16
VMEM_LIMIT = 60 * 1024 * 1024
VMEM_MOST = 67043328
MESH = pl.DeviceIdType.MESH


def nt_dot(left, right):
    return lax.dot_general(left, right, (((1,), (1,)), ((), ())), preferred_element_type=F32)


def tn_dot(left, right):
    return lax.dot_general(left, right, (((0,), (0,)), ((), ())), preferred_element_type=F32)


def nn_dot(left, right):
    return jnp.dot(left, right, preferred_element_type=F32)


def whole(shape):
    return pl.BlockSpec(shape, lambda *_: (0,) * len(shape))


def call(kernel, scalars, operands, outs, name, flops, moved, scratch=()):
    return pl.pallas_call(
        kernel,
        grid_spec=pltpu.PrefetchScalarGridSpec(
            num_scalar_prefetch=1,
            grid=(1,),
            in_specs=[whole(x.shape) for x in operands],
            out_specs=[whole(x.shape) for x in outs],
            scratch_shapes=scratch,
        ),
        out_shape=outs,
        compiler_params=pltpu.CompilerParams(vmem_limit_bytes=VMEM_LIMIT),
        cost_estimate=pl.CostEstimate(flops=flops, bytes_accessed=moved, transcendentals=0),
        name=name,
    )(scalars, *operands)


def rope_tables(length):
    half = HEAD_DIM // 2
    freqs = np.float32(rope_base) ** (-(np.float32(2.0) * np.arange(half, dtype=np.float32)) / np.float32(HEAD_DIM))
    angles = np.arange(length, dtype=np.float32)[:, None] * freqs.astype(np.float32)[None, :]
    cosine, sine = np.cos(angles), np.sin(angles)
    return np.concatenate([cosine, cosine], 1), np.concatenate([-sine, sine], 1)


def swap_halves(values):
    half = HEAD_DIM // 2
    width = values.shape[1]
    lane = lax.broadcasted_iota(jnp.int32, values.shape, 1)
    ahead = pltpu.roll(values, width - half, 1)
    behind = pltpu.roll(values, half, 1)
    return jnp.where(lane % HEAD_DIM < half, ahead, behind)


def norm_back(grad, normed, inverse, gain):
    scaled = grad * gain
    return inverse * (scaled - normed * jnp.mean(scaled * normed, axis=1, keepdims=True))


def ffn_kernel(
    mesh, tiles, parts, x, g, wg, wd, wu, w_last, dwg, dwu, dwd, out_own, out_arrived, dx_own, dx_arrived,
    xt, acc_out, acc_dx, given_out, given_dx, act, dgate, dup, stage, land, gate, send_sems, recv_sems, local_sems,
):
    step = pl.program_id(0)
    rows = x.shape[0] // 2
    links = Links(mesh, send_sems, recv_sems, local_sems)
    chips, local, tile = tiles // parts, wu.shape[0], land.shape[2]
    cols = tile // parts
    gathers, loads = [], []
    for k in range(chips + 1):
        gathers.append(GatherHalf(links, lambda c, k=k: (stage, c, k), lambda o, k=k: (land, k, rows_at(o, local))))
        weight, tile_at = (wu, k) if k < chips else (w_last, chips - 1)
        for c in range(2):
            source = (weight, slice(None), slice((tile_at * 2 + c) * tile, (tile_at * 2 + c + 1) * tile))
            loads.append(links.local(source, (stage, c, k)))

    def begin(k):
        gathers[k].start()
        gathers[k].other_start()

    def turn(k):
        gathers[k].turn()
        gathers[k].turn_late()

    @pl.when(step == 0)
    def _():
        for load in loads:
            load.start()
        links.barrier()
        for load in loads:
            load.wait()
        gathers[0].start()

    @pl.when(step == 0)
    def _():
        acc_out[...] = jnp.zeros_like(acc_out)
        acc_dx[...] = jnp.zeros_like(acc_dx)
        xt[...] = x[...].T
        gathers[0].other_start()

    def first_part():
        turn(0)
        begin(1)
        gathers[0].finish()

    def later_part(k):
        turn(k)
        for n in (2, 3) if k == 1 else (k + 2,):
            if n <= chips:
                begin(n)
        if k == chips - 1:
            turn(chips)

    for k in range(1, chips):
        pl.when(step == (k - 1) * parts + 1)(functools.partial(later_part, k))
    pl.when(step == (chips - 1) * parts)(gathers[chips].finish)
    at = pl.ds(pl.multiple_of(lax.rem(step, parts) * cols, cols), cols)
    chip = step // parts

    @pl.when(chip < chips - 1)
    def _():
        gate[...] = wg[...]

    @pl.when(chip == chips - 1)
    def _():
        gate[...] = land[chips, :, at]

    before = []
    for i in range(2):
        here = slice(i * rows, (i + 1) * rows)
        before.append((nn_dot(x[here, :], gate[...]), nt_dot(g[here, :], wd[...])))
    pl.when(step == 0)(first_part)
    for k in range(1, chips):
        pl.when(step == k * parts)(gathers[k].finish)
    for i in range(2):
        here = slice(i * rows, (i + 1) * rows)
        gate_pre, grad = before[i]
        up = nn_dot(x[here, :], land[chip, :, at])
        sigmoid = jax.nn.sigmoid(gate_pre)
        silu = gate_pre * sigmoid
        hidden = (silu * up).astype(BF16)
        act[here, :] = hidden
        gate_grad = (grad * up * sigmoid * (1.0 + gate_pre * (1.0 - sigmoid))).astype(BF16)
        up_grad = (grad * silu).astype(BF16)
        dgate[here, :] = gate_grad
        dup[here, :] = up_grad
        acc_out[i] += nn_dot(hidden, wd[...])
        acc_dx[i] += nt_dot(gate_grad, gate[...]) + nt_dot(up_grad, land[chip, :, at])
    leaving = [
        links.copy(given_dx, dx_arrived, links.at_core()),
        links.local((acc_dx, 0), dx_own),
        links.copy(given_out, out_arrived, links.at_core()),
        links.local((acc_out, 0), out_own),
    ]

    @pl.when(step == tiles - 1)
    def _():
        given_dx[...] = acc_dx[1].astype(BF16)
        leaving[0].start()
        given_out[...] = acc_out[1].astype(BF16)
        for copies in leaving[1:]:
            copies.start()

    dwg[...] = nn_dot(xt[...], dgate[...]).astype(BF16)
    dwu[...] = nn_dot(xt[...], dup[...]).astype(BF16)
    dwd[...] = tn_dot(act[...], g[...]).astype(BF16)

    @pl.when(step == tiles - 1)
    def _():
        for copies in leaving:
            copies.wait()


def ffn(mesh, x, g, wg, wd, wu, w_last):
    rows, width = x.shape[0] // 2, x.shape[1]
    chips, tile = wg.shape[0] + 1, wg.shape[2]
    parts = 2
    tiles, cols = chips * parts, tile // parts
    local = wu.shape[0]
    keep = lambda shape: pl.BlockSpec(shape, lambda i: (0, 0), pipeline_mode=pl.Buffered(1))
    half = tile * chips
    wide, low = jax.ShapeDtypeStruct((rows, width), F32), jax.ShapeDtypeStruct((rows, width), BF16)
    return pl.pallas_call(
        functools.partial(ffn_kernel, mesh, tiles, parts),
        grid=(tiles,),
        in_specs=[
            keep(x.shape),
            keep(g.shape),
            pl.BlockSpec((None, width, cols), lambda i: (jnp.minimum(i // parts, chips - 2), 0, i % parts)),
            pl.BlockSpec((cols, width), lambda i: (i, 0)),
            pl.BlockSpec(memory_space=pl.ANY),
            pl.BlockSpec(memory_space=pl.ANY),
        ],
        out_specs=[pl.BlockSpec((width, cols), lambda i: (0, i))] * 2
        + [pl.BlockSpec((cols, width), lambda i: (i, 0))]
        + [pl.BlockSpec(memory_space=pl.ANY)] * 4,
        scratch_shapes=[pltpu.VMEM((width, 2 * rows), BF16)]
        + [pltpu.VMEM((2, rows, width), F32)] * 2
        + [pltpu.VMEM((rows, width), BF16)] * 2
        + [pltpu.VMEM((2 * rows, cols), BF16)] * 3
        + [pltpu.VMEM((2, chips + 1, local, tile), BF16), pltpu.VMEM((chips + 1, width, tile), BF16), pltpu.VMEM((width, cols), BF16)]
        + [pltpu.SemaphoreType.DMA((96,)), pltpu.SemaphoreType.DMA((96,)), pltpu.SemaphoreType.DMA((64,))],
        out_shape=[
            jax.ShapeDtypeStruct((width, half), BF16),
            jax.ShapeDtypeStruct((width, half), BF16),
            jax.ShapeDtypeStruct((half, width), BF16),
            wide,
            low,
            wide,
            low,
        ],
        compiler_params=pltpu.CompilerParams(vmem_limit_bytes=VMEM_MOST, collective_id=3, has_side_effects=True),
        cost_estimate=pl.CostEstimate(
            flops=36 * rows * width * half, bytes_accessed=12 * width * half + 20 * rows * width, transcendentals=0
        ),
        name="ffn",
    )(x, g, wg, wd, wu, w_last)


def part(x):
    return x[0].at[x[1:]] if isinstance(x, tuple) else x


def get(x):
    return x[0][x[1:]] if isinstance(x, tuple) else x[...]


def put(x, value):
    if isinstance(x, tuple):
        x[0][x[1:]] = value
    else:
        x[...] = value


class Copy:
    def __init__(self, src, dst, device, send_sem, recv_sem):
        self.src, self.dst, self.device, self.send_sem, self.recv_sem = src, dst, device, send_sem, recv_sem

    def made(self):
        if self.device is None:
            return pltpu.make_async_copy(part(self.src), part(self.dst), part(self.send_sem))
        return pltpu.make_async_remote_copy(
            src_ref=part(self.src),
            dst_ref=part(self.dst),
            send_sem=part(self.send_sem),
            recv_sem=part(self.recv_sem),
            device_id=self.device,
            device_id_type=MESH,
        )

    def start(self):
        self.made().start()

    def wait(self):
        self.made().wait()

    def wait_send(self):
        self.made().wait_send()

    def wait_recv(self):
        self.made().wait_recv()


class Links:
    def __init__(self, mesh, send_sems, recv_sems, local_sems):
        self.ns, self.nf = mesh
        self.na = self.nf // 4
        self.send_sems, self.recv_sems, self.local_sems = send_sems, recv_sems, local_sems
        self.count, self.local_count = 0, 0
        self.z, self.f = lax.axis_index("seq"), lax.axis_index("fsdp")
        self.core = lax.rem(self.f, 2)
        self.b = lax.rem(self.f // 2, 2)
        self.a = self.f // 4

    def chip(self, da, db):
        return lax.rem(self.a + da, self.na) * 2 + lax.rem(self.b + db, 2)

    def at_core(self):
        return (self.z, self.f + 1 - 2 * self.core)

    def at_b(self):
        return (self.z, self.f + 2 - 4 * self.b)

    def at_a(self, d):
        return (self.z, lax.rem(self.f + 4 * d, self.nf))

    def at_z(self, d):
        return (lax.rem(self.z + d, self.ns), self.f)

    def peers(self):
        return [self.at_core(), self.at_b()] + [self.at_a(d) for d in range(1, self.na)] + [self.at_z(d) for d in range(1, self.ns)]

    def barrier(self):
        barrier = pltpu.get_barrier_semaphore()
        peers = self.peers()
        for peer in peers:
            pl.semaphore_signal(barrier, inc=1, device_id=peer, device_id_type=MESH)
        pl.semaphore_wait(barrier, len(peers))

    def copy(self, src, dst, device):
        index = self.count
        self.count += 1
        return Copy(src, dst, device, (self.send_sems, index), (self.recv_sems, index))

    def again(self, src, dst, device):
        index = self.count - 1
        return Copy(src, dst, device, (self.send_sems, index), (self.recv_sems, index))

    def local(self, src, dst):
        index = self.local_count
        self.local_count += 1
        return Copy(src, dst, None, (self.local_sems, index), None)


def line_place(links):
    z, ns = links.z, links.ns
    middle = ns // 2
    step = jnp.where(z < middle, 1, -1)
    end = (z == 0) | (z == ns - 1)
    inner = (z == middle - 1) | (z == middle)
    return end, inner, (z + step, links.f), (z - step, links.f)


GATE_PIECES = 4


def first_piece(ns, columns):
    return columns // GATE_PIECES if ns == 4 else 0


def rows_at(start, size):
    return pl.ds(pl.multiple_of(start * size, size), size)


class ChipSum:
    def __init__(self, links, partial, b_first, arrived, passed, staging):
        self.links, self.partial, self.b_first = links, partial, b_first
        self.arrived, self.passed, self.staging = arrived, passed, staging
        na = links.na
        self.first, self.second = [], []
        if b_first:
            self.kept = [links.chip(da, 0) for da in range(na)]
            for da in range(na):
                self.first.append(links.copy(partial(links.chip(da, 1)), (arrived, da), links.at_b()))
            for d in range(1, na):
                self.second.append(links.copy((arrived, d), (passed, d - 1), links.at_a(d)))
        else:
            self.kept = [links.chip(0, db) for db in range(2)]
            for d in range(1, na):
                for db in range(2):
                    self.first.append(links.copy(partial(links.chip(d, db)), (arrived, (d - 1) * 2 + db), links.at_a(d)))
            self.second.append(links.copy((arrived, 1), (passed, 0), links.at_b()))
        self.loads = [] if staging is None else [links.local(partial(k), (staging, i)) for i, k in enumerate(self.kept)]

    def start(self):
        for copy in self.first:
            copy.start()

    def load(self):
        for load in self.loads:
            load.start()

    def turn(self):
        for load in self.loads:
            load.wait()
        for copy in self.first:
            copy.wait()
        count = len(self.kept)
        for i in [*range(1, count), 0]:
            own = self.partial(self.kept[i]) if self.staging is None else (self.staging, i)
            total = get(own).astype(F32)
            if self.b_first:
                total = total + self.arrived[i].astype(F32)
            else:
                for d in range(self.links.na - 1):
                    total = total + self.arrived[d * 2 + i].astype(F32)
            self.arrived[i] = total.astype(BF16)
            if i > 0 and self.b_first:
                self.second[i - 1].start()
            elif i > 0:
                self.second[0].start()

    def finish(self):
        for copy in self.second:
            copy.wait()
        total = self.arrived[0].astype(F32)
        for i in range(len(self.second)):
            total = total + self.passed[i].astype(F32)
        return total.astype(BF16)


def chip_sum_shapes(na, b_first, rows, columns):
    first = na if b_first else 2 * (na - 1)
    kept = na if b_first else 2
    return [
        pltpu.VMEM((max(first, kept), rows, columns), BF16),
        pltpu.VMEM((na - 1 if b_first else 1, rows, columns), BF16),
        pltpu.VMEM((kept, rows, columns), BF16),
    ]


def flip_core(f):
    return f + 1 - 2 * lax.rem(f, 2)


def flip_b(f):
    return f + 2 - 4 * lax.rem(f // 2, 2)


class Gather:
    def __init__(self, links, own, land, both):
        self.links = links
        f, na, nf = links.f, links.na, links.nf
        to_core, to_b = links.at_core(), links.at_b()

        def move(origin, device, half=None):
            return links.copy(land(origin, half), land(origin, half), device)

        self.given = [links.copy(own, land(f, None), to_core)] if both else []
        self.own = [links.copy(own, land(f, None), to_b)]
        self.own += [links.copy(own, land(f, None), links.at_a(d)) for d in range(1, na)]
        from_b = flip_b(f)
        from_a = [lax.rem(f + nf - 4 * d, nf) for d in range(1, na)]
        if na == 2:
            self.relays = [move(from_b, links.at_a(1), 1), move(from_a[0], to_b, 0)]
            far = [(flip_b(from_a[0]), 0), (flip_b(from_a[0]), 1)]
        else:
            self.relays = [move(origin, to_b) for origin in from_a]
            far = [(flip_b(origin), None) for origin in from_a]
        near = [from_b, *from_a]
        self.near = [move(origin, to_core) for origin in near] if both else []
        self.far = [move(origin, to_core, half) for origin, half in far] if both else []

    def start(self):
        for copies in self.own + self.given:
            copies.start()

    def turn(self):
        for copies in self.own:
            copies.wait()
        for copies in self.relays + self.near:
            copies.start()

    def pass_on(self):
        for copies in self.relays:
            copies.wait()
        for copies in self.far:
            copies.start()

    def finish(self):
        for copies in self.given + self.near + self.far:
            copies.wait()


class GatherHalf:
    def __init__(self, links, stage, land):
        self.links = links
        f, na, nf, core = links.f, links.na, links.nf, links.core
        to_b = links.at_b()

        def move(origin, device):
            return links.copy(land(origin), land(origin), device)

        self.swap = links.copy(stage(1 - core), land(f), links.at_core())
        self.kept = links.local(stage(core), land(f))
        targets = [to_b] + [links.at_a(d) for d in range(1, na)]
        self.own = [links.copy(stage(core), land(f), device) for device in targets]
        self.other = [move(flip_core(f), device) for device in targets]
        from_b = flip_b(f)
        from_a = [lax.rem(f + nf - 4 * d, nf) for d in range(1, na)]
        if na == 2:
            self.relays = [move(from_b, links.at_a(1))]
            self.late = [move(flip_core(from_a[0]), to_b)]
        else:
            self.relays = [move(origin, to_b) for origin in from_a]
            self.late = [move(flip_core(origin), to_b) for origin in from_a]

    def start(self):
        for copies in [self.swap, self.kept, *self.own]:
            copies.start()

    def other_start(self):
        self.swap.wait()
        for copies in self.other:
            copies.start()

    def turn(self):
        for copies in self.own:
            copies.wait()
        for copies in self.relays:
            copies.start()

    def turn_late(self):
        for copies in self.other:
            copies.wait()
        for copies in self.late:
            copies.start()

    def finish(self):
        for copies in [self.kept, *self.relays, *self.late]:
            copies.wait()


def attend_heads(ns, kv, span, qs, ks, vs, out, logs):
    scale = 1.0 / math.sqrt(HEAD_DIM)
    row = lax.broadcasted_iota(jnp.int32, (span, span), 0)
    column = lax.broadcasted_iota(jnp.int32, (span, span), 1)
    causal = row >= column
    lane = lax.broadcasted_iota(jnp.int32, (span, 128), 1)
    for s in range(ns):
        here = slice(s * span, (s + 1) * span)
        stats = jnp.zeros((span, 128), F32)
        for h in range(kv * GROUP):
            g = h // GROUP
            q = qs[h, here, :]
            near = jnp.where(causal, nt_dot(q, ks[g, here, :]) * scale, masked_score)
            top = jnp.max(near, axis=1, keepdims=True)
            if s > 0:
                far = nt_dot(q, ks[g, : s * span, :]) * scale
                top = jnp.maximum(top, jnp.max(far, axis=1, keepdims=True))
            near = jnp.exp(near - top)
            total = jnp.sum(near, axis=1, keepdims=True)
            if s > 0:
                far = jnp.exp(far - top)
                total = total + jnp.sum(far, axis=1, keepdims=True)
            inverse = 1.0 / total
            result = nn_dot((near * inverse).astype(BF16), vs[g, here, :])
            if s > 0:
                result = result + nn_dot((far * inverse).astype(BF16), vs[g, : s * span, :])
            stats = jnp.where(lane == h, top + jnp.log(total), stats)
            out[s, :, h * HEAD_DIM : (h + 1) * HEAD_DIM] = result.astype(BF16)
        logs[here, :] = stats


def fill_tables(cosines, sines, narrow_cosines, narrow_sines, heads):
    end = heads * HEAD_DIM
    cosines[:, end:] = jnp.ones((cosines.shape[0], cosines.shape[1] - end), F32)
    sines[:, end:] = jnp.zeros((cosines.shape[0], cosines.shape[1] - end), F32)
    for h in range(heads):
        at = slice(h * HEAD_DIM, (h + 1) * HEAD_DIM)
        cosines[:, at] = narrow_cosines
        sines[:, at] = narrow_sines


def fore_kernel(
    mesh, count, kv,
    tokens, cotangent, gains_in, wq, wk, wv, wo, wg, wd, narrow_cosines, narrow_sines,
    w_qkv, w_out, w_gate, w_down, first_out, packed, heads_attended, logs, attended_out, hidden_out, second_both, low_both, gains_out,
    rows_in, hidden, first, pack, w_land, wo_land, q_send, q_land, a_send, a_land, stage_gate, gain_send, gain_land,
    qs, ks, vs, log, attended, second, second_abs, low, cosines, sines, send_sems, recv_sems, local_sems,
):
    links = Links(mesh, send_sems, recv_sems, local_sems)
    ns, na, nf = links.ns, links.na, links.nf
    chips = 2 * na
    z, f, core = links.z, links.f, links.core
    rows, width = rows_in.shape
    span = rows // count
    heads = kv * GROUP
    g_width, k_width = heads * HEAD_DIM, kv * HEAD_DIM
    q_width = g_width + 2 * k_width
    local = width // nf
    links.barrier()

    token_load = links.local(tokens, rows_in)
    token_load.start()
    cot_load = links.local(cotangent, hidden)
    cot_load.start()
    gain_send[...] = jnp.zeros_like(gain_send)
    gain_send[0:2, :local] = gains_in[...].astype(F32)
    for j in range(ns):
        pack[j, :, :g_width] = wq[:, j * g_width : (j + 1) * g_width]
        pack[j, :, g_width : g_width + k_width] = wk[:, j * k_width : (j + 1) * k_width]
        pack[j, :, g_width + k_width :] = wv[:, j * k_width : (j + 1) * k_width]

    every = slice(None)

    def piece(start, size, half):
        if half is None:
            return rows_at(start, size)
        return rows_at(start * 2 + half, size // 2)

    units = []
    turns = [*range(1, ns), 0]
    for d in turns:
        g = lax.rem(z + d, ns)
        units.append(Gather(links, (pack, g), lambda o, half, g=g: (w_land, g, piece(o, local, half)), True))
    units.append(Gather(links, wo, lambda o, half: (wo_land, piece(o, local, half)), True))
    depth = wd.shape[0]
    units.append(Gather(links, wd, lambda o, half: (w_down, piece(o // 2, depth, half)), False))
    gate_unit = GatherHalf(links, lambda c: (stage_gate, c), lambda o: (w_gate, every, rows_at(o, local)))
    q_copies, a_copies = [], []
    for d in range(1, ns):
        g = lax.rem(z + d, ns)
        q_copies.append([links.copy((q_send, g, i), (q_land, i, z), links.at_z(d)) for i in range(count)])
    for i in range(count):
        a_copies.append([links.copy((a_send, i, lax.rem(z + d, ns)), (a_land, i, z), links.at_z(d)) for d in range(1, ns)])
    second_copy = links.copy(second_abs, (second_both, pl.ds(rows, rows)), links.at_core())
    low_copy = links.copy(low, (low_both, pl.ds(rows, rows)), links.at_core())

    def gain_at(start, size):
        return (gain_land, pl.ds(start, size))

    pair, chip_four = f // 2 * 2, f // 4 * 4
    gain_copies = [
        [links.copy(gain_at(f, 1), gain_at(f, 1), links.at_core())],
        [links.copy(gain_at(pair, 2), gain_at(pair, 2), links.at_b())],
        [links.copy(gain_at(chip_four, 4), gain_at(chip_four, 4), links.at_a(d)) for d in range(1, na)],
    ]
    stores = []

    def store(src, dst):
        copies = links.local(src, dst)
        copies.start()
        stores.append(copies)

    gain_land[f] = gain_send[...]
    for copies in gain_copies[0]:
        copies.start()
    units[0].start()
    units[1].start()
    for j in range(ns):
        w_land[j, rows_at(f, local), :] = pack[j]
    stage_loads = []
    tile = w_gate.shape[2]
    for c in range(2):
        for k in range(chips - 1):
            source = (wg, every, slice((k * 2 + c) * tile, (k * 2 + c + 1) * tile))
            stage_loads.append(links.local(source, (stage_gate, c, k)))
    for load in stage_loads:
        load.start()
    store_own = [links.local(wo, (wo_land, rows_at(f, local))), links.local(wd, (w_down, rows_at(f // 2, depth)))]
    for copies in store_own:
        copies.start()
    fill_tables(cosines, sines, narrow_cosines[rows_at(z, span), :], narrow_sines[rows_at(z, span), :], heads + kv)
    token_load.wait()
    old = rows_in[...]
    inverse = lax.rsqrt(jnp.mean(old * old, axis=1, keepdims=True) + norm_eps)
    for stage in range(3):
        for copies in gain_copies[stage]:
            copies.wait()
        if stage < 2:
            for copies in gain_copies[stage + 1]:
                copies.start()
    for j in range(nf):
        gains_out[:, j * local : (j + 1) * local] = gain_land[j, 0:2, :local]
    first[...] = (old * inverse * gains_out[0:1, :]).astype(BF16)
    store(first, first_out)

    def project(n):
        g = lax.rem(z + turns[n], ns)
        units[n].finish()
        y = nn_dot(first[...], w_land[g])
        for i in range(count):
            part = y[i * span : (i + 1) * span]
            part = (part * cosines[...] + swap_halves(part) * sines[...]).astype(BF16)
            if turns[n] == 0:
                q_land[i, z] = part
            else:
                q_send[g, i] = part
        if turns[n] > 0:
            q_copies[turns[n] - 1][0].start()
        if n > 0 and turns[n - 1] > 0:
            for copies in q_copies[turns[n - 1] - 1][1:]:
                copies.start()
        store((w_land, g), (w_qkv, g))

    last = len(units)
    for n in range(ns):
        units[n].turn()
        if n + 2 < last:
            units[n + 2].start()
        if n > 0:
            units[n - 1].pass_on()
        if n > 1:
            project(n - 2)
    units[ns].turn()
    for load in stage_loads:
        load.wait()
    gate_unit.start()
    units[ns - 1].pass_on()
    project(ns - 2)
    gate_unit.other_start()
    project(ns - 1)
    units[ns].pass_on()
    cot_load.wait()
    low[...] = hidden[...].astype(BF16)
    low_copy.start()
    store(low, (low_both, pl.ds(0, rows)))

    def attend(i):
        for copies in q_copies:
            copies[i].wait()
        for j in range(ns):
            at = slice(j * span, (j + 1) * span)
            for h in range(heads):
                qs[h, at, :] = q_land[i, j, :, h * HEAD_DIM : (h + 1) * HEAD_DIM]
            for h in range(kv):
                k0, v0 = (heads + h) * HEAD_DIM, (heads + kv + h) * HEAD_DIM
                ks[h, at, :] = q_land[i, j, :, k0 : k0 + HEAD_DIM]
                vs[h, at, :] = q_land[i, j, :, v0 : v0 + HEAD_DIM]
        attend_heads(ns, kv, span, qs, ks, vs, a_send.at[i], log.at[i])
        for copies in a_copies[i]:
            copies.start()
        a_land[i, z] = a_send[i, z]

    for i in range(count):
        attend(i)
        if i == 0:
            units[ns + 1].turn()
            units[ns].finish()
            store_own[0].wait()
            store(wo_land, w_out)
    store(q_land, packed)
    store(a_send, heads_attended)
    store(log, logs)
    for i in range(count):
        for copies in a_copies[i]:
            copies.wait()
        for j in range(ns):
            attended[i * span : (i + 1) * span, j * g_width : (j + 1) * g_width] = a_land[i, j]
    new = rows_in[...] + nn_dot(attended[...], wo_land[...])
    hidden[...] = new
    inverse = lax.rsqrt(jnp.mean(new * new, axis=1, keepdims=True) + norm_eps)
    second_abs[...] = (new * inverse * gains_out[1:2, :]).astype(BF16)
    second_copy.start()
    store(second_abs, (second_both, pl.ds(0, rows)))
    store(attended, attended_out)
    store(hidden, hidden_out)
    units[ns + 1].pass_on()
    gate_unit.turn()
    gate_unit.turn_late()
    gate_unit.finish()
    second_copy.wait()
    low_copy.wait()
    store_own[1].wait()
    for copies in stores:
        copies.wait()


def fore(mesh, count, kv, tokens, cotangent, gains_in, wq, wk, wv, wo, wg, wd, narrow_cosines, narrow_sines):
    ns, nf = mesh
    na = nf // 4
    chips = 2 * na
    rows, width = tokens.shape
    span = rows // count
    length = ns * span
    heads = kv * GROUP
    g_width = heads * HEAD_DIM
    q_width = g_width + 2 * kv * HEAD_DIM
    local, depth = wq.shape[0], wd.shape[0]
    tile = wg.shape[1] // (2 * chips)
    anywhere, vmem = pl.BlockSpec(memory_space=pl.ANY), pl.BlockSpec(memory_space=pltpu.VMEM)
    low = lambda *shape: jax.ShapeDtypeStruct(shape, BF16)
    wide = lambda *shape: jax.ShapeDtypeStruct(shape, F32)
    outs = [
        low(ns, width, q_width),
        low(width, width),
        low(chips - 1, width, tile),
        low(chips * depth, width),
        low(rows, width),
        low(count, ns, span, q_width),
        low(count, ns, span, g_width),
        wide(count, length, 128),
        low(rows, width),
        wide(rows, width),
        low(2 * rows, width),
        low(2 * rows, width),
        wide(2, width),
    ]
    scratch = [
        pltpu.VMEM((rows, width), F32),
        pltpu.VMEM((rows, width), F32),
        pltpu.VMEM((rows, width), BF16),
        pltpu.VMEM((ns, local, q_width), BF16),
        pltpu.VMEM((ns, width, q_width), BF16),
        pltpu.VMEM((width, width), BF16),
        pltpu.VMEM((ns, count, span, q_width), BF16),
        pltpu.VMEM((count, ns, span, q_width), BF16),
        pltpu.VMEM((count, ns, span, g_width), BF16),
        pltpu.VMEM((count, ns, span, g_width), BF16),
        pltpu.VMEM((2, chips - 1, local, tile), BF16),
        pltpu.VMEM((8, 256), F32),
        pltpu.VMEM((nf, 8, 256), F32),
        pltpu.VMEM((heads, length, HEAD_DIM), BF16),
        pltpu.VMEM((kv, length, HEAD_DIM), BF16),
        pltpu.VMEM((kv, length, HEAD_DIM), BF16),
        pltpu.VMEM((count, length, 128), F32),
        pltpu.VMEM((rows, width), BF16),
        pltpu.VMEM((8, 128), BF16),
        pltpu.VMEM((rows, width), BF16),
        pltpu.VMEM((rows, width), BF16),
        pltpu.VMEM((span, q_width), F32),
        pltpu.VMEM((span, q_width), F32),
    ]
    return pl.pallas_call(
        functools.partial(fore_kernel, mesh, count, kv),
        in_specs=[anywhere] * 2 + [vmem] * 4 + [anywhere] * 3 + [vmem] * 2,
        out_specs=[anywhere] * 12 + [vmem],
        out_shape=outs,
        scratch_shapes=scratch
        + [pltpu.SemaphoreType.DMA((160,)), pltpu.SemaphoreType.DMA((160,)), pltpu.SemaphoreType.DMA((64,))],
        compiler_params=pltpu.CompilerParams(vmem_limit_bytes=VMEM_MOST, collective_id=0, has_side_effects=True),
        name="fore",
    )(tokens, cotangent, gains_in, wq, wk, wv, wo, wg, wd, narrow_cosines, narrow_sines)


def attend_back_heads(ns, kv, span, qs, ks, vs, gs, attended, logs, dk, dv, result):
    scale = 1.0 / math.sqrt(HEAD_DIM)
    heads = kv * GROUP
    row = lax.broadcasted_iota(jnp.int32, (span, span), 0)
    column = lax.broadcasted_iota(jnp.int32, (span, span), 1)
    causal = row >= column
    dk[...] = jnp.zeros_like(dk)
    dv[...] = jnp.zeros_like(dv)
    for s in range(ns):
        here = slice(s * span, (s + 1) * span)
        for h in range(heads):
            g = h // GROUP
            q, grad = qs[h, here, :], gs[h, here, :]
            log_total = logs[here, h : h + 1]
            out = attended[s, :, h * HEAD_DIM : (h + 1) * HEAD_DIM]
            delta = jnp.sum(grad.astype(F32) * out.astype(F32), axis=1, keepdims=True)
            k, v = ks[g, here, :], vs[g, here, :]
            near = jnp.where(causal, jnp.exp(nt_dot(q, k) * scale - log_total), 0.0)
            slope = (near * (nt_dot(grad, v) - delta) * scale).astype(BF16)
            dq = nn_dot(slope, k)
            dk[g, here, :] += tn_dot(slope, q)
            dv[g, here, :] += tn_dot(near.astype(BF16), grad)
            if s > 0:
                before = slice(0, s * span)
                k, v = ks[g, before, :], vs[g, before, :]
                far = jnp.exp(nt_dot(q, k) * scale - log_total)
                slope = (far * (nt_dot(grad, v) - delta) * scale).astype(BF16)
                dq = dq + nn_dot(slope, k)
                dk[g, before, :] += tn_dot(slope, q)
                dv[g, before, :] += tn_dot(far.astype(BF16), grad)
            result[here, h * HEAD_DIM : (h + 1) * HEAD_DIM] = dq
    for g in range(kv):
        k0 = (heads + g) * HEAD_DIM
        v0 = (heads + kv + g) * HEAD_DIM
        result[:, k0 : k0 + HEAD_DIM] = dk[g]
        result[:, v0 : v0 + HEAD_DIM] = dv[g]


def back_kernel(
    mesh, count, kv,
    dx_own, dx_other, hidden, cotangent, gains, w_out, w_qkv, packed, attended, logs, cosines, sines, tokens, dwg, dwu,
    high, low_out, out, gain_grads, dqkv, sum_gate, sum_up,
    low, sum_rows, sum_land, dx_land, g_send, g_land, q_send, q_land, swap_send, swap_land, *rest,
):
    parts, (send_sems, recv_sems, local_sems) = rest[:-3], rest[-3:]
    links = Links(mesh, send_sems, recv_sems, local_sems)
    ns, na = links.ns, links.na
    chips = 2 * na
    z, core = links.z, links.core
    rows, width = hidden.shape
    span = rows // count
    length = ns * span
    heads = kv * GROUP
    g_width, q_width = heads * HEAD_DIM, (heads + 2 * kv) * HEAD_DIM
    half = dwg.shape[1]
    block = width // chips
    links.barrier()

    dx_load = links.local(dx_other, dx_land)
    dx_load.start()
    sums = []
    for n, source in enumerate((dwg, dwu)):
        for b_first in (True, False):
            columns = slice(0, half // 2) if b_first else slice(half // 2, half)
            at = (n * 2 + (0 if b_first else 1)) * 3
            partial = lambda k, source=source, columns=columns: (source, rows_at(k, block), columns)
            sums.append(ChipSum(links, partial, b_first, *parts[at : at + 3]))
    for item in sums:
        item.start()
        item.load()

    g_copies, q_copies = [], []
    for i in range(count):
        g_copies.append([links.copy((g_send, i, lax.rem(z + d, ns)), (g_land, i, z), links.at_z(d)) for d in range(1, ns)])
        q_copies.append([links.copy((q_send, i, lax.rem(z + d, ns)), (q_land, z, i), links.at_z(d)) for d in range(1, ns)])

    def out_back(dx, old, grad, w):
        loads = [links.local(dx_own, dx), links.local(hidden, old), links.local(cotangent, grad), links.local(w_out, w)]
        for load in loads:
            load.start()
        dx_load.wait()
        for load in loads[:3]:
            load.wait()
        step = dx[...] + dx_land[...].astype(F32)
        inverse = lax.rsqrt(jnp.mean(old[...] * old[...], axis=1, keepdims=True) + norm_eps)
        normed = old[...] * inverse
        gain_grads[1:2, :] = jnp.sum(step * normed, axis=0, keepdims=True)
        grad[...] = grad[...] + norm_back(step, normed, inverse, gains[1:2, :])
        low[...] = grad[...].astype(BF16)
        stores = [links.local(grad, high), links.local(low, low_out)]
        for store in stores:
            store.start()
        loads[3].wait()
        for i in range(count):
            here = slice(i * span, (i + 1) * span)
            part = nt_dot(low[here, :], w[...]).astype(BF16)
            for j in range(ns):
                g_send[i, j] = part[:, j * g_width : (j + 1) * g_width]
            for copies in g_copies[i]:
                copies.start()
            g_land[i, z] = g_send[i, z]
        for store in stores:
            store.wait()

    pl.run_scoped(
        out_back,
        pltpu.VMEM((rows, width), F32),
        pltpu.VMEM((rows, width), F32),
        pltpu.VMEM((rows, width), F32),
        pltpu.VMEM((width, width), BF16),
    )

    def attention(qkv, mid, log, qs, ks, vs, gs, dk, dv, result, cosine, sine):
        fill_tables(cosine, sine, cosines[...], sines[...], heads + kv)
        for i in range(count):
            loads = [links.local((packed, i), qkv), links.local((attended, i), mid), links.local((logs, i), log)]
            for load in loads:
                load.start()
            for load in loads:
                load.wait()
            for j in range(ns):
                at = slice(j * span, (j + 1) * span)
                for h in range(heads):
                    qs[h, at, :] = qkv[j, :, h * HEAD_DIM : (h + 1) * HEAD_DIM]
                for h in range(kv):
                    k0, v0 = (heads + h) * HEAD_DIM, (heads + kv + h) * HEAD_DIM
                    ks[h, at, :] = qkv[j, :, k0 : k0 + HEAD_DIM]
                    vs[h, at, :] = qkv[j, :, v0 : v0 + HEAD_DIM]
            for copies in g_copies[i]:
                copies.wait()
            for j in range(ns):
                for h in range(heads):
                    gs[h, j * span : (j + 1) * span, :] = g_land[i, j, :, h * HEAD_DIM : (h + 1) * HEAD_DIM]
            attend_back_heads(ns, kv, span, qs, ks, vs, gs, mid, log, dk, dv, result)
            for j in range(ns):
                here = slice(j * span, (j + 1) * span)
                part = result[here, :]
                q_send[i, j] = (part * cosine[here, :] - swap_halves(part) * sine[here, :]).astype(BF16)
            for copies in q_copies[i]:
                copies.start()
            q_land[z, i] = q_send[i, z]
            if i < len(sums) // 2:
                for item in sums[2 * i : 2 * i + 2]:
                    item.turn()

    pl.run_scoped(
        attention,
        pltpu.VMEM((ns, span, q_width), BF16),
        pltpu.VMEM((ns, span, g_width), BF16),
        pltpu.VMEM((length, 128), F32),
        pltpu.VMEM((heads, length, HEAD_DIM), BF16),
        pltpu.VMEM((kv, length, HEAD_DIM), BF16),
        pltpu.VMEM((kv, length, HEAD_DIM), BF16),
        pltpu.VMEM((heads, length, HEAD_DIM), BF16),
        pltpu.VMEM((kv, length, HEAD_DIM), F32),
        pltpu.VMEM((kv, length, HEAD_DIM), F32),
        pltpu.VMEM((length, q_width), F32),
        pltpu.VMEM((length, q_width), F32),
        pltpu.VMEM((length, q_width), F32),
    )

    swaps = []
    local = block // 2
    for item in sums[2 * count :]:
        item.turn()

    def swap(n):
        for m in range(2):
            total = sums[2 * n + m].finish()
            swap_send[n, m, 0] = total[:local]
            swap_send[n, m, 1] = total[local:]
        for m in range(2):
            copies = links.copy((swap_send, n, m, 1 - core), (swap_land, n, m), links.at_core())
            copies.start()
            swaps.append(copies)

    tile = half // chips
    stores = []
    early = first_piece(ns, 2 * half)
    piece = (sum_rows, 0, slice(None), slice(0, max(early, 1)))
    end, inner, inward = line_place(links)[:3]
    early_copy = links.copy(piece, sum_land, inward)

    def combine(n, total):
        for m in range(2):
            swaps[2 * n + m].wait()
            kept, arrived = swap_send[n, m, core], swap_land[n, m]
            for t in range(chips // 2):
                here = slice(t * tile, (t + 1) * tile)
                k = m * (chips // 2) + t
                one, two = kept[:, here], arrived[:, here]
                sum_rows[n, :, 2 * k * tile : (2 * k + 1) * tile] = jnp.where(core == 0, one, two)
                sum_rows[n, :, (2 * k + 1) * tile : (2 * k + 2) * tile] = jnp.where(core == 0, two, one)
        if n == 0 and early:
            pl.when(end)(early_copy.start)
        else:
            copies = links.local((sum_rows, n), total)
            copies.start()
            stores.append(copies)

    def project_back(w, old, base, grad):
        loads = [links.local(tokens, old), links.local(high, base), links.local(w_qkv, w)]
        for load in loads:
            load.start()
        swap(0)
        for load in loads:
            load.wait()
        for i in range(count):
            here = slice(i * span, (i + 1) * span)
            if i == count - 1:
                combine(0, sum_gate)
                swap(1)
                combine(1, sum_up)
            for copies in q_copies[i]:
                copies.wait()
            total = nt_dot(q_land[0, i], w[0])
            for j in range(1, ns):
                total = total + nt_dot(q_land[j, i], w[j])
            grad[here, :] = total
            copies = links.local((q_land, slice(None), i), (dqkv, slice(None), i))
            copies.start()
            stores.append(copies)
            step, rows_old = grad[here, :], old[here, :]
            inverse = lax.rsqrt(jnp.mean(rows_old * rows_old, axis=1, keepdims=True) + norm_eps)
            normed = rows_old * inverse
            part_sum = jnp.sum(step * normed, axis=0, keepdims=True)
            gain_grads[0:1, :] = part_sum if i == 0 else gain_grads[0:1, :] + part_sum
            base[here, :] = base[here, :] + norm_back(step, normed, inverse, gains[0:1, :])
            copies = links.local((base, here), (out, here))
            copies.start()
            stores.append(copies)
        if early:

            @pl.when(inner)
            def _():
                early_copy.wait_recv()
                put(piece, (get(piece).astype(F32) + sum_land[...].astype(F32)).astype(BF16))

            pl.when(end)(early_copy.wait_send)
            copies = links.local((sum_rows, 0), sum_gate)
            copies.start()
            stores.append(copies)
        for copies in stores:
            copies.wait()

    pl.run_scoped(
        project_back,
        pltpu.VMEM((ns, width, q_width), BF16),
        pltpu.VMEM((rows, width), F32),
        pltpu.VMEM((rows, width), F32),
        pltpu.VMEM((rows, width), F32),
    )


def back(mesh, count, kv, dx_own, dx_other, hidden, cotangent, gains, w_out, w_qkv, packed, attended, logs, cosines, sines, tokens, dwg, dwu):
    ns, nf = mesh
    na = nf // 4
    rows, width = hidden.shape
    span = rows // count
    heads = kv * GROUP
    g_width, q_width = heads * HEAD_DIM, (heads + 2 * kv) * HEAD_DIM
    half = dwg.shape[1]
    block = width // (2 * na)
    local = block // 2
    anywhere = pl.BlockSpec(memory_space=pl.ANY)
    vmem = pl.BlockSpec(memory_space=pltpu.VMEM)
    operands = [dx_own, dx_other, hidden, cotangent, gains, w_out, w_qkv, packed, attended, logs, cosines, sines, tokens, dwg, dwu]
    wide = jax.ShapeDtypeStruct((rows, width), F32)
    summed = jax.ShapeDtypeStruct((local, 2 * half), BF16)
    scratch = [
        pltpu.VMEM((rows, width), BF16),
        pltpu.VMEM((2, local, 2 * half), BF16),
        pltpu.VMEM((local, max(first_piece(ns, 2 * half), 128)), BF16),
        pltpu.VMEM((rows, width), BF16),
        pltpu.VMEM((count, ns, span, g_width), BF16),
        pltpu.VMEM((count, ns, span, g_width), BF16),
        pltpu.VMEM((count, ns, span, q_width), BF16),
        pltpu.VMEM((ns, count, span, q_width), BF16),
        pltpu.VMEM((2, 2, 2, local, half // 2), BF16),
        pltpu.VMEM((2, 2, local, half // 2), BF16),
    ]
    for _ in range(2):
        for b_first in (True, False):
            scratch += chip_sum_shapes(na, b_first, block, half // 2)
    return pl.pallas_call(
        functools.partial(back_kernel, mesh, count, kv),
        in_specs=[vmem if x.shape[0] == 2 and x.ndim == 2 or x.shape[1] == HEAD_DIM else anywhere for x in operands],
        out_specs=[anywhere, anywhere, anywhere, vmem, anywhere, anywhere, anywhere],
        out_shape=[
            wide,
            jax.ShapeDtypeStruct((rows, width), BF16),
            wide,
            jax.ShapeDtypeStruct((2, width), F32),
            jax.ShapeDtypeStruct((ns, count, span, q_width), BF16),
            summed,
            summed,
        ],
        scratch_shapes=scratch
        + [pltpu.SemaphoreType.DMA((64,)), pltpu.SemaphoreType.DMA((64,)), pltpu.SemaphoreType.DMA((64,))],
        compiler_params=pltpu.CompilerParams(vmem_limit_bytes=VMEM_MOST, collective_id=1, has_side_effects=True),
        name="back",
    )(*operands)


class LineSum:
    def __init__(self, links, term, first, second, total, out=None, begun=False):
        self.links, self.term, self.first, self.second, self.total = links, term, first, second, total
        self.dtype = (term[0] if isinstance(term, tuple) else term).dtype
        self.deep = links.ns // 2 > 1
        self.begun = begun
        self.end, self.inner, inward, outward = line_place(links)
        moved = self.deep and not begun
        self.inward = links.copy(term, first, inward) if moved else None
        self.onward = links.again(first, first, inward) if moved else None
        self.sum = first if moved else term
        self.across = links.copy(self.sum, second, inward)
        self.outward = links.copy(total, total, outward) if self.deep else None
        self.store = links.local(total, out) if out is not None else None

    def keep(self):
        if self.store is not None:
            self.store.start()

    def add(self, target, one, two):
        put(target, (get(one).astype(F32) + get(two).astype(F32)).astype(self.dtype))

    def begin(self):
        if self.begun:
            pl.when(self.inner)(self.across.start)
        elif self.deep:
            pl.when(self.end)(self.inward.start)
        else:
            self.across.start()

    def relay(self):
        if not self.deep or self.begun:
            return

        @pl.when(jnp.logical_not(self.end))
        def _():
            self.inward.wait_recv()
            self.add(self.first, self.term, self.first)
            pl.when(self.inner)(self.across.start)
            pl.when(jnp.logical_not(self.inner))(self.onward.start)

    def settle(self):
        @pl.when(self.inner)
        def _():
            self.across.wait()
            self.add(self.total, self.sum, self.second)
            if self.deep:
                self.outward.start()
            self.keep()

        if self.deep:

            @pl.when(jnp.logical_not(self.inner | self.end))
            def _():
                self.outward.wait_recv()
                self.outward.start()
                self.keep()

    def finish(self):
        if self.deep:

            @pl.when(self.end)
            def _():
                self.outward.wait_recv()
                self.keep()

            if not self.begun:
                pl.when(jnp.logical_not(self.inner))(self.inward.wait_send)
            pl.when(jnp.logical_not(self.end))(self.outward.wait_send)


def finish_kernel(
    mesh, count, kv,
    term_gate, term_up, dwd, first, dqkv, attended, low, gains,
    out_gate, out_up, out_down, out_out, out_qkv, out_gains,
    tot_gate, tot_up, tot_down, tot_out, tot_qkv, term_down, term_out, term_qkv, in_gate, in_up, in_down, in_out, in_qkv,
    first_both, attended_both, low_both, dq_both, w_out_part, w_qkv_part,
    swap_out, land_out, swap_qkv, land_qkv, gain_terms, gain_lands, *rest,
):
    parts, (send_sems, recv_sems, local_sems) = rest[:-3], rest[-3:]
    links = Links(mesh, send_sems, recv_sems, local_sems)
    ns, na = links.ns, links.na
    chips, per = 2 * na, ns // 2
    core = links.core
    rows, width = first.shape
    q_width = dqkv.shape[3]
    middle = width // 2
    links.barrier()

    def lines(term, inbox, total, out, pieces, begun=False):
        size = term.shape[1] // pieces
        every = slice(None)
        made = []
        for i in range(pieces):
            at = slice(i * size, (i + 1) * size)
            refs = [(ref, *where, every, at) for ref, *where in ((term,), (inbox, 0), (inbox, 1), (total,), (out,))]
            made.append(LineSum(links, *refs, begun and i == 0))
        return made

    gate_lines = lines(term_gate, in_gate, tot_gate, out_gate, GATE_PIECES, first_piece(ns, term_gate.shape[1]) > 0)
    up_lines = lines(term_up, in_up, tot_up, out_up, 4)
    down_lines = lines(term_down, in_down, tot_down, out_down, 4)
    out_lines = lines(term_out, in_out, tot_out, out_out, 2)
    qkv_lines = lines(term_qkv, in_qkv, tot_qkv, out_qkv, 4)
    for line in gate_lines + up_lines:
        line.begin()

    sends = [
        links.copy((dqkv, pl.ds((1 - core) * per, per)), (dq_both, 1), links.at_core()),
        links.copy((low, slice(None), rows_at(1 - core, middle)), (low_both, 1), links.at_core()),
        links.copy(first, (first_both, 1), links.at_core()),
        links.copy(attended, (attended_both, 1), links.at_core()),
    ]
    loads = [
        links.local((low, slice(None), rows_at(core, middle)), (low_both, 0)),
        links.local(attended, (attended_both, 0)),
        links.local(first, (first_both, 0)),
        links.local((dqkv, pl.ds(core * per, per)), (dq_both, 0)),
    ]
    for copies in loads + sends[1:2] + sends[3:4] + sends[2:3] + sends[:1]:
        copies.start()

    down_rows = dwd.shape[0] // chips
    block = width // chips

    def pair(source, row_count, at, staged):
        made = []
        cut = source.shape[1] // 2
        for n, b_first in enumerate((True, False)):
            columns = slice(0, cut) if b_first else slice(cut, 2 * cut)
            partial = lambda k, columns=columns: (source, rows_at(k, row_count), columns)
            refs = parts[at[n] : at[n + 1]]
            made.append(ChipSum(links, partial, b_first, *(refs if staged else (*refs[:2], None))))
        return made

    down = pair(dwd, down_rows, (0, 3, 6), True)
    for item in down:
        item.start()
        item.load()

    gain_copies = [links.copy((gain_terms, 0), (gain_lands, 0), links.at_core()), links.copy((gain_terms, 1), (gain_lands, 1), links.at_b())]
    gain_copies += [links.copy((gain_terms, 2), (gain_lands, 1 + d), links.at_a(d)) for d in range(1, na)]
    gain_line = LineSum(links, (gain_terms, 3), (gain_lands, na + 1), (gain_lands, na + 2), out_gains)
    gain_terms[0] = gains[...]
    gain_copies[0].start()

    def next_gain(i):
        for copies in gain_copies[i : i + 1] if i < 2 else gain_copies[2:]:
            copies.wait()
        if i < 2:
            gain_terms[i + 1] = gain_terms[i] + gain_lands[i]
            for copies in gain_copies[1:2] if i == 0 else gain_copies[2:]:
                copies.start()
        else:
            total = gain_terms[2]
            for d in range(1, na):
                total = total + gain_lands[1 + d]
            gain_terms[3] = total
            gain_line.begin()

    def qkv_part(p):
        columns = slice(p * q_width, (p + 1) * q_width)
        mine, other = dq_both[0, p].reshape(rows, q_width), dq_both[1, p].reshape(rows, q_width)
        for k in range(chips):
            at = slice(k * block, (k + 1) * block)
            total = tn_dot(first_both[0, :, at], mine) + tn_dot(first_both[1, :, at], other)
            w_qkv_part[at, columns] = total.astype(BF16)

    def swap(sums, send, land):
        local = block // 2
        for n, item in enumerate(sums):
            total = item.finish()
            size = total.shape[1]
            send[0, :, n * size : (n + 1) * size] = total[:local]
            send[1, :, n * size : (n + 1) * size] = total[local:]
        copies = links.copy((send, 1 - core), land, links.at_core())
        copies.start()
        return copies

    out_sums = pair(w_out_part, block, (6, 8, 10), False)
    qkv_sums = pair(w_qkv_part, block, (10, 12, 14), False)
    cut = width // 2
    next_gain(0)
    for i in (1, 3):
        sends[i].wait()
    for i in (0, 1):
        loads[i].wait()
    gate_lines[0].relay()
    for k in range(chips):
        at = slice(k * block, (k + 1) * block)
        total = tn_dot(attended_both[0, :, at], low_both[0]) + tn_dot(attended_both[1, :, at], low_both[1])
        w_out_part[at, :] = total.astype(BF16)
    for item in out_sums:
        item.start()
    gate_lines[1].relay()
    next_gain(1)
    for i in (0, 2):
        sends[i].wait()
    for i in (2, 3):
        loads[i].wait()
    gate_lines[0].settle()
    for p in range(per // 2):
        qkv_part(p)
    gate_lines[2].relay()
    next_gain(2)
    gate_lines[1].settle()
    for p in range(per // 2, per):
        qkv_part(p)
    gate_lines[3].relay()
    for item in down:
        item.turn()
    for item in qkv_sums:
        item.start()
    gate_lines[2].settle()
    gain_line.relay()
    gate_lines[3].settle()
    for item in out_sums:
        item.turn()
    up_lines[0].relay()
    gain_line.settle()
    up_lines[1].relay()
    up_lines[0].settle()
    term_down[:, :cut] = down[0].finish()
    term_down[:, cut:] = down[1].finish()
    for line in down_lines:
        line.begin()
    up_lines[2].relay()
    up_lines[1].settle()
    up_lines[3].relay()
    up_lines[2].settle()
    down_lines[0].relay()
    up_lines[3].settle()
    for item in qkv_sums:
        item.turn()
    down_lines[1].relay()
    down_lines[0].settle()
    out_swap = swap(out_sums, swap_out, land_out)
    down_lines[2].relay()
    down_lines[1].settle()
    out_swap.wait()
    kept, arrived = swap_out[core], land_out[...]
    term_out[:, :cut] = jnp.where(core == 0, kept, arrived)
    term_out[:, cut:] = jnp.where(core == 0, arrived, kept)
    for line in out_lines:
        line.begin()
    down_lines[3].relay()
    down_lines[2].settle()
    qkv_swap = swap(qkv_sums, swap_qkv, land_qkv)
    out_lines[0].relay()
    down_lines[3].settle()
    qkv_swap.wait()
    kept, arrived = swap_qkv[core], land_qkv[...]
    for n in range(2):
        group = jnp.where(core == n, kept, arrived)
        for p in range(per):
            taken, start = p * q_width, 0
            for size in (kv * GROUP * HEAD_DIM, kv * HEAD_DIM, kv * HEAD_DIM):
                at = start + (n * per + p) * size
                term_qkv[:, at : at + size] = group[:, taken : taken + size]
                taken, start = taken + size, start + ns * size
    for line in qkv_lines:
        line.begin()
    out_lines[1].relay()
    out_lines[0].settle()
    qkv_lines[0].relay()
    out_lines[1].settle()
    for n in range(1, len(qkv_lines)):
        qkv_lines[n].relay()
        qkv_lines[n - 1].settle()
    qkv_lines[-1].settle()
    every_line = [*gate_lines, *up_lines, gain_line, *down_lines, *out_lines, *qkv_lines]
    for line in every_line:
        line.finish()
    for line in every_line:
        if line.store is not None:
            line.store.wait()


def finish(mesh, count, kv, term_gate, term_up, dwd, first, dqkv, attended, low, gains):
    ns, nf = mesh
    na, per = nf // 4, ns // 2
    rows, width = first.shape
    q_width = dqkv.shape[3]
    local, half = term_gate.shape[0], width // 2
    block = 2 * local
    anywhere, vmem = pl.BlockSpec(memory_space=pl.ANY), pl.BlockSpec(memory_space=pltpu.VMEM)
    down = (dwd.shape[0] // (2 * na), dwd.shape[1])
    shapes = [term_gate.shape, term_up.shape, down, (local, width), (local, ns * q_width)]
    scratch = [pltpu.VMEM(s, BF16) for s in shapes]
    scratch += [pltpu.VMEM(s, BF16) for s in shapes[2:]]
    scratch += [pltpu.VMEM((2,) + tuple(s), BF16) for s in shapes]
    scratch += [
        pltpu.VMEM((2, rows, width), BF16),
        pltpu.VMEM((2, rows, width), BF16),
        pltpu.VMEM((2, rows, half), BF16),
        pltpu.VMEM((2, per, count, rows // count, q_width), BF16),
        pltpu.VMEM((width, half), BF16),
        pltpu.VMEM((width, per * q_width), BF16),
        pltpu.VMEM((2, local, half), BF16),
        pltpu.VMEM((local, half), BF16),
        pltpu.VMEM((2, local, per * q_width), BF16),
        pltpu.VMEM((local, per * q_width), BF16),
        pltpu.VMEM((4, 2, width), F32),
        pltpu.VMEM((na + 3, 2, width), F32),
    ]
    scratch += chip_sum_shapes(na, True, down[0], down[1] // 2) + chip_sum_shapes(na, False, down[0], down[1] // 2)
    for columns in (half // 2, per * q_width // 2):
        for b_first in (True, False):
            scratch += chip_sum_shapes(na, b_first, block, columns)[:2]
    return pl.pallas_call(
        functools.partial(finish_kernel, mesh, count, kv),
        in_specs=[vmem, vmem] + [anywhere] * 5 + [vmem],
        out_specs=[anywhere] * 5 + [vmem],
        out_shape=[jax.ShapeDtypeStruct(s, BF16) for s in shapes] + [jax.ShapeDtypeStruct((2, width), F32)],
        scratch_shapes=scratch
        + [pltpu.SemaphoreType.DMA((128,)), pltpu.SemaphoreType.DMA((128,)), pltpu.SemaphoreType.DMA((64,))],
        compiler_params=pltpu.CompilerParams(vmem_limit_bytes=VMEM_MOST, collective_id=2, has_side_effects=True),
        name="finish",
    )(term_gate, term_up, dwd, first, dqkv, attended, low, gains)


def widen_kernel(cuts, *refs):
    gate, up, down, out, qkv, hidden, own, other = refs[:8]
    o_gate, o_up, o_down, o_out, o_q, o_k, o_v, o_block = refs[8:]
    for source, target in ((gate, o_gate), (up, o_up), (down, o_down), (out, o_out)):
        target[...] = source[...].astype(F32)
    for (start, end), target in zip(cuts, (o_q, o_k, o_v)):
        target[...] = qkv[:, start:end].astype(F32)
    o_block[...] = hidden[...] + own[...] + other[...].astype(F32)


def widen(gate, up, down, out, qkv, hidden, own, other, cuts):
    steps = 4
    operands = [gate, up, down, out, qkv, hidden, own, other]
    rows = out.shape[0]
    shapes = [gate.shape, up.shape, down.shape, out.shape] + [(rows, end - start) for start, end in cuts] + [hidden.shape]
    block = lambda shape: pl.BlockSpec((shape[0] // steps, shape[1]), lambda i: (i, 0))
    return pl.pallas_call(
        functools.partial(widen_kernel, cuts),
        grid=(steps,),
        in_specs=[block(x.shape) for x in operands],
        out_specs=[block(shape) for shape in shapes],
        out_shape=[jax.ShapeDtypeStruct(shape, F32) for shape in shapes],
        compiler_params=pltpu.CompilerParams(vmem_limit_bytes=VMEM_LIMIT),
        cost_estimate=pl.CostEstimate(flops=0, bytes_accessed=40 * rows * gate.shape[1], transcendentals=0),
        name="widen",
    )(*operands)


def solution(mesh):
    ns, nf = mesh.shape["seq"], mesh.shape["fsdp"]
    na = nf // 4
    chips = 2 * na
    kv = KEY_VALUE_HEADS // ns

    def body(tokens, cotangent, attention_gain, feedforward_gain, query_weight, key_matrix, value_matrix, out_weight, gate_weight, up_weight, down_weight):
        count, span, width = tokens.shape
        rows = count * span
        local = query_weight.shape[0]
        sizes = (ns, nf)
        mine = lax.axis_index("fsdp")
        cosines, sines = (jnp.asarray(x) for x in rope_tables(ns * span))
        flat = tokens.reshape(rows, width)
        grad_flat = cotangent.reshape(rows, width)
        (w_qkv, w_out, w_gate, w_down, first, packed, heads_attended, logs, attended, hidden_one, second_both, low_both, gains) = fore(
            sizes, count, kv, flat, grad_flat, jnp.stack([attention_gain, feedforward_gain]),
            query_weight, key_matrix, value_matrix, out_weight, gate_weight, down_weight, cosines, sines,
        )
        dwg, dwu, dwd, out_own, out_arrived, dx_own, dx_arrived = ffn(sizes, second_both, low_both, w_gate, w_down, up_weight, gate_weight)
        high, low, grad_tokens, gain_grads, dqkv, sum_gate, sum_up = back(
            sizes, count, kv, dx_own, dx_arrived, hidden_one, grad_flat, gains, w_out, w_qkv,
            packed, heads_attended, logs, cosines, sines, flat, dwg, dwu,
        )
        *sums, gain_grads = finish(
            sizes, count, kv, sum_gate, sum_up, dwd, first, dqkv, attended, low, gain_grads
        )
        q_end, k_end = ns * kv * GROUP * HEAD_DIM, ns * kv * (GROUP + 1) * HEAD_DIM
        cuts = ((0, q_end), (q_end, k_end), (k_end, sums[4].shape[1]))
        grad_gate, grad_up, grad_down, grad_out, grad_query, grad_key, grad_value, block_out = widen(
            *sums, hidden_one, out_own, out_arrived, cuts
        )
        gain_grads = lax.dynamic_slice(gain_grads, (0, mine * local), (2, local))

        return (
            block_out.reshape(count, span, width),
            grad_tokens.reshape(count, span, width),
            gain_grads[0],
            gain_grads[1],
            grad_query,
            grad_key,
            grad_value,
            grad_out,
            grad_gate,
            grad_up,
            grad_down,
        )

    tokens_spec, gain_spec, weight_spec = P("fsdp", "seq", None), P("fsdp"), P("fsdp", None)
    return jax.shard_map(
        body,
        mesh=mesh,
        in_specs=(tokens_spec, tokens_spec, gain_spec, gain_spec) + (weight_spec,) * 7,
        out_specs=(tokens_spec, tokens_spec, gain_spec, gain_spec) + (weight_spec,) * 7,
        check_vma=False,
    )
```

```python
import functools
import math

import jax
import jax.numpy as jnp
import numpy as np
from jax import lax
from jax.experimental import pallas as pl
from jax.experimental.pallas import tpu as pltpu
from jax.sharding import PartitionSpec as P

QUERY_HEADS = 16
KEY_VALUE_HEADS = 8
HEAD_DIM = 96
GROUP = QUERY_HEADS // KEY_VALUE_HEADS
norm_eps = 1e-05
rope_base = 100000.0
masked_score = -1e30
F32, BF16 = jnp.float32, jnp.bfloat16
VMEM_LIMIT = 60 * 1024 * 1024
VMEM_MOST = 67043328
MESH = pl.DeviceIdType.MESH


def nt_dot(left, right):
    return lax.dot_general(left, right, (((1,), (1,)), ((), ())), preferred_element_type=F32)


def tn_dot(left, right):
    return lax.dot_general(left, right, (((0,), (0,)), ((), ())), preferred_element_type=F32)


def nn_dot(left, right):
    return jnp.dot(left, right, preferred_element_type=F32)


def whole(shape):
    return pl.BlockSpec(shape, lambda *_: (0,) * len(shape))


def call(kernel, scalars, operands, outs, name, flops, moved, scratch=()):
    return pl.pallas_call(
        kernel,
        grid_spec=pltpu.PrefetchScalarGridSpec(
            num_scalar_prefetch=1,
            grid=(1,),
            in_specs=[whole(x.shape) for x in operands],
            out_specs=[whole(x.shape) for x in outs],
            scratch_shapes=scratch,
        ),
        out_shape=outs,
        compiler_params=pltpu.CompilerParams(vmem_limit_bytes=VMEM_LIMIT),
        cost_estimate=pl.CostEstimate(flops=flops, bytes_accessed=moved, transcendentals=0),
        name=name,
    )(scalars, *operands)


def rope_tables(length):
    half = HEAD_DIM // 2
    freqs = np.float32(rope_base) ** (-(np.float32(2.0) * np.arange(half, dtype=np.float32)) / np.float32(HEAD_DIM))
    angles = np.arange(length, dtype=np.float32)[:, None] * freqs.astype(np.float32)[None, :]
    cosine, sine = np.cos(angles), np.sin(angles)
    return np.concatenate([cosine, cosine], 1), np.concatenate([-sine, sine], 1)


def swap_halves(values):
    half = HEAD_DIM // 2
    width = values.shape[1]
    lane = lax.broadcasted_iota(jnp.int32, values.shape, 1)
    ahead = pltpu.roll(values, width - half, 1)
    behind = pltpu.roll(values, half, 1)
    return jnp.where(lane % HEAD_DIM < half, ahead, behind)


def norm_back(grad, normed, inverse, gain):
    scaled = grad * gain
    return inverse * (scaled - normed * jnp.mean(scaled * normed, axis=1, keepdims=True))


def ffn_kernel(
    mesh, tiles, parts, x, g, wg, wd, wu, w_last, dwg, dwu, dwd, out_own, out_arrived, dx_own, dx_arrived,
    xt, acc_out, acc_dx, given_out, given_dx, act, dgate, dup, stage, land, gate, send_sems, recv_sems, local_sems,
):
    step = pl.program_id(0)
    rows = x.shape[0] // 2
    links = Links(mesh, send_sems, recv_sems, local_sems)
    chips, local, tile = tiles // parts, wu.shape[0], land.shape[2]
    cols = tile // parts
    gathers, loads = [], []
    for k in range(chips + 1):
        gathers.append(GatherHalf(links, lambda c, k=k: (stage, c, k), lambda o, k=k: (land, k, rows_at(o, local))))
        weight, tile_at = (wu, k) if k < chips else (w_last, chips - 1)
        for c in range(2):
            source = (weight, slice(None), slice((tile_at * 2 + c) * tile, (tile_at * 2 + c + 1) * tile))
            loads.append(links.local(source, (stage, c, k)))

    def begin(k):
        gathers[k].start()
        gathers[k].other_start()

    def turn(k):
        gathers[k].turn()
        gathers[k].turn_late()

    @pl.when(step == 0)
    def _():
        for load in loads:
            load.start()
        links.barrier()
        for load in loads[:2]:
            load.wait()
        gathers[0].start()
        gathers[0].other_start()
        for load in loads[2:]:
            load.wait()

    @pl.when(step == 0)
    def _():
        acc_out[...] = jnp.zeros_like(acc_out)
        acc_dx[...] = jnp.zeros_like(acc_dx)
        xt[...] = x[...].T

    def first_part():
        turn(0)
        begin(1)
        gathers[0].finish()

    def later_part(k):
        turn(k)
        for n in (2, 3) if k == 1 else (k + 2,):
            if n <= chips:
                begin(n)
        if k == chips - 1:
            turn(chips)

    for k in range(1, chips):
        pl.when(step == (k - 1) * parts + 1)(functools.partial(later_part, k))
    pl.when(step == (chips - 1) * parts)(gathers[chips].finish)
    at = pl.ds(pl.multiple_of(lax.rem(step, parts) * cols, cols), cols)
    chip = step // parts

    @pl.when(chip < chips - 1)
    def _():
        gate[...] = wg[...]

    @pl.when(chip == chips - 1)
    def _():
        gate[...] = land[chips, :, at]

    pl.when(step == 0)(first_part)
    for k in range(1, chips):
        pl.when(step == k * parts)(gathers[k].finish)
    for i in range(2):
        here = slice(i * rows, (i + 1) * rows)
        gate_pre = nn_dot(x[here, :], gate[...])
        up = nn_dot(x[here, :], land[chip, :, at])
        grad = nt_dot(g[here, :], wd[...])
        sigmoid = jax.nn.sigmoid(gate_pre)
        silu = gate_pre * sigmoid
        hidden = (silu * up).astype(BF16)
        act[here, :] = hidden
        gate_grad = (grad * up * sigmoid * (1.0 + gate_pre * (1.0 - sigmoid))).astype(BF16)
        up_grad = (grad * silu).astype(BF16)
        dgate[here, :] = gate_grad
        dup[here, :] = up_grad
        acc_out[i] += nn_dot(hidden, wd[...])
        acc_dx[i] += nt_dot(gate_grad, gate[...]) + nt_dot(up_grad, land[chip, :, at])
    leaving = [
        links.copy(given_dx, dx_arrived, links.at_core()),
        links.local((acc_dx, 0), dx_own),
        links.copy(given_out, out_arrived, links.at_core()),
        links.local((acc_out, 0), out_own),
    ]

    @pl.when(step == tiles - 1)
    def _():
        given_dx[...] = acc_dx[1].astype(BF16)
        leaving[0].start()
        given_out[...] = acc_out[1].astype(BF16)
        for copies in leaving[1:]:
            copies.start()

    dwg[...] = nn_dot(xt[...], dgate[...]).astype(BF16)
    dwu[...] = nn_dot(xt[...], dup[...]).astype(BF16)
    dwd[...] = tn_dot(act[...], g[...]).astype(BF16)

    @pl.when(step == tiles - 1)
    def _():
        for copies in leaving:
            copies.wait()


def ffn(mesh, x, g, wg, wd, wu, w_last):
    rows, width = x.shape[0] // 2, x.shape[1]
    chips, tile = wg.shape[0] + 1, wg.shape[2]
    parts = 2
    tiles, cols = chips * parts, tile // parts
    local = wu.shape[0]
    keep = lambda shape: pl.BlockSpec(shape, lambda i: (0, 0), pipeline_mode=pl.Buffered(1))
    half = tile * chips
    wide, low = jax.ShapeDtypeStruct((rows, width), F32), jax.ShapeDtypeStruct((rows, width), BF16)
    return pl.pallas_call(
        functools.partial(ffn_kernel, mesh, tiles, parts),
        grid=(tiles,),
        in_specs=[
            keep(x.shape),
            keep(g.shape),
            pl.BlockSpec((None, width, cols), lambda i: (jnp.minimum(i // parts, chips - 2), 0, i % parts)),
            pl.BlockSpec((cols, width), lambda i: (i, 0)),
            pl.BlockSpec(memory_space=pl.ANY),
            pl.BlockSpec(memory_space=pl.ANY),
        ],
        out_specs=[pl.BlockSpec((width, cols), lambda i: (0, i))] * 2
        + [pl.BlockSpec((cols, width), lambda i: (i, 0))]
        + [pl.BlockSpec(memory_space=pl.ANY)] * 4,
        scratch_shapes=[pltpu.VMEM((width, 2 * rows), BF16)]
        + [pltpu.VMEM((2, rows, width), F32)] * 2
        + [pltpu.VMEM((rows, width), BF16)] * 2
        + [pltpu.VMEM((2 * rows, cols), BF16)] * 3
        + [pltpu.VMEM((2, chips + 1, local, tile), BF16), pltpu.VMEM((chips + 1, width, tile), BF16), pltpu.VMEM((width, cols), BF16)]
        + [pltpu.SemaphoreType.DMA((96,)), pltpu.SemaphoreType.DMA((96,)), pltpu.SemaphoreType.DMA((64,))],
        out_shape=[
            jax.ShapeDtypeStruct((width, half), BF16),
            jax.ShapeDtypeStruct((width, half), BF16),
            jax.ShapeDtypeStruct((half, width), BF16),
            wide,
            low,
            wide,
            low,
        ],
        compiler_params=pltpu.CompilerParams(vmem_limit_bytes=VMEM_MOST, collective_id=3, has_side_effects=True),
        cost_estimate=pl.CostEstimate(
            flops=36 * rows * width * half, bytes_accessed=12 * width * half + 20 * rows * width, transcendentals=0
        ),
        name="ffn",
    )(x, g, wg, wd, wu, w_last)


def part(x):
    return x[0].at[x[1:]] if isinstance(x, tuple) else x


def get(x):
    return x[0][x[1:]] if isinstance(x, tuple) else x[...]


def put(x, value):
    if isinstance(x, tuple):
        x[0][x[1:]] = value
    else:
        x[...] = value


class Copy:
    def __init__(self, src, dst, device, send_sem, recv_sem):
        self.src, self.dst, self.device, self.send_sem, self.recv_sem = src, dst, device, send_sem, recv_sem

    def made(self):
        if self.device is None:
            return pltpu.make_async_copy(part(self.src), part(self.dst), part(self.send_sem))
        return pltpu.make_async_remote_copy(
            src_ref=part(self.src),
            dst_ref=part(self.dst),
            send_sem=part(self.send_sem),
            recv_sem=part(self.recv_sem),
            device_id=self.device,
            device_id_type=MESH,
        )

    def start(self):
        self.made().start()

    def wait(self):
        self.made().wait()

    def wait_send(self):
        self.made().wait_send()

    def wait_recv(self):
        self.made().wait_recv()


class Links:
    def __init__(self, mesh, send_sems, recv_sems, local_sems):
        self.ns, self.nf = mesh
        self.na = self.nf // 4
        self.send_sems, self.recv_sems, self.local_sems = send_sems, recv_sems, local_sems
        self.count, self.local_count = 0, 0
        self.z, self.f = lax.axis_index("seq"), lax.axis_index("fsdp")
        self.core = lax.rem(self.f, 2)
        self.b = lax.rem(self.f // 2, 2)
        self.a = self.f // 4

    def chip(self, da, db):
        return lax.rem(self.a + da, self.na) * 2 + lax.rem(self.b + db, 2)

    def at_core(self):
        return (self.z, self.f + 1 - 2 * self.core)

    def at_b(self):
        return (self.z, self.f + 2 - 4 * self.b)

    def at_a(self, d):
        return (self.z, lax.rem(self.f + 4 * d, self.nf))

    def at_z(self, d):
        return (lax.rem(self.z + d, self.ns), self.f)

    def peers(self):
        return [self.at_core(), self.at_b()] + [self.at_a(d) for d in range(1, self.na)] + [self.at_z(d) for d in range(1, self.ns)]

    def barrier(self):
        barrier = pltpu.get_barrier_semaphore()
        peers = self.peers()
        for peer in peers:
            pl.semaphore_signal(barrier, inc=1, device_id=peer, device_id_type=MESH)
        pl.semaphore_wait(barrier, len(peers))

    def copy(self, src, dst, device):
        index = self.count
        self.count += 1
        return Copy(src, dst, device, (self.send_sems, index), (self.recv_sems, index))

    def again(self, src, dst, device):
        index = self.count - 1
        return Copy(src, dst, device, (self.send_sems, index), (self.recv_sems, index))

    def local(self, src, dst):
        index = self.local_count
        self.local_count += 1
        return Copy(src, dst, None, (self.local_sems, index), None)


def line_place(links):
    z, ns = links.z, links.ns
    middle = ns // 2
    step = jnp.where(z < middle, 1, -1)
    end = (z == 0) | (z == ns - 1)
    inner = (z == middle - 1) | (z == middle)
    return end, inner, (z + step, links.f), (z - step, links.f)


GATE_PIECES = 4


def first_piece(ns, columns):
    return columns // GATE_PIECES if ns == 4 else 0


def rows_at(start, size):
    return pl.ds(pl.multiple_of(start * size, size), size)


class ChipSum:
    def __init__(self, links, partial, b_first, arrived, passed, staging):
        self.links, self.partial, self.b_first = links, partial, b_first
        self.arrived, self.passed, self.staging = arrived, passed, staging
        na = links.na
        self.first, self.second = [], []
        if b_first:
            self.kept = [links.chip(da, 0) for da in range(na)]
            for da in range(na):
                self.first.append(links.copy(partial(links.chip(da, 1)), (arrived, da), links.at_b()))
            for d in range(1, na):
                self.second.append(links.copy((arrived, d), (passed, d - 1), links.at_a(d)))
        else:
            self.kept = [links.chip(0, db) for db in range(2)]
            for d in range(1, na):
                for db in range(2):
                    self.first.append(links.copy(partial(links.chip(d, db)), (arrived, (d - 1) * 2 + db), links.at_a(d)))
            self.second.append(links.copy((arrived, 1), (passed, 0), links.at_b()))
        self.loads = [] if staging is None else [links.local(partial(k), (staging, i)) for i, k in enumerate(self.kept)]

    def start(self):
        for copy in self.first:
            copy.start()

    def load(self):
        for load in self.loads:
            load.start()

    def turn(self):
        for load in self.loads:
            load.wait()
        for copy in self.first:
            copy.wait()
        count = len(self.kept)
        for i in [*range(1, count), 0]:
            own = self.partial(self.kept[i]) if self.staging is None else (self.staging, i)
            total = get(own).astype(F32)
            if self.b_first:
                total = total + self.arrived[i].astype(F32)
            else:
                for d in range(self.links.na - 1):
                    total = total + self.arrived[d * 2 + i].astype(F32)
            self.arrived[i] = total.astype(BF16)
            if i > 0 and self.b_first:
                self.second[i - 1].start()
            elif i > 0:
                self.second[0].start()

    def finish(self):
        for copy in self.second:
            copy.wait()
        total = self.arrived[0].astype(F32)
        for i in range(len(self.second)):
            total = total + self.passed[i].astype(F32)
        return total.astype(BF16)


def chip_sum_shapes(na, b_first, rows, columns):
    first = na if b_first else 2 * (na - 1)
    kept = na if b_first else 2
    return [
        pltpu.VMEM((max(first, kept), rows, columns), BF16),
        pltpu.VMEM((na - 1 if b_first else 1, rows, columns), BF16),
        pltpu.VMEM((kept, rows, columns), BF16),
    ]


def flip_core(f):
    return f + 1 - 2 * lax.rem(f, 2)


def flip_b(f):
    return f + 2 - 4 * lax.rem(f // 2, 2)


class Gather:
    def __init__(self, links, own, land, both):
        self.links = links
        f, na, nf = links.f, links.na, links.nf
        to_core, to_b = links.at_core(), links.at_b()

        def move(origin, device, half=None):
            return links.copy(land(origin, half), land(origin, half), device)

        self.given = [links.copy(own, land(f, None), to_core)] if both else []
        self.own = [links.copy(own, land(f, None), to_b)]
        self.own += [links.copy(own, land(f, None), links.at_a(d)) for d in range(1, na)]
        from_b = flip_b(f)
        from_a = [lax.rem(f + nf - 4 * d, nf) for d in range(1, na)]
        if na == 2:
            self.relays = [move(from_b, links.at_a(1), 1), move(from_a[0], to_b, 0)]
            far = [(flip_b(from_a[0]), 0), (flip_b(from_a[0]), 1)]
        else:
            self.relays = [move(origin, to_b) for origin in from_a]
            far = [(flip_b(origin), None) for origin in from_a]
        near = [from_b, *from_a]
        self.near = [move(origin, to_core) for origin in near] if both else []
        self.far = [move(origin, to_core, half) for origin, half in far] if both else []

    def start(self):
        for copies in self.own + self.given:
            copies.start()

    def turn(self):
        for copies in self.own:
            copies.wait()
        for copies in self.relays + self.near:
            copies.start()

    def pass_on(self):
        for copies in self.relays:
            copies.wait()
        for copies in self.far:
            copies.start()

    def finish(self):
        for copies in self.given + self.near + self.far:
            copies.wait()


class GatherHalf:
    def __init__(self, links, stage, land):
        self.links = links
        f, na, nf, core = links.f, links.na, links.nf, links.core
        to_b = links.at_b()

        def move(origin, device):
            return links.copy(land(origin), land(origin), device)

        self.swap = links.copy(stage(1 - core), land(f), links.at_core())
        self.kept = links.local(stage(core), land(f))
        targets = [to_b] + [links.at_a(d) for d in range(1, na)]
        self.own = [links.copy(stage(core), land(f), device) for device in targets]
        self.other = [move(flip_core(f), device) for device in targets]
        from_b = flip_b(f)
        from_a = [lax.rem(f + nf - 4 * d, nf) for d in range(1, na)]
        if na == 2:
            self.relays = [move(from_b, links.at_a(1))]
            self.late = [move(flip_core(from_a[0]), to_b)]
        else:
            self.relays = [move(origin, to_b) for origin in from_a]
            self.late = [move(flip_core(origin), to_b) for origin in from_a]

    def start(self):
        for copies in [self.swap, self.kept, *self.own]:
            copies.start()

    def other_start(self):
        self.swap.wait()
        for copies in self.other:
            copies.start()

    def turn(self):
        for copies in self.own:
            copies.wait()
        for copies in self.relays:
            copies.start()

    def turn_late(self):
        for copies in self.other:
            copies.wait()
        for copies in self.late:
            copies.start()

    def finish(self):
        for copies in [self.kept, *self.relays, *self.late]:
            copies.wait()


def attend_heads(ns, kv, span, qs, ks, vs, out, logs):
    scale = 1.0 / math.sqrt(HEAD_DIM)
    row = lax.broadcasted_iota(jnp.int32, (span, span), 0)
    column = lax.broadcasted_iota(jnp.int32, (span, span), 1)
    causal = row >= column
    lane = lax.broadcasted_iota(jnp.int32, (span, 128), 1)
    for s in range(ns):
        here = slice(s * span, (s + 1) * span)
        stats = jnp.zeros((span, 128), F32)
        for h in range(kv * GROUP):
            g = h // GROUP
            q = qs[h, here, :]
            near = jnp.where(causal, nt_dot(q, ks[g, here, :]) * scale, masked_score)
            top = jnp.max(near, axis=1, keepdims=True)
            if s > 0:
                far = nt_dot(q, ks[g, : s * span, :]) * scale
                top = jnp.maximum(top, jnp.max(far, axis=1, keepdims=True))
            near = jnp.exp(near - top)
            total = jnp.sum(near, axis=1, keepdims=True)
            if s > 0:
                far = jnp.exp(far - top)
                total = total + jnp.sum(far, axis=1, keepdims=True)
            inverse = 1.0 / total
            result = nn_dot((near * inverse).astype(BF16), vs[g, here, :])
            if s > 0:
                result = result + nn_dot((far * inverse).astype(BF16), vs[g, : s * span, :])
            stats = jnp.where(lane == h, top + jnp.log(total), stats)
            out[s, :, h * HEAD_DIM : (h + 1) * HEAD_DIM] = result.astype(BF16)
        logs[here, :] = stats


def fill_tables(cosines, sines, narrow_cosines, narrow_sines, heads):
    end = heads * HEAD_DIM
    cosines[:, end:] = jnp.ones((cosines.shape[0], cosines.shape[1] - end), F32)
    sines[:, end:] = jnp.zeros((cosines.shape[0], cosines.shape[1] - end), F32)
    for h in range(heads):
        at = slice(h * HEAD_DIM, (h + 1) * HEAD_DIM)
        cosines[:, at] = narrow_cosines
        sines[:, at] = narrow_sines


def fore_kernel(
    mesh, count, kv,
    tokens, cotangent, gains_in, wq, wk, wv, wo, wg, wd, narrow_cosines, narrow_sines,
    w_qkv, w_out, w_gate, w_down, first_out, packed, heads_attended, logs, attended_out, hidden_out, second_both, low_both, gains_out,
    rows_in, hidden, first, pack, w_land, wo_land, q_send, q_land, a_send, a_land, stage_gate, gain_send, gain_land,
    qs, ks, vs, log, attended, second, second_abs, low, cosines, sines, send_sems, recv_sems, local_sems,
):
    links = Links(mesh, send_sems, recv_sems, local_sems)
    ns, na, nf = links.ns, links.na, links.nf
    chips = 2 * na
    z, f, core = links.z, links.f, links.core
    rows, width = rows_in.shape
    span = rows // count
    heads = kv * GROUP
    g_width, k_width = heads * HEAD_DIM, kv * HEAD_DIM
    q_width = g_width + 2 * k_width
    local = width // nf
    links.barrier()

    token_load = links.local(tokens, rows_in)
    token_load.start()
    cot_load = links.local(cotangent, hidden)
    cot_load.start()
    gain_send[...] = jnp.zeros_like(gain_send)
    gain_send[0:2, :local] = gains_in[...].astype(F32)
    for j in range(ns):
        pack[j, :, :g_width] = wq[:, j * g_width : (j + 1) * g_width]
        pack[j, :, g_width : g_width + k_width] = wk[:, j * k_width : (j + 1) * k_width]
        pack[j, :, g_width + k_width :] = wv[:, j * k_width : (j + 1) * k_width]

    every = slice(None)

    def piece(start, size, half):
        if half is None:
            return rows_at(start, size)
        return rows_at(start * 2 + half, size // 2)

    units = []
    turns = [*range(1, ns), 0]
    for d in turns:
        g = lax.rem(z + d, ns)
        units.append(Gather(links, (pack, g), lambda o, half, g=g: (w_land, g, piece(o, local, half)), True))
    units.append(Gather(links, wo, lambda o, half: (wo_land, piece(o, local, half)), True))
    depth = wd.shape[0]
    units.append(Gather(links, wd, lambda o, half: (w_down, piece(o // 2, depth, half)), False))
    gate_unit = GatherHalf(links, lambda c: (stage_gate, c), lambda o: (w_gate, every, rows_at(o, local)))
    q_copies, a_copies = [], []
    for d in range(1, ns):
        g = lax.rem(z + d, ns)
        q_copies.append([links.copy((q_send, g, i), (q_land, i, z), links.at_z(d)) for i in range(count)])
    for i in range(count):
        a_copies.append([links.copy((a_send, i, lax.rem(z + d, ns)), (a_land, i, z), links.at_z(d)) for d in range(1, ns)])
    second_copy = links.copy(second_abs, (second_both, pl.ds(rows, rows)), links.at_core())
    low_copy = links.copy(low, (low_both, pl.ds(rows, rows)), links.at_core())

    def gain_at(start, size):
        return (gain_land, pl.ds(start, size))

    pair, chip_four = f // 2 * 2, f // 4 * 4
    gain_copies = [
        [links.copy(gain_at(f, 1), gain_at(f, 1), links.at_core())],
        [links.copy(gain_at(pair, 2), gain_at(pair, 2), links.at_b())],
        [links.copy(gain_at(chip_four, 4), gain_at(chip_four, 4), links.at_a(d)) for d in range(1, na)],
    ]
    stores = []

    def store(src, dst):
        copies = links.local(src, dst)
        copies.start()
        stores.append(copies)

    gain_land[f] = gain_send[...]
    for copies in gain_copies[0]:
        copies.start()
    units[0].start()
    units[1].start()
    for j in range(ns):
        w_land[j, rows_at(f, local), :] = pack[j]
    stage_loads = []
    tile = w_gate.shape[2]
    for c in range(2):
        for k in range(chips - 1):
            source = (wg, every, slice((k * 2 + c) * tile, (k * 2 + c + 1) * tile))
            stage_loads.append(links.local(source, (stage_gate, c, k)))
    for load in stage_loads:
        load.start()
    store_own = [links.local(wo, (wo_land, rows_at(f, local))), links.local(wd, (w_down, rows_at(f // 2, depth)))]
    for copies in store_own:
        copies.start()
    fill_tables(cosines, sines, narrow_cosines[rows_at(z, span), :], narrow_sines[rows_at(z, span), :], heads + kv)
    token_load.wait()
    old = rows_in[...]
    inverse = lax.rsqrt(jnp.mean(old * old, axis=1, keepdims=True) + norm_eps)
    for stage in range(3):
        for copies in gain_copies[stage]:
            copies.wait()
        if stage < 2:
            for copies in gain_copies[stage + 1]:
                copies.start()
    for j in range(nf):
        gains_out[:, j * local : (j + 1) * local] = gain_land[j, 0:2, :local]
    first[...] = (old * inverse * gains_out[0:1, :]).astype(BF16)
    store(first, first_out)

    def project(n):
        g = lax.rem(z + turns[n], ns)
        units[n].finish()
        y = nn_dot(first[...], w_land[g])
        for i in range(count):
            part = y[i * span : (i + 1) * span]
            part = (part * cosines[...] + swap_halves(part) * sines[...]).astype(BF16)
            if turns[n] == 0:
                q_land[i, z] = part
            else:
                q_send[g, i] = part
        if turns[n] > 0:
            q_copies[turns[n] - 1][0].start()
        if n > 0 and turns[n - 1] > 0:
            for copies in q_copies[turns[n - 1] - 1][1:]:
                copies.start()
        store((w_land, g), (w_qkv, g))

    last = len(units)
    for n in range(ns):
        units[n].turn()
        if n + 2 < last:
            units[n + 2].start()
        if n > 0:
            units[n - 1].pass_on()
        if n > 1:
            project(n - 2)
    units[ns].turn()
    for load in stage_loads:
        load.wait()
    gate_unit.start()
    units[ns - 1].pass_on()
    project(ns - 2)
    gate_unit.other_start()
    project(ns - 1)
    units[ns].pass_on()
    cot_load.wait()
    low[...] = hidden[...].astype(BF16)
    low_copy.start()
    store(low, (low_both, pl.ds(0, rows)))

    def attend(i):
        for copies in q_copies:
            copies[i].wait()
        for j in range(ns):
            at = slice(j * span, (j + 1) * span)
            for h in range(heads):
                qs[h, at, :] = q_land[i, j, :, h * HEAD_DIM : (h + 1) * HEAD_DIM]
            for h in range(kv):
                k0, v0 = (heads + h) * HEAD_DIM, (heads + kv + h) * HEAD_DIM
                ks[h, at, :] = q_land[i, j, :, k0 : k0 + HEAD_DIM]
                vs[h, at, :] = q_land[i, j, :, v0 : v0 + HEAD_DIM]
        attend_heads(ns, kv, span, qs, ks, vs, a_send.at[i], log.at[i])
        for copies in a_copies[i]:
            copies.start()
        a_land[i, z] = a_send[i, z]

    for i in range(count):
        attend(i)
        if i == 0:
            units[ns + 1].turn()
            units[ns].finish()
            store_own[0].wait()
            store(wo_land, w_out)
    store(q_land, packed)
    store(a_send, heads_attended)
    store(log, logs)
    for i in range(count):
        for copies in a_copies[i]:
            copies.wait()
        for j in range(ns):
            attended[i * span : (i + 1) * span, j * g_width : (j + 1) * g_width] = a_land[i, j]
    new = rows_in[...] + nn_dot(attended[...], wo_land[...])
    hidden[...] = new
    inverse = lax.rsqrt(jnp.mean(new * new, axis=1, keepdims=True) + norm_eps)
    second_abs[...] = (new * inverse * gains_out[1:2, :]).astype(BF16)
    second_copy.start()
    store(second_abs, (second_both, pl.ds(0, rows)))
    store(attended, attended_out)
    store(hidden, hidden_out)
    units[ns + 1].pass_on()
    gate_unit.turn()
    gate_unit.turn_late()
    gate_unit.finish()
    second_copy.wait()
    low_copy.wait()
    store_own[1].wait()
    for copies in stores:
        copies.wait()


def fore(mesh, count, kv, tokens, cotangent, gains_in, wq, wk, wv, wo, wg, wd, narrow_cosines, narrow_sines):
    ns, nf = mesh
    na = nf // 4
    chips = 2 * na
    rows, width = tokens.shape
    span = rows // count
    length = ns * span
    heads = kv * GROUP
    g_width = heads * HEAD_DIM
    q_width = g_width + 2 * kv * HEAD_DIM
    local, depth = wq.shape[0], wd.shape[0]
    tile = wg.shape[1] // (2 * chips)
    anywhere, vmem = pl.BlockSpec(memory_space=pl.ANY), pl.BlockSpec(memory_space=pltpu.VMEM)
    low = lambda *shape: jax.ShapeDtypeStruct(shape, BF16)
    wide = lambda *shape: jax.ShapeDtypeStruct(shape, F32)
    outs = [
        low(ns, width, q_width),
        low(width, width),
        low(chips - 1, width, tile),
        low(chips * depth, width),
        low(rows, width),
        low(count, ns, span, q_width),
        low(count, ns, span, g_width),
        wide(count, length, 128),
        low(rows, width),
        wide(rows, width),
        low(2 * rows, width),
        low(2 * rows, width),
        wide(2, width),
    ]
    scratch = [
        pltpu.VMEM((rows, width), F32),
        pltpu.VMEM((rows, width), F32),
        pltpu.VMEM((rows, width), BF16),
        pltpu.VMEM((ns, local, q_width), BF16),
        pltpu.VMEM((ns, width, q_width), BF16),
        pltpu.VMEM((width, width), BF16),
        pltpu.VMEM((ns, count, span, q_width), BF16),
        pltpu.VMEM((count, ns, span, q_width), BF16),
        pltpu.VMEM((count, ns, span, g_width), BF16),
        pltpu.VMEM((count, ns, span, g_width), BF16),
        pltpu.VMEM((2, chips - 1, local, tile), BF16),
        pltpu.VMEM((8, 256), F32),
        pltpu.VMEM((nf, 8, 256), F32),
        pltpu.VMEM((heads, length, HEAD_DIM), BF16),
        pltpu.VMEM((kv, length, HEAD_DIM), BF16),
        pltpu.VMEM((kv, length, HEAD_DIM), BF16),
        pltpu.VMEM((count, length, 128), F32),
        pltpu.VMEM((rows, width), BF16),
        pltpu.VMEM((8, 128), BF16),
        pltpu.VMEM((rows, width), BF16),
        pltpu.VMEM((rows, width), BF16),
        pltpu.VMEM((span, q_width), F32),
        pltpu.VMEM((span, q_width), F32),
    ]
    return pl.pallas_call(
        functools.partial(fore_kernel, mesh, count, kv),
        in_specs=[anywhere] * 2 + [vmem] * 4 + [anywhere] * 3 + [vmem] * 2,
        out_specs=[anywhere] * 12 + [vmem],
        out_shape=outs,
        scratch_shapes=scratch
        + [pltpu.SemaphoreType.DMA((160,)), pltpu.SemaphoreType.DMA((160,)), pltpu.SemaphoreType.DMA((64,))],
        compiler_params=pltpu.CompilerParams(vmem_limit_bytes=VMEM_MOST, collective_id=0, has_side_effects=True),
        name="fore",
    )(tokens, cotangent, gains_in, wq, wk, wv, wo, wg, wd, narrow_cosines, narrow_sines)


def attend_back_heads(ns, kv, span, qs, ks, vs, gs, attended, logs, dk, dv, result):
    scale = 1.0 / math.sqrt(HEAD_DIM)
    heads = kv * GROUP
    row = lax.broadcasted_iota(jnp.int32, (span, span), 0)
    column = lax.broadcasted_iota(jnp.int32, (span, span), 1)
    causal = row >= column
    dk[...] = jnp.zeros_like(dk)
    dv[...] = jnp.zeros_like(dv)
    for s in range(ns):
        here = slice(s * span, (s + 1) * span)
        for h in range(heads):
            g = h // GROUP
            q, grad = qs[h, here, :], gs[h, here, :]
            log_total = logs[here, h : h + 1]
            out = attended[s, :, h * HEAD_DIM : (h + 1) * HEAD_DIM]
            delta = jnp.sum(grad.astype(F32) * out.astype(F32), axis=1, keepdims=True)
            k, v = ks[g, here, :], vs[g, here, :]
            near = jnp.where(causal, jnp.exp(nt_dot(q, k) * scale - log_total), 0.0)
            slope = (near * (nt_dot(grad, v) - delta) * scale).astype(BF16)
            dq = nn_dot(slope, k)
            dk[g, here, :] += tn_dot(slope, q)
            dv[g, here, :] += tn_dot(near.astype(BF16), grad)
            if s > 0:
                before = slice(0, s * span)
                k, v = ks[g, before, :], vs[g, before, :]
                far = jnp.exp(nt_dot(q, k) * scale - log_total)
                slope = (far * (nt_dot(grad, v) - delta) * scale).astype(BF16)
                dq = dq + nn_dot(slope, k)
                dk[g, before, :] += tn_dot(slope, q)
                dv[g, before, :] += tn_dot(far.astype(BF16), grad)
            result[here, h * HEAD_DIM : (h + 1) * HEAD_DIM] = dq
    for g in range(kv):
        k0 = (heads + g) * HEAD_DIM
        v0 = (heads + kv + g) * HEAD_DIM
        result[:, k0 : k0 + HEAD_DIM] = dk[g]
        result[:, v0 : v0 + HEAD_DIM] = dv[g]


def back_kernel(
    mesh, count, kv,
    dx_own, dx_other, hidden, cotangent, gains, w_out, w_qkv, packed, attended, logs, cosines, sines, tokens, dwg, dwu,
    high, low_out, out, gain_grads, dqkv, sum_gate, sum_up,
    low, sum_rows, sum_land, dx_land, g_send, g_land, q_send, q_land, swap_send, swap_land, *rest,
):
    parts, (send_sems, recv_sems, local_sems) = rest[:-3], rest[-3:]
    links = Links(mesh, send_sems, recv_sems, local_sems)
    ns, na = links.ns, links.na
    chips = 2 * na
    z, core = links.z, links.core
    rows, width = hidden.shape
    span = rows // count
    length = ns * span
    heads = kv * GROUP
    g_width, q_width = heads * HEAD_DIM, (heads + 2 * kv) * HEAD_DIM
    half = dwg.shape[1]
    block = width // chips
    links.barrier()

    dx_load = links.local(dx_other, dx_land)
    dx_load.start()
    sums = []
    for n, source in enumerate((dwg, dwu)):
        for b_first in (True, False):
            columns = slice(0, half // 2) if b_first else slice(half // 2, half)
            at = (n * 2 + (0 if b_first else 1)) * 3
            partial = lambda k, source=source, columns=columns: (source, rows_at(k, block), columns)
            sums.append(ChipSum(links, partial, b_first, *parts[at : at + 3]))
    for item in sums:
        item.start()
        item.load()

    g_copies, q_copies = [], []
    for i in range(count):
        g_copies.append([links.copy((g_send, i, lax.rem(z + d, ns)), (g_land, i, z), links.at_z(d)) for d in range(1, ns)])
        q_copies.append([links.copy((q_send, i, lax.rem(z + d, ns)), (q_land, z, i), links.at_z(d)) for d in range(1, ns)])

    def out_back(dx, old, grad, w):
        loads = [links.local(dx_own, dx), links.local(hidden, old), links.local(cotangent, grad), links.local(w_out, w)]
        for load in loads:
            load.start()
        dx_load.wait()
        for load in loads[:3]:
            load.wait()
        step = dx[...] + dx_land[...].astype(F32)
        inverse = lax.rsqrt(jnp.mean(old[...] * old[...], axis=1, keepdims=True) + norm_eps)
        normed = old[...] * inverse
        gain_grads[1:2, :] = jnp.sum(step * normed, axis=0, keepdims=True)
        grad[...] = grad[...] + norm_back(step, normed, inverse, gains[1:2, :])
        low[...] = grad[...].astype(BF16)
        stores = [links.local(grad, high), links.local(low, low_out)]
        for store in stores:
            store.start()
        loads[3].wait()
        for i in range(count):
            here = slice(i * span, (i + 1) * span)
            part = nt_dot(low[here, :], w[...]).astype(BF16)
            for j in range(ns):
                g_send[i, j] = part[:, j * g_width : (j + 1) * g_width]
            for copies in g_copies[i]:
                copies.start()
            g_land[i, z] = g_send[i, z]
        for store in stores:
            store.wait()

    pl.run_scoped(
        out_back,
        pltpu.VMEM((rows, width), F32),
        pltpu.VMEM((rows, width), F32),
        pltpu.VMEM((rows, width), F32),
        pltpu.VMEM((width, width), BF16),
    )

    def attention(qkv, mid, log, qs, ks, vs, gs, dk, dv, result, cosine, sine):
        fill_tables(cosine, sine, cosines[...], sines[...], heads + kv)
        for i in range(count):
            loads = [links.local((packed, i), qkv), links.local((attended, i), mid), links.local((logs, i), log)]
            for load in loads:
                load.start()
            for load in loads:
                load.wait()
            for j in range(ns):
                at = slice(j * span, (j + 1) * span)
                for h in range(heads):
                    qs[h, at, :] = qkv[j, :, h * HEAD_DIM : (h + 1) * HEAD_DIM]
                for h in range(kv):
                    k0, v0 = (heads + h) * HEAD_DIM, (heads + kv + h) * HEAD_DIM
                    ks[h, at, :] = qkv[j, :, k0 : k0 + HEAD_DIM]
                    vs[h, at, :] = qkv[j, :, v0 : v0 + HEAD_DIM]
            for copies in g_copies[i]:
                copies.wait()
            for j in range(ns):
                for h in range(heads):
                    gs[h, j * span : (j + 1) * span, :] = g_land[i, j, :, h * HEAD_DIM : (h + 1) * HEAD_DIM]
            attend_back_heads(ns, kv, span, qs, ks, vs, gs, mid, log, dk, dv, result)
            for j in range(ns):
                here = slice(j * span, (j + 1) * span)
                part = result[here, :]
                q_send[i, j] = (part * cosine[here, :] - swap_halves(part) * sine[here, :]).astype(BF16)
            for copies in q_copies[i]:
                copies.start()
            q_land[z, i] = q_send[i, z]
            if i < len(sums) // 2:
                for item in sums[2 * i : 2 * i + 2]:
                    item.turn()

    pl.run_scoped(
        attention,
        pltpu.VMEM((ns, span, q_width), BF16),
        pltpu.VMEM((ns, span, g_width), BF16),
        pltpu.VMEM((length, 128), F32),
        pltpu.VMEM((heads, length, HEAD_DIM), BF16),
        pltpu.VMEM((kv, length, HEAD_DIM), BF16),
        pltpu.VMEM((kv, length, HEAD_DIM), BF16),
        pltpu.VMEM((heads, length, HEAD_DIM), BF16),
        pltpu.VMEM((kv, length, HEAD_DIM), F32),
        pltpu.VMEM((kv, length, HEAD_DIM), F32),
        pltpu.VMEM((length, q_width), F32),
        pltpu.VMEM((length, q_width), F32),
        pltpu.VMEM((length, q_width), F32),
    )

    swaps = []
    local = block // 2
    for item in sums[2 * count :]:
        item.turn()

    def swap(n):
        for m in range(2):
            total = sums[2 * n + m].finish()
            swap_send[n, m, 0] = total[:local]
            swap_send[n, m, 1] = total[local:]
        for m in range(2):
            copies = links.copy((swap_send, n, m, 1 - core), (swap_land, n, m), links.at_core())
            copies.start()
            swaps.append(copies)

    tile = half // chips
    stores = []
    early = first_piece(ns, 2 * half)
    piece = (sum_rows, 0, slice(None), slice(0, max(early, 1)))
    end, inner, inward = line_place(links)[:3]
    early_copy = links.copy(piece, sum_land, inward)

    def combine(n, total):
        for m in range(2):
            swaps[2 * n + m].wait()
            kept, arrived = swap_send[n, m, core], swap_land[n, m]
            for t in range(chips // 2):
                here = slice(t * tile, (t + 1) * tile)
                k = m * (chips // 2) + t
                one, two = kept[:, here], arrived[:, here]
                sum_rows[n, :, 2 * k * tile : (2 * k + 1) * tile] = jnp.where(core == 0, one, two)
                sum_rows[n, :, (2 * k + 1) * tile : (2 * k + 2) * tile] = jnp.where(core == 0, two, one)
        if n == 0 and early:
            pl.when(end)(early_copy.start)
        else:
            copies = links.local((sum_rows, n), total)
            copies.start()
            stores.append(copies)

    def project_back(w, old, base, grad):
        loads = [links.local(tokens, old), links.local(high, base), links.local(w_qkv, w)]
        for load in loads:
            load.start()
        swap(0)
        for load in loads:
            load.wait()
        for i in range(count):
            here = slice(i * span, (i + 1) * span)
            if i == count - 1:
                combine(0, sum_gate)
                swap(1)
                combine(1, sum_up)
            for copies in q_copies[i]:
                copies.wait()
            total = nt_dot(q_land[0, i], w[0])
            for j in range(1, ns):
                total = total + nt_dot(q_land[j, i], w[j])
            grad[here, :] = total
            copies = links.local((q_land, slice(None), i), (dqkv, slice(None), i))
            copies.start()
            stores.append(copies)
            step, rows_old = grad[here, :], old[here, :]
            inverse = lax.rsqrt(jnp.mean(rows_old * rows_old, axis=1, keepdims=True) + norm_eps)
            normed = rows_old * inverse
            part_sum = jnp.sum(step * normed, axis=0, keepdims=True)
            gain_grads[0:1, :] = part_sum if i == 0 else gain_grads[0:1, :] + part_sum
            base[here, :] = base[here, :] + norm_back(step, normed, inverse, gains[0:1, :])
            copies = links.local((base, here), (out, here))
            copies.start()
            stores.append(copies)
        if early:

            @pl.when(inner)
            def _():
                early_copy.wait_recv()
                put(piece, (get(piece).astype(F32) + sum_land[...].astype(F32)).astype(BF16))

            pl.when(end)(early_copy.wait_send)
            copies = links.local((sum_rows, 0), sum_gate)
            copies.start()
            stores.append(copies)
        for copies in stores:
            copies.wait()

    pl.run_scoped(
        project_back,
        pltpu.VMEM((ns, width, q_width), BF16),
        pltpu.VMEM((rows, width), F32),
        pltpu.VMEM((rows, width), F32),
        pltpu.VMEM((rows, width), F32),
    )


def back(mesh, count, kv, dx_own, dx_other, hidden, cotangent, gains, w_out, w_qkv, packed, attended, logs, cosines, sines, tokens, dwg, dwu):
    ns, nf = mesh
    na = nf // 4
    rows, width = hidden.shape
    span = rows // count
    heads = kv * GROUP
    g_width, q_width = heads * HEAD_DIM, (heads + 2 * kv) * HEAD_DIM
    half = dwg.shape[1]
    block = width // (2 * na)
    local = block // 2
    anywhere = pl.BlockSpec(memory_space=pl.ANY)
    vmem = pl.BlockSpec(memory_space=pltpu.VMEM)
    operands = [dx_own, dx_other, hidden, cotangent, gains, w_out, w_qkv, packed, attended, logs, cosines, sines, tokens, dwg, dwu]
    wide = jax.ShapeDtypeStruct((rows, width), F32)
    summed = jax.ShapeDtypeStruct((local, 2 * half), BF16)
    scratch = [
        pltpu.VMEM((rows, width), BF16),
        pltpu.VMEM((2, local, 2 * half), BF16),
        pltpu.VMEM((local, max(first_piece(ns, 2 * half), 128)), BF16),
        pltpu.VMEM((rows, width), BF16),
        pltpu.VMEM((count, ns, span, g_width), BF16),
        pltpu.VMEM((count, ns, span, g_width), BF16),
        pltpu.VMEM((count, ns, span, q_width), BF16),
        pltpu.VMEM((ns, count, span, q_width), BF16),
        pltpu.VMEM((2, 2, 2, local, half // 2), BF16),
        pltpu.VMEM((2, 2, local, half // 2), BF16),
    ]
    for _ in range(2):
        for b_first in (True, False):
            scratch += chip_sum_shapes(na, b_first, block, half // 2)
    return pl.pallas_call(
        functools.partial(back_kernel, mesh, count, kv),
        in_specs=[vmem if x.shape[0] == 2 and x.ndim == 2 or x.shape[1] == HEAD_DIM else anywhere for x in operands],
        out_specs=[anywhere, anywhere, anywhere, vmem, anywhere, anywhere, anywhere],
        out_shape=[
            wide,
            jax.ShapeDtypeStruct((rows, width), BF16),
            wide,
            jax.ShapeDtypeStruct((2, width), F32),
            jax.ShapeDtypeStruct((ns, count, span, q_width), BF16),
            summed,
            summed,
        ],
        scratch_shapes=scratch
        + [pltpu.SemaphoreType.DMA((64,)), pltpu.SemaphoreType.DMA((64,)), pltpu.SemaphoreType.DMA((64,))],
        compiler_params=pltpu.CompilerParams(vmem_limit_bytes=VMEM_MOST, collective_id=1, has_side_effects=True),
        name="back",
    )(*operands)


class LineSum:
    def __init__(self, links, term, first, second, total, out=None, begun=False):
        self.links, self.term, self.first, self.second, self.total = links, term, first, second, total
        self.dtype = (term[0] if isinstance(term, tuple) else term).dtype
        self.deep = links.ns // 2 > 1
        self.begun = begun
        self.end, self.inner, inward, outward = line_place(links)
        moved = self.deep and not begun
        self.inward = links.copy(term, first, inward) if moved else None
        self.onward = links.again(first, first, inward) if moved else None
        self.sum = first if moved else term
        self.across = links.copy(self.sum, second, inward)
        self.outward = links.copy(total, total, outward) if self.deep else None
        self.store = links.local(total, out) if out is not None else None

    def keep(self):
        if self.store is not None:
            self.store.start()

    def add(self, target, one, two):
        put(target, (get(one).astype(F32) + get(two).astype(F32)).astype(self.dtype))

    def begin(self):
        if self.begun:
            pl.when(self.inner)(self.across.start)
        elif self.deep:
            pl.when(self.end)(self.inward.start)
        else:
            self.across.start()

    def relay(self):
        if not self.deep or self.begun:
            return

        @pl.when(jnp.logical_not(self.end))
        def _():
            self.inward.wait_recv()
            self.add(self.first, self.term, self.first)
            pl.when(self.inner)(self.across.start)
            pl.when(jnp.logical_not(self.inner))(self.onward.start)

    def settle(self):
        @pl.when(self.inner)
        def _():
            self.across.wait()
            self.add(self.total, self.sum, self.second)
            if self.deep:
                self.outward.start()
            self.keep()

        if self.deep:

            @pl.when(jnp.logical_not(self.inner | self.end))
            def _():
                self.outward.wait_recv()
                self.outward.start()
                self.keep()

    def finish(self):
        if self.deep:

            @pl.when(self.end)
            def _():
                self.outward.wait_recv()
                self.keep()

            if not self.begun:
                pl.when(jnp.logical_not(self.inner))(self.inward.wait_send)
            pl.when(jnp.logical_not(self.end))(self.outward.wait_send)


def finish_kernel(
    mesh, count, kv,
    term_gate, term_up, dwd, first, dqkv, attended, low, gains,
    out_gate, out_up, out_down, out_out, out_qkv, out_gains,
    tot_gate, tot_up, tot_down, tot_out, tot_qkv, term_down, term_out, term_qkv, in_gate, in_up, in_down, in_out, in_qkv,
    first_both, attended_both, low_both, dq_both, w_out_part, w_qkv_part,
    swap_out, land_out, swap_qkv, land_qkv, gain_terms, gain_lands, *rest,
):
    parts, (send_sems, recv_sems, local_sems) = rest[:-3], rest[-3:]
    links = Links(mesh, send_sems, recv_sems, local_sems)
    ns, na = links.ns, links.na
    chips, per = 2 * na, ns // 2
    core = links.core
    rows, width = first.shape
    q_width = dqkv.shape[3]
    middle = width // 2
    links.barrier()

    def lines(term, inbox, total, out, pieces, begun=False):
        size = term.shape[1] // pieces
        every = slice(None)
        made = []
        for i in range(pieces):
            at = slice(i * size, (i + 1) * size)
            refs = [(ref, *where, every, at) for ref, *where in ((term,), (inbox, 0), (inbox, 1), (total,), (out,))]
            made.append(LineSum(links, *refs, begun and i == 0))
        return made

    gate_lines = lines(term_gate, in_gate, tot_gate, out_gate, GATE_PIECES, first_piece(ns, term_gate.shape[1]) > 0)
    up_lines = lines(term_up, in_up, tot_up, out_up, 4)
    down_lines = lines(term_down, in_down, tot_down, out_down, 4)
    out_lines = lines(term_out, in_out, tot_out, out_out, 2)
    qkv_lines = lines(term_qkv, in_qkv, tot_qkv, out_qkv, 4)
    for line in gate_lines + up_lines:
        line.begin()

    sends = [
        links.copy((dqkv, pl.ds((1 - core) * per, per)), (dq_both, 1), links.at_core()),
        links.copy((low, slice(None), rows_at(1 - core, middle)), (low_both, 1), links.at_core()),
        links.copy(first, (first_both, 1), links.at_core()),
        links.copy(attended, (attended_both, 1), links.at_core()),
    ]
    loads = [
        links.local((low, slice(None), rows_at(core, middle)), (low_both, 0)),
        links.local(attended, (attended_both, 0)),
        links.local(first, (first_both, 0)),
        links.local((dqkv, pl.ds(core * per, per)), (dq_both, 0)),
    ]
    for copies in loads + sends[1:2] + sends[3:4] + sends[2:3] + sends[:1]:
        copies.start()

    down_rows = dwd.shape[0] // chips
    block = width // chips

    def pair(source, row_count, at, staged):
        made = []
        cut = source.shape[1] // 2
        for n, b_first in enumerate((True, False)):
            columns = slice(0, cut) if b_first else slice(cut, 2 * cut)
            partial = lambda k, columns=columns: (source, rows_at(k, row_count), columns)
            refs = parts[at[n] : at[n + 1]]
            made.append(ChipSum(links, partial, b_first, *(refs if staged else (*refs[:2], None))))
        return made

    down = pair(dwd, down_rows, (0, 3, 6), True)
    for item in down:
        item.start()
        item.load()

    gain_copies = [links.copy((gain_terms, 0), (gain_lands, 0), links.at_core()), links.copy((gain_terms, 1), (gain_lands, 1), links.at_b())]
    gain_copies += [links.copy((gain_terms, 2), (gain_lands, 1 + d), links.at_a(d)) for d in range(1, na)]
    gain_line = LineSum(links, (gain_terms, 3), (gain_lands, na + 1), (gain_lands, na + 2), out_gains)
    gain_terms[0] = gains[...]
    gain_copies[0].start()

    def next_gain(i):
        for copies in gain_copies[i : i + 1] if i < 2 else gain_copies[2:]:
            copies.wait()
        if i < 2:
            gain_terms[i + 1] = gain_terms[i] + gain_lands[i]
            for copies in gain_copies[1:2] if i == 0 else gain_copies[2:]:
                copies.start()
        else:
            total = gain_terms[2]
            for d in range(1, na):
                total = total + gain_lands[1 + d]
            gain_terms[3] = total
            gain_line.begin()

    def qkv_part(p):
        columns = slice(p * q_width, (p + 1) * q_width)
        mine, other = dq_both[0, p].reshape(rows, q_width), dq_both[1, p].reshape(rows, q_width)
        for k in range(chips):
            at = slice(k * block, (k + 1) * block)
            total = tn_dot(first_both[0, :, at], mine) + tn_dot(first_both[1, :, at], other)
            w_qkv_part[at, columns] = total.astype(BF16)

    def swap(sums, send, land):
        local = block // 2
        for n, item in enumerate(sums):
            total = item.finish()
            size = total.shape[1]
            send[0, :, n * size : (n + 1) * size] = total[:local]
            send[1, :, n * size : (n + 1) * size] = total[local:]
        copies = links.copy((send, 1 - core), land, links.at_core())
        copies.start()
        return copies

    out_sums = pair(w_out_part, block, (6, 8, 10), False)
    qkv_sums = pair(w_qkv_part, block, (10, 12, 14), False)
    cut = width // 2
    next_gain(0)
    for i in (1, 3):
        sends[i].wait()
    for i in (0, 1):
        loads[i].wait()
    gate_lines[0].relay()
    for k in range(chips):
        at = slice(k * block, (k + 1) * block)
        total = tn_dot(attended_both[0, :, at], low_both[0]) + tn_dot(attended_both[1, :, at], low_both[1])
        w_out_part[at, :] = total.astype(BF16)
    for item in out_sums:
        item.start()
    gate_lines[1].relay()
    next_gain(1)
    for i in (0, 2):
        sends[i].wait()
    for i in (2, 3):
        loads[i].wait()
    gate_lines[0].settle()
    for p in range(per // 2):
        qkv_part(p)
    gate_lines[2].relay()
    next_gain(2)
    gate_lines[1].settle()
    for p in range(per // 2, per):
        qkv_part(p)
    gate_lines[3].relay()
    for item in down:
        item.turn()
    for item in qkv_sums:
        item.start()
    gate_lines[2].settle()
    gain_line.relay()
    gate_lines[3].settle()
    for item in out_sums:
        item.turn()
    up_lines[0].relay()
    gain_line.settle()
    up_lines[1].relay()
    up_lines[0].settle()
    term_down[:, :cut] = down[0].finish()
    term_down[:, cut:] = down[1].finish()
    for line in down_lines:
        line.begin()
    up_lines[2].relay()
    up_lines[1].settle()
    up_lines[3].relay()
    up_lines[2].settle()
    down_lines[0].relay()
    up_lines[3].settle()
    for item in qkv_sums:
        item.turn()
    down_lines[1].relay()
    down_lines[0].settle()
    out_swap = swap(out_sums, swap_out, land_out)
    down_lines[2].relay()
    down_lines[1].settle()
    out_swap.wait()
    kept, arrived = swap_out[core], land_out[...]
    term_out[:, :cut] = jnp.where(core == 0, kept, arrived)
    term_out[:, cut:] = jnp.where(core == 0, arrived, kept)
    for line in out_lines:
        line.begin()
    down_lines[3].relay()
    down_lines[2].settle()
    qkv_swap = swap(qkv_sums, swap_qkv, land_qkv)
    out_lines[0].relay()
    down_lines[3].settle()
    qkv_swap.wait()
    kept, arrived = swap_qkv[core], land_qkv[...]
    for n in range(2):
        group = jnp.where(core == n, kept, arrived)
        for p in range(per):
            taken, start = p * q_width, 0
            for size in (kv * GROUP * HEAD_DIM, kv * HEAD_DIM, kv * HEAD_DIM):
                at = start + (n * per + p) * size
                term_qkv[:, at : at + size] = group[:, taken : taken + size]
                taken, start = taken + size, start + ns * size
    for line in qkv_lines:
        line.begin()
    out_lines[1].relay()
    out_lines[0].settle()
    qkv_lines[0].relay()
    out_lines[1].settle()
    for n in range(1, len(qkv_lines)):
        qkv_lines[n].relay()
        qkv_lines[n - 1].settle()
    qkv_lines[-1].settle()
    every_line = [*gate_lines, *up_lines, gain_line, *down_lines, *out_lines, *qkv_lines]
    for line in every_line:
        line.finish()
    for line in every_line:
        if line.store is not None:
            line.store.wait()


def finish(mesh, count, kv, term_gate, term_up, dwd, first, dqkv, attended, low, gains):
    ns, nf = mesh
    na, per = nf // 4, ns // 2
    rows, width = first.shape
    q_width = dqkv.shape[3]
    local, half = term_gate.shape[0], width // 2
    block = 2 * local
    anywhere, vmem = pl.BlockSpec(memory_space=pl.ANY), pl.BlockSpec(memory_space=pltpu.VMEM)
    down = (dwd.shape[0] // (2 * na), dwd.shape[1])
    shapes = [term_gate.shape, term_up.shape, down, (local, width), (local, ns * q_width)]
    scratch = [pltpu.VMEM(s, BF16) for s in shapes]
    scratch += [pltpu.VMEM(s, BF16) for s in shapes[2:]]
    scratch += [pltpu.VMEM((2,) + tuple(s), BF16) for s in shapes]
    scratch += [
        pltpu.VMEM((2, rows, width), BF16),
        pltpu.VMEM((2, rows, width), BF16),
        pltpu.VMEM((2, rows, half), BF16),
        pltpu.VMEM((2, per, count, rows // count, q_width), BF16),
        pltpu.VMEM((width, half), BF16),
        pltpu.VMEM((width, per * q_width), BF16),
        pltpu.VMEM((2, local, half), BF16),
        pltpu.VMEM((local, half), BF16),
        pltpu.VMEM((2, local, per * q_width), BF16),
        pltpu.VMEM((local, per * q_width), BF16),
        pltpu.VMEM((4, 2, width), F32),
        pltpu.VMEM((na + 3, 2, width), F32),
    ]
    scratch += chip_sum_shapes(na, True, down[0], down[1] // 2) + chip_sum_shapes(na, False, down[0], down[1] // 2)
    for columns in (half // 2, per * q_width // 2):
        for b_first in (True, False):
            scratch += chip_sum_shapes(na, b_first, block, columns)[:2]
    return pl.pallas_call(
        functools.partial(finish_kernel, mesh, count, kv),
        in_specs=[vmem, vmem] + [anywhere] * 5 + [vmem],
        out_specs=[anywhere] * 5 + [vmem],
        out_shape=[jax.ShapeDtypeStruct(s, BF16) for s in shapes] + [jax.ShapeDtypeStruct((2, width), F32)],
        scratch_shapes=scratch
        + [pltpu.SemaphoreType.DMA((128,)), pltpu.SemaphoreType.DMA((128,)), pltpu.SemaphoreType.DMA((64,))],
        compiler_params=pltpu.CompilerParams(vmem_limit_bytes=VMEM_MOST, collective_id=2, has_side_effects=True),
        name="finish",
    )(term_gate, term_up, dwd, first, dqkv, attended, low, gains)


def widen_kernel(cuts, *refs):
    gate, up, down, out, qkv, hidden, own, other = refs[:8]
    o_gate, o_up, o_down, o_out, o_q, o_k, o_v, o_block = refs[8:]
    for source, target in ((gate, o_gate), (up, o_up), (down, o_down), (out, o_out)):
        target[...] = source[...].astype(F32)
    for (start, end), target in zip(cuts, (o_q, o_k, o_v)):
        target[...] = qkv[:, start:end].astype(F32)
    o_block[...] = hidden[...] + own[...] + other[...].astype(F32)


def widen(gate, up, down, out, qkv, hidden, own, other, cuts):
    steps = 4
    operands = [gate, up, down, out, qkv, hidden, own, other]
    rows = out.shape[0]
    shapes = [gate.shape, up.shape, down.shape, out.shape] + [(rows, end - start) for start, end in cuts] + [hidden.shape]
    block = lambda shape: pl.BlockSpec((shape[0] // steps, shape[1]), lambda i: (i, 0))
    return pl.pallas_call(
        functools.partial(widen_kernel, cuts),
        grid=(steps,),
        in_specs=[block(x.shape) for x in operands],
        out_specs=[block(shape) for shape in shapes],
        out_shape=[jax.ShapeDtypeStruct(shape, F32) for shape in shapes],
        compiler_params=pltpu.CompilerParams(vmem_limit_bytes=VMEM_LIMIT),
        cost_estimate=pl.CostEstimate(flops=0, bytes_accessed=40 * rows * gate.shape[1], transcendentals=0),
        name="widen",
    )(*operands)


def solution(mesh):
    ns, nf = mesh.shape["seq"], mesh.shape["fsdp"]
    na = nf // 4
    chips = 2 * na
    kv = KEY_VALUE_HEADS // ns

    def body(tokens, cotangent, attention_gain, feedforward_gain, query_weight, key_matrix, value_matrix, out_weight, gate_weight, up_weight, down_weight):
        count, span, width = tokens.shape
        rows = count * span
        local = query_weight.shape[0]
        sizes = (ns, nf)
        mine = lax.axis_index("fsdp")
        cosines, sines = (jnp.asarray(x) for x in rope_tables(ns * span))
        flat = tokens.reshape(rows, width)
        grad_flat = cotangent.reshape(rows, width)
        (w_qkv, w_out, w_gate, w_down, first, packed, heads_attended, logs, attended, hidden_one, second_both, low_both, gains) = fore(
            sizes, count, kv, flat, grad_flat, jnp.stack([attention_gain, feedforward_gain]),
            query_weight, key_matrix, value_matrix, out_weight, gate_weight, down_weight, cosines, sines,
        )
        dwg, dwu, dwd, out_own, out_arrived, dx_own, dx_arrived = ffn(sizes, second_both, low_both, w_gate, w_down, up_weight, gate_weight)
        high, low, grad_tokens, gain_grads, dqkv, sum_gate, sum_up = back(
            sizes, count, kv, dx_own, dx_arrived, hidden_one, grad_flat, gains, w_out, w_qkv,
            packed, heads_attended, logs, cosines, sines, flat, dwg, dwu,
        )
        *sums, gain_grads = finish(
            sizes, count, kv, sum_gate, sum_up, dwd, first, dqkv, attended, low, gain_grads
        )
        q_end, k_end = ns * kv * GROUP * HEAD_DIM, ns * kv * (GROUP + 1) * HEAD_DIM
        cuts = ((0, q_end), (q_end, k_end), (k_end, sums[4].shape[1]))
        grad_gate, grad_up, grad_down, grad_out, grad_query, grad_key, grad_value, block_out = widen(
            *sums, hidden_one, out_own, out_arrived, cuts
        )
        gain_grads = lax.dynamic_slice(gain_grads, (0, mine * local), (2, local))

        return (
            block_out.reshape(count, span, width),
            grad_tokens.reshape(count, span, width),
            gain_grads[0],
            gain_grads[1],
            grad_query,
            grad_key,
            grad_value,
            grad_out,
            grad_gate,
            grad_up,
            grad_down,
        )

    tokens_spec, gain_spec, weight_spec = P("fsdp", "seq", None), P("fsdp"), P("fsdp", None)
    return jax.shard_map(
        body,
        mesh=mesh,
        in_specs=(tokens_spec, tokens_spec, gain_spec, gain_spec) + (weight_spec,) * 7,
        out_specs=(tokens_spec, tokens_spec, gain_spec, gain_spec) + (weight_spec,) * 7,
        check_vma=False,
    )
```

```python
import functools
import math

import jax
import jax.numpy as jnp
import numpy as np
from jax import lax
from jax.experimental import pallas as pl
from jax.experimental.pallas import tpu as pltpu
from jax.sharding import PartitionSpec as P

QUERY_HEADS = 16
KEY_VALUE_HEADS = 8
HEAD_DIM = 96
GROUP = QUERY_HEADS // KEY_VALUE_HEADS
norm_eps = 1e-05
rope_base = 100000.0
masked_score = -1e30
F32, BF16 = jnp.float32, jnp.bfloat16
VMEM_LIMIT = 60 * 1024 * 1024
VMEM_MOST = 67043328
MESH = pl.DeviceIdType.MESH


def nt_dot(left, right):
    return lax.dot_general(left, right, (((1,), (1,)), ((), ())), preferred_element_type=F32)


def tn_dot(left, right):
    return lax.dot_general(left, right, (((0,), (0,)), ((), ())), preferred_element_type=F32)


def nn_dot(left, right):
    return jnp.dot(left, right, preferred_element_type=F32)


def whole(shape):
    return pl.BlockSpec(shape, lambda *_: (0,) * len(shape))


def call(kernel, scalars, operands, outs, name, flops, moved, scratch=()):
    return pl.pallas_call(
        kernel,
        grid_spec=pltpu.PrefetchScalarGridSpec(
            num_scalar_prefetch=1,
            grid=(1,),
            in_specs=[whole(x.shape) for x in operands],
            out_specs=[whole(x.shape) for x in outs],
            scratch_shapes=scratch,
        ),
        out_shape=outs,
        compiler_params=pltpu.CompilerParams(vmem_limit_bytes=VMEM_LIMIT),
        cost_estimate=pl.CostEstimate(flops=flops, bytes_accessed=moved, transcendentals=0),
        name=name,
    )(scalars, *operands)


def rope_tables(length):
    half = HEAD_DIM // 2
    freqs = np.float32(rope_base) ** (-(np.float32(2.0) * np.arange(half, dtype=np.float32)) / np.float32(HEAD_DIM))
    angles = np.arange(length, dtype=np.float32)[:, None] * freqs.astype(np.float32)[None, :]
    cosine, sine = np.cos(angles), np.sin(angles)
    return np.concatenate([cosine, cosine], 1), np.concatenate([-sine, sine], 1)


def swap_halves(values):
    half = HEAD_DIM // 2
    width = values.shape[1]
    lane = lax.broadcasted_iota(jnp.int32, values.shape, 1)
    ahead = pltpu.roll(values, width - half, 1)
    behind = pltpu.roll(values, half, 1)
    return jnp.where(lane % HEAD_DIM < half, ahead, behind)


def norm_back(grad, normed, inverse, gain):
    scaled = grad * gain
    return inverse * (scaled - normed * jnp.mean(scaled * normed, axis=1, keepdims=True))


def ffn_kernel(
    mesh, tiles, parts, x, g, wg, wd, wu, w_last, dwg, dwu, dwd, out_own, out_arrived, dx_own, dx_arrived,
    xt, acc_out, acc_dx, given_out, given_dx, act, dgate, dup, stage, land, gate, send_sems, recv_sems, local_sems,
):
    step = pl.program_id(0)
    rows = x.shape[0] // 2
    links = Links(mesh, send_sems, recv_sems, local_sems)
    chips, local, tile = tiles // parts, wu.shape[0], land.shape[2]
    cols = tile // parts
    gathers, loads = [], []
    for k in range(chips + 1):
        gathers.append(GatherHalf(links, lambda c, k=k: (stage, c, k), lambda o, k=k: (land, k, rows_at(o, local))))
        weight, tile_at = (wu, k) if k < chips else (w_last, chips - 1)
        for c in range(2):
            source = (weight, slice(None), slice((tile_at * 2 + c) * tile, (tile_at * 2 + c + 1) * tile))
            loads.append(links.local(source, (stage, c, k)))

    def begin(k):
        gathers[k].start()
        gathers[k].other_start()

    def turn(k):
        gathers[k].turn()
        gathers[k].turn_late()

    @pl.when(step == 0)
    def _():
        for load in loads:
            load.start()
        links.barrier()
        for load in loads[:2]:
            load.wait()
        gathers[0].start()
        gathers[0].other_start()
        for load in loads[2:]:
            load.wait()

    @pl.when(step == 0)
    def _():
        acc_out[...] = jnp.zeros_like(acc_out)
        acc_dx[...] = jnp.zeros_like(acc_dx)
        xt[...] = x[...].T

    def first_part():
        turn(0)
        begin(1)
        gathers[0].finish()

    def later_part(k):
        turn(k)
        for n in (2, 3) if k == 1 else (k + 2,):
            if n <= chips:
                begin(n)
        if k == chips - 1:
            turn(chips)

    for k in range(1, chips):
        pl.when(step == (k - 1) * parts + 1)(functools.partial(later_part, k))
    pl.when(step == (chips - 1) * parts)(gathers[chips].finish)
    at = pl.ds(pl.multiple_of(lax.rem(step, parts) * cols, cols), cols)
    chip = step // parts

    @pl.when(chip < chips - 1)
    def _():
        gate[...] = wg[...]

    @pl.when(chip == chips - 1)
    def _():
        gate[...] = land[chips, :, at]

    pl.when(step == 0)(first_part)
    for k in range(1, chips):
        pl.when(step == k * parts)(gathers[k].finish)
    for i in range(2):
        here = slice(i * rows, (i + 1) * rows)
        gate_pre = nn_dot(x[here, :], gate[...])
        up = nn_dot(x[here, :], land[chip, :, at])
        grad = nt_dot(g[here, :], wd[...])
        sigmoid = jax.nn.sigmoid(gate_pre)
        silu = gate_pre * sigmoid
        hidden = (silu * up).astype(BF16)
        act[here, :] = hidden
        gate_grad = (grad * up * sigmoid * (1.0 + gate_pre * (1.0 - sigmoid))).astype(BF16)
        up_grad = (grad * silu).astype(BF16)
        dgate[here, :] = gate_grad
        dup[here, :] = up_grad
        acc_out[i] += nn_dot(hidden, wd[...])
        acc_dx[i] += nt_dot(gate_grad, gate[...]) + nt_dot(up_grad, land[chip, :, at])
    leaving = [
        links.copy(given_dx, dx_arrived, links.at_core()),
        links.local((acc_dx, 0), dx_own),
        links.copy(given_out, out_arrived, links.at_core()),
        links.local((acc_out, 0), out_own),
    ]

    @pl.when(step == tiles - 1)
    def _():
        given_dx[...] = acc_dx[1].astype(BF16)
        leaving[0].start()
        given_out[...] = acc_out[1].astype(BF16)
        for copies in leaving[1:]:
            copies.start()

    dwg[...] = nn_dot(xt[...], dgate[...]).astype(BF16)
    dwu[...] = nn_dot(xt[...], dup[...]).astype(BF16)
    dwd[...] = tn_dot(act[...], g[...]).astype(BF16)

    @pl.when(step == tiles - 1)
    def _():
        for copies in leaving:
            copies.wait()


def ffn(mesh, x, g, wg, wd, wu, w_last):
    rows, width = x.shape[0] // 2, x.shape[1]
    chips, tile = wg.shape[0] + 1, wg.shape[2]
    parts = 2
    tiles, cols = chips * parts, tile // parts
    local = wu.shape[0]
    keep = lambda shape: pl.BlockSpec(shape, lambda i: (0, 0), pipeline_mode=pl.Buffered(1))
    half = tile * chips
    wide, low = jax.ShapeDtypeStruct((rows, width), F32), jax.ShapeDtypeStruct((rows, width), BF16)
    return pl.pallas_call(
        functools.partial(ffn_kernel, mesh, tiles, parts),
        grid=(tiles,),
        in_specs=[
            keep(x.shape),
            keep(g.shape),
            pl.BlockSpec((None, width, cols), lambda i: (jnp.minimum(i // parts, chips - 2), 0, i % parts)),
            pl.BlockSpec((cols, width), lambda i: (i, 0)),
            pl.BlockSpec(memory_space=pl.ANY),
            pl.BlockSpec(memory_space=pl.ANY),
        ],
        out_specs=[pl.BlockSpec((width, cols), lambda i: (0, i))] * 2
        + [pl.BlockSpec((cols, width), lambda i: (i, 0))]
        + [pl.BlockSpec(memory_space=pl.ANY)] * 4,
        scratch_shapes=[pltpu.VMEM((width, 2 * rows), BF16)]
        + [pltpu.VMEM((2, rows, width), F32)] * 2
        + [pltpu.VMEM((rows, width), BF16)] * 2
        + [pltpu.VMEM((2 * rows, cols), BF16)] * 3
        + [pltpu.VMEM((2, chips + 1, local, tile), BF16), pltpu.VMEM((chips + 1, width, tile), BF16), pltpu.VMEM((width, cols), BF16)]
        + [pltpu.SemaphoreType.DMA((96,)), pltpu.SemaphoreType.DMA((96,)), pltpu.SemaphoreType.DMA((64,))],
        out_shape=[
            jax.ShapeDtypeStruct((width, half), BF16),
            jax.ShapeDtypeStruct((width, half), BF16),
            jax.ShapeDtypeStruct((half, width), BF16),
            wide,
            low,
            wide,
            low,
        ],
        compiler_params=pltpu.CompilerParams(vmem_limit_bytes=VMEM_MOST, collective_id=3, has_side_effects=True),
        cost_estimate=pl.CostEstimate(
            flops=36 * rows * width * half, bytes_accessed=12 * width * half + 20 * rows * width, transcendentals=0
        ),
        name="ffn",
    )(x, g, wg, wd, wu, w_last)


def part(x):
    return x[0].at[x[1:]] if isinstance(x, tuple) else x


def get(x):
    return x[0][x[1:]] if isinstance(x, tuple) else x[...]


def put(x, value):
    if isinstance(x, tuple):
        x[0][x[1:]] = value
    else:
        x[...] = value


class Copy:
    def __init__(self, src, dst, device, send_sem, recv_sem):
        self.src, self.dst, self.device, self.send_sem, self.recv_sem = src, dst, device, send_sem, recv_sem

    def made(self):
        if self.device is None:
            return pltpu.make_async_copy(part(self.src), part(self.dst), part(self.send_sem))
        return pltpu.make_async_remote_copy(
            src_ref=part(self.src),
            dst_ref=part(self.dst),
            send_sem=part(self.send_sem),
            recv_sem=part(self.recv_sem),
            device_id=self.device,
            device_id_type=MESH,
        )

    def start(self):
        self.made().start()

    def wait(self):
        self.made().wait()

    def wait_send(self):
        self.made().wait_send()

    def wait_recv(self):
        self.made().wait_recv()


class Links:
    def __init__(self, mesh, send_sems, recv_sems, local_sems):
        self.ns, self.nf = mesh
        self.na = self.nf // 4
        self.send_sems, self.recv_sems, self.local_sems = send_sems, recv_sems, local_sems
        self.count, self.local_count = 0, 0
        self.z, self.f = lax.axis_index("seq"), lax.axis_index("fsdp")
        self.core = lax.rem(self.f, 2)
        self.b = lax.rem(self.f // 2, 2)
        self.a = self.f // 4

    def chip(self, da, db):
        return lax.rem(self.a + da, self.na) * 2 + lax.rem(self.b + db, 2)

    def at_core(self):
        return (self.z, self.f + 1 - 2 * self.core)

    def at_b(self):
        return (self.z, self.f + 2 - 4 * self.b)

    def at_a(self, d):
        return (self.z, lax.rem(self.f + 4 * d, self.nf))

    def at_z(self, d):
        return (lax.rem(self.z + d, self.ns), self.f)

    def peers(self):
        return [self.at_core(), self.at_b()] + [self.at_a(d) for d in range(1, self.na)] + [self.at_z(d) for d in range(1, self.ns)]

    def barrier(self):
        barrier = pltpu.get_barrier_semaphore()
        peers = self.peers()
        for peer in peers:
            pl.semaphore_signal(barrier, inc=1, device_id=peer, device_id_type=MESH)
        pl.semaphore_wait(barrier, len(peers))

    def copy(self, src, dst, device):
        index = self.count
        self.count += 1
        return Copy(src, dst, device, (self.send_sems, index), (self.recv_sems, index))

    def again(self, src, dst, device):
        index = self.count - 1
        return Copy(src, dst, device, (self.send_sems, index), (self.recv_sems, index))

    def local(self, src, dst):
        index = self.local_count
        self.local_count += 1
        return Copy(src, dst, None, (self.local_sems, index), None)


def line_place(links):
    z, ns = links.z, links.ns
    middle = ns // 2
    step = jnp.where(z < middle, 1, -1)
    end = (z == 0) | (z == ns - 1)
    inner = (z == middle - 1) | (z == middle)
    return end, inner, (z + step, links.f), (z - step, links.f)


GATE_PIECES = 4


def first_piece(ns, columns):
    return columns // GATE_PIECES if ns == 4 else 0


def rows_at(start, size):
    return pl.ds(pl.multiple_of(start * size, size), size)


class ChipSum:
    def __init__(self, links, partial, b_first, arrived, passed, staging):
        self.links, self.partial, self.b_first = links, partial, b_first
        self.arrived, self.passed, self.staging = arrived, passed, staging
        na = links.na
        self.first, self.second = [], []
        if b_first:
            self.kept = [links.chip(da, 0) for da in range(na)]
            for da in range(na):
                self.first.append(links.copy(partial(links.chip(da, 1)), (arrived, da), links.at_b()))
            for d in range(1, na):
                self.second.append(links.copy((arrived, d), (passed, d - 1), links.at_a(d)))
        else:
            self.kept = [links.chip(0, db) for db in range(2)]
            for d in range(1, na):
                for db in range(2):
                    self.first.append(links.copy(partial(links.chip(d, db)), (arrived, (d - 1) * 2 + db), links.at_a(d)))
            self.second.append(links.copy((arrived, 1), (passed, 0), links.at_b()))
        self.loads = [] if staging is None else [links.local(partial(k), (staging, i)) for i, k in enumerate(self.kept)]

    def start(self):
        for copy in self.first:
            copy.start()

    def load(self):
        for load in self.loads:
            load.start()

    def turn(self):
        for load in self.loads:
            load.wait()
        for copy in self.first:
            copy.wait()
        count = len(self.kept)
        for i in [*range(1, count), 0]:
            own = self.partial(self.kept[i]) if self.staging is None else (self.staging, i)
            total = get(own).astype(F32)
            if self.b_first:
                total = total + self.arrived[i].astype(F32)
            else:
                for d in range(self.links.na - 1):
                    total = total + self.arrived[d * 2 + i].astype(F32)
            self.arrived[i] = total.astype(BF16)
            if i > 0 and self.b_first:
                self.second[i - 1].start()
            elif i > 0:
                self.second[0].start()

    def finish(self):
        for copy in self.second:
            copy.wait()
        total = self.arrived[0].astype(F32)
        for i in range(len(self.second)):
            total = total + self.passed[i].astype(F32)
        return total.astype(BF16)


def chip_sum_shapes(na, b_first, rows, columns):
    first = na if b_first else 2 * (na - 1)
    kept = na if b_first else 2
    return [
        pltpu.VMEM((max(first, kept), rows, columns), BF16),
        pltpu.VMEM((na - 1 if b_first else 1, rows, columns), BF16),
        pltpu.VMEM((kept, rows, columns), BF16),
    ]


def flip_core(f):
    return f + 1 - 2 * lax.rem(f, 2)


def flip_b(f):
    return f + 2 - 4 * lax.rem(f // 2, 2)


class Gather:
    def __init__(self, links, own, land, both):
        self.links = links
        f, na, nf = links.f, links.na, links.nf
        to_core, to_b = links.at_core(), links.at_b()

        def move(origin, device, half=None):
            return links.copy(land(origin, half), land(origin, half), device)

        self.given = [links.copy(own, land(f, None), to_core)] if both else []
        self.own = [links.copy(own, land(f, None), to_b)]
        self.own += [links.copy(own, land(f, None), links.at_a(d)) for d in range(1, na)]
        from_b = flip_b(f)
        from_a = [lax.rem(f + nf - 4 * d, nf) for d in range(1, na)]
        if na == 2:
            self.relays = [move(from_b, links.at_a(1), 1), move(from_a[0], to_b, 0)]
            far = [(flip_b(from_a[0]), 0), (flip_b(from_a[0]), 1)]
        else:
            self.relays = [move(origin, to_b) for origin in from_a]
            far = [(flip_b(origin), None) for origin in from_a]
        near = [from_b, *from_a]
        self.near = [move(origin, to_core) for origin in near] if both else []
        self.far = [move(origin, to_core, half) for origin, half in far] if both else []

    def start(self):
        for copies in self.own + self.given:
            copies.start()

    def turn(self):
        for copies in self.own:
            copies.wait()
        for copies in self.relays + self.near:
            copies.start()

    def pass_on(self):
        for copies in self.relays:
            copies.wait()
        for copies in self.far:
            copies.start()

    def finish(self):
        for copies in self.given + self.near + self.far:
            copies.wait()


class GatherHalf:
    def __init__(self, links, stage, land):
        self.links = links
        f, na, nf, core = links.f, links.na, links.nf, links.core
        to_b = links.at_b()

        def move(origin, device):
            return links.copy(land(origin), land(origin), device)

        self.swap = links.copy(stage(1 - core), land(f), links.at_core())
        self.kept = links.local(stage(core), land(f))
        targets = [to_b] + [links.at_a(d) for d in range(1, na)]
        self.own = [links.copy(stage(core), land(f), device) for device in targets]
        self.other = [move(flip_core(f), device) for device in targets]
        from_b = flip_b(f)
        from_a = [lax.rem(f + nf - 4 * d, nf) for d in range(1, na)]
        if na == 2:
            self.relays = [move(from_b, links.at_a(1))]
            self.late = [move(flip_core(from_a[0]), to_b)]
        else:
            self.relays = [move(origin, to_b) for origin in from_a]
            self.late = [move(flip_core(origin), to_b) for origin in from_a]

    def start(self):
        for copies in [self.swap, self.kept, *self.own]:
            copies.start()

    def other_start(self):
        self.swap.wait()
        for copies in self.other:
            copies.start()

    def turn(self):
        for copies in self.own:
            copies.wait()
        for copies in self.relays:
            copies.start()

    def turn_late(self):
        for copies in self.other:
            copies.wait()
        for copies in self.late:
            copies.start()

    def finish(self):
        for copies in [self.kept, *self.relays, *self.late]:
            copies.wait()


def attend_heads(ns, kv, span, qs, ks, vs, out, logs):
    scale = 1.0 / math.sqrt(HEAD_DIM)
    row = lax.broadcasted_iota(jnp.int32, (span, span), 0)
    column = lax.broadcasted_iota(jnp.int32, (span, span), 1)
    causal = row >= column
    lane = lax.broadcasted_iota(jnp.int32, (span, 128), 1)
    for s in range(ns):
        here = slice(s * span, (s + 1) * span)
        stats = jnp.zeros((span, 128), F32)
        for h in range(kv * GROUP):
            g = h // GROUP
            q = qs[h, here, :]
            near = jnp.where(causal, nt_dot(q, ks[g, here, :]) * scale, masked_score)
            top = jnp.max(near, axis=1, keepdims=True)
            if s > 0:
                far = nt_dot(q, ks[g, : s * span, :]) * scale
                top = jnp.maximum(top, jnp.max(far, axis=1, keepdims=True))
            near = jnp.exp(near - top)
            total = jnp.sum(near, axis=1, keepdims=True)
            if s > 0:
                far = jnp.exp(far - top)
                total = total + jnp.sum(far, axis=1, keepdims=True)
            inverse = 1.0 / total
            result = nn_dot((near * inverse).astype(BF16), vs[g, here, :])
            if s > 0:
                result = result + nn_dot((far * inverse).astype(BF16), vs[g, : s * span, :])
            stats = jnp.where(lane == h, top + jnp.log(total), stats)
            out[s, :, h * HEAD_DIM : (h + 1) * HEAD_DIM] = result.astype(BF16)
        logs[here, :] = stats


def fill_tables(cosines, sines, narrow_cosines, narrow_sines, heads):
    end = heads * HEAD_DIM
    cosines[:, end:] = jnp.ones((cosines.shape[0], cosines.shape[1] - end), F32)
    sines[:, end:] = jnp.zeros((cosines.shape[0], cosines.shape[1] - end), F32)
    for h in range(heads):
        at = slice(h * HEAD_DIM, (h + 1) * HEAD_DIM)
        cosines[:, at] = narrow_cosines
        sines[:, at] = narrow_sines


def fore_kernel(
    mesh, count, kv,
    tokens, cotangent, gains_in, wq, wk, wv, wo, wg, wd, narrow_cosines, narrow_sines,
    w_qkv, w_out, w_gate, w_down, first_out, packed, heads_attended, logs, attended_out, hidden_out, second_both, low_both, gains_out,
    rows_in, hidden, first, pack, w_land, wo_land, q_send, q_land, a_send, a_land, stage_gate, gain_send, gain_land,
    qs, ks, vs, log, attended, second, second_abs, low, cosines, sines, send_sems, recv_sems, local_sems,
):
    links = Links(mesh, send_sems, recv_sems, local_sems)
    ns, na, nf = links.ns, links.na, links.nf
    chips = 2 * na
    z, f, core = links.z, links.f, links.core
    rows, width = rows_in.shape
    span = rows // count
    heads = kv * GROUP
    g_width, k_width = heads * HEAD_DIM, kv * HEAD_DIM
    q_width = g_width + 2 * k_width
    local = width // nf
    links.barrier()

    token_load = links.local(tokens, rows_in)
    token_load.start()
    cot_load = links.local(cotangent, hidden)
    cot_load.start()
    gain_send[...] = jnp.zeros_like(gain_send)
    gain_send[0:2, :local] = gains_in[...].astype(F32)
    for j in range(ns):
        pack[j, :, :g_width] = wq[:, j * g_width : (j + 1) * g_width]
        pack[j, :, g_width : g_width + k_width] = wk[:, j * k_width : (j + 1) * k_width]
        pack[j, :, g_width + k_width :] = wv[:, j * k_width : (j + 1) * k_width]

    every = slice(None)

    def piece(start, size, half):
        if half is None:
            return rows_at(start, size)
        return rows_at(start * 2 + half, size // 2)

    units = []
    turns = [*range(1, ns), 0]
    for d in turns:
        g = lax.rem(z + d, ns)
        units.append(Gather(links, (pack, g), lambda o, half, g=g: (w_land, g, piece(o, local, half)), True))
    units.append(Gather(links, wo, lambda o, half: (wo_land, piece(o, local, half)), True))
    depth = wd.shape[0]
    units.append(Gather(links, wd, lambda o, half: (w_down, piece(o // 2, depth, half)), False))
    gate_unit = GatherHalf(links, lambda c: (stage_gate, c), lambda o: (w_gate, every, rows_at(o, local)))
    q_copies, a_copies = [], []
    for d in range(1, ns):
        g = lax.rem(z + d, ns)
        q_copies.append([links.copy((q_send, g, i), (q_land, i, z), links.at_z(d)) for i in range(count)])
    for i in range(count):
        a_copies.append([links.copy((a_send, i, lax.rem(z + d, ns)), (a_land, i, z), links.at_z(d)) for d in range(1, ns)])
    second_copy = links.copy(second_abs, (second_both, pl.ds(rows, rows)), links.at_core())
    low_copy = links.copy(low, (low_both, pl.ds(rows, rows)), links.at_core())

    def gain_at(start, size):
        return (gain_land, pl.ds(start, size))

    pair, chip_four = f // 2 * 2, f // 4 * 4
    gain_copies = [
        [links.copy(gain_at(f, 1), gain_at(f, 1), links.at_core())],
        [links.copy(gain_at(pair, 2), gain_at(pair, 2), links.at_b())],
        [links.copy(gain_at(chip_four, 4), gain_at(chip_four, 4), links.at_a(d)) for d in range(1, na)],
    ]
    stores = []

    def store(src, dst):
        copies = links.local(src, dst)
        copies.start()
        stores.append(copies)

    gain_land[f] = gain_send[...]
    for copies in gain_copies[0]:
        copies.start()
    units[0].start()
    units[1].start()
    for j in range(ns):
        w_land[j, rows_at(f, local), :] = pack[j]
    stage_loads = []
    tile = w_gate.shape[2]
    for c in range(2):
        for k in range(chips - 1):
            source = (wg, every, slice((k * 2 + c) * tile, (k * 2 + c + 1) * tile))
            stage_loads.append(links.local(source, (stage_gate, c, k)))
    for load in stage_loads:
        load.start()
    store_own = [links.local(wo, (wo_land, rows_at(f, local))), links.local(wd, (w_down, rows_at(f // 2, depth)))]
    for copies in store_own:
        copies.start()
    fill_tables(cosines, sines, narrow_cosines[rows_at(z, span), :], narrow_sines[rows_at(z, span), :], heads + kv)
    token_load.wait()
    old = rows_in[...]
    inverse = lax.rsqrt(jnp.mean(old * old, axis=1, keepdims=True) + norm_eps)
    for stage in range(3):
        for copies in gain_copies[stage]:
            copies.wait()
        if stage < 2:
            for copies in gain_copies[stage + 1]:
                copies.start()
    for j in range(nf):
        gains_out[:, j * local : (j + 1) * local] = gain_land[j, 0:2, :local]
    first[...] = (old * inverse * gains_out[0:1, :]).astype(BF16)
    store(first, first_out)

    def project(n):
        g = lax.rem(z + turns[n], ns)
        units[n].finish()
        y = nn_dot(first[...], w_land[g])
        for i in range(count):
            part = y[i * span : (i + 1) * span]
            part = (part * cosines[...] + swap_halves(part) * sines[...]).astype(BF16)
            if turns[n] == 0:
                q_land[i, z] = part
            else:
                q_send[g, i] = part
        if turns[n] > 0:
            q_copies[turns[n] - 1][0].start()
        if n > 0 and turns[n - 1] > 0:
            for copies in q_copies[turns[n - 1] - 1][1:]:
                copies.start()
        store((w_land, g), (w_qkv, g))

    last = len(units)
    for n in range(ns):
        units[n].turn()
        if n + 2 < last:
            units[n + 2].start()
        if n > 0:
            units[n - 1].pass_on()
        if n > 1:
            project(n - 2)
    units[ns].turn()
    for load in stage_loads:
        load.wait()
    gate_unit.start()
    units[ns - 1].pass_on()
    project(ns - 2)
    gate_unit.other_start()
    project(ns - 1)
    units[ns].pass_on()
    cot_load.wait()
    low[...] = hidden[...].astype(BF16)
    low_copy.start()
    store(low, (low_both, pl.ds(0, rows)))

    def attend(i):
        for copies in q_copies:
            copies[i].wait()
        for j in range(ns):
            at = slice(j * span, (j + 1) * span)
            for h in range(heads):
                qs[h, at, :] = q_land[i, j, :, h * HEAD_DIM : (h + 1) * HEAD_DIM]
            for h in range(kv):
                k0, v0 = (heads + h) * HEAD_DIM, (heads + kv + h) * HEAD_DIM
                ks[h, at, :] = q_land[i, j, :, k0 : k0 + HEAD_DIM]
                vs[h, at, :] = q_land[i, j, :, v0 : v0 + HEAD_DIM]
        attend_heads(ns, kv, span, qs, ks, vs, a_send.at[i], log.at[i])
        for copies in a_copies[i]:
            copies.start()
        a_land[i, z] = a_send[i, z]

    for i in range(count):
        attend(i)
        if i == 0:
            units[ns + 1].turn()
            units[ns].finish()
            store_own[0].wait()
            store(wo_land, w_out)
    store(q_land, packed)
    store(a_send, heads_attended)
    store(log, logs)
    for i in range(count):
        for copies in a_copies[i]:
            copies.wait()
        for j in range(ns):
            attended[i * span : (i + 1) * span, j * g_width : (j + 1) * g_width] = a_land[i, j]
    new = rows_in[...] + nn_dot(attended[...], wo_land[...])
    hidden[...] = new
    inverse = lax.rsqrt(jnp.mean(new * new, axis=1, keepdims=True) + norm_eps)
    second_abs[...] = (new * inverse * gains_out[1:2, :]).astype(BF16)
    second_copy.start()
    store(second_abs, (second_both, pl.ds(0, rows)))
    store(attended, attended_out)
    store(hidden, hidden_out)
    units[ns + 1].pass_on()
    gate_unit.turn()
    gate_unit.turn_late()
    gate_unit.finish()
    second_copy.wait()
    low_copy.wait()
    store_own[1].wait()
    for copies in stores:
        copies.wait()


def fore(mesh, count, kv, tokens, cotangent, gains_in, wq, wk, wv, wo, wg, wd, narrow_cosines, narrow_sines):
    ns, nf = mesh
    na = nf // 4
    chips = 2 * na
    rows, width = tokens.shape
    span = rows // count
    length = ns * span
    heads = kv * GROUP
    g_width = heads * HEAD_DIM
    q_width = g_width + 2 * kv * HEAD_DIM
    local, depth = wq.shape[0], wd.shape[0]
    tile = wg.shape[1] // (2 * chips)
    anywhere, vmem = pl.BlockSpec(memory_space=pl.ANY), pl.BlockSpec(memory_space=pltpu.VMEM)
    low = lambda *shape: jax.ShapeDtypeStruct(shape, BF16)
    wide = lambda *shape: jax.ShapeDtypeStruct(shape, F32)
    outs = [
        low(ns, width, q_width),
        low(width, width),
        low(chips - 1, width, tile),
        low(chips * depth, width),
        low(rows, width),
        low(count, ns, span, q_width),
        low(count, ns, span, g_width),
        wide(count, length, 128),
        low(rows, width),
        wide(rows, width),
        low(2 * rows, width),
        low(2 * rows, width),
        wide(2, width),
    ]
    scratch = [
        pltpu.VMEM((rows, width), F32),
        pltpu.VMEM((rows, width), F32),
        pltpu.VMEM((rows, width), BF16),
        pltpu.VMEM((ns, local, q_width), BF16),
        pltpu.VMEM((ns, width, q_width), BF16),
        pltpu.VMEM((width, width), BF16),
        pltpu.VMEM((ns, count, span, q_width), BF16),
        pltpu.VMEM((count, ns, span, q_width), BF16),
        pltpu.VMEM((count, ns, span, g_width), BF16),
        pltpu.VMEM((count, ns, span, g_width), BF16),
        pltpu.VMEM((2, chips - 1, local, tile), BF16),
        pltpu.VMEM((8, 256), F32),
        pltpu.VMEM((nf, 8, 256), F32),
        pltpu.VMEM((heads, length, HEAD_DIM), BF16),
        pltpu.VMEM((kv, length, HEAD_DIM), BF16),
        pltpu.VMEM((kv, length, HEAD_DIM), BF16),
        pltpu.VMEM((count, length, 128), F32),
        pltpu.VMEM((rows, width), BF16),
        pltpu.VMEM((8, 128), BF16),
        pltpu.VMEM((rows, width), BF16),
        pltpu.VMEM((rows, width), BF16),
        pltpu.VMEM((span, q_width), F32),
        pltpu.VMEM((span, q_width), F32),
    ]
    return pl.pallas_call(
        functools.partial(fore_kernel, mesh, count, kv),
        in_specs=[anywhere] * 2 + [vmem] * 4 + [anywhere] * 3 + [vmem] * 2,
        out_specs=[anywhere] * 12 + [vmem],
        out_shape=outs,
        scratch_shapes=scratch
        + [pltpu.SemaphoreType.DMA((160,)), pltpu.SemaphoreType.DMA((160,)), pltpu.SemaphoreType.DMA((64,))],
        compiler_params=pltpu.CompilerParams(vmem_limit_bytes=VMEM_MOST, collective_id=0, has_side_effects=True),
        name="fore",
    )(tokens, cotangent, gains_in, wq, wk, wv, wo, wg, wd, narrow_cosines, narrow_sines)


def attend_back_heads(ns, kv, span, qs, ks, vs, gs, attended, logs, dk, dv, result):
    scale = 1.0 / math.sqrt(HEAD_DIM)
    heads = kv * GROUP
    row = lax.broadcasted_iota(jnp.int32, (span, span), 0)
    column = lax.broadcasted_iota(jnp.int32, (span, span), 1)
    causal = row >= column
    dk[...] = jnp.zeros_like(dk)
    dv[...] = jnp.zeros_like(dv)
    for s in range(ns):
        here = slice(s * span, (s + 1) * span)
        for h in range(heads):
            g = h // GROUP
            q, grad = qs[h, here, :], gs[h, here, :]
            log_total = logs[here, h : h + 1]
            out = attended[s, :, h * HEAD_DIM : (h + 1) * HEAD_DIM]
            delta = jnp.sum(grad.astype(F32) * out.astype(F32), axis=1, keepdims=True)
            k, v = ks[g, here, :], vs[g, here, :]
            near = jnp.where(causal, jnp.exp(nt_dot(q, k) * scale - log_total), 0.0)
            slope = (near * (nt_dot(grad, v) - delta) * scale).astype(BF16)
            dq = nn_dot(slope, k)
            dk[g, here, :] += tn_dot(slope, q)
            dv[g, here, :] += tn_dot(near.astype(BF16), grad)
            if s > 0:
                before = slice(0, s * span)
                k, v = ks[g, before, :], vs[g, before, :]
                far = jnp.exp(nt_dot(q, k) * scale - log_total)
                slope = (far * (nt_dot(grad, v) - delta) * scale).astype(BF16)
                dq = dq + nn_dot(slope, k)
                dk[g, before, :] += tn_dot(slope, q)
                dv[g, before, :] += tn_dot(far.astype(BF16), grad)
            result[here, h * HEAD_DIM : (h + 1) * HEAD_DIM] = dq
    for g in range(kv):
        k0 = (heads + g) * HEAD_DIM
        v0 = (heads + kv + g) * HEAD_DIM
        result[:, k0 : k0 + HEAD_DIM] = dk[g]
        result[:, v0 : v0 + HEAD_DIM] = dv[g]


def back_kernel(
    mesh, count, kv,
    dx_own, dx_other, hidden, cotangent, gains, w_out, w_qkv, packed, attended, logs, cosines, sines, tokens, dwg, dwu,
    high, low_out, out, gain_grads, dqkv, sum_gate, sum_up,
    low, sum_rows, sum_land, dx_land, g_send, g_land, q_send, q_land, swap_send, swap_land, *rest,
):
    parts, (send_sems, recv_sems, local_sems) = rest[:-3], rest[-3:]
    links = Links(mesh, send_sems, recv_sems, local_sems)
    ns, na = links.ns, links.na
    chips = 2 * na
    z, core = links.z, links.core
    rows, width = hidden.shape
    span = rows // count
    length = ns * span
    heads = kv * GROUP
    g_width, q_width = heads * HEAD_DIM, (heads + 2 * kv) * HEAD_DIM
    half = dwg.shape[1]
    block = width // chips
    links.barrier()

    sums = []
    for n, source in enumerate((dwg, dwu)):
        for b_first in (True, False):
            columns = slice(0, half // 2) if b_first else slice(half // 2, half)
            at = (n * 2 + (0 if b_first else 1)) * 3
            partial = lambda k, source=source, columns=columns: (source, rows_at(k, block), columns)
            sums.append(ChipSum(links, partial, b_first, *parts[at : at + 3]))
    for item in sums:
        item.start()
        item.load()

    g_copies, q_copies = [], []
    for i in range(count):
        g_copies.append([links.copy((g_send, i, lax.rem(z + d, ns)), (g_land, i, z), links.at_z(d)) for d in range(1, ns)])
        q_copies.append([links.copy((q_send, i, lax.rem(z + d, ns)), (q_land, z, i), links.at_z(d)) for d in range(1, ns)])

    def out_back(dx, old, grad, w):
        load_sets, store_sets = [], []
        for i in range(count):
            here = pl.ds(i * span, span)
            pairs = ((dx_own, dx), (dx_other, dx_land), (hidden, old), (cotangent, grad))
            load_sets.append([links.local((source, here), (target, here)) for source, target in pairs])
            store_sets.append([links.local((grad, here), (high, here)), links.local((low, here), (low_out, here))])
        w_load = links.local(w_out, w)
        for load in load_sets[0] + [w_load] + [load for loads in load_sets[1:] for load in loads]:
            load.start()
        for i in range(count):
            here = slice(i * span, (i + 1) * span)
            for load in load_sets[i]:
                load.wait()
            step, rows_old = dx[here, :] + dx_land[here, :].astype(F32), old[here, :]
            inverse = lax.rsqrt(jnp.mean(rows_old * rows_old, axis=1, keepdims=True) + norm_eps)
            normed = rows_old * inverse
            part_sum = jnp.sum(step * normed, axis=0, keepdims=True)
            gain_grads[1:2, :] = part_sum if i == 0 else gain_grads[1:2, :] + part_sum
            total = grad[here, :] + norm_back(step, normed, inverse, gains[1:2, :])
            grad[here, :] = total
            low[here, :] = total.astype(BF16)
            for copies in store_sets[i]:
                copies.start()
            if i == 0:
                w_load.wait()
            out_part = nt_dot(low[here, :], w[...]).astype(BF16)
            for j in range(ns):
                g_send[i, j] = out_part[:, j * g_width : (j + 1) * g_width]
            for copies in g_copies[i]:
                copies.start()
            g_land[i, z] = g_send[i, z]
        for copies in [copies for stores in store_sets for copies in stores]:
            copies.wait()

    pl.run_scoped(
        out_back,
        pltpu.VMEM((rows, width), F32),
        pltpu.VMEM((rows, width), F32),
        pltpu.VMEM((rows, width), F32),
        pltpu.VMEM((width, width), BF16),
    )

    def attention(qkv, mid, log, qs, ks, vs, gs, dk, dv, result, cosine, sine):
        fill_tables(cosine, sine, cosines[...], sines[...], heads + kv)
        for i in range(count):
            loads = [links.local((packed, i), qkv), links.local((attended, i), mid), links.local((logs, i), log)]
            for load in loads:
                load.start()
            for load in loads:
                load.wait()
            for j in range(ns):
                at = slice(j * span, (j + 1) * span)
                for h in range(heads):
                    qs[h, at, :] = qkv[j, :, h * HEAD_DIM : (h + 1) * HEAD_DIM]
                for h in range(kv):
                    k0, v0 = (heads + h) * HEAD_DIM, (heads + kv + h) * HEAD_DIM
                    ks[h, at, :] = qkv[j, :, k0 : k0 + HEAD_DIM]
                    vs[h, at, :] = qkv[j, :, v0 : v0 + HEAD_DIM]
            for copies in g_copies[i]:
                copies.wait()
            for j in range(ns):
                for h in range(heads):
                    gs[h, j * span : (j + 1) * span, :] = g_land[i, j, :, h * HEAD_DIM : (h + 1) * HEAD_DIM]
            attend_back_heads(ns, kv, span, qs, ks, vs, gs, mid, log, dk, dv, result)
            for j in range(ns):
                here = slice(j * span, (j + 1) * span)
                part = result[here, :]
                q_send[i, j] = (part * cosine[here, :] - swap_halves(part) * sine[here, :]).astype(BF16)
            for copies in q_copies[i]:
                copies.start()
            q_land[z, i] = q_send[i, z]
            if i < len(sums) // 2:
                for item in sums[2 * i : 2 * i + 2]:
                    item.turn()

    pl.run_scoped(
        attention,
        pltpu.VMEM((ns, span, q_width), BF16),
        pltpu.VMEM((ns, span, g_width), BF16),
        pltpu.VMEM((length, 128), F32),
        pltpu.VMEM((heads, length, HEAD_DIM), BF16),
        pltpu.VMEM((kv, length, HEAD_DIM), BF16),
        pltpu.VMEM((kv, length, HEAD_DIM), BF16),
        pltpu.VMEM((heads, length, HEAD_DIM), BF16),
        pltpu.VMEM((kv, length, HEAD_DIM), F32),
        pltpu.VMEM((kv, length, HEAD_DIM), F32),
        pltpu.VMEM((length, q_width), F32),
        pltpu.VMEM((length, q_width), F32),
        pltpu.VMEM((length, q_width), F32),
    )

    swaps = []
    local = block // 2
    for item in sums[2 * count :]:
        item.turn()

    def swap(n):
        for m in range(2):
            total = sums[2 * n + m].finish()
            swap_send[n, m, 0] = total[:local]
            swap_send[n, m, 1] = total[local:]
        for m in range(2):
            copies = links.copy((swap_send, n, m, 1 - core), (swap_land, n, m), links.at_core())
            copies.start()
            swaps.append(copies)

    tile = half // chips
    stores = []
    early = first_piece(ns, 2 * half)
    piece = (sum_rows, 0, slice(None), slice(0, max(early, 1)))
    end, inner, inward = line_place(links)[:3]
    early_copy = links.copy(piece, sum_land, inward)

    def combine(n, total):
        for m in range(2):
            swaps[2 * n + m].wait()
            kept, arrived = swap_send[n, m, core], swap_land[n, m]
            for t in range(chips // 2):
                here = slice(t * tile, (t + 1) * tile)
                k = m * (chips // 2) + t
                one, two = kept[:, here], arrived[:, here]
                sum_rows[n, :, 2 * k * tile : (2 * k + 1) * tile] = jnp.where(core == 0, one, two)
                sum_rows[n, :, (2 * k + 1) * tile : (2 * k + 2) * tile] = jnp.where(core == 0, two, one)
        if n == 0 and early:
            pl.when(end)(early_copy.start)
        else:
            copies = links.local((sum_rows, n), total)
            copies.start()
            stores.append(copies)

    def project_back(w, old, base, grad):
        loads = [links.local(tokens, old), links.local(high, base), links.local(w_qkv, w)]
        for load in loads:
            load.start()
        swap(0)
        for load in loads:
            load.wait()
        for i in range(count):
            here = slice(i * span, (i + 1) * span)
            if i == count - 1:
                combine(0, sum_gate)
                swap(1)
                combine(1, sum_up)
            for copies in q_copies[i]:
                copies.wait()
            total = nt_dot(q_land[0, i], w[0])
            for j in range(1, ns):
                total = total + nt_dot(q_land[j, i], w[j])
            grad[here, :] = total
            copies = links.local((q_land, slice(None), i), (dqkv, slice(None), i))
            copies.start()
            stores.append(copies)
            step, rows_old = grad[here, :], old[here, :]
            inverse = lax.rsqrt(jnp.mean(rows_old * rows_old, axis=1, keepdims=True) + norm_eps)
            normed = rows_old * inverse
            part_sum = jnp.sum(step * normed, axis=0, keepdims=True)
            gain_grads[0:1, :] = part_sum if i == 0 else gain_grads[0:1, :] + part_sum
            base[here, :] = base[here, :] + norm_back(step, normed, inverse, gains[0:1, :])
            copies = links.local((base, here), (out, here))
            copies.start()
            stores.append(copies)
        if early:

            @pl.when(inner)
            def _():
                early_copy.wait_recv()
                put(piece, (get(piece).astype(F32) + sum_land[...].astype(F32)).astype(BF16))

            pl.when(end)(early_copy.wait_send)
            copies = links.local((sum_rows, 0), sum_gate)
            copies.start()
            stores.append(copies)
        for copies in stores:
            copies.wait()

    pl.run_scoped(
        project_back,
        pltpu.VMEM((ns, width, q_width), BF16),
        pltpu.VMEM((rows, width), F32),
        pltpu.VMEM((rows, width), F32),
        pltpu.VMEM((rows, width), F32),
    )


def back(mesh, count, kv, dx_own, dx_other, hidden, cotangent, gains, w_out, w_qkv, packed, attended, logs, cosines, sines, tokens, dwg, dwu):
    ns, nf = mesh
    na = nf // 4
    rows, width = hidden.shape
    span = rows // count
    heads = kv * GROUP
    g_width, q_width = heads * HEAD_DIM, (heads + 2 * kv) * HEAD_DIM
    half = dwg.shape[1]
    block = width // (2 * na)
    local = block // 2
    anywhere = pl.BlockSpec(memory_space=pl.ANY)
    vmem = pl.BlockSpec(memory_space=pltpu.VMEM)
    operands = [dx_own, dx_other, hidden, cotangent, gains, w_out, w_qkv, packed, attended, logs, cosines, sines, tokens, dwg, dwu]
    wide = jax.ShapeDtypeStruct((rows, width), F32)
    summed = jax.ShapeDtypeStruct((local, 2 * half), BF16)
    scratch = [
        pltpu.VMEM((rows, width), BF16),
        pltpu.VMEM((2, local, 2 * half), BF16),
        pltpu.VMEM((local, max(first_piece(ns, 2 * half), 128)), BF16),
        pltpu.VMEM((rows, width), BF16),
        pltpu.VMEM((count, ns, span, g_width), BF16),
        pltpu.VMEM((count, ns, span, g_width), BF16),
        pltpu.VMEM((count, ns, span, q_width), BF16),
        pltpu.VMEM((ns, count, span, q_width), BF16),
        pltpu.VMEM((2, 2, 2, local, half // 2), BF16),
        pltpu.VMEM((2, 2, local, half // 2), BF16),
    ]
    for _ in range(2):
        for b_first in (True, False):
            scratch += chip_sum_shapes(na, b_first, block, half // 2)
    return pl.pallas_call(
        functools.partial(back_kernel, mesh, count, kv),
        in_specs=[vmem if x.shape[0] == 2 and x.ndim == 2 or x.shape[1] == HEAD_DIM else anywhere for x in operands],
        out_specs=[anywhere, anywhere, anywhere, vmem, anywhere, anywhere, anywhere],
        out_shape=[
            wide,
            jax.ShapeDtypeStruct((rows, width), BF16),
            wide,
            jax.ShapeDtypeStruct((2, width), F32),
            jax.ShapeDtypeStruct((ns, count, span, q_width), BF16),
            summed,
            summed,
        ],
        scratch_shapes=scratch
        + [pltpu.SemaphoreType.DMA((64,)), pltpu.SemaphoreType.DMA((64,)), pltpu.SemaphoreType.DMA((64,))],
        compiler_params=pltpu.CompilerParams(vmem_limit_bytes=VMEM_MOST, collective_id=1, has_side_effects=True),
        name="back",
    )(*operands)


class LineSum:
    def __init__(self, links, term, first, second, total, out=None, begun=False):
        self.links, self.term, self.first, self.second, self.total = links, term, first, second, total
        self.dtype = (term[0] if isinstance(term, tuple) else term).dtype
        self.deep = links.ns // 2 > 1
        self.begun = begun
        self.end, self.inner, inward, outward = line_place(links)
        moved = self.deep and not begun
        self.inward = links.copy(term, first, inward) if moved else None
        self.onward = links.again(first, first, inward) if moved else None
        self.sum = first if moved else term
        self.across = links.copy(self.sum, second, inward)
        self.outward = links.copy(total, total, outward) if self.deep else None
        self.store = links.local(total, out) if out is not None else None

    def keep(self):
        if self.store is not None:
            self.store.start()

    def add(self, target, one, two):
        put(target, (get(one).astype(F32) + get(two).astype(F32)).astype(self.dtype))

    def begin(self):
        if self.begun:
            pl.when(self.inner)(self.across.start)
        elif self.deep:
            pl.when(self.end)(self.inward.start)
        else:
            self.across.start()

    def relay(self):
        if not self.deep or self.begun:
            return

        @pl.when(jnp.logical_not(self.end))
        def _():
            self.inward.wait_recv()
            self.add(self.first, self.term, self.first)
            pl.when(self.inner)(self.across.start)
            pl.when(jnp.logical_not(self.inner))(self.onward.start)

    def settle(self):
        @pl.when(self.inner)
        def _():
            self.across.wait()
            self.add(self.total, self.sum, self.second)
            if self.deep:
                self.outward.start()
            self.keep()

        if self.deep:

            @pl.when(jnp.logical_not(self.inner | self.end))
            def _():
                self.outward.wait_recv()
                self.outward.start()
                self.keep()

    def finish(self):
        if self.deep:

            @pl.when(self.end)
            def _():
                self.outward.wait_recv()
                self.keep()

            if not self.begun:
                pl.when(jnp.logical_not(self.inner))(self.inward.wait_send)
            pl.when(jnp.logical_not(self.end))(self.outward.wait_send)


def finish_kernel(
    mesh, count, kv,
    gate_in, up_in, dwd, first, dqkv, attended, low, gains,
    out_gate, out_up, out_down, out_out, out_qkv, out_gains,
    tot_gate, tot_up, tot_down, tot_out, tot_qkv, term_gate, term_up, term_down, term_out, term_qkv, in_gate, in_up, in_down, in_out, in_qkv,
    first_both, attended_both, low_both, dq_both, w_out_part, w_qkv_part,
    swap_out, land_out, swap_qkv, land_qkv, gain_terms, gain_lands, *rest,
):
    parts, (send_sems, recv_sems, local_sems) = rest[:-3], rest[-3:]
    links = Links(mesh, send_sems, recv_sems, local_sems)
    ns, na = links.ns, links.na
    chips, per = 2 * na, ns // 2
    core = links.core
    rows, width = first.shape
    q_width = dqkv.shape[3]
    middle = width // 2

    def lines(term, inbox, total, out, pieces, begun=False):
        size = term.shape[1] // pieces
        every = slice(None)
        made = []
        for i in range(pieces):
            at = slice(i * size, (i + 1) * size)
            refs = [(ref, *where, every, at) for ref, *where in ((term,), (inbox, 0), (inbox, 1), (total,), (out,))]
            made.append(LineSum(links, *refs, begun and i == 0))
        return made

    gate_lines = lines(term_gate, in_gate, tot_gate, out_gate, GATE_PIECES, first_piece(ns, term_gate.shape[1]) > 0)
    up_lines = lines(term_up, in_up, tot_up, out_up, 4)
    down_lines = lines(term_down, in_down, tot_down, out_down, 4)
    out_lines = lines(term_out, in_out, tot_out, out_out, 2)
    qkv_lines = lines(term_qkv, in_qkv, tot_qkv, out_qkv, 4)
    term_loads = []
    for source, some in ((gate_in, gate_lines), (up_in, up_lines)):
        for line in some:
            term_loads.append(links.local((source, *line.term[1:]), line.term))
    for load in term_loads:
        load.start()
    links.barrier()
    for load, line in zip(term_loads, gate_lines + up_lines):
        load.wait()
        line.begin()

    sends = [
        links.copy((dqkv, pl.ds((1 - core) * per, per)), (dq_both, 1), links.at_core()),
        links.copy((low, slice(None), rows_at(1 - core, middle)), (low_both, 1), links.at_core()),
        links.copy(first, (first_both, 1), links.at_core()),
        links.copy(attended, (attended_both, 1), links.at_core()),
    ]
    loads = [
        links.local((low, slice(None), rows_at(core, middle)), (low_both, 0)),
        links.local(attended, (attended_both, 0)),
        links.local(first, (first_both, 0)),
        links.local((dqkv, pl.ds(core * per, per)), (dq_both, 0)),
    ]
    for copies in loads + sends[1:2] + sends[3:4] + sends[2:3] + sends[:1]:
        copies.start()

    down_rows = dwd.shape[0] // chips
    block = width // chips

    def pair(source, row_count, at, staged):
        made = []
        cut = source.shape[1] // 2
        for n, b_first in enumerate((True, False)):
            columns = slice(0, cut) if b_first else slice(cut, 2 * cut)
            partial = lambda k, columns=columns: (source, rows_at(k, row_count), columns)
            refs = parts[at[n] : at[n + 1]]
            made.append(ChipSum(links, partial, b_first, *(refs if staged else (*refs[:2], None))))
        return made

    down = pair(dwd, down_rows, (0, 3, 6), True)
    for item in down:
        item.start()
        item.load()

    gain_copies = [links.copy((gain_terms, 0), (gain_lands, 0), links.at_core()), links.copy((gain_terms, 1), (gain_lands, 1), links.at_b())]
    gain_copies += [links.copy((gain_terms, 2), (gain_lands, 1 + d), links.at_a(d)) for d in range(1, na)]
    gain_line = LineSum(links, (gain_terms, 3), (gain_lands, na + 1), (gain_lands, na + 2), out_gains)
    gain_terms[0] = gains[...]
    gain_copies[0].start()

    def next_gain(i):
        for copies in gain_copies[i : i + 1] if i < 2 else gain_copies[2:]:
            copies.wait()
        if i < 2:
            gain_terms[i + 1] = gain_terms[i] + gain_lands[i]
            for copies in gain_copies[1:2] if i == 0 else gain_copies[2:]:
                copies.start()
        else:
            total = gain_terms[2]
            for d in range(1, na):
                total = total + gain_lands[1 + d]
            gain_terms[3] = total
            gain_line.begin()

    def qkv_part(p):
        columns = slice(p * q_width, (p + 1) * q_width)
        mine, other = dq_both[0, p].reshape(rows, q_width), dq_both[1, p].reshape(rows, q_width)
        for k in range(chips):
            at = slice(k * block, (k + 1) * block)
            total = tn_dot(first_both[0, :, at], mine) + tn_dot(first_both[1, :, at], other)
            w_qkv_part[at, columns] = total.astype(BF16)

    def swap(sums, send, land):
        local = block // 2
        for n, item in enumerate(sums):
            total = item.finish()
            size = total.shape[1]
            send[0, :, n * size : (n + 1) * size] = total[:local]
            send[1, :, n * size : (n + 1) * size] = total[local:]
        copies = links.copy((send, 1 - core), land, links.at_core())
        copies.start()
        return copies

    out_sums = pair(w_out_part, block, (6, 8, 10), False)
    qkv_sums = pair(w_qkv_part, block, (10, 12, 14), False)
    cut = width // 2
    next_gain(0)
    for i in (1, 3):
        sends[i].wait()
    for i in (0, 1):
        loads[i].wait()
    gate_lines[0].relay()
    for k in range(chips):
        at = slice(k * block, (k + 1) * block)
        total = tn_dot(attended_both[0, :, at], low_both[0]) + tn_dot(attended_both[1, :, at], low_both[1])
        w_out_part[at, :] = total.astype(BF16)
    for item in out_sums:
        item.start()
    gate_lines[1].relay()
    next_gain(1)
    for i in (0, 2):
        sends[i].wait()
    for i in (2, 3):
        loads[i].wait()
    gate_lines[0].settle()
    for p in range(per // 2):
        qkv_part(p)
    gate_lines[2].relay()
    next_gain(2)
    gate_lines[1].settle()
    for p in range(per // 2, per):
        qkv_part(p)
    gate_lines[3].relay()
    for item in down:
        item.turn()
    for item in qkv_sums:
        item.start()
    gate_lines[2].settle()
    gain_line.relay()
    gate_lines[3].settle()
    for item in out_sums:
        item.turn()
    up_lines[0].relay()
    gain_line.settle()
    up_lines[1].relay()
    up_lines[0].settle()
    term_down[:, :cut] = down[0].finish()
    term_down[:, cut:] = down[1].finish()
    for line in down_lines:
        line.begin()
    up_lines[2].relay()
    up_lines[1].settle()
    up_lines[3].relay()
    up_lines[2].settle()
    down_lines[0].relay()
    up_lines[3].settle()
    for item in qkv_sums:
        item.turn()
    down_lines[1].relay()
    down_lines[0].settle()
    out_swap = swap(out_sums, swap_out, land_out)
    down_lines[2].relay()
    down_lines[1].settle()
    out_swap.wait()
    kept, arrived = swap_out[core], land_out[...]
    term_out[:, :cut] = jnp.where(core == 0, kept, arrived)
    term_out[:, cut:] = jnp.where(core == 0, arrived, kept)
    for line in out_lines:
        line.begin()
    down_lines[3].relay()
    down_lines[2].settle()
    qkv_swap = swap(qkv_sums, swap_qkv, land_qkv)
    out_lines[0].relay()
    down_lines[3].settle()
    qkv_swap.wait()
    kept, arrived = swap_qkv[core], land_qkv[...]
    for n in range(2):
        group = jnp.where(core == n, kept, arrived)
        for p in range(per):
            taken, start = p * q_width, 0
            for size in (kv * GROUP * HEAD_DIM, kv * HEAD_DIM, kv * HEAD_DIM):
                at = start + (n * per + p) * size
                term_qkv[:, at : at + size] = group[:, taken : taken + size]
                taken, start = taken + size, start + ns * size
    for line in qkv_lines:
        line.begin()
    out_lines[1].relay()
    out_lines[0].settle()
    qkv_lines[0].relay()
    out_lines[1].settle()
    for n in range(1, len(qkv_lines)):
        qkv_lines[n].relay()
        qkv_lines[n - 1].settle()
    qkv_lines[-1].settle()
    every_line = [*gate_lines, *up_lines, gain_line, *down_lines, *out_lines, *qkv_lines]
    for line in every_line:
        line.finish()
    for line in every_line:
        if line.store is not None:
            line.store.wait()


def finish(mesh, count, kv, term_gate, term_up, dwd, first, dqkv, attended, low, gains):
    ns, nf = mesh
    na, per = nf // 4, ns // 2
    rows, width = first.shape
    q_width = dqkv.shape[3]
    local, half = term_gate.shape[0], width // 2
    block = 2 * local
    anywhere, vmem = pl.BlockSpec(memory_space=pl.ANY), pl.BlockSpec(memory_space=pltpu.VMEM)
    down = (dwd.shape[0] // (2 * na), dwd.shape[1])
    shapes = [term_gate.shape, term_up.shape, down, (local, width), (local, ns * q_width)]
    scratch = [pltpu.VMEM(s, BF16) for s in shapes]
    scratch += [pltpu.VMEM(s, BF16) for s in shapes]
    scratch += [pltpu.VMEM((2,) + tuple(s), BF16) for s in shapes]
    scratch += [
        pltpu.VMEM((2, rows, width), BF16),
        pltpu.VMEM((2, rows, width), BF16),
        pltpu.VMEM((2, rows, half), BF16),
        pltpu.VMEM((2, per, count, rows // count, q_width), BF16),
        pltpu.VMEM((width, half), BF16),
        pltpu.VMEM((width, per * q_width), BF16),
        pltpu.VMEM((2, local, half), BF16),
        pltpu.VMEM((local, half), BF16),
        pltpu.VMEM((2, local, per * q_width), BF16),
        pltpu.VMEM((local, per * q_width), BF16),
        pltpu.VMEM((4, 2, width), F32),
        pltpu.VMEM((na + 3, 2, width), F32),
    ]
    scratch += chip_sum_shapes(na, True, down[0], down[1] // 2) + chip_sum_shapes(na, False, down[0], down[1] // 2)
    for columns in (half // 2, per * q_width // 2):
        for b_first in (True, False):
            scratch += chip_sum_shapes(na, b_first, block, columns)[:2]
    return pl.pallas_call(
        functools.partial(finish_kernel, mesh, count, kv),
        in_specs=[anywhere] * 7 + [vmem],
        out_specs=[anywhere] * 5 + [vmem],
        out_shape=[jax.ShapeDtypeStruct(s, BF16) for s in shapes] + [jax.ShapeDtypeStruct((2, width), F32)],
        scratch_shapes=scratch
        + [pltpu.SemaphoreType.DMA((128,)), pltpu.SemaphoreType.DMA((128,)), pltpu.SemaphoreType.DMA((64,))],
        compiler_params=pltpu.CompilerParams(vmem_limit_bytes=VMEM_MOST, collective_id=2, has_side_effects=True),
        name="finish",
    )(term_gate, term_up, dwd, first, dqkv, attended, low, gains)


def widen_kernel(cuts, *refs):
    gate, up, down, out, qkv, hidden, own, other = refs[:8]
    o_gate, o_up, o_down, o_out, o_q, o_k, o_v, o_block = refs[8:]
    for source, target in ((gate, o_gate), (up, o_up), (down, o_down), (out, o_out)):
        target[...] = source[...].astype(F32)
    for (start, end), target in zip(cuts, (o_q, o_k, o_v)):
        target[...] = qkv[:, start:end].astype(F32)
    o_block[...] = hidden[...] + own[...] + other[...].astype(F32)


def widen(gate, up, down, out, qkv, hidden, own, other, cuts):
    steps = 8 if out.shape[0] % 64 == 0 else 4
    operands = [gate, up, down, out, qkv, hidden, own, other]
    rows = out.shape[0]
    shapes = [gate.shape, up.shape, down.shape, out.shape] + [(rows, end - start) for start, end in cuts] + [hidden.shape]
    block = lambda shape: pl.BlockSpec((shape[0] // steps, shape[1]), lambda i: (i, 0))
    return pl.pallas_call(
        functools.partial(widen_kernel, cuts),
        grid=(steps,),
        in_specs=[block(x.shape) for x in operands],
        out_specs=[block(shape) for shape in shapes],
        out_shape=[jax.ShapeDtypeStruct(shape, F32) for shape in shapes],
        compiler_params=pltpu.CompilerParams(vmem_limit_bytes=VMEM_LIMIT),
        cost_estimate=pl.CostEstimate(flops=0, bytes_accessed=40 * rows * gate.shape[1], transcendentals=0),
        name="widen",
    )(*operands)


def solution(mesh):
    ns, nf = mesh.shape["seq"], mesh.shape["fsdp"]
    na = nf // 4
    chips = 2 * na
    kv = KEY_VALUE_HEADS // ns

    def body(tokens, cotangent, attention_gain, feedforward_gain, query_weight, key_matrix, value_matrix, out_weight, gate_weight, up_weight, down_weight):
        count, span, width = tokens.shape
        rows = count * span
        local = query_weight.shape[0]
        sizes = (ns, nf)
        mine = lax.axis_index("fsdp")
        cosines, sines = (jnp.asarray(x) for x in rope_tables(ns * span))
        flat = tokens.reshape(rows, width)
        grad_flat = cotangent.reshape(rows, width)
        (w_qkv, w_out, w_gate, w_down, first, packed, heads_attended, logs, attended, hidden_one, second_both, low_both, gains) = fore(
            sizes, count, kv, flat, grad_flat, jnp.stack([attention_gain, feedforward_gain]),
            query_weight, key_matrix, value_matrix, out_weight, gate_weight, down_weight, cosines, sines,
        )
        dwg, dwu, dwd, out_own, out_arrived, dx_own, dx_arrived = ffn(sizes, second_both, low_both, w_gate, w_down, up_weight, gate_weight)
        high, low, grad_tokens, gain_grads, dqkv, sum_gate, sum_up = back(
            sizes, count, kv, dx_own, dx_arrived, hidden_one, grad_flat, gains, w_out, w_qkv,
            packed, heads_attended, logs, cosines, sines, flat, dwg, dwu,
        )
        *sums, gain_grads = finish(
            sizes, count, kv, sum_gate, sum_up, dwd, first, dqkv, attended, low, gain_grads
        )
        q_end, k_end = ns * kv * GROUP * HEAD_DIM, ns * kv * (GROUP + 1) * HEAD_DIM
        cuts = ((0, q_end), (q_end, k_end), (k_end, sums[4].shape[1]))
        grad_gate, grad_up, grad_down, grad_out, grad_query, grad_key, grad_value, block_out = widen(
            *sums, hidden_one, out_own, out_arrived, cuts
        )
        gain_grads = lax.dynamic_slice(gain_grads, (0, mine * local), (2, local))

        return (
            block_out.reshape(count, span, width),
            grad_tokens.reshape(count, span, width),
            gain_grads[0],
            gain_grads[1],
            grad_query,
            grad_key,
            grad_value,
            grad_out,
            grad_gate,
            grad_up,
            grad_down,
        )

    tokens_spec, gain_spec, weight_spec = P("fsdp", "seq", None), P("fsdp"), P("fsdp", None)
    return jax.shard_map(
        body,
        mesh=mesh,
        in_specs=(tokens_spec, tokens_spec, gain_spec, gain_spec) + (weight_spec,) * 7,
        out_specs=(tokens_spec, tokens_spec, gain_spec, gain_spec) + (weight_spec,) * 7,
        check_vma=False,
    )
```

```python
import functools
import math

import jax
import jax.numpy as jnp
import numpy as np
from jax import lax
from jax.experimental import pallas as pl
from jax.experimental.pallas import tpu as pltpu
from jax.sharding import PartitionSpec as P

QUERY_HEADS = 16
KEY_VALUE_HEADS = 8
HEAD_DIM = 96
GROUP = QUERY_HEADS // KEY_VALUE_HEADS
norm_eps = 1e-05
rope_base = 100000.0
masked_score = -1e30
F32, BF16 = jnp.float32, jnp.bfloat16
VMEM_LIMIT = 60 * 1024 * 1024
VMEM_MOST = 67043328
MESH = pl.DeviceIdType.MESH


def nt_dot(left, right):
    return lax.dot_general(left, right, (((1,), (1,)), ((), ())), preferred_element_type=F32)


def tn_dot(left, right):
    return lax.dot_general(left, right, (((0,), (0,)), ((), ())), preferred_element_type=F32)


def nn_dot(left, right):
    return jnp.dot(left, right, preferred_element_type=F32)


def whole(shape):
    return pl.BlockSpec(shape, lambda *_: (0,) * len(shape))


def call(kernel, scalars, operands, outs, name, flops, moved, scratch=()):
    return pl.pallas_call(
        kernel,
        grid_spec=pltpu.PrefetchScalarGridSpec(
            num_scalar_prefetch=1,
            grid=(1,),
            in_specs=[whole(x.shape) for x in operands],
            out_specs=[whole(x.shape) for x in outs],
            scratch_shapes=scratch,
        ),
        out_shape=outs,
        compiler_params=pltpu.CompilerParams(vmem_limit_bytes=VMEM_LIMIT),
        cost_estimate=pl.CostEstimate(flops=flops, bytes_accessed=moved, transcendentals=0),
        name=name,
    )(scalars, *operands)


def rope_tables(length):
    half = HEAD_DIM // 2
    freqs = np.float32(rope_base) ** (-(np.float32(2.0) * np.arange(half, dtype=np.float32)) / np.float32(HEAD_DIM))
    angles = np.arange(length, dtype=np.float32)[:, None] * freqs.astype(np.float32)[None, :]
    cosine, sine = np.cos(angles), np.sin(angles)
    return np.concatenate([cosine, cosine], 1), np.concatenate([-sine, sine], 1)


def swap_halves(values):
    half = HEAD_DIM // 2
    width = values.shape[1]
    lane = lax.broadcasted_iota(jnp.int32, values.shape, 1)
    ahead = pltpu.roll(values, width - half, 1)
    behind = pltpu.roll(values, half, 1)
    return jnp.where(lane % HEAD_DIM < half, ahead, behind)


def norm_back(grad, normed, inverse, gain):
    scaled = grad * gain
    return inverse * (scaled - normed * jnp.mean(scaled * normed, axis=1, keepdims=True))


def ffn_kernel(
    mesh, tiles, parts, x, g, wg, wd, wu, w_last, dwg, dwu, dwd, out_own, out_arrived, dx_own, dx_arrived,
    xt, acc_out, acc_dx, given_out, given_dx, act, dgate, dup, stage, land, gate, send_sems, recv_sems, local_sems,
):
    step = pl.program_id(0)
    rows = x.shape[0] // 2
    links = Links(mesh, send_sems, recv_sems, local_sems)
    chips, local, tile = tiles // parts, wu.shape[0], land.shape[2]
    cols = tile // parts
    gathers, loads = [], []
    for k in range(chips + 1):
        gathers.append(GatherHalf(links, lambda c, k=k: (stage, c, k), lambda o, k=k: (land, k, rows_at(o, local))))
        weight, tile_at = (wu, k) if k < chips else (w_last, chips - 1)
        for c in range(2):
            source = (weight, slice(None), slice((tile_at * 2 + c) * tile, (tile_at * 2 + c + 1) * tile))
            loads.append(links.local(source, (stage, c, k)))

    def begin(k):
        gathers[k].start()
        gathers[k].other_start()

    def turn(k):
        gathers[k].turn()
        gathers[k].turn_late()

    @pl.when(step == 0)
    def _():
        for load in loads:
            load.start()
        links.barrier()
        for load in loads[:2]:
            load.wait()
        gathers[0].start()
        gathers[0].other_start()
        for load in loads[2:]:
            load.wait()

    @pl.when(step == 0)
    def _():
        acc_out[...] = jnp.zeros_like(acc_out)
        acc_dx[...] = jnp.zeros_like(acc_dx)
        xt[...] = x[...].T

    def first_part():
        turn(0)
        begin(1)
        gathers[0].finish()

    def later_part(k):
        turn(k)
        for n in (2, 3) if k == 1 else (k + 2,):
            if n <= chips:
                begin(n)
        if k == chips - 1:
            turn(chips)

    for k in range(1, chips):
        pl.when(step == (k - 1) * parts + 1)(functools.partial(later_part, k))
    pl.when(step == (chips - 1) * parts)(gathers[chips].finish)
    at = pl.ds(pl.multiple_of(lax.rem(step, parts) * cols, cols), cols)
    chip = step // parts

    @pl.when(chip < chips - 1)
    def _():
        gate[...] = wg[...]

    @pl.when(chip == chips - 1)
    def _():
        gate[...] = land[chips, :, at]

    pl.when(step == 0)(first_part)
    for k in range(1, chips):
        pl.when(step == k * parts)(gathers[k].finish)
    for i in range(2):
        here = slice(i * rows, (i + 1) * rows)
        gate_pre = nn_dot(x[here, :], gate[...])
        up = nn_dot(x[here, :], land[chip, :, at])
        grad = nt_dot(g[here, :], wd[...])
        sigmoid = jax.nn.sigmoid(gate_pre)
        silu = gate_pre * sigmoid
        hidden = (silu * up).astype(BF16)
        act[here, :] = hidden
        gate_grad = (grad * up * sigmoid * (1.0 + gate_pre * (1.0 - sigmoid))).astype(BF16)
        up_grad = (grad * silu).astype(BF16)
        dgate[here, :] = gate_grad
        dup[here, :] = up_grad
        acc_out[i] += nn_dot(hidden, wd[...])
        acc_dx[i] += nt_dot(gate_grad, gate[...]) + nt_dot(up_grad, land[chip, :, at])
    leaving = [
        links.copy(given_dx, dx_arrived, links.at_core()),
        links.local((acc_dx, 0), dx_own),
        links.copy(given_out, out_arrived, links.at_core()),
        links.local((acc_out, 0), out_own),
    ]

    @pl.when(step == tiles - 1)
    def _():
        given_dx[...] = acc_dx[1].astype(BF16)
        leaving[0].start()
        given_out[...] = acc_out[1].astype(BF16)
        for copies in leaving[1:]:
            copies.start()

    dwg[...] = nn_dot(xt[...], dgate[...]).astype(BF16)
    dwu[...] = nn_dot(xt[...], dup[...]).astype(BF16)
    dwd[...] = tn_dot(act[...], g[...]).astype(BF16)

    @pl.when(step == tiles - 1)
    def _():
        for copies in leaving:
            copies.wait()


def ffn(mesh, x, g, wg, wd, wu, w_last):
    rows, width = x.shape[0] // 2, x.shape[1]
    chips, tile = wg.shape[0] + 1, wg.shape[2]
    parts = 2
    tiles, cols = chips * parts, tile // parts
    local = wu.shape[0]
    keep = lambda shape: pl.BlockSpec(shape, lambda i: (0, 0), pipeline_mode=pl.Buffered(1))
    half = tile * chips
    wide, low = jax.ShapeDtypeStruct((rows, width), F32), jax.ShapeDtypeStruct((rows, width), BF16)
    return pl.pallas_call(
        functools.partial(ffn_kernel, mesh, tiles, parts),
        grid=(tiles,),
        in_specs=[
            keep(x.shape),
            keep(g.shape),
            pl.BlockSpec((None, width, cols), lambda i: (jnp.minimum(i // parts, chips - 2), 0, i % parts)),
            pl.BlockSpec((cols, width), lambda i: (i, 0)),
            pl.BlockSpec(memory_space=pl.ANY),
            pl.BlockSpec(memory_space=pl.ANY),
        ],
        out_specs=[pl.BlockSpec((width, cols), lambda i: (0, i))] * 2
        + [pl.BlockSpec((cols, width), lambda i: (i, 0))]
        + [pl.BlockSpec(memory_space=pl.ANY)] * 4,
        scratch_shapes=[pltpu.VMEM((width, 2 * rows), BF16)]
        + [pltpu.VMEM((2, rows, width), F32)] * 2
        + [pltpu.VMEM((rows, width), BF16)] * 2
        + [pltpu.VMEM((2 * rows, cols), BF16)] * 3
        + [pltpu.VMEM((2, chips + 1, local, tile), BF16), pltpu.VMEM((chips + 1, width, tile), BF16), pltpu.VMEM((width, cols), BF16)]
        + [pltpu.SemaphoreType.DMA((96,)), pltpu.SemaphoreType.DMA((96,)), pltpu.SemaphoreType.DMA((64,))],
        out_shape=[
            jax.ShapeDtypeStruct((width, half), BF16),
            jax.ShapeDtypeStruct((width, half), BF16),
            jax.ShapeDtypeStruct((half, width), BF16),
            wide,
            low,
            wide,
            low,
        ],
        compiler_params=pltpu.CompilerParams(vmem_limit_bytes=VMEM_MOST, collective_id=3, has_side_effects=True),
        cost_estimate=pl.CostEstimate(
            flops=36 * rows * width * half, bytes_accessed=12 * width * half + 20 * rows * width, transcendentals=0
        ),
        name="ffn",
    )(x, g, wg, wd, wu, w_last)


def part(x):
    return x[0].at[x[1:]] if isinstance(x, tuple) else x


def get(x):
    return x[0][x[1:]] if isinstance(x, tuple) else x[...]


def put(x, value):
    if isinstance(x, tuple):
        x[0][x[1:]] = value
    else:
        x[...] = value


class Copy:
    def __init__(self, src, dst, device, send_sem, recv_sem):
        self.src, self.dst, self.device, self.send_sem, self.recv_sem = src, dst, device, send_sem, recv_sem

    def made(self):
        if self.device is None:
            return pltpu.make_async_copy(part(self.src), part(self.dst), part(self.send_sem))
        return pltpu.make_async_remote_copy(
            src_ref=part(self.src),
            dst_ref=part(self.dst),
            send_sem=part(self.send_sem),
            recv_sem=part(self.recv_sem),
            device_id=self.device,
            device_id_type=MESH,
        )

    def start(self):
        self.made().start()

    def wait(self):
        self.made().wait()

    def wait_send(self):
        self.made().wait_send()

    def wait_recv(self):
        self.made().wait_recv()


class Links:
    def __init__(self, mesh, send_sems, recv_sems, local_sems):
        self.ns, self.nf = mesh
        self.na = self.nf // 4
        self.send_sems, self.recv_sems, self.local_sems = send_sems, recv_sems, local_sems
        self.count, self.local_count = 0, 0
        self.z, self.f = lax.axis_index("seq"), lax.axis_index("fsdp")
        self.core = lax.rem(self.f, 2)
        self.b = lax.rem(self.f // 2, 2)
        self.a = self.f // 4

    def chip(self, da, db):
        return lax.rem(self.a + da, self.na) * 2 + lax.rem(self.b + db, 2)

    def at_core(self):
        return (self.z, self.f + 1 - 2 * self.core)

    def at_b(self):
        return (self.z, self.f + 2 - 4 * self.b)

    def at_a(self, d):
        return (self.z, lax.rem(self.f + 4 * d, self.nf))

    def at_z(self, d):
        return (lax.rem(self.z + d, self.ns), self.f)

    def peers(self):
        return [self.at_core(), self.at_b()] + [self.at_a(d) for d in range(1, self.na)] + [self.at_z(d) for d in range(1, self.ns)]

    def barrier(self):
        barrier = pltpu.get_barrier_semaphore()
        peers = self.peers()
        for peer in peers:
            pl.semaphore_signal(barrier, inc=1, device_id=peer, device_id_type=MESH)
        pl.semaphore_wait(barrier, len(peers))

    def copy(self, src, dst, device):
        index = self.count
        self.count += 1
        return Copy(src, dst, device, (self.send_sems, index), (self.recv_sems, index))

    def again(self, src, dst, device):
        index = self.count - 1
        return Copy(src, dst, device, (self.send_sems, index), (self.recv_sems, index))

    def local(self, src, dst):
        index = self.local_count
        self.local_count += 1
        return Copy(src, dst, None, (self.local_sems, index), None)


def line_place(links):
    z, ns = links.z, links.ns
    middle = ns // 2
    step = jnp.where(z < middle, 1, -1)
    end = (z == 0) | (z == ns - 1)
    inner = (z == middle - 1) | (z == middle)
    return end, inner, (z + step, links.f), (z - step, links.f)


GATE_PIECES = 4


def first_piece(ns, columns):
    return columns // GATE_PIECES if ns == 4 else 0


def rows_at(start, size):
    return pl.ds(pl.multiple_of(start * size, size), size)


class ChipSum:
    def __init__(self, links, partial, b_first, arrived, passed, staging):
        self.links, self.partial, self.b_first = links, partial, b_first
        self.arrived, self.passed, self.staging = arrived, passed, staging
        na = links.na
        self.first, self.second = [], []
        if b_first:
            self.kept = [links.chip(da, 0) for da in range(na)]
            for da in range(na):
                self.first.append(links.copy(partial(links.chip(da, 1)), (arrived, da), links.at_b()))
            for d in range(1, na):
                self.second.append(links.copy((arrived, d), (passed, d - 1), links.at_a(d)))
        else:
            self.kept = [links.chip(0, db) for db in range(2)]
            for d in range(1, na):
                for db in range(2):
                    self.first.append(links.copy(partial(links.chip(d, db)), (arrived, (d - 1) * 2 + db), links.at_a(d)))
            self.second.append(links.copy((arrived, 1), (passed, 0), links.at_b()))
        self.loads = [] if staging is None else [links.local(partial(k), (staging, i)) for i, k in enumerate(self.kept)]

    def start(self):
        for copy in self.first:
            copy.start()

    def load(self):
        for load in self.loads:
            load.start()

    def turn(self):
        for load in self.loads:
            load.wait()
        for copy in self.first:
            copy.wait()
        count = len(self.kept)
        for i in [*range(1, count), 0]:
            own = self.partial(self.kept[i]) if self.staging is None else (self.staging, i)
            total = get(own).astype(F32)
            if self.b_first:
                total = total + self.arrived[i].astype(F32)
            else:
                for d in range(self.links.na - 1):
                    total = total + self.arrived[d * 2 + i].astype(F32)
            self.arrived[i] = total.astype(BF16)
            if i > 0 and self.b_first:
                self.second[i - 1].start()
            elif i > 0:
                self.second[0].start()

    def finish(self):
        for copy in self.second:
            copy.wait()
        total = self.arrived[0].astype(F32)
        for i in range(len(self.second)):
            total = total + self.passed[i].astype(F32)
        return total.astype(BF16)


def chip_sum_shapes(na, b_first, rows, columns):
    first = na if b_first else 2 * (na - 1)
    kept = na if b_first else 2
    return [
        pltpu.VMEM((max(first, kept), rows, columns), BF16),
        pltpu.VMEM((na - 1 if b_first else 1, rows, columns), BF16),
        pltpu.VMEM((kept, rows, columns), BF16),
    ]


def flip_core(f):
    return f + 1 - 2 * lax.rem(f, 2)


def flip_b(f):
    return f + 2 - 4 * lax.rem(f // 2, 2)


class Gather:
    def __init__(self, links, own, land, both):
        self.links = links
        f, na, nf = links.f, links.na, links.nf
        to_core, to_b = links.at_core(), links.at_b()

        def move(origin, device, half=None):
            return links.copy(land(origin, half), land(origin, half), device)

        self.given = [links.copy(own, land(f, None), to_core)] if both else []
        self.own = [links.copy(own, land(f, None), to_b)]
        self.own += [links.copy(own, land(f, None), links.at_a(d)) for d in range(1, na)]
        from_b = flip_b(f)
        from_a = [lax.rem(f + nf - 4 * d, nf) for d in range(1, na)]
        if na == 2:
            self.relays = [move(from_b, links.at_a(1), 1), move(from_a[0], to_b, 0)]
            far = [(flip_b(from_a[0]), 0), (flip_b(from_a[0]), 1)]
        else:
            self.relays = [move(origin, to_b) for origin in from_a]
            far = [(flip_b(origin), None) for origin in from_a]
        near = [from_b, *from_a]
        self.near = [move(origin, to_core) for origin in near] if both else []
        self.far = [move(origin, to_core, half) for origin, half in far] if both else []

    def start(self):
        for copies in self.own + self.given:
            copies.start()

    def turn(self):
        for copies in self.own:
            copies.wait()
        for copies in self.relays + self.near:
            copies.start()

    def pass_on(self):
        for copies in self.relays:
            copies.wait()
        for copies in self.far:
            copies.start()

    def finish(self):
        for copies in self.given + self.near + self.far:
            copies.wait()


class GatherHalf:
    def __init__(self, links, stage, land):
        self.links = links
        f, na, nf, core = links.f, links.na, links.nf, links.core
        to_b = links.at_b()

        def move(origin, device):
            return links.copy(land(origin), land(origin), device)

        self.swap = links.copy(stage(1 - core), land(f), links.at_core())
        self.kept = links.local(stage(core), land(f))
        targets = [to_b] + [links.at_a(d) for d in range(1, na)]
        self.own = [links.copy(stage(core), land(f), device) for device in targets]
        self.other = [move(flip_core(f), device) for device in targets]
        from_b = flip_b(f)
        from_a = [lax.rem(f + nf - 4 * d, nf) for d in range(1, na)]
        if na == 2:
            self.relays = [move(from_b, links.at_a(1))]
            self.late = [move(flip_core(from_a[0]), to_b)]
        else:
            self.relays = [move(origin, to_b) for origin in from_a]
            self.late = [move(flip_core(origin), to_b) for origin in from_a]

    def start(self):
        for copies in [self.swap, self.kept, *self.own]:
            copies.start()

    def other_start(self):
        self.swap.wait()
        for copies in self.other:
            copies.start()

    def turn(self):
        for copies in self.own:
            copies.wait()
        for copies in self.relays:
            copies.start()

    def turn_late(self):
        for copies in self.other:
            copies.wait()
        for copies in self.late:
            copies.start()

    def finish(self):
        for copies in [self.kept, *self.relays, *self.late]:
            copies.wait()


def attend_heads(ns, kv, span, qs, ks, vs, out, logs):
    scale = 1.0 / math.sqrt(HEAD_DIM)
    row = lax.broadcasted_iota(jnp.int32, (span, span), 0)
    column = lax.broadcasted_iota(jnp.int32, (span, span), 1)
    causal = row >= column
    lane = lax.broadcasted_iota(jnp.int32, (span, 128), 1)
    for s in range(ns):
        here = slice(s * span, (s + 1) * span)
        stats = jnp.zeros((span, 128), F32)
        for h in range(kv * GROUP):
            g = h // GROUP
            q = qs[h, here, :]
            near = jnp.where(causal, nt_dot(q, ks[g, here, :]) * scale, masked_score)
            top = jnp.max(near, axis=1, keepdims=True)
            if s > 0:
                far = nt_dot(q, ks[g, : s * span, :]) * scale
                top = jnp.maximum(top, jnp.max(far, axis=1, keepdims=True))
            near = jnp.exp(near - top)
            total = jnp.sum(near, axis=1, keepdims=True)
            if s > 0:
                far = jnp.exp(far - top)
                total = total + jnp.sum(far, axis=1, keepdims=True)
            inverse = 1.0 / total
            result = nn_dot((near * inverse).astype(BF16), vs[g, here, :])
            if s > 0:
                result = result + nn_dot((far * inverse).astype(BF16), vs[g, : s * span, :])
            stats = jnp.where(lane == h, top + jnp.log(total), stats)
            out[s, :, h * HEAD_DIM : (h + 1) * HEAD_DIM] = result.astype(BF16)
        logs[here, :] = stats


def fill_tables(cosines, sines, narrow_cosines, narrow_sines, heads):
    end = heads * HEAD_DIM
    cosines[:, end:] = jnp.ones((cosines.shape[0], cosines.shape[1] - end), F32)
    sines[:, end:] = jnp.zeros((cosines.shape[0], cosines.shape[1] - end), F32)
    for h in range(heads):
        at = slice(h * HEAD_DIM, (h + 1) * HEAD_DIM)
        cosines[:, at] = narrow_cosines
        sines[:, at] = narrow_sines


def fore_kernel(
    mesh, count, kv,
    tokens, cotangent, gains_in, wq, wk, wv, wo, wg, wd, narrow_cosines, narrow_sines,
    w_qkv, w_out, w_gate, w_down, first_out, packed, heads_attended, logs, attended_out, hidden_out, second_both, low_both, gains_out,
    rows_in, hidden, first, pack, w_land, wo_land, q_send, q_land, a_send, a_land, stage_gate, gain_send, gain_land,
    qs, ks, vs, log, attended, second, second_abs, low, cosines, sines, send_sems, recv_sems, local_sems,
):
    links = Links(mesh, send_sems, recv_sems, local_sems)
    ns, na, nf = links.ns, links.na, links.nf
    chips = 2 * na
    z, f, core = links.z, links.f, links.core
    rows, width = rows_in.shape
    span = rows // count
    heads = kv * GROUP
    g_width, k_width = heads * HEAD_DIM, kv * HEAD_DIM
    q_width = g_width + 2 * k_width
    local = width // nf
    links.barrier()

    token_load = links.local(tokens, rows_in)
    token_load.start()
    cot_load = links.local(cotangent, hidden)
    cot_load.start()
    gain_send[...] = jnp.zeros_like(gain_send)
    gain_send[0:2, :local] = gains_in[...].astype(F32)
    for j in range(ns):
        pack[j, :, :g_width] = wq[:, j * g_width : (j + 1) * g_width]
        pack[j, :, g_width : g_width + k_width] = wk[:, j * k_width : (j + 1) * k_width]
        pack[j, :, g_width + k_width :] = wv[:, j * k_width : (j + 1) * k_width]

    every = slice(None)

    def piece(start, size, half):
        if half is None:
            return rows_at(start, size)
        return rows_at(start * 2 + half, size // 2)

    units = []
    turns = [*range(1, ns), 0]
    for d in turns:
        g = lax.rem(z + d, ns)
        units.append(Gather(links, (pack, g), lambda o, half, g=g: (w_land, g, piece(o, local, half)), True))
    units.append(Gather(links, wo, lambda o, half: (wo_land, piece(o, local, half)), True))
    depth = wd.shape[0]
    units.append(Gather(links, wd, lambda o, half: (w_down, piece(o // 2, depth, half)), False))
    gate_unit = GatherHalf(links, lambda c: (stage_gate, c), lambda o: (w_gate, every, rows_at(o, local)))
    q_copies, a_copies = [], []
    for d in range(1, ns):
        g = lax.rem(z + d, ns)
        q_copies.append([links.copy((q_send, g, i), (q_land, i, z), links.at_z(d)) for i in range(count)])
    for i in range(count):
        a_copies.append([links.copy((a_send, i, lax.rem(z + d, ns)), (a_land, i, z), links.at_z(d)) for d in range(1, ns)])
    second_copy = links.copy(second_abs, (second_both, pl.ds(rows, rows)), links.at_core())
    low_copy = links.copy(low, (low_both, pl.ds(rows, rows)), links.at_core())

    def gain_at(start, size):
        return (gain_land, pl.ds(start, size))

    pair, chip_four = f // 2 * 2, f // 4 * 4
    gain_copies = [
        [links.copy(gain_at(f, 1), gain_at(f, 1), links.at_core())],
        [links.copy(gain_at(pair, 2), gain_at(pair, 2), links.at_b())],
        [links.copy(gain_at(chip_four, 4), gain_at(chip_four, 4), links.at_a(d)) for d in range(1, na)],
    ]
    stores = []

    def store(src, dst):
        copies = links.local(src, dst)
        copies.start()
        stores.append(copies)

    gain_land[f] = gain_send[...]
    for copies in gain_copies[0]:
        copies.start()
    units[0].start()
    units[1].start()
    for j in range(ns):
        w_land[j, rows_at(f, local), :] = pack[j]
    stage_loads = []
    tile = w_gate.shape[2]
    for c in range(2):
        for k in range(chips - 1):
            source = (wg, every, slice((k * 2 + c) * tile, (k * 2 + c + 1) * tile))
            stage_loads.append(links.local(source, (stage_gate, c, k)))
    for load in stage_loads:
        load.start()
    store_own = [links.local(wo, (wo_land, rows_at(f, local))), links.local(wd, (w_down, rows_at(f // 2, depth)))]
    for copies in store_own:
        copies.start()
    fill_tables(cosines, sines, narrow_cosines[rows_at(z, span), :], narrow_sines[rows_at(z, span), :], heads + kv)
    token_load.wait()
    old = rows_in[...]
    inverse = lax.rsqrt(jnp.mean(old * old, axis=1, keepdims=True) + norm_eps)
    for stage in range(3):
        for copies in gain_copies[stage]:
            copies.wait()
        if stage < 2:
            for copies in gain_copies[stage + 1]:
                copies.start()
    for j in range(nf):
        gains_out[:, j * local : (j + 1) * local] = gain_land[j, 0:2, :local]
    first[...] = (old * inverse * gains_out[0:1, :]).astype(BF16)
    store(first, first_out)

    def project(n):
        g = lax.rem(z + turns[n], ns)
        units[n].finish()
        y = nn_dot(first[...], w_land[g])
        for i in range(count):
            part = y[i * span : (i + 1) * span]
            part = (part * cosines[...] + swap_halves(part) * sines[...]).astype(BF16)
            if turns[n] == 0:
                q_land[i, z] = part
            else:
                q_send[g, i] = part
        if turns[n] > 0:
            q_copies[turns[n] - 1][0].start()
        if n > 0 and turns[n - 1] > 0:
            for copies in q_copies[turns[n - 1] - 1][1:]:
                copies.start()
        store((w_land, g), (w_qkv, g))

    last = len(units)
    for n in range(ns):
        units[n].turn()
        if n + 2 < last:
            units[n + 2].start()
        if n > 0:
            units[n - 1].pass_on()
        if n > 1:
            project(n - 2)
    units[ns].turn()
    for load in stage_loads:
        load.wait()
    gate_unit.start()
    units[ns - 1].pass_on()
    project(ns - 2)
    gate_unit.other_start()
    project(ns - 1)
    units[ns].pass_on()
    cot_load.wait()
    low[...] = hidden[...].astype(BF16)
    low_copy.start()
    store(low, (low_both, pl.ds(0, rows)))

    def attend(i):
        for copies in q_copies:
            copies[i].wait()
        for j in range(ns):
            at = slice(j * span, (j + 1) * span)
            for h in range(heads):
                qs[h, at, :] = q_land[i, j, :, h * HEAD_DIM : (h + 1) * HEAD_DIM]
            for h in range(kv):
                k0, v0 = (heads + h) * HEAD_DIM, (heads + kv + h) * HEAD_DIM
                ks[h, at, :] = q_land[i, j, :, k0 : k0 + HEAD_DIM]
                vs[h, at, :] = q_land[i, j, :, v0 : v0 + HEAD_DIM]
        attend_heads(ns, kv, span, qs, ks, vs, a_send.at[i], log.at[i])
        for copies in a_copies[i]:
            copies.start()
        a_land[i, z] = a_send[i, z]

    for i in range(count):
        attend(i)
        if i == 0:
            units[ns + 1].turn()
            units[ns].finish()
            store_own[0].wait()
            store(wo_land, w_out)
    store(q_land, packed)
    store(a_send, heads_attended)
    store(log, logs)
    for i in range(count):
        for copies in a_copies[i]:
            copies.wait()
        for j in range(ns):
            attended[i * span : (i + 1) * span, j * g_width : (j + 1) * g_width] = a_land[i, j]
    new = rows_in[...] + nn_dot(attended[...], wo_land[...])
    hidden[...] = new
    inverse = lax.rsqrt(jnp.mean(new * new, axis=1, keepdims=True) + norm_eps)
    second_abs[...] = (new * inverse * gains_out[1:2, :]).astype(BF16)
    second_copy.start()
    store(second_abs, (second_both, pl.ds(0, rows)))
    store(attended, attended_out)
    store(hidden, hidden_out)
    units[ns + 1].pass_on()
    gate_unit.turn()
    gate_unit.turn_late()
    gate_unit.finish()
    second_copy.wait()
    low_copy.wait()
    store_own[1].wait()
    for copies in stores:
        copies.wait()


def fore(mesh, count, kv, tokens, cotangent, gains_in, wq, wk, wv, wo, wg, wd, narrow_cosines, narrow_sines):
    ns, nf = mesh
    na = nf // 4
    chips = 2 * na
    rows, width = tokens.shape
    span = rows // count
    length = ns * span
    heads = kv * GROUP
    g_width = heads * HEAD_DIM
    q_width = g_width + 2 * kv * HEAD_DIM
    local, depth = wq.shape[0], wd.shape[0]
    tile = wg.shape[1] // (2 * chips)
    anywhere, vmem = pl.BlockSpec(memory_space=pl.ANY), pl.BlockSpec(memory_space=pltpu.VMEM)
    low = lambda *shape: jax.ShapeDtypeStruct(shape, BF16)
    wide = lambda *shape: jax.ShapeDtypeStruct(shape, F32)
    outs = [
        low(ns, width, q_width),
        low(width, width),
        low(chips - 1, width, tile),
        low(chips * depth, width),
        low(rows, width),
        low(count, ns, span, q_width),
        low(count, ns, span, g_width),
        wide(count, length, 128),
        low(rows, width),
        wide(rows, width),
        low(2 * rows, width),
        low(2 * rows, width),
        wide(2, width),
    ]
    scratch = [
        pltpu.VMEM((rows, width), F32),
        pltpu.VMEM((rows, width), F32),
        pltpu.VMEM((rows, width), BF16),
        pltpu.VMEM((ns, local, q_width), BF16),
        pltpu.VMEM((ns, width, q_width), BF16),
        pltpu.VMEM((width, width), BF16),
        pltpu.VMEM((ns, count, span, q_width), BF16),
        pltpu.VMEM((count, ns, span, q_width), BF16),
        pltpu.VMEM((count, ns, span, g_width), BF16),
        pltpu.VMEM((count, ns, span, g_width), BF16),
        pltpu.VMEM((2, chips - 1, local, tile), BF16),
        pltpu.VMEM((8, 256), F32),
        pltpu.VMEM((nf, 8, 256), F32),
        pltpu.VMEM((heads, length, HEAD_DIM), BF16),
        pltpu.VMEM((kv, length, HEAD_DIM), BF16),
        pltpu.VMEM((kv, length, HEAD_DIM), BF16),
        pltpu.VMEM((count, length, 128), F32),
        pltpu.VMEM((rows, width), BF16),
        pltpu.VMEM((8, 128), BF16),
        pltpu.VMEM((rows, width), BF16),
        pltpu.VMEM((rows, width), BF16),
        pltpu.VMEM((span, q_width), F32),
        pltpu.VMEM((span, q_width), F32),
    ]
    return pl.pallas_call(
        functools.partial(fore_kernel, mesh, count, kv),
        in_specs=[anywhere] * 2 + [vmem] * 4 + [anywhere] * 3 + [vmem] * 2,
        out_specs=[anywhere] * 12 + [vmem],
        out_shape=outs,
        scratch_shapes=scratch
        + [pltpu.SemaphoreType.DMA((160,)), pltpu.SemaphoreType.DMA((160,)), pltpu.SemaphoreType.DMA((64,))],
        compiler_params=pltpu.CompilerParams(vmem_limit_bytes=VMEM_MOST, collective_id=0, has_side_effects=True),
        name="fore",
    )(tokens, cotangent, gains_in, wq, wk, wv, wo, wg, wd, narrow_cosines, narrow_sines)


def attend_back_heads(ns, kv, span, qs, ks, vs, gs, attended, logs, dk, dv, result):
    scale = 1.0 / math.sqrt(HEAD_DIM)
    heads = kv * GROUP
    row = lax.broadcasted_iota(jnp.int32, (span, span), 0)
    column = lax.broadcasted_iota(jnp.int32, (span, span), 1)
    causal = row >= column
    dk[...] = jnp.zeros_like(dk)
    dv[...] = jnp.zeros_like(dv)
    for s in range(ns):
        here = slice(s * span, (s + 1) * span)
        for h in range(heads):
            g = h // GROUP
            q, grad = qs[h, here, :], gs[h, here, :]
            log_total = logs[here, h : h + 1]
            out = attended[s, :, h * HEAD_DIM : (h + 1) * HEAD_DIM]
            delta = jnp.sum(grad.astype(F32) * out.astype(F32), axis=1, keepdims=True)
            k, v = ks[g, here, :], vs[g, here, :]
            near = jnp.where(causal, jnp.exp(nt_dot(q, k) * scale - log_total), 0.0)
            slope = (near * (nt_dot(grad, v) - delta) * scale).astype(BF16)
            dq = nn_dot(slope, k)
            dk[g, here, :] += tn_dot(slope, q)
            dv[g, here, :] += tn_dot(near.astype(BF16), grad)
            if s > 0:
                before = slice(0, s * span)
                k, v = ks[g, before, :], vs[g, before, :]
                far = jnp.exp(nt_dot(q, k) * scale - log_total)
                slope = (far * (nt_dot(grad, v) - delta) * scale).astype(BF16)
                dq = dq + nn_dot(slope, k)
                dk[g, before, :] += tn_dot(slope, q)
                dv[g, before, :] += tn_dot(far.astype(BF16), grad)
            result[here, h * HEAD_DIM : (h + 1) * HEAD_DIM] = dq
    for g in range(kv):
        k0 = (heads + g) * HEAD_DIM
        v0 = (heads + kv + g) * HEAD_DIM
        result[:, k0 : k0 + HEAD_DIM] = dk[g]
        result[:, v0 : v0 + HEAD_DIM] = dv[g]


def back_kernel(
    mesh, count, kv,
    dx_own, dx_other, hidden, cotangent, gains, w_out, w_qkv, packed, attended, logs, cosines, sines, tokens, dwg, dwu,
    high, low_out, out, gain_grads, dqkv, sum_gate, sum_up,
    low, sum_rows, sum_land, dx_land, g_send, g_land, q_send, q_land, swap_send, swap_land, *rest,
):
    parts, (send_sems, recv_sems, local_sems) = rest[:-3], rest[-3:]
    links = Links(mesh, send_sems, recv_sems, local_sems)
    ns, na = links.ns, links.na
    chips = 2 * na
    z, core = links.z, links.core
    rows, width = hidden.shape
    span = rows // count
    length = ns * span
    heads = kv * GROUP
    g_width, q_width = heads * HEAD_DIM, (heads + 2 * kv) * HEAD_DIM
    half = dwg.shape[1]
    block = width // chips
    links.barrier()

    sums = []
    for n, source in enumerate((dwg, dwu)):
        for b_first in (True, False):
            columns = slice(0, half // 2) if b_first else slice(half // 2, half)
            at = (n * 2 + (0 if b_first else 1)) * 3
            partial = lambda k, source=source, columns=columns: (source, rows_at(k, block), columns)
            sums.append(ChipSum(links, partial, b_first, *parts[at : at + 3]))
    for item in sums:
        item.start()
        item.load()

    g_copies, q_copies = [], []
    for i in range(count):
        g_copies.append([links.copy((g_send, i, lax.rem(z + d, ns)), (g_land, i, z), links.at_z(d)) for d in range(1, ns)])
        q_copies.append([links.copy((q_send, i, lax.rem(z + d, ns)), (q_land, z, i), links.at_z(d)) for d in range(1, ns)])

    def out_back(dx, old, grad, w):
        load_sets, store_sets = [], []
        for i in range(count):
            here = pl.ds(i * span, span)
            pairs = ((dx_own, dx), (dx_other, dx_land), (hidden, old), (cotangent, grad))
            load_sets.append([links.local((source, here), (target, here)) for source, target in pairs])
            store_sets.append([links.local((grad, here), (high, here)), links.local((low, here), (low_out, here))])
        w_load = links.local(w_out, w)
        for load in load_sets[0] + [w_load] + [load for loads in load_sets[1:] for load in loads]:
            load.start()
        for i in range(count):
            here = slice(i * span, (i + 1) * span)
            for load in load_sets[i]:
                load.wait()
            step, rows_old = dx[here, :] + dx_land[here, :].astype(F32), old[here, :]
            inverse = lax.rsqrt(jnp.mean(rows_old * rows_old, axis=1, keepdims=True) + norm_eps)
            normed = rows_old * inverse
            part_sum = jnp.sum(step * normed, axis=0, keepdims=True)
            gain_grads[1:2, :] = part_sum if i == 0 else gain_grads[1:2, :] + part_sum
            total = grad[here, :] + norm_back(step, normed, inverse, gains[1:2, :])
            grad[here, :] = total
            low[here, :] = total.astype(BF16)
            for copies in store_sets[i]:
                copies.start()
            if i == 0:
                w_load.wait()
            out_part = nt_dot(low[here, :], w[...]).astype(BF16)
            for j in range(ns):
                g_send[i, j] = out_part[:, j * g_width : (j + 1) * g_width]
            for copies in g_copies[i]:
                copies.start()
            g_land[i, z] = g_send[i, z]
        for copies in [copies for stores in store_sets for copies in stores]:
            copies.wait()

    pl.run_scoped(
        out_back,
        pltpu.VMEM((rows, width), F32),
        pltpu.VMEM((rows, width), F32),
        pltpu.VMEM((rows, width), F32),
        pltpu.VMEM((width, width), BF16),
    )

    def attention(qkv, mid, log, qs, ks, vs, gs, dk, dv, result, cosine, sine):
        fill_tables(cosine, sine, cosines[...], sines[...], heads + kv)
        for i in range(count):
            loads = [links.local((packed, i), qkv), links.local((attended, i), mid), links.local((logs, i), log)]
            for load in loads:
                load.start()
            for load in loads:
                load.wait()
            for j in range(ns):
                at = slice(j * span, (j + 1) * span)
                for h in range(heads):
                    qs[h, at, :] = qkv[j, :, h * HEAD_DIM : (h + 1) * HEAD_DIM]
                for h in range(kv):
                    k0, v0 = (heads + h) * HEAD_DIM, (heads + kv + h) * HEAD_DIM
                    ks[h, at, :] = qkv[j, :, k0 : k0 + HEAD_DIM]
                    vs[h, at, :] = qkv[j, :, v0 : v0 + HEAD_DIM]
            for copies in g_copies[i]:
                copies.wait()
            for j in range(ns):
                for h in range(heads):
                    gs[h, j * span : (j + 1) * span, :] = g_land[i, j, :, h * HEAD_DIM : (h + 1) * HEAD_DIM]
            attend_back_heads(ns, kv, span, qs, ks, vs, gs, mid, log, dk, dv, result)
            for j in range(ns):
                here = slice(j * span, (j + 1) * span)
                part = result[here, :]
                q_send[i, j] = (part * cosine[here, :] - swap_halves(part) * sine[here, :]).astype(BF16)
            for copies in q_copies[i]:
                copies.start()
            q_land[z, i] = q_send[i, z]
            if i < len(sums) // 2:
                for item in sums[2 * i : 2 * i + 2]:
                    item.turn()

    pl.run_scoped(
        attention,
        pltpu.VMEM((ns, span, q_width), BF16),
        pltpu.VMEM((ns, span, g_width), BF16),
        pltpu.VMEM((length, 128), F32),
        pltpu.VMEM((heads, length, HEAD_DIM), BF16),
        pltpu.VMEM((kv, length, HEAD_DIM), BF16),
        pltpu.VMEM((kv, length, HEAD_DIM), BF16),
        pltpu.VMEM((heads, length, HEAD_DIM), BF16),
        pltpu.VMEM((kv, length, HEAD_DIM), F32),
        pltpu.VMEM((kv, length, HEAD_DIM), F32),
        pltpu.VMEM((length, q_width), F32),
        pltpu.VMEM((length, q_width), F32),
        pltpu.VMEM((length, q_width), F32),
    )

    swaps = []
    local = block // 2
    for item in sums[2 * count :]:
        item.turn()

    def swap(n):
        for m in range(2):
            total = sums[2 * n + m].finish()
            swap_send[n, m, 0] = total[:local]
            swap_send[n, m, 1] = total[local:]
        for m in range(2):
            copies = links.copy((swap_send, n, m, 1 - core), (swap_land, n, m), links.at_core())
            copies.start()
            swaps.append(copies)

    tile = half // chips
    stores = []
    early = first_piece(ns, 2 * half)
    piece = (sum_rows, 0, slice(None), slice(0, max(early, 1)))
    end, inner, inward = line_place(links)[:3]
    early_copy = links.copy(piece, sum_land, inward)

    def combine(n, total):
        for m in range(2):
            swaps[2 * n + m].wait()
            kept, arrived = swap_send[n, m, core], swap_land[n, m]
            for t in range(chips // 2):
                here = slice(t * tile, (t + 1) * tile)
                k = m * (chips // 2) + t
                one, two = kept[:, here], arrived[:, here]
                sum_rows[n, :, 2 * k * tile : (2 * k + 1) * tile] = jnp.where(core == 0, one, two)
                sum_rows[n, :, (2 * k + 1) * tile : (2 * k + 2) * tile] = jnp.where(core == 0, two, one)
        if n == 0 and early:
            pl.when(end)(early_copy.start)
        else:
            copies = links.local((sum_rows, n), total)
            copies.start()
            stores.append(copies)

    def project_back(w, old, base, grad):
        loads = [links.local(tokens, old), links.local(high, base), links.local(w_qkv, w)]
        for load in loads:
            load.start()
        swap(0)
        for load in loads:
            load.wait()
        for i in range(count):
            here = slice(i * span, (i + 1) * span)
            if i == count - 1:
                combine(0, sum_gate)
                swap(1)
                combine(1, sum_up)
            for copies in q_copies[i]:
                copies.wait()
            total = nt_dot(q_land[0, i], w[0])
            for j in range(1, ns):
                total = total + nt_dot(q_land[j, i], w[j])
            grad[here, :] = total
            copies = links.local((q_land, slice(None), i), (dqkv, slice(None), i))
            copies.start()
            stores.append(copies)
            step, rows_old = grad[here, :], old[here, :]
            inverse = lax.rsqrt(jnp.mean(rows_old * rows_old, axis=1, keepdims=True) + norm_eps)
            normed = rows_old * inverse
            part_sum = jnp.sum(step * normed, axis=0, keepdims=True)
            gain_grads[0:1, :] = part_sum if i == 0 else gain_grads[0:1, :] + part_sum
            base[here, :] = base[here, :] + norm_back(step, normed, inverse, gains[0:1, :])
            copies = links.local((base, here), (out, here))
            copies.start()
            stores.append(copies)
        if early:

            @pl.when(inner)
            def _():
                early_copy.wait_recv()
                put(piece, (get(piece).astype(F32) + sum_land[...].astype(F32)).astype(BF16))

            pl.when(end)(early_copy.wait_send)
            copies = links.local((sum_rows, 0), sum_gate)
            copies.start()
            stores.append(copies)
        for copies in stores:
            copies.wait()

    pl.run_scoped(
        project_back,
        pltpu.VMEM((ns, width, q_width), BF16),
        pltpu.VMEM((rows, width), F32),
        pltpu.VMEM((rows, width), F32),
        pltpu.VMEM((rows, width), F32),
    )


def back(mesh, count, kv, dx_own, dx_other, hidden, cotangent, gains, w_out, w_qkv, packed, attended, logs, cosines, sines, tokens, dwg, dwu):
    ns, nf = mesh
    na = nf // 4
    rows, width = hidden.shape
    span = rows // count
    heads = kv * GROUP
    g_width, q_width = heads * HEAD_DIM, (heads + 2 * kv) * HEAD_DIM
    half = dwg.shape[1]
    block = width // (2 * na)
    local = block // 2
    anywhere = pl.BlockSpec(memory_space=pl.ANY)
    vmem = pl.BlockSpec(memory_space=pltpu.VMEM)
    operands = [dx_own, dx_other, hidden, cotangent, gains, w_out, w_qkv, packed, attended, logs, cosines, sines, tokens, dwg, dwu]
    wide = jax.ShapeDtypeStruct((rows, width), F32)
    summed = jax.ShapeDtypeStruct((local, 2 * half), BF16)
    scratch = [
        pltpu.VMEM((rows, width), BF16),
        pltpu.VMEM((2, local, 2 * half), BF16),
        pltpu.VMEM((local, max(first_piece(ns, 2 * half), 128)), BF16),
        pltpu.VMEM((rows, width), BF16),
        pltpu.VMEM((count, ns, span, g_width), BF16),
        pltpu.VMEM((count, ns, span, g_width), BF16),
        pltpu.VMEM((count, ns, span, q_width), BF16),
        pltpu.VMEM((ns, count, span, q_width), BF16),
        pltpu.VMEM((2, 2, 2, local, half // 2), BF16),
        pltpu.VMEM((2, 2, local, half // 2), BF16),
    ]
    for _ in range(2):
        for b_first in (True, False):
            scratch += chip_sum_shapes(na, b_first, block, half // 2)
    return pl.pallas_call(
        functools.partial(back_kernel, mesh, count, kv),
        in_specs=[vmem if x.shape[0] == 2 and x.ndim == 2 or x.shape[1] == HEAD_DIM else anywhere for x in operands],
        out_specs=[anywhere, anywhere, anywhere, vmem, anywhere, anywhere, anywhere],
        out_shape=[
            wide,
            jax.ShapeDtypeStruct((rows, width), BF16),
            wide,
            jax.ShapeDtypeStruct((2, width), F32),
            jax.ShapeDtypeStruct((ns, count, span, q_width), BF16),
            summed,
            summed,
        ],
        scratch_shapes=scratch
        + [pltpu.SemaphoreType.DMA((64,)), pltpu.SemaphoreType.DMA((64,)), pltpu.SemaphoreType.DMA((64,))],
        compiler_params=pltpu.CompilerParams(vmem_limit_bytes=VMEM_MOST, collective_id=1, has_side_effects=True),
        name="back",
    )(*operands)


class LineSum:
    def __init__(self, links, term, first, second, total, out=None, begun=False):
        self.links, self.term, self.first, self.second, self.total = links, term, first, second, total
        self.dtype = (term[0] if isinstance(term, tuple) else term).dtype
        self.deep = links.ns // 2 > 1
        self.begun = begun
        self.end, self.inner, inward, outward = line_place(links)
        moved = self.deep and not begun
        self.inward = links.copy(term, first, inward) if moved else None
        self.onward = links.again(first, first, inward) if moved else None
        self.sum = first if moved else term
        self.across = links.copy(self.sum, second, inward)
        self.outward = links.copy(total, total, outward) if self.deep else None
        self.store = links.local(total, out) if out is not None else None

    def keep(self):
        if self.store is not None:
            self.store.start()

    def add(self, target, one, two):
        put(target, (get(one).astype(F32) + get(two).astype(F32)).astype(self.dtype))

    def begin(self):
        if self.begun:
            pl.when(self.inner)(self.across.start)
        elif self.deep:
            pl.when(self.end)(self.inward.start)
        else:
            self.across.start()

    def relay(self):
        if not self.deep or self.begun:
            return

        @pl.when(jnp.logical_not(self.end))
        def _():
            self.inward.wait_recv()
            self.add(self.first, self.term, self.first)
            pl.when(self.inner)(self.across.start)
            pl.when(jnp.logical_not(self.inner))(self.onward.start)

    def settle(self):
        @pl.when(self.inner)
        def _():
            self.across.wait()
            self.add(self.total, self.sum, self.second)
            if self.deep:
                self.outward.start()
            self.keep()

        if self.deep:

            @pl.when(jnp.logical_not(self.inner | self.end))
            def _():
                self.outward.wait_recv()
                self.outward.start()
                self.keep()

    def finish(self):
        if self.deep:

            @pl.when(self.end)
            def _():
                self.outward.wait_recv()
                self.keep()

            if not self.begun:
                pl.when(jnp.logical_not(self.inner))(self.inward.wait_send)
            pl.when(jnp.logical_not(self.end))(self.outward.wait_send)


def finish_kernel(
    mesh, count, kv,
    gate_in, up_in, dwd, first, dqkv, attended, low, gains,
    out_gate, out_up, out_down, out_out, out_qkv, out_gains,
    tot_gate, tot_up, tot_down, tot_out, tot_qkv, term_gate, term_up, term_down, term_out, term_qkv, in_gate, in_up, in_down, in_out, in_qkv,
    first_both, attended_both, low_both, dq_both, w_out_part, w_qkv_part,
    swap_out, land_out, swap_qkv, land_qkv, gain_terms, gain_lands, *rest,
):
    parts, (send_sems, recv_sems, local_sems) = rest[:-3], rest[-3:]
    links = Links(mesh, send_sems, recv_sems, local_sems)
    ns, na = links.ns, links.na
    chips, per = 2 * na, ns // 2
    core = links.core
    rows, width = first.shape
    q_width = dqkv.shape[3]
    middle = width // 2

    def lines(term, inbox, total, out, pieces, begun=False):
        size = term.shape[1] // pieces
        every = slice(None)
        made = []
        for i in range(pieces):
            at = slice(i * size, (i + 1) * size)
            refs = [(ref, *where, every, at) for ref, *where in ((term,), (inbox, 0), (inbox, 1), (total,), (out,))]
            made.append(LineSum(links, *refs, begun and i == 0))
        return made

    gate_lines = lines(term_gate, in_gate, tot_gate, out_gate, GATE_PIECES, first_piece(ns, term_gate.shape[1]) > 0)
    up_lines = lines(term_up, in_up, tot_up, out_up, 4)
    down_lines = lines(term_down, in_down, tot_down, out_down, 4)
    out_lines = lines(term_out, in_out, tot_out, out_out, 2)
    qkv_lines = lines(term_qkv, in_qkv, tot_qkv, out_qkv, 4)
    term_loads = []
    for source, some in ((gate_in, gate_lines), (up_in, up_lines)):
        for line in some:
            term_loads.append(links.local((source, *line.term[1:]), line.term))
    for load in term_loads:
        load.start()
    links.barrier()
    for load, line in zip(term_loads, gate_lines + up_lines):
        load.wait()
        line.begin()

    sends = [
        links.copy((dqkv, pl.ds((1 - core) * per, per)), (dq_both, 1), links.at_core()),
        links.copy((low, slice(None), rows_at(1 - core, middle)), (low_both, 1), links.at_core()),
        links.copy(first, (first_both, 1), links.at_core()),
        links.copy(attended, (attended_both, 1), links.at_core()),
    ]
    loads = [
        links.local((low, slice(None), rows_at(core, middle)), (low_both, 0)),
        links.local(attended, (attended_both, 0)),
        links.local(first, (first_both, 0)),
        links.local((dqkv, pl.ds(core * per, per)), (dq_both, 0)),
    ]
    for copies in loads + sends[1:2] + sends[3:4] + sends[2:3] + sends[:1]:
        copies.start()

    down_rows = dwd.shape[0] // chips
    block = width // chips

    def pair(source, row_count, at, staged):
        made = []
        cut = source.shape[1] // 2
        for n, b_first in enumerate((True, False)):
            columns = slice(0, cut) if b_first else slice(cut, 2 * cut)
            partial = lambda k, columns=columns: (source, rows_at(k, row_count), columns)
            refs = parts[at[n] : at[n + 1]]
            made.append(ChipSum(links, partial, b_first, *(refs if staged else (*refs[:2], None))))
        return made

    down = pair(dwd, down_rows, (0, 3, 6), True)
    for item in down:
        item.start()
        item.load()

    gain_copies = [links.copy((gain_terms, 0), (gain_lands, 0), links.at_core()), links.copy((gain_terms, 1), (gain_lands, 1), links.at_b())]
    gain_copies += [links.copy((gain_terms, 2), (gain_lands, 1 + d), links.at_a(d)) for d in range(1, na)]
    gain_line = LineSum(links, (gain_terms, 3), (gain_lands, na + 1), (gain_lands, na + 2), out_gains)
    gain_terms[0] = gains[...]
    gain_copies[0].start()

    def next_gain(i):
        for copies in gain_copies[i : i + 1] if i < 2 else gain_copies[2:]:
            copies.wait()
        if i < 2:
            gain_terms[i + 1] = gain_terms[i] + gain_lands[i]
            for copies in gain_copies[1:2] if i == 0 else gain_copies[2:]:
                copies.start()
        else:
            total = gain_terms[2]
            for d in range(1, na):
                total = total + gain_lands[1 + d]
            gain_terms[3] = total
            gain_line.begin()

    def qkv_part(p):
        columns = slice(p * q_width, (p + 1) * q_width)
        mine, other = dq_both[0, p].reshape(rows, q_width), dq_both[1, p].reshape(rows, q_width)
        for k in range(chips):
            at = slice(k * block, (k + 1) * block)
            total = tn_dot(first_both[0, :, at], mine) + tn_dot(first_both[1, :, at], other)
            w_qkv_part[at, columns] = total.astype(BF16)

    def swap(sums, send, land):
        local = block // 2
        for n, item in enumerate(sums):
            total = item.finish()
            size = total.shape[1]
            send[0, :, n * size : (n + 1) * size] = total[:local]
            send[1, :, n * size : (n + 1) * size] = total[local:]
        copies = links.copy((send, 1 - core), land, links.at_core())
        copies.start()
        return copies

    out_sums = pair(w_out_part, block, (6, 8, 10), False)
    qkv_sums = pair(w_qkv_part, block, (10, 12, 14), False)
    cut = width // 2
    next_gain(0)
    for i in (1, 3):
        sends[i].wait()
    for i in (0, 1):
        loads[i].wait()
    gate_lines[0].relay()
    for k in range(chips):
        at = slice(k * block, (k + 1) * block)
        total = tn_dot(attended_both[0, :, at], low_both[0]) + tn_dot(attended_both[1, :, at], low_both[1])
        w_out_part[at, :] = total.astype(BF16)
    for item in out_sums:
        item.start()
    gate_lines[1].relay()
    next_gain(1)
    for i in (0, 2):
        sends[i].wait()
    for i in (2, 3):
        loads[i].wait()
    gate_lines[0].settle()
    for p in range(per // 2):
        qkv_part(p)
    gate_lines[2].relay()
    next_gain(2)
    gate_lines[1].settle()
    for p in range(per // 2, per):
        qkv_part(p)
    gate_lines[3].relay()
    for item in down:
        item.turn()
    for item in qkv_sums:
        item.start()
    gate_lines[2].settle()
    gain_line.relay()
    up_lines[0].relay()
    gate_lines[3].settle()
    for item in out_sums:
        item.turn()
    up_lines[1].relay()
    up_lines[0].settle()
    gain_line.settle()
    up_lines[2].relay()
    up_lines[1].settle()
    term_down[:, :cut] = down[0].finish()
    term_down[:, cut:] = down[1].finish()
    for line in down_lines:
        line.begin()
    up_lines[3].relay()
    up_lines[2].settle()
    down_lines[0].relay()
    up_lines[3].settle()
    for item in qkv_sums:
        item.turn()
    down_lines[1].relay()
    down_lines[0].settle()
    out_swap = swap(out_sums, swap_out, land_out)
    down_lines[2].relay()
    down_lines[1].settle()
    out_swap.wait()
    kept, arrived = swap_out[core], land_out[...]
    term_out[:, :cut] = jnp.where(core == 0, kept, arrived)
    term_out[:, cut:] = jnp.where(core == 0, arrived, kept)
    for line in out_lines:
        line.begin()
    down_lines[3].relay()
    down_lines[2].settle()
    qkv_swap = swap(qkv_sums, swap_qkv, land_qkv)
    out_lines[0].relay()
    down_lines[3].settle()
    qkv_swap.wait()
    kept, arrived = swap_qkv[core], land_qkv[...]
    for n in range(2):
        group = jnp.where(core == n, kept, arrived)
        for p in range(per):
            taken, start = p * q_width, 0
            for size in (kv * GROUP * HEAD_DIM, kv * HEAD_DIM, kv * HEAD_DIM):
                at = start + (n * per + p) * size
                term_qkv[:, at : at + size] = group[:, taken : taken + size]
                taken, start = taken + size, start + ns * size
    for line in qkv_lines:
        line.begin()
    out_lines[1].relay()
    out_lines[0].settle()
    qkv_lines[0].relay()
    out_lines[1].settle()
    for n in range(1, len(qkv_lines)):
        qkv_lines[n].relay()
        qkv_lines[n - 1].settle()
    qkv_lines[-1].settle()
    every_line = [*gate_lines, *up_lines, gain_line, *down_lines, *out_lines, *qkv_lines]
    for line in every_line:
        line.finish()
    for line in every_line:
        if line.store is not None:
            line.store.wait()


def finish(mesh, count, kv, term_gate, term_up, dwd, first, dqkv, attended, low, gains):
    ns, nf = mesh
    na, per = nf // 4, ns // 2
    rows, width = first.shape
    q_width = dqkv.shape[3]
    local, half = term_gate.shape[0], width // 2
    block = 2 * local
    anywhere, vmem = pl.BlockSpec(memory_space=pl.ANY), pl.BlockSpec(memory_space=pltpu.VMEM)
    down = (dwd.shape[0] // (2 * na), dwd.shape[1])
    shapes = [term_gate.shape, term_up.shape, down, (local, width), (local, ns * q_width)]
    scratch = [pltpu.VMEM(s, BF16) for s in shapes]
    scratch += [pltpu.VMEM(s, BF16) for s in shapes]
    scratch += [pltpu.VMEM((2,) + tuple(s), BF16) for s in shapes]
    scratch += [
        pltpu.VMEM((2, rows, width), BF16),
        pltpu.VMEM((2, rows, width), BF16),
        pltpu.VMEM((2, rows, half), BF16),
        pltpu.VMEM((2, per, count, rows // count, q_width), BF16),
        pltpu.VMEM((width, half), BF16),
        pltpu.VMEM((width, per * q_width), BF16),
        pltpu.VMEM((2, local, half), BF16),
        pltpu.VMEM((local, half), BF16),
        pltpu.VMEM((2, local, per * q_width), BF16),
        pltpu.VMEM((local, per * q_width), BF16),
        pltpu.VMEM((4, 2, width), F32),
        pltpu.VMEM((na + 3, 2, width), F32),
    ]
    scratch += chip_sum_shapes(na, True, down[0], down[1] // 2) + chip_sum_shapes(na, False, down[0], down[1] // 2)
    for columns in (half // 2, per * q_width // 2):
        for b_first in (True, False):
            scratch += chip_sum_shapes(na, b_first, block, columns)[:2]
    return pl.pallas_call(
        functools.partial(finish_kernel, mesh, count, kv),
        in_specs=[anywhere] * 7 + [vmem],
        out_specs=[anywhere] * 5 + [vmem],
        out_shape=[jax.ShapeDtypeStruct(s, BF16) for s in shapes] + [jax.ShapeDtypeStruct((2, width), F32)],
        scratch_shapes=scratch
        + [pltpu.SemaphoreType.DMA((128,)), pltpu.SemaphoreType.DMA((128,)), pltpu.SemaphoreType.DMA((64,))],
        compiler_params=pltpu.CompilerParams(vmem_limit_bytes=VMEM_MOST, collective_id=2, has_side_effects=True),
        name="finish",
    )(term_gate, term_up, dwd, first, dqkv, attended, low, gains)


def widen_kernel(cuts, *refs):
    gate, up, down, out, qkv, hidden, own, other = refs[:8]
    o_gate, o_up, o_down, o_out, o_q, o_k, o_v, o_block = refs[8:]
    for source, target in ((gate, o_gate), (up, o_up), (down, o_down), (out, o_out)):
        target[...] = source[...].astype(F32)
    for (start, end), target in zip(cuts, (o_q, o_k, o_v)):
        target[...] = qkv[:, start:end].astype(F32)
    o_block[...] = hidden[...] + own[...] + other[...].astype(F32)


def widen(gate, up, down, out, qkv, hidden, own, other, cuts):
    steps = 4
    operands = [gate, up, down, out, qkv, hidden, own, other]
    rows = out.shape[0]
    shapes = [gate.shape, up.shape, down.shape, out.shape] + [(rows, end - start) for start, end in cuts] + [hidden.shape]
    block = lambda shape: pl.BlockSpec((shape[0] // steps, shape[1]), lambda i: (i, 0))
    return pl.pallas_call(
        functools.partial(widen_kernel, cuts),
        grid=(steps,),
        in_specs=[block(x.shape) for x in operands],
        out_specs=[block(shape) for shape in shapes],
        out_shape=[jax.ShapeDtypeStruct(shape, F32) for shape in shapes],
        compiler_params=pltpu.CompilerParams(vmem_limit_bytes=VMEM_LIMIT),
        cost_estimate=pl.CostEstimate(flops=0, bytes_accessed=40 * rows * gate.shape[1], transcendentals=0),
        name="widen",
    )(*operands)


def solution(mesh):
    ns, nf = mesh.shape["seq"], mesh.shape["fsdp"]
    na = nf // 4
    chips = 2 * na
    kv = KEY_VALUE_HEADS // ns

    def body(tokens, cotangent, attention_gain, feedforward_gain, query_weight, key_matrix, value_matrix, out_weight, gate_weight, up_weight, down_weight):
        count, span, width = tokens.shape
        rows = count * span
        local = query_weight.shape[0]
        sizes = (ns, nf)
        mine = lax.axis_index("fsdp")
        cosines, sines = (jnp.asarray(x) for x in rope_tables(ns * span))
        flat = tokens.reshape(rows, width)
        grad_flat = cotangent.reshape(rows, width)
        (w_qkv, w_out, w_gate, w_down, first, packed, heads_attended, logs, attended, hidden_one, second_both, low_both, gains) = fore(
            sizes, count, kv, flat, grad_flat, jnp.stack([attention_gain, feedforward_gain]),
            query_weight, key_matrix, value_matrix, out_weight, gate_weight, down_weight, cosines, sines,
        )
        dwg, dwu, dwd, out_own, out_arrived, dx_own, dx_arrived = ffn(sizes, second_both, low_both, w_gate, w_down, up_weight, gate_weight)
        high, low, grad_tokens, gain_grads, dqkv, sum_gate, sum_up = back(
            sizes, count, kv, dx_own, dx_arrived, hidden_one, grad_flat, gains, w_out, w_qkv,
            packed, heads_attended, logs, cosines, sines, flat, dwg, dwu,
        )
        *sums, gain_grads = finish(
            sizes, count, kv, sum_gate, sum_up, dwd, first, dqkv, attended, low, gain_grads
        )
        q_end, k_end = ns * kv * GROUP * HEAD_DIM, ns * kv * (GROUP + 1) * HEAD_DIM
        cuts = ((0, q_end), (q_end, k_end), (k_end, sums[4].shape[1]))
        grad_gate, grad_up, grad_down, grad_out, grad_query, grad_key, grad_value, block_out = widen(
            *sums, hidden_one, out_own, out_arrived, cuts
        )
        gain_grads = lax.dynamic_slice(gain_grads, (0, mine * local), (2, local))

        return (
            block_out.reshape(count, span, width),
            grad_tokens.reshape(count, span, width),
            gain_grads[0],
            gain_grads[1],
            grad_query,
            grad_key,
            grad_value,
            grad_out,
            grad_gate,
            grad_up,
            grad_down,
        )

    tokens_spec, gain_spec, weight_spec = P("fsdp", "seq", None), P("fsdp"), P("fsdp", None)
    return jax.shard_map(
        body,
        mesh=mesh,
        in_specs=(tokens_spec, tokens_spec, gain_spec, gain_spec) + (weight_spec,) * 7,
        out_specs=(tokens_spec, tokens_spec, gain_spec, gain_spec) + (weight_spec,) * 7,
        check_vma=False,
    )
```

```python
import functools
import math

import jax
import jax.numpy as jnp
import numpy as np
from jax import lax
from jax.experimental import pallas as pl
from jax.experimental.pallas import tpu as pltpu
from jax.sharding import PartitionSpec as P

QUERY_HEADS = 16
KEY_VALUE_HEADS = 8
HEAD_DIM = 96
GROUP = QUERY_HEADS // KEY_VALUE_HEADS
norm_eps = 1e-05
rope_base = 100000.0
masked_score = -1e30
F32, BF16 = jnp.float32, jnp.bfloat16
VMEM_LIMIT = 60 * 1024 * 1024
VMEM_MOST = 67043328
MESH = pl.DeviceIdType.MESH


def nt_dot(left, right):
    return lax.dot_general(left, right, (((1,), (1,)), ((), ())), preferred_element_type=F32)


def tn_dot(left, right):
    return lax.dot_general(left, right, (((0,), (0,)), ((), ())), preferred_element_type=F32)


def nn_dot(left, right):
    return jnp.dot(left, right, preferred_element_type=F32)


def whole(shape):
    return pl.BlockSpec(shape, lambda *_: (0,) * len(shape))


def call(kernel, scalars, operands, outs, name, flops, moved, scratch=()):
    return pl.pallas_call(
        kernel,
        grid_spec=pltpu.PrefetchScalarGridSpec(
            num_scalar_prefetch=1,
            grid=(1,),
            in_specs=[whole(x.shape) for x in operands],
            out_specs=[whole(x.shape) for x in outs],
            scratch_shapes=scratch,
        ),
        out_shape=outs,
        compiler_params=pltpu.CompilerParams(vmem_limit_bytes=VMEM_LIMIT),
        cost_estimate=pl.CostEstimate(flops=flops, bytes_accessed=moved, transcendentals=0),
        name=name,
    )(scalars, *operands)


def rope_tables(length):
    half = HEAD_DIM // 2
    freqs = np.float32(rope_base) ** (-(np.float32(2.0) * np.arange(half, dtype=np.float32)) / np.float32(HEAD_DIM))
    angles = np.arange(length, dtype=np.float32)[:, None] * freqs.astype(np.float32)[None, :]
    cosine, sine = np.cos(angles), np.sin(angles)
    return np.concatenate([cosine, cosine], 1), np.concatenate([-sine, sine], 1)


def swap_halves(values):
    half = HEAD_DIM // 2
    width = values.shape[1]
    lane = lax.broadcasted_iota(jnp.int32, values.shape, 1)
    ahead = pltpu.roll(values, width - half, 1)
    behind = pltpu.roll(values, half, 1)
    return jnp.where(lane % HEAD_DIM < half, ahead, behind)


def norm_back(grad, normed, inverse, gain):
    scaled = grad * gain
    return inverse * (scaled - normed * jnp.mean(scaled * normed, axis=1, keepdims=True))


def ffn_kernel(
    mesh, tiles, parts, x, g, wg, wd, wu, w_last, dwg, dwu, dwd, out_own, out_arrived, dx_own, dx_arrived,
    xt, acc_out, acc_dx, given_out, given_dx, act, dgate, dup, stage, land, gate, send_sems, recv_sems, local_sems,
):
    step = pl.program_id(0)
    rows = x.shape[0] // 2
    links = Links(mesh, send_sems, recv_sems, local_sems)
    chips, local, tile = tiles // parts, wu.shape[0], land.shape[2]
    cols = tile // parts
    gathers, loads, first = [], [], []
    every = slice(None)
    for r in range(parts):
        here = slice(r * cols, (r + 1) * cols)
        first.append(GatherHalf(links, lambda c, here=here: (stage, c, 0, every, here), lambda o, here=here: (land, 0, rows_at(o, local), here)))
    for k in range(chips + 1):
        if k > 0:
            gathers.append(GatherHalf(links, lambda c, k=k: (stage, c, k), lambda o, k=k: (land, k, rows_at(o, local))))
        else:
            gathers.append(None)
        weight, tile_at = (wu, k) if k < chips else (w_last, chips - 1)
        for c in range(2):
            source = (weight, every, slice((tile_at * 2 + c) * tile, (tile_at * 2 + c + 1) * tile))
            loads.append(links.local(source, (stage, c, k)))

    def begin(k):
        gathers[k].start()
        gathers[k].other_start()

    def turn(k):
        gathers[k].turn()
        gathers[k].turn_late()

    @pl.when(step == 0)
    def _():
        for load in loads:
            load.start()
        links.barrier()
        for load in loads[:2]:
            load.wait()
        first[0].start()
        first[0].other_start()
        for load in loads[2:]:
            load.wait()

    @pl.when(step == 0)
    def _():
        acc_out[...] = jnp.zeros_like(acc_out)
        acc_dx[...] = jnp.zeros_like(acc_dx)
        xt[...] = x[...].T

    def first_part():
        first[0].turn()
        first[0].turn_late()
        for n in range(1, parts):
            first[n].start()
            first[n].other_start()
        first[0].finish()

    def second_part():
        for n in range(1, parts):
            first[n].turn()
            first[n].turn_late()
        begin(1)

    def third_part():
        for n in range(1, parts):
            first[n].finish()

    def later_part(k):
        turn(k)
        for n in (2, 3) if k == 1 else (k + 2,):
            if n <= chips:
                begin(n)
        if k == chips - 1:
            turn(chips)

    for k in range(1, chips):
        if k > 1:
            pl.when(step == (k - 1) * parts + 1)(functools.partial(later_part, k))
    pl.when(step == (chips - 1) * parts)(gathers[chips].finish)
    at = pl.ds(pl.multiple_of(lax.rem(step, parts) * cols, cols), cols)
    chip = step // parts

    @pl.when(chip < chips - 1)
    def _():
        gate[...] = wg[...]

    @pl.when(chip == chips - 1)
    def _():
        gate[...] = land[chips, :, at]

    pl.when(step == 0)(first_part)
    pl.when(step == 1)(third_part)
    for k in range(1, chips):
        pl.when(step == k * parts)(gathers[k].finish)
    for i in range(2):
        here = slice(i * rows, (i + 1) * rows)
        if i == 1:
            pl.when(step == 0)(second_part)
            pl.when(step == 1)(functools.partial(later_part, 1))
        gate_pre = nn_dot(x[here, :], gate[...])
        up = nn_dot(x[here, :], land[chip, :, at])
        grad = nt_dot(g[here, :], wd[...])
        sigmoid = jax.nn.sigmoid(gate_pre)
        silu = gate_pre * sigmoid
        hidden = (silu * up).astype(BF16)
        act[here, :] = hidden
        gate_grad = (grad * up * sigmoid * (1.0 + gate_pre * (1.0 - sigmoid))).astype(BF16)
        up_grad = (grad * silu).astype(BF16)
        dgate[here, :] = gate_grad
        dup[here, :] = up_grad
        acc_out[i] += nn_dot(hidden, wd[...])
        acc_dx[i] += nt_dot(gate_grad, gate[...]) + nt_dot(up_grad, land[chip, :, at])
    leaving = [
        links.copy(given_dx, dx_arrived, links.at_core()),
        links.local((acc_dx, 0), dx_own),
        links.copy(given_out, out_arrived, links.at_core()),
        links.local((acc_out, 0), out_own),
    ]

    @pl.when(step == tiles - 1)
    def _():
        given_dx[...] = acc_dx[1].astype(BF16)
        leaving[0].start()
        given_out[...] = acc_out[1].astype(BF16)
        for copies in leaving[1:]:
            copies.start()

    dwg[...] = nn_dot(xt[...], dgate[...]).astype(BF16)
    dwu[...] = nn_dot(xt[...], dup[...]).astype(BF16)
    dwd[...] = tn_dot(act[...], g[...]).astype(BF16)

    @pl.when(step == tiles - 1)
    def _():
        for copies in leaving:
            copies.wait()


def ffn(mesh, x, g, wg, wd, wu, w_last):
    rows, width = x.shape[0] // 2, x.shape[1]
    chips, tile = wg.shape[0] + 1, wg.shape[2]
    parts = 2
    tiles, cols = chips * parts, tile // parts
    local = wu.shape[0]
    keep = lambda shape: pl.BlockSpec(shape, lambda i: (0, 0), pipeline_mode=pl.Buffered(1))
    half = tile * chips
    wide, low = jax.ShapeDtypeStruct((rows, width), F32), jax.ShapeDtypeStruct((rows, width), BF16)
    return pl.pallas_call(
        functools.partial(ffn_kernel, mesh, tiles, parts),
        grid=(tiles,),
        in_specs=[
            keep(x.shape),
            keep(g.shape),
            pl.BlockSpec((None, width, cols), lambda i: (jnp.minimum(i // parts, chips - 2), 0, i % parts)),
            pl.BlockSpec((cols, width), lambda i: (i, 0)),
            pl.BlockSpec(memory_space=pl.ANY),
            pl.BlockSpec(memory_space=pl.ANY),
        ],
        out_specs=[pl.BlockSpec((width, cols), lambda i: (0, i))] * 2
        + [pl.BlockSpec((cols, width), lambda i: (i, 0))]
        + [pl.BlockSpec(memory_space=pl.ANY)] * 4,
        scratch_shapes=[pltpu.VMEM((width, 2 * rows), BF16)]
        + [pltpu.VMEM((2, rows, width), F32)] * 2
        + [pltpu.VMEM((rows, width), BF16)] * 2
        + [pltpu.VMEM((2 * rows, cols), BF16)] * 3
        + [pltpu.VMEM((2, chips + 1, local, tile), BF16), pltpu.VMEM((chips + 1, width, tile), BF16), pltpu.VMEM((width, cols), BF16)]
        + [pltpu.SemaphoreType.DMA((96,)), pltpu.SemaphoreType.DMA((96,)), pltpu.SemaphoreType.DMA((64,))],
        out_shape=[
            jax.ShapeDtypeStruct((width, half), BF16),
            jax.ShapeDtypeStruct((width, half), BF16),
            jax.ShapeDtypeStruct((half, width), BF16),
            wide,
            low,
            wide,
            low,
        ],
        compiler_params=pltpu.CompilerParams(vmem_limit_bytes=VMEM_MOST, collective_id=3, has_side_effects=True),
        cost_estimate=pl.CostEstimate(
            flops=36 * rows * width * half, bytes_accessed=12 * width * half + 20 * rows * width, transcendentals=0
        ),
        name="ffn",
    )(x, g, wg, wd, wu, w_last)


def part(x):
    return x[0].at[x[1:]] if isinstance(x, tuple) else x


def get(x):
    return x[0][x[1:]] if isinstance(x, tuple) else x[...]


def put(x, value):
    if isinstance(x, tuple):
        x[0][x[1:]] = value
    else:
        x[...] = value


class Copy:
    def __init__(self, src, dst, device, send_sem, recv_sem):
        self.src, self.dst, self.device, self.send_sem, self.recv_sem = src, dst, device, send_sem, recv_sem

    def made(self):
        if self.device is None:
            return pltpu.make_async_copy(part(self.src), part(self.dst), part(self.send_sem))
        return pltpu.make_async_remote_copy(
            src_ref=part(self.src),
            dst_ref=part(self.dst),
            send_sem=part(self.send_sem),
            recv_sem=part(self.recv_sem),
            device_id=self.device,
            device_id_type=MESH,
        )

    def start(self):
        self.made().start()

    def wait(self):
        self.made().wait()

    def wait_send(self):
        self.made().wait_send()

    def wait_recv(self):
        self.made().wait_recv()


class Links:
    def __init__(self, mesh, send_sems, recv_sems, local_sems):
        self.ns, self.nf = mesh
        self.na = self.nf // 4
        self.send_sems, self.recv_sems, self.local_sems = send_sems, recv_sems, local_sems
        self.count, self.local_count = 0, 0
        self.z, self.f = lax.axis_index("seq"), lax.axis_index("fsdp")
        self.core = lax.rem(self.f, 2)
        self.b = lax.rem(self.f // 2, 2)
        self.a = self.f // 4

    def chip(self, da, db):
        return lax.rem(self.a + da, self.na) * 2 + lax.rem(self.b + db, 2)

    def at_core(self):
        return (self.z, self.f + 1 - 2 * self.core)

    def at_b(self):
        return (self.z, self.f + 2 - 4 * self.b)

    def at_a(self, d):
        return (self.z, lax.rem(self.f + 4 * d, self.nf))

    def at_z(self, d):
        return (lax.rem(self.z + d, self.ns), self.f)

    def peers(self):
        return [self.at_core(), self.at_b()] + [self.at_a(d) for d in range(1, self.na)] + [self.at_z(d) for d in range(1, self.ns)]

    def barrier(self):
        barrier = pltpu.get_barrier_semaphore()
        peers = self.peers()
        for peer in peers:
            pl.semaphore_signal(barrier, inc=1, device_id=peer, device_id_type=MESH)
        pl.semaphore_wait(barrier, len(peers))

    def copy(self, src, dst, device):
        index = self.count
        self.count += 1
        return Copy(src, dst, device, (self.send_sems, index), (self.recv_sems, index))

    def again(self, src, dst, device):
        index = self.count - 1
        return Copy(src, dst, device, (self.send_sems, index), (self.recv_sems, index))

    def local(self, src, dst):
        index = self.local_count
        self.local_count += 1
        return Copy(src, dst, None, (self.local_sems, index), None)


def line_place(links):
    z, ns = links.z, links.ns
    middle = ns // 2
    step = jnp.where(z < middle, 1, -1)
    end = (z == 0) | (z == ns - 1)
    inner = (z == middle - 1) | (z == middle)
    return end, inner, (z + step, links.f), (z - step, links.f)


GATE_PIECES = 4


def first_piece(ns, columns):
    return columns // GATE_PIECES if ns == 4 else 0


def rows_at(start, size):
    return pl.ds(pl.multiple_of(start * size, size), size)


class ChipSum:
    def __init__(self, links, partial, b_first, arrived, passed, staging):
        self.links, self.partial, self.b_first = links, partial, b_first
        self.arrived, self.passed, self.staging = arrived, passed, staging
        na = links.na
        self.first, self.second = [], []
        if b_first:
            self.kept = [links.chip(da, 0) for da in range(na)]
            for da in range(na):
                self.first.append(links.copy(partial(links.chip(da, 1)), (arrived, da), links.at_b()))
            for d in range(1, na):
                self.second.append(links.copy((arrived, d), (passed, d - 1), links.at_a(d)))
        else:
            self.kept = [links.chip(0, db) for db in range(2)]
            for d in range(1, na):
                for db in range(2):
                    self.first.append(links.copy(partial(links.chip(d, db)), (arrived, (d - 1) * 2 + db), links.at_a(d)))
            self.second.append(links.copy((arrived, 1), (passed, 0), links.at_b()))
        self.loads = [] if staging is None else [links.local(partial(k), (staging, i)) for i, k in enumerate(self.kept)]

    def start(self):
        for copy in self.first:
            copy.start()

    def load(self):
        for load in self.loads:
            load.start()

    def turn(self):
        for load in self.loads:
            load.wait()
        for copy in self.first:
            copy.wait()
        count = len(self.kept)
        for i in [*range(1, count), 0]:
            own = self.partial(self.kept[i]) if self.staging is None else (self.staging, i)
            total = get(own).astype(F32)
            if self.b_first:
                total = total + self.arrived[i].astype(F32)
            else:
                for d in range(self.links.na - 1):
                    total = total + self.arrived[d * 2 + i].astype(F32)
            self.arrived[i] = total.astype(BF16)
            if i > 0 and self.b_first:
                self.second[i - 1].start()
            elif i > 0:
                self.second[0].start()

    def finish(self):
        for copy in self.second:
            copy.wait()
        total = self.arrived[0].astype(F32)
        for i in range(len(self.second)):
            total = total + self.passed[i].astype(F32)
        return total.astype(BF16)


def chip_sum_shapes(na, b_first, rows, columns):
    first = na if b_first else 2 * (na - 1)
    kept = na if b_first else 2
    return [
        pltpu.VMEM((max(first, kept), rows, columns), BF16),
        pltpu.VMEM((na - 1 if b_first else 1, rows, columns), BF16),
        pltpu.VMEM((kept, rows, columns), BF16),
    ]


def flip_core(f):
    return f + 1 - 2 * lax.rem(f, 2)


def flip_b(f):
    return f + 2 - 4 * lax.rem(f // 2, 2)


class Gather:
    def __init__(self, links, own, land, both):
        self.links = links
        f, na, nf = links.f, links.na, links.nf
        to_core, to_b = links.at_core(), links.at_b()

        def move(origin, device, half=None):
            return links.copy(land(origin, half), land(origin, half), device)

        self.given = [links.copy(own, land(f, None), to_core)] if both else []
        self.own = [links.copy(own, land(f, None), to_b)]
        self.own += [links.copy(own, land(f, None), links.at_a(d)) for d in range(1, na)]
        from_b = flip_b(f)
        from_a = [lax.rem(f + nf - 4 * d, nf) for d in range(1, na)]
        if na == 2:
            self.relays = [move(from_b, links.at_a(1), 1), move(from_a[0], to_b, 0)]
            far = [(flip_b(from_a[0]), 0), (flip_b(from_a[0]), 1)]
        else:
            self.relays = [move(origin, to_b) for origin in from_a]
            far = [(flip_b(origin), None) for origin in from_a]
        near = [from_b, *from_a]
        self.near = [move(origin, to_core) for origin in near] if both else []
        self.far = [move(origin, to_core, half) for origin, half in far] if both else []

    def start(self):
        for copies in self.own + self.given:
            copies.start()

    def turn(self):
        for copies in self.own:
            copies.wait()
        for copies in self.relays + self.near:
            copies.start()

    def pass_on(self):
        for copies in self.relays:
            copies.wait()
        for copies in self.far:
            copies.start()

    def finish(self):
        for copies in self.given + self.near + self.far:
            copies.wait()


class GatherHalf:
    def __init__(self, links, stage, land):
        self.links = links
        f, na, nf, core = links.f, links.na, links.nf, links.core
        to_b = links.at_b()

        def move(origin, device):
            return links.copy(land(origin), land(origin), device)

        self.swap = links.copy(stage(1 - core), land(f), links.at_core())
        self.kept = links.local(stage(core), land(f))
        targets = [to_b] + [links.at_a(d) for d in range(1, na)]
        self.own = [links.copy(stage(core), land(f), device) for device in targets]
        self.other = [move(flip_core(f), device) for device in targets]
        from_b = flip_b(f)
        from_a = [lax.rem(f + nf - 4 * d, nf) for d in range(1, na)]
        if na == 2:
            self.relays = [move(from_b, links.at_a(1))]
            self.late = [move(flip_core(from_a[0]), to_b)]
        else:
            self.relays = [move(origin, to_b) for origin in from_a]
            self.late = [move(flip_core(origin), to_b) for origin in from_a]

    def start(self):
        for copies in [self.swap, self.kept, *self.own]:
            copies.start()

    def other_start(self):
        self.swap.wait()
        for copies in self.other:
            copies.start()

    def turn(self):
        for copies in self.own:
            copies.wait()
        for copies in self.relays:
            copies.start()

    def turn_late(self):
        for copies in self.other:
            copies.wait()
        for copies in self.late:
            copies.start()

    def finish(self):
        for copies in [self.kept, *self.relays, *self.late]:
            copies.wait()


def attend_heads(ns, kv, span, qs, ks, vs, out, logs):
    scale = 1.0 / math.sqrt(HEAD_DIM)
    row = lax.broadcasted_iota(jnp.int32, (span, span), 0)
    column = lax.broadcasted_iota(jnp.int32, (span, span), 1)
    causal = row >= column
    lane = lax.broadcasted_iota(jnp.int32, (span, 128), 1)
    for s in range(ns):
        here = slice(s * span, (s + 1) * span)
        stats = jnp.zeros((span, 128), F32)
        for h in range(kv * GROUP):
            g = h // GROUP
            q = qs[h, here, :]
            near = jnp.where(causal, nt_dot(q, ks[g, here, :]) * scale, masked_score)
            top = jnp.max(near, axis=1, keepdims=True)
            if s > 0:
                far = nt_dot(q, ks[g, : s * span, :]) * scale
                top = jnp.maximum(top, jnp.max(far, axis=1, keepdims=True))
            near = jnp.exp(near - top)
            total = jnp.sum(near, axis=1, keepdims=True)
            if s > 0:
                far = jnp.exp(far - top)
                total = total + jnp.sum(far, axis=1, keepdims=True)
            inverse = 1.0 / total
            result = nn_dot((near * inverse).astype(BF16), vs[g, here, :])
            if s > 0:
                result = result + nn_dot((far * inverse).astype(BF16), vs[g, : s * span, :])
            stats = jnp.where(lane == h, top + jnp.log(total), stats)
            out[s, :, h * HEAD_DIM : (h + 1) * HEAD_DIM] = result.astype(BF16)
        logs[here, :] = stats


def fill_tables(cosines, sines, narrow_cosines, narrow_sines, heads):
    end = heads * HEAD_DIM
    cosines[:, end:] = jnp.ones((cosines.shape[0], cosines.shape[1] - end), F32)
    sines[:, end:] = jnp.zeros((cosines.shape[0], cosines.shape[1] - end), F32)
    for h in range(heads):
        at = slice(h * HEAD_DIM, (h + 1) * HEAD_DIM)
        cosines[:, at] = narrow_cosines
        sines[:, at] = narrow_sines


def fore_kernel(
    mesh, count, kv,
    tokens, cotangent, gains_in, wq, wk, wv, wo, wg, wd, narrow_cosines, narrow_sines,
    w_qkv, w_out, w_gate, w_down, first_out, packed, heads_attended, logs, attended_out, hidden_out, second_both, low_both, gains_out,
    rows_in, hidden, first, pack, w_land, wo_land, q_send, q_land, a_send, a_land, stage_gate, gain_send, gain_land,
    qs, ks, vs, log, attended, second, second_abs, low, cosines, sines, send_sems, recv_sems, local_sems,
):
    links = Links(mesh, send_sems, recv_sems, local_sems)
    ns, na, nf = links.ns, links.na, links.nf
    chips = 2 * na
    z, f, core = links.z, links.f, links.core
    rows, width = rows_in.shape
    span = rows // count
    heads = kv * GROUP
    g_width, k_width = heads * HEAD_DIM, kv * HEAD_DIM
    q_width = g_width + 2 * k_width
    local = width // nf
    links.barrier()

    token_load = links.local(tokens, rows_in)
    token_load.start()
    cot_load = links.local(cotangent, hidden)
    cot_load.start()
    gain_send[...] = jnp.zeros_like(gain_send)
    gain_send[0:2, :local] = gains_in[...].astype(F32)
    for j in range(ns):
        pack[j, :, :g_width] = wq[:, j * g_width : (j + 1) * g_width]
        pack[j, :, g_width : g_width + k_width] = wk[:, j * k_width : (j + 1) * k_width]
        pack[j, :, g_width + k_width :] = wv[:, j * k_width : (j + 1) * k_width]

    every = slice(None)

    def piece(start, size, half):
        if half is None:
            return rows_at(start, size)
        return rows_at(start * 2 + half, size // 2)

    units = []
    turns = [*range(1, ns), 0]
    for d in turns:
        g = lax.rem(z + d, ns)
        units.append(Gather(links, (pack, g), lambda o, half, g=g: (w_land, g, piece(o, local, half)), True))
    units.append(Gather(links, wo, lambda o, half: (wo_land, piece(o, local, half)), True))
    depth = wd.shape[0]
    units.append(Gather(links, wd, lambda o, half: (w_down, piece(o // 2, depth, half)), False))
    gate_unit = GatherHalf(links, lambda c: (stage_gate, c), lambda o: (w_gate, every, rows_at(o, local)))
    q_copies, a_copies = [], []
    for d in range(1, ns):
        g = lax.rem(z + d, ns)
        q_copies.append([links.copy((q_send, g, i), (q_land, i, z), links.at_z(d)) for i in range(count)])
    for i in range(count):
        a_copies.append([links.copy((a_send, i, lax.rem(z + d, ns)), (a_land, i, z), links.at_z(d)) for d in range(1, ns)])
    second_copy = links.copy(second_abs, (second_both, pl.ds(rows, rows)), links.at_core())
    low_copy = links.copy(low, (low_both, pl.ds(rows, rows)), links.at_core())

    def gain_at(start, size):
        return (gain_land, pl.ds(start, size))

    pair, chip_four = f // 2 * 2, f // 4 * 4
    gain_copies = [
        [links.copy(gain_at(f, 1), gain_at(f, 1), links.at_core())],
        [links.copy(gain_at(pair, 2), gain_at(pair, 2), links.at_b())],
        [links.copy(gain_at(chip_four, 4), gain_at(chip_four, 4), links.at_a(d)) for d in range(1, na)],
    ]
    stores = []

    def store(src, dst):
        copies = links.local(src, dst)
        copies.start()
        stores.append(copies)

    gain_land[f] = gain_send[...]
    for copies in gain_copies[0]:
        copies.start()
    units[0].start()
    units[1].start()
    for j in range(ns):
        w_land[j, rows_at(f, local), :] = pack[j]
    stage_loads = []
    tile = w_gate.shape[2]
    for c in range(2):
        for k in range(chips - 1):
            source = (wg, every, slice((k * 2 + c) * tile, (k * 2 + c + 1) * tile))
            stage_loads.append(links.local(source, (stage_gate, c, k)))
    for load in stage_loads:
        load.start()
    store_own = [links.local(wo, (wo_land, rows_at(f, local))), links.local(wd, (w_down, rows_at(f // 2, depth)))]
    for copies in store_own:
        copies.start()
    fill_tables(cosines, sines, narrow_cosines[rows_at(z, span), :], narrow_sines[rows_at(z, span), :], heads + kv)
    token_load.wait()
    old = rows_in[...]
    inverse = lax.rsqrt(jnp.mean(old * old, axis=1, keepdims=True) + norm_eps)
    for stage in range(3):
        for copies in gain_copies[stage]:
            copies.wait()
        if stage < 2:
            for copies in gain_copies[stage + 1]:
                copies.start()
    for j in range(nf):
        gains_out[:, j * local : (j + 1) * local] = gain_land[j, 0:2, :local]
    first[...] = (old * inverse * gains_out[0:1, :]).astype(BF16)
    store(first, first_out)

    def project(n):
        g = lax.rem(z + turns[n], ns)
        units[n].finish()
        y = nn_dot(first[...], w_land[g])
        for i in range(count):
            part = y[i * span : (i + 1) * span]
            part = (part * cosines[...] + swap_halves(part) * sines[...]).astype(BF16)
            if turns[n] == 0:
                q_land[i, z] = part
            else:
                q_send[g, i] = part
        if turns[n] > 0:
            q_copies[turns[n] - 1][0].start()
        if n > 0 and turns[n - 1] > 0:
            for copies in q_copies[turns[n - 1] - 1][1:]:
                copies.start()
        store((w_land, g), (w_qkv, g))

    last = len(units)
    for n in range(ns):
        units[n].turn()
        if n + 2 < last:
            units[n + 2].start()
        if n > 0:
            units[n - 1].pass_on()
        if n > 1:
            project(n - 2)
    units[ns].turn()
    for load in stage_loads:
        load.wait()
    gate_unit.start()
    units[ns - 1].pass_on()
    project(ns - 2)
    gate_unit.other_start()
    project(ns - 1)
    units[ns].pass_on()
    cot_load.wait()
    low[...] = hidden[...].astype(BF16)
    low_copy.start()
    store(low, (low_both, pl.ds(0, rows)))

    def attend(i):
        for copies in q_copies:
            copies[i].wait()
        for j in range(ns):
            at = slice(j * span, (j + 1) * span)
            for h in range(heads):
                qs[h, at, :] = q_land[i, j, :, h * HEAD_DIM : (h + 1) * HEAD_DIM]
            for h in range(kv):
                k0, v0 = (heads + h) * HEAD_DIM, (heads + kv + h) * HEAD_DIM
                ks[h, at, :] = q_land[i, j, :, k0 : k0 + HEAD_DIM]
                vs[h, at, :] = q_land[i, j, :, v0 : v0 + HEAD_DIM]
        attend_heads(ns, kv, span, qs, ks, vs, a_send.at[i], log.at[i])
        for copies in a_copies[i]:
            copies.start()
        a_land[i, z] = a_send[i, z]

    for i in range(count):
        attend(i)
        if i == 0:
            units[ns + 1].turn()
            units[ns].finish()
            store_own[0].wait()
            store(wo_land, w_out)
    store(q_land, packed)
    store(a_send, heads_attended)
    store(log, logs)
    for i in range(count):
        for copies in a_copies[i]:
            copies.wait()
        for j in range(ns):
            attended[i * span : (i + 1) * span, j * g_width : (j + 1) * g_width] = a_land[i, j]
    new = rows_in[...] + nn_dot(attended[...], wo_land[...])
    hidden[...] = new
    inverse = lax.rsqrt(jnp.mean(new * new, axis=1, keepdims=True) + norm_eps)
    second_abs[...] = (new * inverse * gains_out[1:2, :]).astype(BF16)
    second_copy.start()
    store(second_abs, (second_both, pl.ds(0, rows)))
    store(attended, attended_out)
    store(hidden, hidden_out)
    units[ns + 1].pass_on()
    gate_unit.turn()
    gate_unit.turn_late()
    gate_unit.finish()
    second_copy.wait()
    low_copy.wait()
    store_own[1].wait()
    for copies in stores:
        copies.wait()


def fore(mesh, count, kv, tokens, cotangent, gains_in, wq, wk, wv, wo, wg, wd, narrow_cosines, narrow_sines):
    ns, nf = mesh
    na = nf // 4
    chips = 2 * na
    rows, width = tokens.shape
    span = rows // count
    length = ns * span
    heads = kv * GROUP
    g_width = heads * HEAD_DIM
    q_width = g_width + 2 * kv * HEAD_DIM
    local, depth = wq.shape[0], wd.shape[0]
    tile = wg.shape[1] // (2 * chips)
    anywhere, vmem = pl.BlockSpec(memory_space=pl.ANY), pl.BlockSpec(memory_space=pltpu.VMEM)
    low = lambda *shape: jax.ShapeDtypeStruct(shape, BF16)
    wide = lambda *shape: jax.ShapeDtypeStruct(shape, F32)
    outs = [
        low(ns, width, q_width),
        low(width, width),
        low(chips - 1, width, tile),
        low(chips * depth, width),
        low(rows, width),
        low(count, ns, span, q_width),
        low(count, ns, span, g_width),
        wide(count, length, 128),
        low(rows, width),
        wide(rows, width),
        low(2 * rows, width),
        low(2 * rows, width),
        wide(2, width),
    ]
    scratch = [
        pltpu.VMEM((rows, width), F32),
        pltpu.VMEM((rows, width), F32),
        pltpu.VMEM((rows, width), BF16),
        pltpu.VMEM((ns, local, q_width), BF16),
        pltpu.VMEM((ns, width, q_width), BF16),
        pltpu.VMEM((width, width), BF16),
        pltpu.VMEM((ns, count, span, q_width), BF16),
        pltpu.VMEM((count, ns, span, q_width), BF16),
        pltpu.VMEM((count, ns, span, g_width), BF16),
        pltpu.VMEM((count, ns, span, g_width), BF16),
        pltpu.VMEM((2, chips - 1, local, tile), BF16),
        pltpu.VMEM((8, 256), F32),
        pltpu.VMEM((nf, 8, 256), F32),
        pltpu.VMEM((heads, length, HEAD_DIM), BF16),
        pltpu.VMEM((kv, length, HEAD_DIM), BF16),
        pltpu.VMEM((kv, length, HEAD_DIM), BF16),
        pltpu.VMEM((count, length, 128), F32),
        pltpu.VMEM((rows, width), BF16),
        pltpu.VMEM((8, 128), BF16),
        pltpu.VMEM((rows, width), BF16),
        pltpu.VMEM((rows, width), BF16),
        pltpu.VMEM((span, q_width), F32),
        pltpu.VMEM((span, q_width), F32),
    ]
    return pl.pallas_call(
        functools.partial(fore_kernel, mesh, count, kv),
        in_specs=[anywhere] * 2 + [vmem] * 4 + [anywhere] * 3 + [vmem] * 2,
        out_specs=[anywhere] * 12 + [vmem],
        out_shape=outs,
        scratch_shapes=scratch
        + [pltpu.SemaphoreType.DMA((160,)), pltpu.SemaphoreType.DMA((160,)), pltpu.SemaphoreType.DMA((64,))],
        compiler_params=pltpu.CompilerParams(vmem_limit_bytes=VMEM_MOST, collective_id=0, has_side_effects=True),
        name="fore",
    )(tokens, cotangent, gains_in, wq, wk, wv, wo, wg, wd, narrow_cosines, narrow_sines)


def attend_back_heads(ns, kv, span, qs, ks, vs, gs, attended, logs, dk, dv, result):
    scale = 1.0 / math.sqrt(HEAD_DIM)
    heads = kv * GROUP
    row = lax.broadcasted_iota(jnp.int32, (span, span), 0)
    column = lax.broadcasted_iota(jnp.int32, (span, span), 1)
    causal = row >= column
    dk[...] = jnp.zeros_like(dk)
    dv[...] = jnp.zeros_like(dv)
    for s in range(ns):
        here = slice(s * span, (s + 1) * span)
        for h in range(heads):
            g = h // GROUP
            q, grad = qs[h, here, :], gs[h, here, :]
            log_total = logs[here, h : h + 1]
            out = attended[s, :, h * HEAD_DIM : (h + 1) * HEAD_DIM]
            delta = jnp.sum(grad.astype(F32) * out.astype(F32), axis=1, keepdims=True)
            k, v = ks[g, here, :], vs[g, here, :]
            near = jnp.where(causal, jnp.exp(nt_dot(q, k) * scale - log_total), 0.0)
            slope = (near * (nt_dot(grad, v) - delta) * scale).astype(BF16)
            dq = nn_dot(slope, k)
            dk[g, here, :] += tn_dot(slope, q)
            dv[g, here, :] += tn_dot(near.astype(BF16), grad)
            if s > 0:
                before = slice(0, s * span)
                k, v = ks[g, before, :], vs[g, before, :]
                far = jnp.exp(nt_dot(q, k) * scale - log_total)
                slope = (far * (nt_dot(grad, v) - delta) * scale).astype(BF16)
                dq = dq + nn_dot(slope, k)
                dk[g, before, :] += tn_dot(slope, q)
                dv[g, before, :] += tn_dot(far.astype(BF16), grad)
            result[here, h * HEAD_DIM : (h + 1) * HEAD_DIM] = dq
    for g in range(kv):
        k0 = (heads + g) * HEAD_DIM
        v0 = (heads + kv + g) * HEAD_DIM
        result[:, k0 : k0 + HEAD_DIM] = dk[g]
        result[:, v0 : v0 + HEAD_DIM] = dv[g]


def back_kernel(
    mesh, count, kv,
    dx_own, dx_other, hidden, cotangent, gains, w_out, w_qkv, packed, attended, logs, cosines, sines, tokens, dwg, dwu,
    high, low_out, out, gain_grads, dqkv, sum_gate, sum_up,
    low, sum_rows, sum_land, dx_land, g_send, g_land, q_send, q_land, swap_send, swap_land, *rest,
):
    parts, (send_sems, recv_sems, local_sems) = rest[:-3], rest[-3:]
    links = Links(mesh, send_sems, recv_sems, local_sems)
    ns, na = links.ns, links.na
    chips = 2 * na
    z, core = links.z, links.core
    rows, width = hidden.shape
    span = rows // count
    length = ns * span
    heads = kv * GROUP
    g_width, q_width = heads * HEAD_DIM, (heads + 2 * kv) * HEAD_DIM
    half = dwg.shape[1]
    block = width // chips
    links.barrier()

    sums = []
    for n, source in enumerate((dwg, dwu)):
        for b_first in (True, False):
            columns = slice(0, half // 2) if b_first else slice(half // 2, half)
            at = (n * 2 + (0 if b_first else 1)) * 3
            partial = lambda k, source=source, columns=columns: (source, rows_at(k, block), columns)
            sums.append(ChipSum(links, partial, b_first, *parts[at : at + 3]))
    for item in sums:
        item.start()
        item.load()

    g_copies, q_copies = [], []
    for i in range(count):
        g_copies.append([links.copy((g_send, i, lax.rem(z + d, ns)), (g_land, i, z), links.at_z(d)) for d in range(1, ns)])
        q_copies.append([links.copy((q_send, i, lax.rem(z + d, ns)), (q_land, z, i), links.at_z(d)) for d in range(1, ns)])

    def out_back(dx, old, grad, w):
        load_sets, store_sets = [], []
        for i in range(count):
            here = pl.ds(i * span, span)
            pairs = ((dx_own, dx), (dx_other, dx_land), (hidden, old), (cotangent, grad))
            load_sets.append([links.local((source, here), (target, here)) for source, target in pairs])
            store_sets.append([links.local((grad, here), (high, here)), links.local((low, here), (low_out, here))])
        w_load = links.local(w_out, w)
        for load in load_sets[0] + [w_load] + [load for loads in load_sets[1:] for load in loads]:
            load.start()
        for i in range(count):
            here = slice(i * span, (i + 1) * span)
            for load in load_sets[i]:
                load.wait()
            step, rows_old = dx[here, :] + dx_land[here, :].astype(F32), old[here, :]
            inverse = lax.rsqrt(jnp.mean(rows_old * rows_old, axis=1, keepdims=True) + norm_eps)
            normed = rows_old * inverse
            part_sum = jnp.sum(step * normed, axis=0, keepdims=True)
            gain_grads[1:2, :] = part_sum if i == 0 else gain_grads[1:2, :] + part_sum
            total = grad[here, :] + norm_back(step, normed, inverse, gains[1:2, :])
            grad[here, :] = total
            low[here, :] = total.astype(BF16)
            for copies in store_sets[i]:
                copies.start()
            if i == 0:
                w_load.wait()
            out_part = nt_dot(low[here, :], w[...]).astype(BF16)
            for j in range(ns):
                g_send[i, j] = out_part[:, j * g_width : (j + 1) * g_width]
            for copies in g_copies[i]:
                copies.start()
            g_land[i, z] = g_send[i, z]
        for copies in [copies for stores in store_sets for copies in stores]:
            copies.wait()

    pl.run_scoped(
        out_back,
        pltpu.VMEM((rows, width), F32),
        pltpu.VMEM((rows, width), F32),
        pltpu.VMEM((rows, width), F32),
        pltpu.VMEM((width, width), BF16),
    )

    def attention(qkv, mid, log, qs, ks, vs, gs, dk, dv, result, cosine, sine):
        fill_tables(cosine, sine, cosines[...], sines[...], heads + kv)
        for i in range(count):
            loads = [links.local((packed, i), qkv), links.local((attended, i), mid), links.local((logs, i), log)]
            for load in loads:
                load.start()
            for load in loads:
                load.wait()
            for j in range(ns):
                at = slice(j * span, (j + 1) * span)
                for h in range(heads):
                    qs[h, at, :] = qkv[j, :, h * HEAD_DIM : (h + 1) * HEAD_DIM]
                for h in range(kv):
                    k0, v0 = (heads + h) * HEAD_DIM, (heads + kv + h) * HEAD_DIM
                    ks[h, at, :] = qkv[j, :, k0 : k0 + HEAD_DIM]
                    vs[h, at, :] = qkv[j, :, v0 : v0 + HEAD_DIM]
            for copies in g_copies[i]:
                copies.wait()
            for j in range(ns):
                for h in range(heads):
                    gs[h, j * span : (j + 1) * span, :] = g_land[i, j, :, h * HEAD_DIM : (h + 1) * HEAD_DIM]
            attend_back_heads(ns, kv, span, qs, ks, vs, gs, mid, log, dk, dv, result)
            for j in range(ns):
                here = slice(j * span, (j + 1) * span)
                part = result[here, :]
                q_send[i, j] = (part * cosine[here, :] - swap_halves(part) * sine[here, :]).astype(BF16)
            for copies in q_copies[i]:
                copies.start()
            q_land[z, i] = q_send[i, z]
            if i < len(sums) // 2:
                for item in sums[2 * i : 2 * i + 2]:
                    item.turn()

    pl.run_scoped(
        attention,
        pltpu.VMEM((ns, span, q_width), BF16),
        pltpu.VMEM((ns, span, g_width), BF16),
        pltpu.VMEM((length, 128), F32),
        pltpu.VMEM((heads, length, HEAD_DIM), BF16),
        pltpu.VMEM((kv, length, HEAD_DIM), BF16),
        pltpu.VMEM((kv, length, HEAD_DIM), BF16),
        pltpu.VMEM((heads, length, HEAD_DIM), BF16),
        pltpu.VMEM((kv, length, HEAD_DIM), F32),
        pltpu.VMEM((kv, length, HEAD_DIM), F32),
        pltpu.VMEM((length, q_width), F32),
        pltpu.VMEM((length, q_width), F32),
        pltpu.VMEM((length, q_width), F32),
    )

    swaps = []
    local = block // 2
    for item in sums[2 * count :]:
        item.turn()

    def swap(n):
        for m in range(2):
            total = sums[2 * n + m].finish()
            swap_send[n, m, 0] = total[:local]
            swap_send[n, m, 1] = total[local:]
        for m in range(2):
            copies = links.copy((swap_send, n, m, 1 - core), (swap_land, n, m), links.at_core())
            copies.start()
            swaps.append(copies)

    tile = half // chips
    stores = []
    early = first_piece(ns, 2 * half)
    piece = (sum_rows, 0, slice(None), slice(0, max(early, 1)))
    end, inner, inward = line_place(links)[:3]
    early_copy = links.copy(piece, sum_land, inward)

    def combine(n, total):
        for m in range(2):
            swaps[2 * n + m].wait()
            kept, arrived = swap_send[n, m, core], swap_land[n, m]
            for t in range(chips // 2):
                here = slice(t * tile, (t + 1) * tile)
                k = m * (chips // 2) + t
                one, two = kept[:, here], arrived[:, here]
                sum_rows[n, :, 2 * k * tile : (2 * k + 1) * tile] = jnp.where(core == 0, one, two)
                sum_rows[n, :, (2 * k + 1) * tile : (2 * k + 2) * tile] = jnp.where(core == 0, two, one)
        if n == 0 and early:
            pl.when(end)(early_copy.start)
        else:
            copies = links.local((sum_rows, n), total)
            copies.start()
            stores.append(copies)

    def project_back(w, old, base, grad):
        loads = [links.local(tokens, old), links.local(high, base), links.local(w_qkv, w)]
        for load in loads:
            load.start()
        swap(0)
        for load in loads:
            load.wait()
        for i in range(count):
            here = slice(i * span, (i + 1) * span)
            if i == count - 1:
                combine(0, sum_gate)
                swap(1)
                combine(1, sum_up)
            for copies in q_copies[i]:
                copies.wait()
            total = nt_dot(q_land[0, i], w[0])
            for j in range(1, ns):
                total = total + nt_dot(q_land[j, i], w[j])
            grad[here, :] = total
            copies = links.local((q_land, slice(None), i), (dqkv, slice(None), i))
            copies.start()
            stores.append(copies)
            step, rows_old = grad[here, :], old[here, :]
            inverse = lax.rsqrt(jnp.mean(rows_old * rows_old, axis=1, keepdims=True) + norm_eps)
            normed = rows_old * inverse
            part_sum = jnp.sum(step * normed, axis=0, keepdims=True)
            gain_grads[0:1, :] = part_sum if i == 0 else gain_grads[0:1, :] + part_sum
            base[here, :] = base[here, :] + norm_back(step, normed, inverse, gains[0:1, :])
            copies = links.local((base, here), (out, here))
            copies.start()
            stores.append(copies)
        if early:

            @pl.when(inner)
            def _():
                early_copy.wait_recv()
                put(piece, (get(piece).astype(F32) + sum_land[...].astype(F32)).astype(BF16))

            pl.when(end)(early_copy.wait_send)
            copies = links.local((sum_rows, 0), sum_gate)
            copies.start()
            stores.append(copies)
        for copies in stores:
            copies.wait()

    pl.run_scoped(
        project_back,
        pltpu.VMEM((ns, width, q_width), BF16),
        pltpu.VMEM((rows, width), F32),
        pltpu.VMEM((rows, width), F32),
        pltpu.VMEM((rows, width), F32),
    )


def back(mesh, count, kv, dx_own, dx_other, hidden, cotangent, gains, w_out, w_qkv, packed, attended, logs, cosines, sines, tokens, dwg, dwu):
    ns, nf = mesh
    na = nf // 4
    rows, width = hidden.shape
    span = rows // count
    heads = kv * GROUP
    g_width, q_width = heads * HEAD_DIM, (heads + 2 * kv) * HEAD_DIM
    half = dwg.shape[1]
    block = width // (2 * na)
    local = block // 2
    anywhere = pl.BlockSpec(memory_space=pl.ANY)
    vmem = pl.BlockSpec(memory_space=pltpu.VMEM)
    operands = [dx_own, dx_other, hidden, cotangent, gains, w_out, w_qkv, packed, attended, logs, cosines, sines, tokens, dwg, dwu]
    wide = jax.ShapeDtypeStruct((rows, width), F32)
    summed = jax.ShapeDtypeStruct((local, 2 * half), BF16)
    scratch = [
        pltpu.VMEM((rows, width), BF16),
        pltpu.VMEM((2, local, 2 * half), BF16),
        pltpu.VMEM((local, max(first_piece(ns, 2 * half), 128)), BF16),
        pltpu.VMEM((rows, width), BF16),
        pltpu.VMEM((count, ns, span, g_width), BF16),
        pltpu.VMEM((count, ns, span, g_width), BF16),
        pltpu.VMEM((count, ns, span, q_width), BF16),
        pltpu.VMEM((ns, count, span, q_width), BF16),
        pltpu.VMEM((2, 2, 2, local, half // 2), BF16),
        pltpu.VMEM((2, 2, local, half // 2), BF16),
    ]
    for _ in range(2):
        for b_first in (True, False):
            scratch += chip_sum_shapes(na, b_first, block, half // 2)
    return pl.pallas_call(
        functools.partial(back_kernel, mesh, count, kv),
        in_specs=[vmem if x.shape[0] == 2 and x.ndim == 2 or x.shape[1] == HEAD_DIM else anywhere for x in operands],
        out_specs=[anywhere, anywhere, anywhere, vmem, anywhere, anywhere, anywhere],
        out_shape=[
            wide,
            jax.ShapeDtypeStruct((rows, width), BF16),
            wide,
            jax.ShapeDtypeStruct((2, width), F32),
            jax.ShapeDtypeStruct((ns, count, span, q_width), BF16),
            summed,
            summed,
        ],
        scratch_shapes=scratch
        + [pltpu.SemaphoreType.DMA((64,)), pltpu.SemaphoreType.DMA((64,)), pltpu.SemaphoreType.DMA((64,))],
        compiler_params=pltpu.CompilerParams(vmem_limit_bytes=VMEM_MOST, collective_id=1, has_side_effects=True),
        name="back",
    )(*operands)


class LineSum:
    def __init__(self, links, term, first, second, total, out=None, begun=False):
        self.links, self.term, self.first, self.second, self.total = links, term, first, second, total
        self.dtype = (term[0] if isinstance(term, tuple) else term).dtype
        self.deep = links.ns // 2 > 1
        self.begun = begun
        self.end, self.inner, inward, outward = line_place(links)
        moved = self.deep and not begun
        self.inward = links.copy(term, first, inward) if moved else None
        self.onward = links.again(first, first, inward) if moved else None
        self.sum = first if moved else term
        self.across = links.copy(self.sum, second, inward)
        self.outward = links.copy(total, total, outward) if self.deep else None
        self.store = links.local(total, out) if out is not None else None

    def keep(self):
        if self.store is not None:
            self.store.start()

    def add(self, target, one, two):
        put(target, (get(one).astype(F32) + get(two).astype(F32)).astype(self.dtype))

    def begin(self):
        if self.begun:
            pl.when(self.inner)(self.across.start)
        elif self.deep:
            pl.when(self.end)(self.inward.start)
        else:
            self.across.start()

    def relay(self):
        if not self.deep or self.begun:
            return

        @pl.when(jnp.logical_not(self.end))
        def _():
            self.inward.wait_recv()
            self.add(self.first, self.term, self.first)
            pl.when(self.inner)(self.across.start)
            pl.when(jnp.logical_not(self.inner))(self.onward.start)

    def settle(self):
        @pl.when(self.inner)
        def _():
            self.across.wait()
            self.add(self.total, self.sum, self.second)
            if self.deep:
                self.outward.start()
            self.keep()

        if self.deep:

            @pl.when(jnp.logical_not(self.inner | self.end))
            def _():
                self.outward.wait_recv()
                self.outward.start()
                self.keep()

    def finish(self):
        if self.deep:

            @pl.when(self.end)
            def _():
                self.outward.wait_recv()
                self.keep()

            if not self.begun:
                pl.when(jnp.logical_not(self.inner))(self.inward.wait_send)
            pl.when(jnp.logical_not(self.end))(self.outward.wait_send)


def finish_kernel(
    mesh, count, kv,
    gate_in, up_in, dwd, first, dqkv, attended, low, gains,
    out_gate, out_up, out_down, out_out, out_qkv, out_gains,
    tot_gate, tot_up, tot_down, tot_out, tot_qkv, term_gate, term_up, term_down, term_out, term_qkv, in_gate, in_up, in_down, in_out, in_qkv,
    first_both, attended_both, low_both, dq_both, w_out_part, w_qkv_part,
    swap_out, land_out, swap_qkv, land_qkv, gain_terms, gain_lands, *rest,
):
    parts, (send_sems, recv_sems, local_sems) = rest[:-3], rest[-3:]
    links = Links(mesh, send_sems, recv_sems, local_sems)
    ns, na = links.ns, links.na
    chips, per = 2 * na, ns // 2
    core = links.core
    rows, width = first.shape
    q_width = dqkv.shape[3]
    middle = width // 2

    def lines(term, inbox, total, out, pieces, begun=False):
        size = term.shape[1] // pieces
        every = slice(None)
        made = []
        for i in range(pieces):
            at = slice(i * size, (i + 1) * size)
            refs = [(ref, *where, every, at) for ref, *where in ((term,), (inbox, 0), (inbox, 1), (total,), (out,))]
            made.append(LineSum(links, *refs, begun and i == 0))
        return made

    gate_lines = lines(term_gate, in_gate, tot_gate, out_gate, GATE_PIECES, first_piece(ns, term_gate.shape[1]) > 0)
    up_lines = lines(term_up, in_up, tot_up, out_up, 4)
    down_lines = lines(term_down, in_down, tot_down, out_down, 4)
    out_lines = lines(term_out, in_out, tot_out, out_out, 2)
    qkv_lines = lines(term_qkv, in_qkv, tot_qkv, out_qkv, 4)
    term_loads = []
    for source, some in ((gate_in, gate_lines), (up_in, up_lines)):
        for line in some:
            term_loads.append(links.local((source, *line.term[1:]), line.term))
    for load in term_loads:
        load.start()
    links.barrier()
    for load, line in zip(term_loads, gate_lines + up_lines):
        load.wait()
        line.begin()

    sends = [
        links.copy((dqkv, pl.ds((1 - core) * per, per)), (dq_both, 1), links.at_core()),
        links.copy((low, slice(None), rows_at(1 - core, middle)), (low_both, 1), links.at_core()),
        links.copy(first, (first_both, 1), links.at_core()),
        links.copy(attended, (attended_both, 1), links.at_core()),
    ]
    loads = [
        links.local((low, slice(None), rows_at(core, middle)), (low_both, 0)),
        links.local(attended, (attended_both, 0)),
        links.local(first, (first_both, 0)),
        links.local((dqkv, pl.ds(core * per, per)), (dq_both, 0)),
    ]
    for copies in loads + sends[1:2] + sends[3:4] + sends[2:3] + sends[:1]:
        copies.start()

    down_rows = dwd.shape[0] // chips
    block = width // chips

    def pair(source, row_count, at, staged):
        made = []
        cut = source.shape[1] // 2
        for n, b_first in enumerate((True, False)):
            columns = slice(0, cut) if b_first else slice(cut, 2 * cut)
            partial = lambda k, columns=columns: (source, rows_at(k, row_count), columns)
            refs = parts[at[n] : at[n + 1]]
            made.append(ChipSum(links, partial, b_first, *(refs if staged else (*refs[:2], None))))
        return made

    down = pair(dwd, down_rows, (0, 3, 6), True)
    for item in down:
        item.start()
        item.load()

    gain_copies = [links.copy((gain_terms, 0), (gain_lands, 0), links.at_core()), links.copy((gain_terms, 1), (gain_lands, 1), links.at_b())]
    gain_copies += [links.copy((gain_terms, 2), (gain_lands, 1 + d), links.at_a(d)) for d in range(1, na)]
    gain_line = LineSum(links, (gain_terms, 3), (gain_lands, na + 1), (gain_lands, na + 2), out_gains)
    gain_terms[0] = gains[...]
    gain_copies[0].start()

    def next_gain(i):
        for copies in gain_copies[i : i + 1] if i < 2 else gain_copies[2:]:
            copies.wait()
        if i < 2:
            gain_terms[i + 1] = gain_terms[i] + gain_lands[i]
            for copies in gain_copies[1:2] if i == 0 else gain_copies[2:]:
                copies.start()
        else:
            total = gain_terms[2]
            for d in range(1, na):
                total = total + gain_lands[1 + d]
            gain_terms[3] = total
            gain_line.begin()

    def qkv_part(p):
        columns = slice(p * q_width, (p + 1) * q_width)
        mine, other = dq_both[0, p].reshape(rows, q_width), dq_both[1, p].reshape(rows, q_width)
        for k in range(chips):
            at = slice(k * block, (k + 1) * block)
            total = tn_dot(first_both[0, :, at], mine) + tn_dot(first_both[1, :, at], other)
            w_qkv_part[at, columns] = total.astype(BF16)

    def swap(sums, send, land):
        local = block // 2
        for n, item in enumerate(sums):
            total = item.finish()
            size = total.shape[1]
            send[0, :, n * size : (n + 1) * size] = total[:local]
            send[1, :, n * size : (n + 1) * size] = total[local:]
        copies = links.copy((send, 1 - core), land, links.at_core())
        copies.start()
        return copies

    out_sums = pair(w_out_part, block, (6, 8, 10), False)
    qkv_sums = pair(w_qkv_part, block, (10, 12, 14), False)
    cut = width // 2
    next_gain(0)
    for i in (1, 3):
        sends[i].wait()
    for i in (0, 1):
        loads[i].wait()
    gate_lines[0].relay()
    for k in range(chips):
        at = slice(k * block, (k + 1) * block)
        total = tn_dot(attended_both[0, :, at], low_both[0]) + tn_dot(attended_both[1, :, at], low_both[1])
        w_out_part[at, :] = total.astype(BF16)
    for item in out_sums:
        item.start()
    gate_lines[1].relay()
    next_gain(1)
    for i in (0, 2):
        sends[i].wait()
    for i in (2, 3):
        loads[i].wait()
    gate_lines[0].settle()
    for p in range(per // 2):
        qkv_part(p)
    gate_lines[2].relay()
    next_gain(2)
    gate_lines[1].settle()
    for p in range(per // 2, per):
        qkv_part(p)
    gate_lines[3].relay()
    for item in down:
        item.turn()
    for item in qkv_sums:
        item.start()
    gate_lines[2].settle()
    gain_line.relay()
    up_lines[0].relay()
    gate_lines[3].settle()
    for item in out_sums:
        item.turn()
    up_lines[1].relay()
    up_lines[0].settle()
    gain_line.settle()
    up_lines[2].relay()
    up_lines[1].settle()
    term_down[:, :cut] = down[0].finish()
    term_down[:, cut:] = down[1].finish()
    for line in down_lines:
        line.begin()
    up_lines[3].relay()
    up_lines[2].settle()
    down_lines[0].relay()
    up_lines[3].settle()
    for item in qkv_sums:
        item.turn()
    down_lines[1].relay()
    down_lines[0].settle()
    out_swap = swap(out_sums, swap_out, land_out)
    down_lines[2].relay()
    down_lines[1].settle()
    out_swap.wait()
    kept, arrived = swap_out[core], land_out[...]
    term_out[:, :cut] = jnp.where(core == 0, kept, arrived)
    term_out[:, cut:] = jnp.where(core == 0, arrived, kept)
    for line in out_lines:
        line.begin()
    down_lines[3].relay()
    down_lines[2].settle()
    qkv_swap = swap(qkv_sums, swap_qkv, land_qkv)
    out_lines[0].relay()
    down_lines[3].settle()
    qkv_swap.wait()
    kept, arrived = swap_qkv[core], land_qkv[...]
    for n in range(2):
        group = jnp.where(core == n, kept, arrived)
        for p in range(per):
            taken, start = p * q_width, 0
            for size in (kv * GROUP * HEAD_DIM, kv * HEAD_DIM, kv * HEAD_DIM):
                at = start + (n * per + p) * size
                term_qkv[:, at : at + size] = group[:, taken : taken + size]
                taken, start = taken + size, start + ns * size
    for line in qkv_lines:
        line.begin()
    out_lines[1].relay()
    out_lines[0].settle()
    qkv_lines[0].relay()
    out_lines[1].settle()
    for n in range(1, len(qkv_lines)):
        qkv_lines[n].relay()
        qkv_lines[n - 1].settle()
    qkv_lines[-1].settle()
    every_line = [*gate_lines, *up_lines, gain_line, *down_lines, *out_lines, *qkv_lines]
    for line in every_line:
        line.finish()
    for line in every_line:
        if line.store is not None:
            line.store.wait()


def finish(mesh, count, kv, term_gate, term_up, dwd, first, dqkv, attended, low, gains):
    ns, nf = mesh
    na, per = nf // 4, ns // 2
    rows, width = first.shape
    q_width = dqkv.shape[3]
    local, half = term_gate.shape[0], width // 2
    block = 2 * local
    anywhere, vmem = pl.BlockSpec(memory_space=pl.ANY), pl.BlockSpec(memory_space=pltpu.VMEM)
    down = (dwd.shape[0] // (2 * na), dwd.shape[1])
    shapes = [term_gate.shape, term_up.shape, down, (local, width), (local, ns * q_width)]
    scratch = [pltpu.VMEM(s, BF16) for s in shapes]
    scratch += [pltpu.VMEM(s, BF16) for s in shapes]
    scratch += [pltpu.VMEM((2,) + tuple(s), BF16) for s in shapes]
    scratch += [
        pltpu.VMEM((2, rows, width), BF16),
        pltpu.VMEM((2, rows, width), BF16),
        pltpu.VMEM((2, rows, half), BF16),
        pltpu.VMEM((2, per, count, rows // count, q_width), BF16),
        pltpu.VMEM((width, half), BF16),
        pltpu.VMEM((width, per * q_width), BF16),
        pltpu.VMEM((2, local, half), BF16),
        pltpu.VMEM((local, half), BF16),
        pltpu.VMEM((2, local, per * q_width), BF16),
        pltpu.VMEM((local, per * q_width), BF16),
        pltpu.VMEM((4, 2, width), F32),
        pltpu.VMEM((na + 3, 2, width), F32),
    ]
    scratch += chip_sum_shapes(na, True, down[0], down[1] // 2) + chip_sum_shapes(na, False, down[0], down[1] // 2)
    for columns in (half // 2, per * q_width // 2):
        for b_first in (True, False):
            scratch += chip_sum_shapes(na, b_first, block, columns)[:2]
    return pl.pallas_call(
        functools.partial(finish_kernel, mesh, count, kv),
        in_specs=[anywhere] * 7 + [vmem],
        out_specs=[anywhere] * 5 + [vmem],
        out_shape=[jax.ShapeDtypeStruct(s, BF16) for s in shapes] + [jax.ShapeDtypeStruct((2, width), F32)],
        scratch_shapes=scratch
        + [pltpu.SemaphoreType.DMA((128,)), pltpu.SemaphoreType.DMA((128,)), pltpu.SemaphoreType.DMA((64,))],
        compiler_params=pltpu.CompilerParams(vmem_limit_bytes=VMEM_MOST, collective_id=2, has_side_effects=True),
        name="finish",
    )(term_gate, term_up, dwd, first, dqkv, attended, low, gains)


def widen_kernel(cuts, *refs):
    gate, up, down, out, qkv, hidden, own, other = refs[:8]
    o_gate, o_up, o_down, o_out, o_q, o_k, o_v, o_block = refs[8:]
    for source, target in ((gate, o_gate), (up, o_up), (down, o_down), (out, o_out)):
        target[...] = source[...].astype(F32)
    for (start, end), target in zip(cuts, (o_q, o_k, o_v)):
        target[...] = qkv[:, start:end].astype(F32)
    o_block[...] = hidden[...] + own[...] + other[...].astype(F32)


def widen(gate, up, down, out, qkv, hidden, own, other, cuts):
    steps = 4
    operands = [gate, up, down, out, qkv, hidden, own, other]
    rows = out.shape[0]
    shapes = [gate.shape, up.shape, down.shape, out.shape] + [(rows, end - start) for start, end in cuts] + [hidden.shape]
    block = lambda shape: pl.BlockSpec((shape[0] // steps, shape[1]), lambda i: (i, 0))
    return pl.pallas_call(
        functools.partial(widen_kernel, cuts),
        grid=(steps,),
        in_specs=[block(x.shape) for x in operands],
        out_specs=[block(shape) for shape in shapes],
        out_shape=[jax.ShapeDtypeStruct(shape, F32) for shape in shapes],
        compiler_params=pltpu.CompilerParams(vmem_limit_bytes=VMEM_LIMIT),
        cost_estimate=pl.CostEstimate(flops=0, bytes_accessed=40 * rows * gate.shape[1], transcendentals=0),
        name="widen",
    )(*operands)


def solution(mesh):
    ns, nf = mesh.shape["seq"], mesh.shape["fsdp"]
    na = nf // 4
    chips = 2 * na
    kv = KEY_VALUE_HEADS // ns

    def body(tokens, cotangent, attention_gain, feedforward_gain, query_weight, key_matrix, value_matrix, out_weight, gate_weight, up_weight, down_weight):
        count, span, width = tokens.shape
        rows = count * span
        local = query_weight.shape[0]
        sizes = (ns, nf)
        mine = lax.axis_index("fsdp")
        cosines, sines = (jnp.asarray(x) for x in rope_tables(ns * span))
        flat = tokens.reshape(rows, width)
        grad_flat = cotangent.reshape(rows, width)
        (w_qkv, w_out, w_gate, w_down, first, packed, heads_attended, logs, attended, hidden_one, second_both, low_both, gains) = fore(
            sizes, count, kv, flat, grad_flat, jnp.stack([attention_gain, feedforward_gain]),
            query_weight, key_matrix, value_matrix, out_weight, gate_weight, down_weight, cosines, sines,
        )
        dwg, dwu, dwd, out_own, out_arrived, dx_own, dx_arrived = ffn(sizes, second_both, low_both, w_gate, w_down, up_weight, gate_weight)
        high, low, grad_tokens, gain_grads, dqkv, sum_gate, sum_up = back(
            sizes, count, kv, dx_own, dx_arrived, hidden_one, grad_flat, gains, w_out, w_qkv,
            packed, heads_attended, logs, cosines, sines, flat, dwg, dwu,
        )
        *sums, gain_grads = finish(
            sizes, count, kv, sum_gate, sum_up, dwd, first, dqkv, attended, low, gain_grads
        )
        q_end, k_end = ns * kv * GROUP * HEAD_DIM, ns * kv * (GROUP + 1) * HEAD_DIM
        cuts = ((0, q_end), (q_end, k_end), (k_end, sums[4].shape[1]))
        grad_gate, grad_up, grad_down, grad_out, grad_query, grad_key, grad_value, block_out = widen(
            *sums, hidden_one, out_own, out_arrived, cuts
        )
        gain_grads = lax.dynamic_slice(gain_grads, (0, mine * local), (2, local))

        return (
            block_out.reshape(count, span, width),
            grad_tokens.reshape(count, span, width),
            gain_grads[0],
            gain_grads[1],
            grad_query,
            grad_key,
            grad_value,
            grad_out,
            grad_gate,
            grad_up,
            grad_down,
        )

    tokens_spec, gain_spec, weight_spec = P("fsdp", "seq", None), P("fsdp"), P("fsdp", None)
    return jax.shard_map(
        body,
        mesh=mesh,
        in_specs=(tokens_spec, tokens_spec, gain_spec, gain_spec) + (weight_spec,) * 7,
        out_specs=(tokens_spec, tokens_spec, gain_spec, gain_spec) + (weight_spec,) * 7,
        check_vma=False,
    )
```
